64 devices in a mesh: dp: 4 (over x, y), tp: 16 (over z, core).
Axes of the slice: x: 2, y: 2, z: 8, core: 2. Of those that a mesh axis runs over, the one named last changes fastest.
The devices are a block of a 4x4x8 slice.
Arguments:
- x_in: bfloat16 [8192, 2048], P(('dp', 'tp')), parts along dimension 0
- grad_y: bfloat16 [8192, 2048], P(('dp', 'tp')), parts along dimension 0
- norm_gain: float32 [2, 2048], replicated
- w_qkv: bfloat16 [2, 2048, 6144], P(None, None, 'tp')
- w_out: bfloat16 [2, 2048, 2048], P(None, 'tp')
- w_gate: bfloat16 [2, 2048, 8192], P(None, None, 'tp')
- w_up: bfloat16 [2, 2048, 8192], P(None, None, 'tp')
- w_down: bfloat16 [2, 8192, 2048], P(None, 'tp')
Outputs:
- output 1: bfloat16 [8192, 2048], P(('dp', 'tp')), parts along dimension 0
- output 2: float32 [8, 2048], P('dp'), parts along dimension 0
- output 3: bfloat16 [8, 2048, 6144], P('dp', None, 'tp'), parts along dimension 0
- output 4: bfloat16 [8, 2048, 2048], P('dp', 'tp'), parts along dimension 0
- output 5: bfloat16 [8, 2048, 8192], P('dp', None, 'tp'), parts along dimension 0
- output 6: bfloat16 [8, 2048, 8192], P('dp', None, 'tp'), parts along dimension 0
- output 7: bfloat16 [8, 8192, 2048], P('dp', 'tp'), parts along dimension 0
There are 4 independent parts. The reference program is written for one: setup_inputs(seed, part) draws one part's arguments, and reference() takes and returns one part's arrays. A program takes and returns all parts, laid end to end along the dimension named above; an argument that names none is the same for every part.
All inputs are finite; a program needn't handle non-finite values.
Results may differ from the reference program's by a relative error of at most 0.0158805.
Values are sent between devices in bfloat16 or wider.
A program may use at most 768 MiB of HBM per device.

```python
import jax
import jax.numpy as jnp
from jax import lax

SEQ_LEN = 2048
D_MODEL = 2048
D_FF = 8192
HEADS = 16
KV_HEADS = 16
HEAD_DIM = 128
LAYERS = 2

GROUP_SIZE = HEADS // KV_HEADS
QKV_COLS = (HEADS + 2 * KV_HEADS) * HEAD_DIM
NORM_EPS = 1e-5
ROPE_BASE = 10000.0


def setup_inputs(seed: int = 0, part: int = 0) -> dict:
    data_keys = jax.random.split(jax.random.fold_in(jax.random.key(seed), part), 2)
    weight_keys = jax.random.split(jax.random.key(seed + 1), 6)
    x_in = jax.random.normal(data_keys[0], (SEQ_LEN, D_MODEL), jnp.float32)
    grad_y = jax.random.normal(data_keys[1], (SEQ_LEN, D_MODEL), jnp.float32)
    norm_gain = 1.0 + 0.3 * jax.random.normal(weight_keys[0], (LAYERS, D_MODEL), jnp.float32)
    w_qkv = jax.random.normal(weight_keys[1], (LAYERS, D_MODEL, QKV_COLS), jnp.float32) * D_MODEL ** -0.5
    w_out = jax.random.normal(weight_keys[2], (LAYERS, HEADS * HEAD_DIM, D_MODEL), jnp.float32) * (HEADS * HEAD_DIM) ** -0.5
    w_gate = jax.random.normal(weight_keys[3], (LAYERS, D_MODEL, D_FF), jnp.float32) * D_MODEL ** -0.5
    w_up = jax.random.normal(weight_keys[4], (LAYERS, D_MODEL, D_FF), jnp.float32) * D_MODEL ** -0.5
    w_down = jax.random.normal(weight_keys[5], (LAYERS, D_FF, D_MODEL), jnp.float32) * D_FF ** -0.5
    return {'x_in': x_in.astype(jnp.bfloat16), 'grad_y': grad_y.astype(jnp.bfloat16), 'norm_gain': norm_gain, 'w_qkv': w_qkv.astype(jnp.bfloat16), 'w_out': w_out.astype(jnp.bfloat16), 'w_gate': w_gate.astype(jnp.bfloat16), 'w_up': w_up.astype(jnp.bfloat16), 'w_down': w_down.astype(jnp.bfloat16)}


def rope_tables():
    half_dim = HEAD_DIM // 2
    freqs = ROPE_BASE ** (-2.0 * jnp.arange(half_dim, dtype=jnp.float32) / HEAD_DIM)
    angles = jnp.arange(SEQ_LEN, dtype=jnp.float32)[:, None] * freqs[None, :]
    return jnp.cos(angles)[:, None, None, :], jnp.sin(angles)[:, None, None, :]


def rotate(values, cos_tab, sin_tab):
    half_dim = values.shape[-1] // 2
    lower_half = values[..., :half_dim]
    upper_half = values[..., half_dim:]
    return jnp.concatenate([lower_half * cos_tab - upper_half * sin_tab, upper_half * cos_tab + lower_half * sin_tab], axis=-1)


def rms_scale(x_f32, gain_row):
    inv_rms = lax.rsqrt(jnp.mean(x_f32 * x_f32, axis=-1, keepdims=True) + NORM_EPS)
    return x_f32 * inv_rms * gain_row


def group_attention(operands):
    query, keys_rot, values_v = operands
    causal = jnp.arange(SEQ_LEN)[:, None] >= jnp.arange(SEQ_LEN)[None, :]
    scores = jnp.einsum('sgd,td->gst', query.astype(jnp.float32), keys_rot.astype(jnp.float32)) * HEAD_DIM ** -0.5
    attn_prob = jax.nn.softmax(jnp.where(causal, scores, -1e30), axis=-1).astype(jnp.bfloat16)
    return jnp.einsum('gst,td->sgd', attn_prob.astype(jnp.float32), values_v.astype(jnp.float32)).astype(jnp.bfloat16)


def decoder_block(x_cur, gain_row, w_qkv_l, w_out_l, w_gate_l, w_up_l, w_down_l, cos_tab, sin_tab):
    x_f32 = x_cur.astype(jnp.float32)
    normed = rms_scale(x_f32, gain_row).astype(jnp.bfloat16).astype(jnp.float32)
    qkv_all = jnp.dot(normed, w_qkv_l.astype(jnp.float32), preferred_element_type=jnp.float32).astype(jnp.bfloat16)
    qkv_all = qkv_all.reshape(SEQ_LEN, KV_HEADS, GROUP_SIZE + 2, HEAD_DIM)
    rotated = rotate(qkv_all[:, :, :GROUP_SIZE + 1].astype(jnp.float32), cos_tab, sin_tab).astype(jnp.bfloat16)
    operands = (jnp.moveaxis(rotated[:, :, :GROUP_SIZE], 1, 0), jnp.moveaxis(rotated[:, :, GROUP_SIZE], 1, 0), jnp.moveaxis(qkv_all[:, :, GROUP_SIZE + 1], 1, 0))
    attn_out = lax.map(jax.checkpoint(group_attention), operands)
    attn_out = jnp.moveaxis(attn_out, 0, 1).reshape(SEQ_LEN, HEADS * HEAD_DIM)
    gate_act = jnp.dot(normed, w_gate_l.astype(jnp.float32), preferred_element_type=jnp.float32).astype(jnp.bfloat16)
    up_act = jnp.dot(normed, w_up_l.astype(jnp.float32), preferred_element_type=jnp.float32).astype(jnp.bfloat16)
    hidden = (jax.nn.silu(gate_act.astype(jnp.float32)) * up_act.astype(jnp.float32)).astype(jnp.bfloat16)
    block_sum = x_f32 + jnp.dot(attn_out.astype(jnp.float32), w_out_l.astype(jnp.float32), preferred_element_type=jnp.float32) + jnp.dot(hidden.astype(jnp.float32), w_down_l.astype(jnp.float32), preferred_element_type=jnp.float32)
    return block_sum.astype(jnp.bfloat16)


def stack_forward(x_in, norm_gain, w_qkv, w_out, w_gate, w_up, w_down):
    cos_tab, sin_tab = rope_tables()

    def body(x_cur, layer_weights):
        gain_row, w_qkv_l, w_out_l, w_gate_l, w_up_l, w_down_l = layer_weights
        return decoder_block(x_cur, gain_row, w_qkv_l, w_out_l, w_gate_l, w_up_l, w_down_l, cos_tab, sin_tab), None

    return lax.scan(body, x_in, (norm_gain, w_qkv, w_out, w_gate, w_up, w_down))[0]


def reference(x_in, grad_y, norm_gain, w_qkv, w_out, w_gate, w_up, w_down):
    pullback = jax.vjp(stack_forward, x_in, norm_gain, w_qkv, w_out, w_gate, w_up, w_down)[1]
    grad_x, grad_gain, grad_qkv, grad_out, grad_gate, grad_up, grad_down = pullback(grad_y)
    return (grad_x, grad_gain, grad_qkv, grad_out, grad_gate, grad_up, grad_down)
```

```python
import functools

import jax
import jax.numpy as jnp
from jax import lax
from jax.experimental import pallas as pl
from jax.experimental.pallas import tpu as pltpu
from jax.sharding import PartitionSpec as P

HEAD_DIM = 128
NORM_EPS = 1e-5
ROPE_BASE = 10000.0
MESH = pl.DeviceIdType.MESH
NP = 4
F32 = jnp.float32
BF16 = jnp.bfloat16


def dot_nn(a, b):
    return lax.dot_general(a, b, (((1,), (0,)), ((), ())), preferred_element_type=F32)


def dot_nt(a, b):
    return lax.dot_general(a, b, (((1,), (1,)), ((), ())), preferred_element_type=F32)


def dot_tn(a, b):
    return lax.dot_general(a, b, (((0,), (0,)), ((), ())), preferred_element_type=F32)


def aligned(index, size):
    return pl.multiple_of(index, size)


class Place:
    def __init__(self, tp_size):
        index = lax.axis_index('tp')
        self.ring = tp_size // 2
        self.half = self.ring // 2
        self.core = lax.rem(index, 2)
        self.chip = lax.div(index, 2)
        self.right = {'tp': self.near(1) * 2 + self.core}
        self.left = {'tp': self.near(-1) * 2 + self.core}
        self.mate = {'tp': self.chip * 2 + 1 - self.core}

    def near(self, step):
        return lax.rem(self.chip + step + self.ring, self.ring)

    def barrier(self, others=()):
        sem = pltpu.get_barrier_semaphore()
        peers = [self.right, self.left, self.mate] + list(others)
        for peer in peers:
            pl.semaphore_signal(sem, inc=1, device_id=peer, device_id_type=MESH)
        pl.semaphore_wait(sem, len(peers))


class Gather:
    def __init__(self, place, buf, shard_rows, sems):
        self.place, self.buf, self.shard = place, buf, shard_rows
        self.rows = shard_rows // NP
        self.events = (place.half - 1) * NP + NP // 2
        self.send_r, self.recv_r, self.send_l, self.recv_l, self.send_m, self.recv_m = sems

    @staticmethod
    def scratch(half):
        events = (half - 1) * NP + NP // 2
        return [pltpu.SemaphoreType.DMA((n,)) for n in (events, events, events, events, 2 * events + NP, 2 * events + NP)]

    def view(self, chip, core, piece):
        start = (chip * 2 + core) * self.shard + piece * self.rows
        return self.buf.at[pl.ds(aligned(start, self.rows), self.rows)]

    def own_rows(self):
        start = (self.place.chip * 2 + self.place.core) * self.shard
        return pl.ds(aligned(start, self.shard), self.shard)

    def to_right(self, event, view):
        return pltpu.make_async_remote_copy(view, view, self.send_r.at[event], self.recv_r.at[event], self.place.right, MESH)

    def to_left(self, event, view):
        return pltpu.make_async_remote_copy(view, view, self.send_l.at[event], self.recv_l.at[event], self.place.left, MESH)

    def to_mate(self, slot, view):
        return pltpu.make_async_remote_copy(view, view, self.send_m.at[slot], self.recv_m.at[slot], self.place.mate, MESH)

    def start(self):
        place = self.place
        for piece in range(NP):
            self.to_right(piece, self.view(place.chip, place.core, piece)).start()
            self.to_left(piece, self.view(place.chip, place.core, NP - 1 - piece)).start()
        for piece in range(NP):
            self.to_mate(2 * self.events + piece, self.view(place.chip, place.core, piece)).start()

    def views(self, event):
        step = lax.div(event, NP) + 1
        piece = lax.rem(event, NP)
        from_left = self.view(self.place.near(-step), self.place.core, piece)
        from_right = self.view(self.place.near(step), self.place.core, NP - 1 - piece)
        return from_left, from_right

    def event(self, event, forward=None):
        from_left, from_right = self.views(event)
        self.to_right(event, from_left).wait_recv()
        self.pass_on(event, forward, lambda: self.to_right(event + NP, from_left).start())
        self.to_mate(event, from_left).start()
        self.to_left(event, from_right).wait_recv()
        self.pass_on(event, forward, lambda: self.to_left(event + NP, from_right).start())
        self.to_mate(self.events + event, from_right).start()

    def pass_on(self, event, forward, send):
        if forward is None:
            pl.when(event + NP < self.events)(send)
        elif forward:
            send()

    def mate_wait(self, first, count):
        for offset in range(count):
            self.to_mate(first + offset, self.view(self.place.chip, 1 - self.place.core, 0)).wait_recv()

    def mate_wait_all(self):
        def body(slot, carry):
            self.mate_wait(slot, 1)
            return carry
        lax.fori_loop(0, 2 * self.events + NP, body, 0)

    def mate_wait_last(self):
        first = (self.place.half - 1) * NP
        self.mate_wait(first, NP // 2)
        self.mate_wait(self.events + first, NP // 2)

    def mate_wait_chip(self, distance, rightward):
        ring_first = lax.select(rightward, self.events, 0) + (distance - 1) * NP
        self.mate_wait(lax.select(distance == 0, 2 * self.events, ring_first), NP)

    def finish(self):
        view = self.view(self.place.chip, self.place.core, 0)

        def ring(event, carry):
            self.to_right(event, view).wait_send()
            self.to_left(event, view).wait_send()
            return carry
        lax.fori_loop(0, self.events, ring, 0)

        def across(slot, carry):
            self.to_mate(slot, view).wait_send()
            return carry
        lax.fori_loop(0, 2 * self.events + NP, across, 0)


class Reduce:
    def __init__(self, place, part, shard_rows, refs):
        self.place, self.part, self.shard = place, part, shard_rows
        self.events = (place.half - 1) * NP + NP // 2
        self.ring_r, self.ring_l, self.acc, self.stage = refs[:4]
        self.send_r, self.recv_r, self.send_l, self.recv_l, self.send_m, self.recv_m = refs[4:]

    @staticmethod
    def scratch(half, shard_rows, width):
        events = (half - 1) * NP + NP // 2
        shapes = [(events,), (events,), (2 * events + NP,), (6, 2)]
        sems = (events, events, events, events, 2 * events + NP, 2 * events + NP)
        return [pltpu.VMEM(s + (shard_rows, width), F32) for s in shapes] + [pltpu.SemaphoreType.DMA((n,)) for n in sems]

    def slot(self, event, way):
        return lax.rem(event, 2) * 2 + way

    def mate_copy(self, slot, index):
        return pltpu.make_async_remote_copy(
            self.stage.at[slot, 1 - self.place.core], self.acc.at[index], self.send_m.at[index], self.recv_m.at[index],
            self.place.mate, MESH)

    def ring_copy(self, event, way):
        if way == 0:
            return pltpu.make_async_remote_copy(
                self.acc.at[2 * event], self.ring_r.at[event], self.send_r.at[event], self.recv_r.at[event], self.place.right, MESH)
        return pltpu.make_async_remote_copy(
            self.acc.at[2 * event + 1], self.ring_l.at[event], self.send_l.at[event], self.recv_l.at[event], self.place.left, MESH)

    def fill(self, chip, piece, slot, index):
        value = self.part(chip, piece)
        self.stage[slot, 0] = value[:self.shard]
        self.stage[slot, 1] = value[self.shard:]
        self.mate_copy(slot, index).start()

    def prepare(self, event, reuse=True):
        shifted = event + NP // 2
        distance = self.place.half - lax.div(shifted, NP)
        piece = lax.rem(shifted, NP)
        for way in range(2):
            slot = self.slot(event, way)
            if reuse:
                self.mate_copy(slot, 2 * (event - 2) + way).wait_send()
            if way == 0:
                self.fill(self.place.near(distance), piece, slot, 2 * event)
            else:
                self.fill(self.place.near(-distance), NP - 1 - piece, slot, 2 * event + 1)

    def prepare_own(self, second):
        event = self.events + (1 if second else 0)
        for way in range(2):
            slot = 4 + way if second else self.slot(self.events, way)
            if not second:
                self.mate_copy(slot, 2 * (event - 2) + way).wait_send()
            self.fill(self.place.chip, (2 if second else 0) + way, slot, 2 * event + way)

    def event(self, event, arrives):
        for way in range(2):
            index = 2 * event + way
            slot = self.slot(event, way)
            self.mate_copy(slot, index).wait_recv()
            total = self.stage[slot, self.place.core] + self.acc[index]
            if arrives:
                self.ring_copy(event - NP, way).wait_recv()
                ring = self.ring_r if way == 0 else self.ring_l
                total = total + ring[event - NP]
            self.acc[index] = total
            self.ring_copy(event, way).start()

    def final(self, piece):
        last = self.events - NP
        index = 2 * self.events + piece
        slot = piece % 2 + (4 if piece >= 2 else 2 * (self.events % 2))
        self.mate_copy(slot, index).wait_recv()
        self.ring_copy(last + piece, 0).wait_recv()
        self.ring_copy(last + NP - 1 - piece, 1).wait_recv()
        return ((self.stage[slot, self.place.core] + self.acc[index])
                + (self.ring_r[last + piece] + self.ring_l[last + NP - 1 - piece]))

    def final_order(self):
        return range(NP)

    def finish(self):
        for event in range(self.events - 1, self.events + 2):
            for way in range(2):
                self.mate_copy(0, 2 * event + way).wait_send()

        def ring(event, carry):
            self.ring_copy(event, 0).wait_send()
            self.ring_copy(event, 1).wait_send()
            return carry
        lax.fori_loop(0, self.events, ring, 0)

    def run(self, filler):
        self.prepare(0, reuse=False)

        def first(event, carry):
            self.event(event, False)

            @pl.when(event < 1)
            def _():
                self.prepare(event + 1, reuse=False)

            @pl.when(event >= 1)
            def _():
                self.prepare(event + 1)
            filler(event)
            return carry

        def later(event, carry):
            self.event(event, True)

            @pl.when(event + 1 < self.events)
            def _():
                self.prepare(event + 1)

            @pl.when(event + 1 == self.events)
            def _():
                self.prepare_own(False)

            @pl.when(event == NP)
            def _():
                self.prepare_own(True)
            filler(event)
            return carry
        lax.fori_loop(0, NP, first, 0)
        lax.fori_loop(NP, self.events, later, 0)


def rope_pair(table):
    lanes = lax.broadcasted_iota(jnp.int32, table.shape, 1)
    swapped = pltpu.roll(table, HEAD_DIM // 2, 1)
    low = lanes < HEAD_DIM // 2
    return jnp.where(low, table, swapped), jnp.where(low, -swapped, table)


def rope(values, table, inverse=False):
    cos2, sin2 = rope_pair(table)
    turned = pltpu.roll(values, HEAD_DIM // 2, 1)
    if inverse:
        return values * cos2 - turned * sin2
    return values * cos2 + turned * sin2


def norm_forward(x_f32, gain_row):
    inv = lax.rsqrt(jnp.mean(x_f32 * x_f32, axis=-1, keepdims=True) + NORM_EPS)
    return (x_f32 * inv * gain_row).astype(BF16)


def norm_backward(x_f32, gain_row, d_normed):
    inv = lax.rsqrt(jnp.mean(x_f32 * x_f32, axis=-1, keepdims=True) + NORM_EPS)
    unit = x_f32 * inv
    d_unit = d_normed * gain_row
    d_x = inv * (d_unit - unit * jnp.mean(d_unit * unit, axis=-1, keepdims=True))
    return d_x, jnp.sum(d_normed * unit, axis=0, keepdims=True)


def attention_block(row0, rows, keys, refs, forward, backward):
    q_ref, k_ref, v_ref, table_ref, read_da, write_o, dx_ref, dk_ref, dv_ref = refs
    here = pl.ds(aligned(row0, rows), rows)
    scale = HEAD_DIM ** -0.5
    query = q_ref[here]
    scores = dot_nt(query, k_ref[0:keys]) * scale
    row_id = row0 + lax.broadcasted_iota(jnp.int32, scores.shape, 0)
    col_id = lax.broadcasted_iota(jnp.int32, scores.shape, 1)
    scores = jnp.where(row_id >= col_id, scores, -1e30)
    expd = jnp.exp(scores - jnp.max(scores, axis=-1, keepdims=True))
    prob = expd * (1.0 / jnp.sum(expd, axis=-1, keepdims=True))
    prob_b = prob.astype(BF16)
    d_attn = read_da(here) if backward else None
    if forward:
        write_o(here, dot_nn(prob_b, v_ref[0:keys]).astype(BF16))
    if backward:
        dv_ref[0:keys] += dot_tn(prob_b, d_attn)
        d_prob = dot_nt(d_attn, v_ref[0:keys]).astype(BF16).astype(F32)
        row_dot = jnp.sum(prob * d_prob, axis=-1, keepdims=True)
        d_scores = (prob * (d_prob - row_dot) * scale).astype(BF16)
        d_query = dot_nn(d_scores, k_ref[0:keys]).astype(BF16).astype(F32)
        dx_ref[here, 0:HEAD_DIM] = rope(d_query, table_ref[here], inverse=True).astype(BF16)
        dk_ref[0:keys] += dot_tn(d_scores, query)


def store_keys_values(dx_ref, dk_ref, dv_ref, table_ref, rows):
    def body(block, carry):
        here = pl.ds(aligned(block * rows, rows), rows)
        d_key = dk_ref[here].astype(BF16).astype(F32)
        dx_ref[here, HEAD_DIM:2 * HEAD_DIM] = rope(d_key, table_ref[here], inverse=True).astype(BF16)
        dx_ref[here, 2 * HEAD_DIM:3 * HEAD_DIM] = dv_ref[here].astype(BF16)
        return carry
    lax.fori_loop(0, dx_ref.shape[0] // rows, body, 0)


def gated_pull(gate, up, d_hidden):
    sig = jax.nn.sigmoid(gate)
    silu = gate * sig
    d_silu = d_hidden * up
    return (silu * up).astype(BF16), (d_silu * sig + d_silu * silu * (1.0 - sig)).astype(BF16), (d_hidden * silu).astype(BF16)


class Copies:
    def __init__(self, sems):
        self.sems, self.used = sems, 0

    def start(self, src, dst):
        copy = pltpu.make_async_copy(src, dst, self.sems.at[self.used])
        self.used += 1
        copy.start()
        return copy


def gather_units(gather, unit, event):
    step = lax.div(event, NP) + 1
    piece = lax.rem(event, NP)
    last = gather.events - 1
    own = event == 1
    near = (event >= NP) & (lax.rem(event, 2) == 0)
    final = event == last

    @pl.when(own | near | final)
    def _():
        distance = step - 1
        rightward = final | (piece != 0)
        gather.mate_wait_chip(distance, rightward)
        chip = gather.place.near(lax.select(rightward, distance, -distance))
        unit(chip)


def kernel_first(tp_size, x_ref, gain_ref, gy_hbm, table_hbm, wqkv_hbm, wout_hbm, wgate_hbm, wup_hbm, wdown_hbm,
                 x1_out, u1_out, u0_out, gy_out, q_out, k_out, v_out, o_out, ab_out, dah_out, *scratch):
    n_gather, n_reduce = 6, 10
    (u_ref, g_ref, wc_ref, wo_ref, wo1_ref, q_ref, k_ref, v_ref, om_ref, ab_ref, dah_ref, table_ref, y_ref, local) = scratch[:14]
    sems_u = scratch[14:14 + n_gather]
    sems_g = scratch[14 + n_gather:14 + 2 * n_gather]
    refs_r = scratch[14 + 2 * n_gather:]
    place = Place(tp_size)
    shard, width = x_ref.shape
    pair = 2 * shard
    chips = place.ring
    head_cols = wqkv_hbm.shape[2]
    ff = wgate_hbm.shape[2]
    piece_cols = width // NP

    loads = Copies(local)
    gu = Gather(place, u_ref, shard, sems_u)
    gg = Gather(place, g_ref, shard, sems_g)
    load_g = loads.start(gy_hbm, g_ref.at[gg.own_rows()])
    load_w = [loads.start(wqkv_hbm.at[0], wc_ref.at[:, 0:head_cols]),
              loads.start(wgate_hbm.at[0], wc_ref.at[:, head_cols:head_cols + ff]),
              loads.start(wup_hbm.at[0], wc_ref.at[:, head_cols + ff:head_cols + 2 * ff]),
              loads.start(table_hbm, table_ref)]
    load_o = []
    for piece in range(NP):
        cols = slice(piece * piece_cols, (piece + 1) * piece_cols)
        load_o.append(loads.start(wout_hbm.at[0, :, cols], wo_ref.at[piece, 0:HEAD_DIM]))
        load_o.append(loads.start(wdown_hbm.at[0, :, cols], wo_ref.at[piece, HEAD_DIM:HEAD_DIM + ff]))
    load_o.append(loads.start(wout_hbm.at[1], wo1_ref.at[0:HEAD_DIM]))
    load_o.append(loads.start(wdown_hbm.at[1], wo1_ref.at[HEAD_DIM:HEAD_DIM + ff]))

    x_f32 = x_ref[...].astype(F32)
    u_own = norm_forward(x_f32, gain_ref[0:1])
    u_ref[gu.own_rows()] = u_own
    u0_out[...] = u_own
    place.barrier()
    gu.start()
    load_g.wait()
    for copy in load_w:
        copy.wait()

    n_out = loads.used

    def ab_copy(slot, here):
        return pltpu.make_async_copy(ab_ref.at[slot], ab_out.at[here], local.at[n_out + slot])

    def unit(count, chip):
        here = pl.ds(aligned(chip * pair, pair), pair)
        slot = lax.rem(count, 2)
        rows_u = u_ref[here]
        qkv = dot_nn(rows_u, wc_ref[:, 0:head_cols]).astype(BF16)
        table = table_ref[here]
        q_ref[here] = rope(qkv[:, 0:HEAD_DIM].astype(F32), table).astype(BF16)
        k_ref[here] = rope(qkv[:, HEAD_DIM:2 * HEAD_DIM].astype(F32), table).astype(BF16)
        v_ref[here] = qkv[:, 2 * HEAD_DIM:3 * HEAD_DIM]

        @pl.when(count >= 2)
        def _():
            ab_copy(slot, here).wait()
        gate = dot_nn(rows_u, wc_ref[:, head_cols:head_cols + ff]).astype(BF16)
        up = dot_nn(rows_u, wc_ref[:, head_cols + ff:head_cols + 2 * ff]).astype(BF16)
        ab_ref[slot, :, 0:ff] = gate
        ab_ref[slot, :, ff:2 * ff] = up
        gate_f, up_f = gate.astype(F32), up.astype(F32)
        om_ref[here, HEAD_DIM:HEAD_DIM + ff] = (gate_f * jax.nn.sigmoid(gate_f) * up_f).astype(BF16)
        ab_copy(slot, here).start()

    def unit_count(event):
        return lax.select(event == 1, 0, lax.select(event == gu.events - 1, chips - 2, lax.div(event, 2) - 1))

    def loop_u(event, carry):
        gu.event(event)

        @pl.when(event == gu.events - NP)
        def _():
            gg.start()
        gather_units(gu, functools.partial(unit, unit_count(event)), event)
        return carry
    lax.fori_loop(0, gu.events, loop_u, 0)
    gu.mate_wait_last()
    unit(jnp.int32(chips - 1), place.near(place.half))

    def write_o(here, value):
        om_ref[here, 0:HEAD_DIM] = value

    blocks = chips
    refs_a = (q_ref, k_ref, v_ref, table_ref, None, write_o, None, None, None)

    def loop_g(event, carry):
        gg.event(event, forward=True)

        @pl.when(event < blocks)
        def _():
            attention_block(event * pair, pair, chips * pair, refs_a, True, False)
        return carry
    lax.fori_loop(0, gg.events - NP, loop_g, 0)
    for copy in load_o:
        copy.wait()

    outs = Copies(local)
    outs.used = n_out + 2
    saves = [outs.start(q_ref, q_out), outs.start(k_ref, k_out), outs.start(v_ref, v_out),
             outs.start(om_ref.at[:, 0:HEAD_DIM], o_out)]
    n_dah = outs.used + 1

    def gy_copy():
        return pltpu.make_async_copy(g_ref, gy_out, local.at[n_dah - 1])

    def dah_copy(slot, here):
        return pltpu.make_async_copy(dah_ref.at[slot], dah_out.at[here], local.at[n_dah + slot])

    def part(chip, piece):
        here = pl.ds(aligned(chip * pair, pair), pair)
        return dot_nn(om_ref[here], wo_ref[piece])

    reduce = Reduce(place, part, shard, refs_r)

    def filler(event):
        @pl.when(event < NP)
        def _():
            gg.event(gg.events - NP + event, forward=False)

        @pl.when(event == NP - 1)
        def _():
            gg.mate_wait_all()
            gy_copy().start()

        @pl.when((event >= NP) & (event < NP + chips))
        def _():
            block = event - NP
            here = pl.ds(aligned(block * pair, pair), pair)
            slot = lax.rem(block, 2)

            @pl.when(block >= 2)
            def _():
                dah_copy(slot, here).wait()
            dah_ref[slot] = dot_nt(g_ref[here], wo1_ref[...]).astype(BF16)
            dah_copy(slot, here).start()

    reduce.run(filler)
    for piece in reduce.final_order():
        y_ref[:, piece * piece_cols:(piece + 1) * piece_cols] = reduce.final(piece)
    x_next = (x_ref[...].astype(F32) + y_ref[...]).astype(BF16)
    x1_out[...] = x_next
    u1_out[...] = norm_forward(x_next.astype(F32), gain_ref[1:2])
    gu.finish()
    gg.finish()
    reduce.finish()
    for copy in saves:
        copy.wait()
    gy_copy().wait()
    for slot in range(2):
        ab_copy(slot, pl.ds(0, pair)).wait()
        dah_copy(slot, pl.ds(0, pair)).wait()


def weight_grads_u(block, u_ref, dx_ref, stage_ref, outs, sems, head_cols, ff):
    rows = stage_ref.shape[1]
    slot = lax.rem(block, 2)
    here = pl.ds(aligned(block * rows, rows), rows)

    def copies():
        bounds = (0, head_cols, head_cols + ff, head_cols + 2 * ff)
        return [pltpu.make_async_copy(stage_ref.at[slot, :, bounds[i]:bounds[i + 1]], outs[i].at[here], sems.at[slot, i]) for i in range(3)]

    @pl.when(block >= 2)
    def _():
        for copy in copies():
            copy.wait()
    stage_ref[slot] = dot_tn(u_ref[:, here], dx_ref[...]).astype(BF16)
    for copy in copies():
        copy.start()


def weight_grads_u_wait(stage_ref, outs, sems, head_cols, ff):
    rows = stage_ref.shape[1]
    bounds = (0, head_cols, head_cols + ff, head_cols + 2 * ff)
    for slot in range(2):
        for i in range(3):
            pltpu.make_async_copy(stage_ref.at[slot, :, bounds[i]:bounds[i + 1]], outs[i].at[pl.ds(0, rows)], sems.at[slot, i]).wait()


def weight_grads_h(piece, ho_ref, read_dy, stage_ref, outs, sems, ff):
    cols = stage_ref.shape[2]
    stage_ref[piece] = dot_tn(ho_ref[...], read_dy(piece)).astype(BF16)
    for copy in h_copies(piece, stage_ref, outs, sems, ff):
        copy.start()


def h_copies(piece, stage_ref, outs, sems, ff):
    cols = stage_ref.shape[2]
    there = pl.ds(aligned(piece * cols, cols), cols)
    return [pltpu.make_async_copy(stage_ref.at[piece, 0:HEAD_DIM], outs[0].at[:, there], sems.at[piece, 0]),
            pltpu.make_async_copy(stage_ref.at[piece, HEAD_DIM:HEAD_DIM + ff], outs[1].at[:, there], sems.at[piece, 1])]


def kernel_last_block(tp_size, x_ref, dy_ref, gain_ref, u_hbm, gy_hbm, dah_hbm, table_hbm, wqkv_hbm, wgate_hbm, wup_hbm,
                      dx_out, gain_out, gqkv_out, gout_out, ggate_out, gup_out, gdown_out, *scratch):
    n_gather = 6
    (u_ref, wc_ref, dx_ref, ho_ref, gy_ref, q_ref, k_ref, v_ref, dk_ref, dv_ref, table_ref, y_ref, gs_ref, hs_ref, local,
     sems_gs, sems_hs, sems_gy) = scratch[:18]
    sems_u = scratch[18:18 + n_gather]
    refs_r = scratch[18 + n_gather:]
    place = Place(tp_size)
    shard, width = x_ref.shape
    pair = 2 * shard
    chips = place.ring
    head_cols = wqkv_hbm.shape[2]
    ff = wgate_hbm.shape[2]
    piece_cols = width // NP

    loads = Copies(local)
    gu = Gather(place, u_ref, shard, sems_u)
    load_u = loads.start(u_hbm, u_ref.at[gu.own_rows()])
    load_w = [loads.start(wqkv_hbm.at[1], wc_ref.at[:, 0:head_cols]),
              loads.start(wgate_hbm.at[1], wc_ref.at[:, head_cols:head_cols + ff]),
              loads.start(wup_hbm.at[1], wc_ref.at[:, head_cols + ff:head_cols + 2 * ff]),
              loads.start(table_hbm, table_ref),
              loads.start(dah_hbm, ho_ref)]

    def gy_load(piece):
        slot = piece % 2 if isinstance(piece, int) else lax.rem(piece, 2)
        cols = pl.ds(aligned(piece * piece_cols, piece_cols), piece_cols)
        return pltpu.make_async_copy(gy_hbm.at[:, cols], gy_ref.at[slot], sems_gy.at[slot])

    gy_load(0).start()
    gy_load(1).start()
    place.barrier()
    load_u.wait()
    gu.start()
    dk_ref[...] = jnp.zeros_like(dk_ref)
    dv_ref[...] = jnp.zeros_like(dv_ref)
    for copy in load_w:
        copy.wait()

    def unit(chip):
        here = pl.ds(aligned(chip * pair, pair), pair)
        rows_u = u_ref[here]
        qkv = dot_nn(rows_u, wc_ref[:, 0:head_cols]).astype(BF16)
        table = table_ref[here]
        q_ref[here] = rope(qkv[:, 0:HEAD_DIM].astype(F32), table).astype(BF16)
        k_ref[here] = rope(qkv[:, HEAD_DIM:2 * HEAD_DIM].astype(F32), table).astype(BF16)
        v_ref[here] = qkv[:, 2 * HEAD_DIM:3 * HEAD_DIM]
        gate = dot_nn(rows_u, wc_ref[:, head_cols:head_cols + ff]).astype(BF16).astype(F32)
        up = dot_nn(rows_u, wc_ref[:, head_cols + ff:head_cols + 2 * ff]).astype(BF16).astype(F32)
        d_hidden = ho_ref[here, HEAD_DIM:HEAD_DIM + ff].astype(F32)
        hidden, d_gate, d_up = gated_pull(gate, up, d_hidden)
        ho_ref[here, HEAD_DIM:HEAD_DIM + ff] = hidden
        dx_ref[here, head_cols:head_cols + ff] = d_gate
        dx_ref[here, head_cols + ff:head_cols + 2 * ff] = d_up

    def loop_u(event, carry):
        gu.event(event)
        gather_units(gu, unit, event)
        return carry
    lax.fori_loop(0, gu.events, loop_u, 0)
    gu.mate_wait_last()
    unit(place.near(place.half))

    def read_da(here):
        return ho_ref[here, 0:HEAD_DIM]

    def write_o(here, value):
        ho_ref[here, 0:HEAD_DIM] = value

    refs_a = (q_ref, k_ref, v_ref, table_ref, read_da, write_o, dx_ref, dk_ref, dv_ref)
    groups = 4
    for group in range(groups):
        def body(block, carry, group=group):
            attention_block(block * pair, pair, (group + 1) * (chips * pair // groups), refs_a, True, True)
            return carry
        lax.fori_loop(group * chips // groups, (group + 1) * chips // groups, body, 0)
    store_keys_values(dx_ref, dk_ref, dv_ref, table_ref, pair)

    def part(chip, piece):
        here = pl.ds(aligned(chip * pair, pair), pair)
        return dot_nt(dx_ref[here], wc_ref[pl.ds(aligned(piece * piece_cols, piece_cols), piece_cols)])

    reduce = Reduce(place, part, shard, refs_r)
    outs_u = (gqkv_out, ggate_out, gup_out)
    outs_h = (gout_out, gdown_out)

    def read_dy(piece):
        return gy_ref[lax.rem(piece, 2)]

    def filler(event):
        @pl.when(event < NP)
        def _():
            gy_load(event).wait()
            weight_grads_h(event, ho_ref, read_dy, hs_ref, outs_h, sems_hs, ff)

            @pl.when(event + 2 < NP)
            def _():
                gy_load(event + 2).start()

        @pl.when((event >= NP) & (event < NP + chips))
        def _():
            weight_grads_u(event - NP, u_ref, dx_ref, gs_ref, outs_u, sems_gs, head_cols, ff)

    reduce.run(filler)
    for piece in reduce.final_order():
        y_ref[:, piece * piece_cols:(piece + 1) * piece_cols] = reduce.final(piece)
    d_normed = y_ref[...].astype(BF16).astype(F32)
    d_x, gain_part = norm_backward(x_ref[...].astype(F32), gain_ref[1:2], d_normed)
    dx_out[...] = (dy_ref[...].astype(F32) + d_x).astype(BF16)
    gain_out[...] = gain_part
    gu.finish()
    reduce.finish()
    for piece in range(NP):
        for copy in h_copies(piece, hs_ref, outs_h, sems_hs, ff):
            copy.wait()
    weight_grads_u_wait(gs_ref, outs_u, sems_gs, head_cols, ff)


def kernel_first_block(tp_size, x_ref, dy_ref, gain_ref, gain1_ref, u_hbm, q_hbm, k_hbm, v_hbm, o_hbm, ab_hbm, table_hbm,
                       wqkv_hbm, wout_hbm, wgate_hbm, wup_hbm, wdown_hbm,
                       dx_out, gain_out, gqkv_out, gout_out, ggate_out, gup_out, gdown_out, *scratch):
    n_gather = 6
    (u_ref, g_ref, wc_ref, dx_ref, ho_ref, q_ref, k_ref, v_ref, dk_ref, dv_ref, table_ref, y_ref, gs_ref, hs_ref,
     pair_ref, all_ref, local, sems_gs, sems_hs, sem_ps, sem_pr, sem_as, sem_ar) = scratch[:23]
    sems_u = scratch[23:23 + n_gather]
    sems_g = scratch[23 + n_gather:23 + 2 * n_gather]
    refs_r = scratch[23 + 2 * n_gather:]
    place = Place(tp_size)
    shard, width = x_ref.shape
    pair = 2 * shard
    chips = place.ring
    head_cols = wqkv_hbm.shape[2]
    ff = wgate_hbm.shape[2]
    piece_cols = width // NP

    loads = Copies(local)
    gu = Gather(place, u_ref, shard, sems_u)
    gg = Gather(place, g_ref, shard, sems_g)
    load_u = loads.start(u_hbm, u_ref.at[gu.own_rows()])
    load_h = []
    for piece in range(NP):
        cols = slice(piece * piece_cols, (piece + 1) * piece_cols)
        load_h.append(loads.start(wout_hbm.at[0, :, cols], hs_ref.at[piece, 0:HEAD_DIM]))
        load_h.append(loads.start(wdown_hbm.at[0, :, cols], hs_ref.at[piece, HEAD_DIM:HEAD_DIM + ff]))
    load_h.append(loads.start(ab_hbm, dx_ref.at[:, head_cols:head_cols + 2 * ff]))
    load_a = [loads.start(q_hbm, q_ref), loads.start(k_hbm, k_ref), loads.start(v_hbm, v_ref),
              loads.start(o_hbm, ho_ref.at[:, 0:HEAD_DIM]),
              loads.start(table_hbm, table_ref),
              loads.start(wqkv_hbm.at[0], wc_ref.at[:, 0:head_cols]),
              loads.start(wgate_hbm.at[0], wc_ref.at[:, head_cols:head_cols + ff]),
              loads.start(wup_hbm.at[0], wc_ref.at[:, head_cols + ff:head_cols + 2 * ff])]

    g_ref[gg.own_rows()] = dy_ref[...]
    others = [{'tp': place.near(step) * 2 + place.core} for step in range(2, chips - 1)]
    place.barrier(others)
    gg.start()
    dk_ref[...] = jnp.zeros_like(dk_ref)
    dv_ref[...] = jnp.zeros_like(dv_ref)
    load_u.wait()
    for copy in load_h:
        copy.wait()

    def unit(chip):
        here = pl.ds(aligned(chip * pair, pair), pair)
        dah = dot_nt(g_ref[here, 0:piece_cols], hs_ref[0])
        for piece in range(1, NP):
            dah = dah + dot_nt(g_ref[here, piece * piece_cols:(piece + 1) * piece_cols], hs_ref[piece])
        dx_ref[here, 0:HEAD_DIM] = dah[:, 0:HEAD_DIM].astype(BF16)
        d_hidden = dah[:, HEAD_DIM:HEAD_DIM + ff].astype(BF16).astype(F32)
        gate = dx_ref[here, head_cols:head_cols + ff].astype(F32)
        up = dx_ref[here, head_cols + ff:head_cols + 2 * ff].astype(F32)
        hidden, d_gate, d_up = gated_pull(gate, up, d_hidden)
        ho_ref[here, HEAD_DIM:HEAD_DIM + ff] = hidden
        dx_ref[here, head_cols:head_cols + ff] = d_gate
        dx_ref[here, head_cols + ff:head_cols + 2 * ff] = d_up

    def loop_g(event, carry):
        gg.event(event)

        @pl.when(event == gg.events - NP)
        def _():
            gu.start()
        gather_units(gg, unit, event)
        return carry
    lax.fori_loop(0, gg.events, loop_g, 0)
    gg.mate_wait_last()
    unit(place.near(place.half))
    for copy in load_a:
        copy.wait()

    def read_da(here):
        return dx_ref[here, 0:HEAD_DIM]

    refs_a = (q_ref, k_ref, v_ref, table_ref, read_da, None, dx_ref, dk_ref, dv_ref)
    step_rows = shard

    def loop_u(event, carry):
        gu.event(event, forward=True)

        @pl.when(event < chips)
        def _():
            def body(sub, inner):
                attention_block((event * 2 + sub) * step_rows, step_rows, chips * pair, refs_a, False, True)
                return inner
            lax.fori_loop(0, 2, body, 0)
        return carry
    lax.fori_loop(0, gu.events - NP, loop_u, 0)
    store_keys_values(dx_ref, dk_ref, dv_ref, table_ref, pair)

    def part(chip, piece):
        here = pl.ds(aligned(chip * pair, pair), pair)
        return dot_nt(dx_ref[here], wc_ref[pl.ds(aligned(piece * piece_cols, piece_cols), piece_cols)])

    reduce = Reduce(place, part, shard, refs_r)
    outs_u = (gqkv_out, ggate_out, gup_out)
    outs_h = (gout_out, gdown_out)

    def read_dy(piece):
        return g_ref[:, pl.ds(aligned(piece * piece_cols, piece_cols), piece_cols)]

    def filler(event):
        @pl.when(event < NP)
        def _():
            gu.event(gu.events - NP + event, forward=False)
            weight_grads_h(event, ho_ref, read_dy, hs_ref, outs_h, sems_hs, ff)

        @pl.when(event == NP - 1)
        def _():
            gu.mate_wait_all()

        @pl.when((event >= NP) & (event < NP + chips))
        def _():
            weight_grads_u(event - NP, u_ref, dx_ref, gs_ref, outs_u, sems_gs, head_cols, ff)

    reduce.run(filler)
    for piece in reduce.final_order():
        y_ref[:, piece * piece_cols:(piece + 1) * piece_cols] = reduce.final(piece)
    d_normed = y_ref[...].astype(BF16).astype(F32)
    d_x, gain_part = norm_backward(x_ref[...].astype(F32), gain_ref[0:1], d_normed)

    lanes = 128
    tiles = width // lanes
    for tile in range(tiles):
        pair_ref[0, tile:tile + 1] = gain_part[:, tile * lanes:(tile + 1) * lanes]
        pair_ref[0, tiles + tile:tiles + tile + 1] = gain1_ref[:, tile * lanes:(tile + 1) * lanes]
    cross = pltpu.make_async_remote_copy(pair_ref.at[0], pair_ref.at[1], sem_ps, sem_pr, place.mate, MESH)
    cross.start()
    dx_out[...] = (dy_ref[...].astype(F32) + d_x).astype(BF16)
    cross.wait()
    all_ref[place.chip] = pair_ref[0] + pair_ref[1]

    def spread(step):
        return pltpu.make_async_remote_copy(
            all_ref.at[place.chip], all_ref.at[place.chip], sem_as.at[step - 1], sem_ar.at[step - 1],
            {'tp': place.near(step) * 2 + place.core}, MESH)
    for step in range(1, chips):
        spread(step).start()
    gu.finish()
    gg.finish()
    reduce.finish()
    for piece in range(NP):
        for copy in h_copies(piece, hs_ref, outs_h, sems_hs, ff):
            copy.wait()
    weight_grads_u_wait(gs_ref, outs_u, sems_gs, head_cols, ff)
    for step in range(1, chips):
        spread(step).wait()
    total = all_ref[0]
    for chip in range(1, chips):
        total = total + all_ref[chip]
    gain_out[...] = total


def solution(mesh):
    tp_size = mesh.shape['tp']
    half = tp_size // 4
    row_spec = P(('dp', 'tp'), None)
    col_spec = P(None, None, 'tp')
    inner_spec = P(None, 'tp', None)

    def device_program(x_loc, dy_loc, norm_gain, w_qkv, w_out, w_gate, w_up, w_down):
        shard, width = x_loc.shape
        seq = shard * tp_size
        pair = 2 * shard
        chips = tp_size // 2
        head_cols = w_qkv.shape[2]
        ff = w_gate.shape[2]
        cols = head_cols + 2 * ff
        piece_cols = width // NP
        vmem, anyspace = pl.BlockSpec(memory_space=pltpu.VMEM), pl.BlockSpec(memory_space=pl.ANY)
        shape = jax.ShapeDtypeStruct
        dma = pltpu.SemaphoreType.DMA

        half_dim = HEAD_DIM // 2
        freqs = ROPE_BASE ** (-2.0 * jnp.arange(half_dim, dtype=F32) / HEAD_DIM)
        angles = jnp.arange(seq, dtype=F32)[:, None] * freqs[None, :]
        table = jnp.concatenate([jnp.cos(angles), jnp.sin(angles)], axis=1)

        def params(number):
            return pltpu.CompilerParams(collective_id=number, has_side_effects=True, vmem_limit_bytes=67043328)

        rows_shape = shape((shard, width), BF16)
        head_shape = shape((seq, HEAD_DIM), BF16)
        gathers = Gather.scratch(half)
        reduces = Reduce.scratch(half, shard, piece_cols)
        x1, u1, u0, gy_full, q0, k0, v0, o0, ab0, dah1 = pl.pallas_call(
            functools.partial(kernel_first, tp_size),
            out_shape=(rows_shape, rows_shape, rows_shape, shape((seq, width), BF16), head_shape, head_shape, head_shape, head_shape,
                       shape((seq, 2 * ff), BF16), shape((seq, HEAD_DIM + ff), BF16)),
            in_specs=[vmem, vmem] + [anyspace] * 7,
            out_specs=(vmem, vmem, vmem) + (anyspace,) * 7,
            scratch_shapes=[
                pltpu.VMEM((seq, width), BF16), pltpu.VMEM((seq, width), BF16), pltpu.VMEM((width, cols), BF16),
                pltpu.VMEM((NP, HEAD_DIM + ff, piece_cols), BF16), pltpu.VMEM((HEAD_DIM + ff, width), BF16),
                pltpu.VMEM((seq, HEAD_DIM), BF16), pltpu.VMEM((seq, HEAD_DIM), BF16), pltpu.VMEM((seq, HEAD_DIM), BF16),
                pltpu.VMEM((seq, HEAD_DIM + ff), BF16), pltpu.VMEM((2, pair, 2 * ff), BF16), pltpu.VMEM((2, pair, HEAD_DIM + ff), BF16),
                pltpu.VMEM((seq, HEAD_DIM), F32), pltpu.VMEM((shard, width), F32), dma((32,))] + gathers + gathers + reduces,
            compiler_params=params(1), name='first_forward',
        )(x_loc, norm_gain, dy_loc, table, w_qkv, w_out, w_gate, w_up, w_down)

        grad_shapes = (rows_shape, shape((1, width), F32), shape((width, head_cols), BF16), shape((HEAD_DIM, width), BF16),
                       shape((width, ff), BF16), shape((width, ff), BF16), shape((ff, width), BF16))
        dx1, gain1, gqkv1, gout1, ggate1, gup1, gdown1 = pl.pallas_call(
            functools.partial(kernel_last_block, tp_size),
            out_shape=grad_shapes,
            in_specs=[vmem, vmem, vmem] + [anyspace] * 7,
            out_specs=(vmem, vmem) + (anyspace,) * 5,
            scratch_shapes=[
                pltpu.VMEM((seq, width), BF16), pltpu.VMEM((width, cols), BF16), pltpu.VMEM((seq, cols), BF16),
                pltpu.VMEM((seq, HEAD_DIM + ff), BF16), pltpu.VMEM((2, seq, piece_cols), BF16),
                pltpu.VMEM((seq, HEAD_DIM), BF16), pltpu.VMEM((seq, HEAD_DIM), BF16), pltpu.VMEM((seq, HEAD_DIM), BF16),
                pltpu.VMEM((seq, HEAD_DIM), F32), pltpu.VMEM((seq, HEAD_DIM), F32), pltpu.VMEM((seq, HEAD_DIM), F32),
                pltpu.VMEM((shard, width), F32), pltpu.VMEM((2, width // chips, cols), BF16),
                pltpu.VMEM((NP, HEAD_DIM + ff, piece_cols), BF16),
                dma((16,)), dma((2, 3)), dma((NP, 2)), dma((2,))] + gathers + reduces,
            compiler_params=params(2), name='last_block',
        )(x1, dy_loc, norm_gain, u1, gy_full, dah1, table, w_qkv, w_gate, w_up)

        grad_shapes = (rows_shape, shape((2 * width // 128, 128), F32)) + grad_shapes[2:]
        grad_x, gains, gqkv0, gout0, ggate0, gup0, gdown0 = pl.pallas_call(
            functools.partial(kernel_first_block, tp_size),
            out_shape=grad_shapes,
            in_specs=[vmem] * 4 + [anyspace] * 12,
            out_specs=(vmem, vmem) + (anyspace,) * 5,
            scratch_shapes=[
                pltpu.VMEM((seq, width), BF16), pltpu.VMEM((seq, width), BF16), pltpu.VMEM((width, cols), BF16), pltpu.VMEM((seq, cols), BF16),
                pltpu.VMEM((seq, HEAD_DIM + ff), BF16),
                pltpu.VMEM((seq, HEAD_DIM), BF16), pltpu.VMEM((seq, HEAD_DIM), BF16), pltpu.VMEM((seq, HEAD_DIM), BF16),
                pltpu.VMEM((seq, HEAD_DIM), F32), pltpu.VMEM((seq, HEAD_DIM), F32), pltpu.VMEM((seq, HEAD_DIM), F32),
                pltpu.VMEM((shard, width), F32), pltpu.VMEM((2, width // chips, cols), BF16),
                pltpu.VMEM((NP, HEAD_DIM + ff, piece_cols), BF16),
                pltpu.VMEM((2, 2 * width // 128, 128), F32), pltpu.VMEM((chips, 2 * width // 128, 128), F32),
                dma((32,)), dma((2, 3)), dma((NP, 2)), dma(()), dma(()), dma((chips - 1,)), dma((chips - 1,))] + gathers + gathers + reduces,
            compiler_params=params(3), name='first_block',
        )(x_loc, dx1, norm_gain, gain1, u0, q0, k0, v0, o0, ab0, table, w_qkv, w_out, w_gate, w_up, w_down)

        grad_gain = gains.reshape(2, width)
        return (grad_x, grad_gain, jnp.stack([gqkv0, gqkv1]), jnp.stack([gout0, gout1]), jnp.stack([ggate0, ggate1]),
                jnp.stack([gup0, gup1]), jnp.stack([gdown0, gdown1]))

    return jax.shard_map(device_program, mesh=mesh, in_specs=(row_spec, row_spec, P(None, None), col_spec, inner_spec, col_spec, col_spec, inner_spec), out_specs=(row_spec, P('dp', None), P('dp', None, 'tp'), P('dp', 'tp', None), P('dp', None, 'tp'), P('dp', None, 'tp'), P('dp', 'tp', None)), check_vma=False)
```

```python
import functools

import jax
import jax.numpy as jnp
import numpy as np
from jax import lax
from jax.experimental import pallas as pl
from jax.experimental.pallas import tpu as pltpu
from jax.sharding import PartitionSpec as P

HEAD_DIM = 128
NORM_EPS = 1e-5
ROPE_BASE = 10000.0
MESH = pl.DeviceIdType.MESH
NP = 4
F32 = jnp.float32
BF16 = jnp.bfloat16


def dot_nn(a, b):
    return lax.dot_general(a, b, (((1,), (0,)), ((), ())), preferred_element_type=F32)


def dot_nt(a, b):
    return lax.dot_general(a, b, (((1,), (1,)), ((), ())), preferred_element_type=F32)


def dot_tn(a, b):
    return lax.dot_general(a, b, (((0,), (0,)), ((), ())), preferred_element_type=F32)


def aligned(index, size):
    return pl.multiple_of(index, size)


class Place:
    def __init__(self, tp_size):
        index = lax.axis_index('tp')
        self.ring = tp_size // 2
        self.half = self.ring // 2
        self.core = lax.rem(index, 2)
        self.chip = lax.div(index, 2)
        self.right = {'tp': self.near(1) * 2 + self.core}
        self.left = {'tp': self.near(-1) * 2 + self.core}
        self.mate = {'tp': self.chip * 2 + 1 - self.core}

    def near(self, step):
        return lax.rem(self.chip + step + self.ring, self.ring)

    def barrier(self, others=()):
        sem = pltpu.get_barrier_semaphore()
        peers = [self.right, self.left, self.mate] + list(others)
        for peer in peers:
            pl.semaphore_signal(sem, inc=1, device_id=peer, device_id_type=MESH)
        pl.semaphore_wait(sem, len(peers))


class Gather:
    def __init__(self, place, buf, shard_rows, sems):
        self.place, self.buf, self.shard = place, buf, shard_rows
        self.rows = shard_rows // NP
        self.events = (place.half - 1) * NP + NP // 2
        self.send_r, self.recv_r, self.send_l, self.recv_l, self.send_m, self.recv_m = sems

    @staticmethod
    def scratch(half):
        events = (half - 1) * NP + NP // 2
        return [pltpu.SemaphoreType.DMA((n,)) for n in (events, events, events, events, 2 * events + NP, 2 * events + NP)]

    def view(self, chip, core, piece):
        start = (chip * 2 + core) * self.shard + piece * self.rows
        return self.buf.at[pl.ds(aligned(start, self.rows), self.rows)]

    def own_rows(self):
        start = (self.place.chip * 2 + self.place.core) * self.shard
        return pl.ds(aligned(start, self.shard), self.shard)

    def to_right(self, event, view):
        return pltpu.make_async_remote_copy(view, view, self.send_r.at[event], self.recv_r.at[event], self.place.right, MESH)

    def to_left(self, event, view):
        return pltpu.make_async_remote_copy(view, view, self.send_l.at[event], self.recv_l.at[event], self.place.left, MESH)

    def to_mate(self, slot, view):
        return pltpu.make_async_remote_copy(view, view, self.send_m.at[slot], self.recv_m.at[slot], self.place.mate, MESH)

    def start(self):
        place = self.place
        for piece in range(NP):
            self.to_right(piece, self.view(place.chip, place.core, piece)).start()
            self.to_left(piece, self.view(place.chip, place.core, NP - 1 - piece)).start()
        for piece in range(NP):
            self.to_mate(2 * self.events + piece, self.view(place.chip, place.core, piece)).start()

    def views(self, event):
        step = lax.div(event, NP) + 1
        piece = lax.rem(event, NP)
        from_left = self.view(self.place.near(-step), self.place.core, piece)
        from_right = self.view(self.place.near(step), self.place.core, NP - 1 - piece)
        return from_left, from_right

    def event(self, event, forward=None):
        from_left, from_right = self.views(event)
        self.to_right(event, from_left).wait_recv()
        self.pass_on(event, forward, lambda: self.to_right(event + NP, from_left).start())
        self.to_mate(event, from_left).start()
        self.to_left(event, from_right).wait_recv()
        self.pass_on(event, forward, lambda: self.to_left(event + NP, from_right).start())
        self.to_mate(self.events + event, from_right).start()

    def pass_on(self, event, forward, send):
        if forward is None:
            pl.when(event + NP < self.events)(send)
        elif forward:
            send()

    def mate_wait(self, first, count):
        for offset in range(count):
            self.to_mate(first + offset, self.view(self.place.chip, 1 - self.place.core, 0)).wait_recv()

    def mate_wait_all(self):
        def body(slot, carry):
            self.mate_wait(slot, 1)
            return carry
        lax.fori_loop(0, 2 * self.events + NP, body, 0)

    def mate_wait_last(self):
        first = (self.place.half - 1) * NP
        self.mate_wait(first, NP // 2)
        self.mate_wait(self.events + first, NP // 2)

    def mate_wait_chip(self, distance, rightward):
        ring_first = lax.select(rightward, self.events, 0) + jnp.maximum(distance - 1, 0) * NP
        self.mate_wait(lax.select(distance == 0, 2 * self.events, ring_first), NP)

    def finish(self):
        view = self.view(self.place.chip, self.place.core, 0)

        def ring(event, carry):
            self.to_right(event, view).wait_send()
            self.to_left(event, view).wait_send()
            return carry
        lax.fori_loop(0, self.events, ring, 0)

        def across(slot, carry):
            self.to_mate(slot, view).wait_send()
            return carry
        lax.fori_loop(0, 2 * self.events + NP, across, 0)


class Reduce:
    SLOTS = 6

    def __init__(self, place, part, shard_rows, refs):
        self.place, self.part, self.shard = place, part, shard_rows
        self.events = (place.half - 1) * NP + NP // 2
        self.ring, self.acc, self.stage, self.send_n, self.recv_n, self.send_m, self.recv_m = refs

    @staticmethod
    def scratch(half, shard_rows, width):
        events = (half - 1) * NP + NP // 2
        shapes = [(2, events), (2 * events + NP,), (Reduce.SLOTS, 2)]
        sems = [(2, events), (2, events), (2 * events + NP,), (2 * events + NP,)]
        return [pltpu.VMEM(s + (shard_rows, width), F32) for s in shapes] + [pltpu.SemaphoreType.DMA(s) for s in sems]

    def mate_copy(self, term):
        return pltpu.make_async_remote_copy(
            self.stage.at[lax.rem(term, self.SLOTS), 1 - self.place.core], self.acc.at[term], self.send_m.at[term], self.recv_m.at[term],
            self.place.mate, MESH)

    def ring_copy(self, event, way):
        to = {'tp': self.place.near(1 - 2 * way) * 2 + self.place.core}
        return pltpu.make_async_remote_copy(
            self.acc.at[2 * event + way], self.ring.at[way, event], self.send_n.at[way, event], self.recv_n.at[way, event], to, MESH)

    def fill(self, term):
        @pl.when(term >= self.SLOTS)
        def _():
            self.mate_copy(jnp.maximum(term - self.SLOTS, 0)).wait_send()
        slot = lax.rem(term, self.SLOTS)
        way = lax.rem(term, 2)
        shifted = lax.div(term, 2) + NP // 2
        travels = term < 2 * self.events
        distance = jnp.maximum(self.place.half - lax.div(shifted, NP), 0)
        turn = lax.rem(shifted, NP)
        piece = lax.select(travels, lax.select(way == 0, turn, NP - 1 - turn), lax.rem(jnp.maximum(term - 2 * self.events, 0), NP))
        value = self.part(self.place.near((1 - 2 * way) * distance), piece)
        self.stage[slot, 0] = value[:self.shard]
        self.stage[slot, 1] = value[self.shard:]
        self.mate_copy(term).start()

    def event(self, event):
        def add(way, carry):
            term = 2 * event + way
            self.mate_copy(term).wait_recv()
            self.acc[term] += self.stage[lax.rem(term, self.SLOTS), self.place.core]

            @pl.when(event >= NP)
            def _():
                before = jnp.maximum(event - NP, 0)
                self.ring_copy(before, way).wait_recv()
                self.acc[term] += self.ring[way, before]
            self.ring_copy(event, way).start()
            return carry
        lax.fori_loop(0, 2, add, 0)

    def final(self, piece):
        last = self.events - NP
        term = 2 * self.events + piece
        self.mate_copy(term).wait_recv()
        self.ring_copy(last + piece, 0).wait_recv()
        self.ring_copy(last + NP - 1 - piece, 1).wait_recv()
        return ((self.stage[term % self.SLOTS, self.place.core] + self.acc[term])
                + (self.ring[0, last + piece] + self.ring[1, last + NP - 1 - piece]))

    def finish(self):
        def across(term, carry):
            self.mate_copy(term).wait_send()
            return carry
        terms = 2 * self.events + NP
        lax.fori_loop(terms - self.SLOTS, terms, across, 0)

        def ring(event, carry):
            self.ring_copy(event, 0).wait_send()
            self.ring_copy(event, 1).wait_send()
            return carry
        lax.fori_loop(0, self.events, ring, 0)

    def run(self, filler):
        def body(turn, carry):
            event = jnp.maximum(turn - 1, 0)
            travels = (turn >= 1) & (turn <= self.events)

            @pl.when(travels)
            def _():
                self.event(event)

            def ahead(way, inner):
                self.fill(2 * turn + way)
                return inner
            lax.fori_loop(0, 2, ahead, 0)

            @pl.when(travels)
            def _():
                filler(event)
            return carry
        lax.fori_loop(0, self.events + 2, body, 0)


def rope_pair(table):
    lanes = lax.broadcasted_iota(jnp.int32, table.shape, 1)
    swapped = pltpu.roll(table, HEAD_DIM // 2, 1)
    low = lanes < HEAD_DIM // 2
    return jnp.where(low, table, swapped), jnp.where(low, -swapped, table)


def fill_table(freqs, table_ref):
    rows = 64
    blocks = table_ref.shape[0] // rows

    def cos_sin(count, scale):
        steps = lax.broadcasted_iota(jnp.int32, (count, HEAD_DIM), 0) * scale
        angles = steps.astype(F32) * freqs
        return jnp.cos(angles), jnp.sin(angles)
    cos_low, sin_low = cos_sin(rows, 1)
    cos_high, sin_high = cos_sin(max(blocks, 8), rows)
    low = lax.broadcasted_iota(jnp.int32, (1, HEAD_DIM), 1) < HEAD_DIM // 2
    first = jnp.where(low, cos_high, sin_high)
    second = jnp.where(low, -sin_high, cos_high)
    for block in range(blocks):
        table_ref[block * rows:(block + 1) * rows] = first[block:block + 1] * cos_low + second[block:block + 1] * sin_low


def rope(values, table, inverse=False):
    cos2, sin2 = rope_pair(table)
    turned = pltpu.roll(values, HEAD_DIM // 2, 1)
    if inverse:
        return values * cos2 - turned * sin2
    return values * cos2 + turned * sin2


def norm_forward(x_f32, gain_row):
    inv = lax.rsqrt(jnp.mean(x_f32 * x_f32, axis=-1, keepdims=True) + NORM_EPS)
    return (x_f32 * inv * gain_row).astype(BF16)


def norm_backward(x_f32, gain_row, d_normed):
    inv = lax.rsqrt(jnp.mean(x_f32 * x_f32, axis=-1, keepdims=True) + NORM_EPS)
    unit = x_f32 * inv
    d_unit = d_normed * gain_row
    d_x = inv * (d_unit - unit * jnp.mean(d_unit * unit, axis=-1, keepdims=True))
    return d_x, jnp.sum(d_normed * unit, axis=0, keepdims=True)


def attention_block(row0, rows, keys, refs, forward, backward):
    q_ref, k_ref, v_ref, table_ref, read_da, write_o, dx_ref, dk_ref, dv_ref = refs
    here = pl.ds(aligned(row0, rows), rows)
    scale = HEAD_DIM ** -0.5
    query = q_ref[here]
    scores = dot_nt(query, k_ref[0:keys]) * scale
    row_id = row0 + lax.broadcasted_iota(jnp.int32, scores.shape, 0)
    col_id = lax.broadcasted_iota(jnp.int32, scores.shape, 1)
    scores = jnp.where(row_id >= col_id, scores, -1e30)
    expd = jnp.exp(scores - jnp.max(scores, axis=-1, keepdims=True))
    prob = expd * (1.0 / jnp.sum(expd, axis=-1, keepdims=True))
    prob_b = prob.astype(BF16)
    d_attn = read_da(here) if backward else None
    if forward:
        write_o(here, dot_nn(prob_b, v_ref[0:keys]).astype(BF16))
    if backward:
        dv_ref[0:keys] += dot_tn(prob_b, d_attn)
        d_prob = dot_nt(d_attn, v_ref[0:keys]).astype(BF16).astype(F32)
        row_dot = jnp.sum(prob * d_prob, axis=-1, keepdims=True)
        d_scores = (prob * (d_prob - row_dot) * scale).astype(BF16)
        d_query = dot_nn(d_scores, k_ref[0:keys]).astype(BF16).astype(F32)
        dx_ref[here, 0:HEAD_DIM] = rope(d_query, table_ref[here], inverse=True).astype(BF16)
        dk_ref[0:keys] += dot_tn(d_scores, query)


def store_keys_values(dx_ref, dk_ref, dv_ref, table_ref, rows):
    def body(block, carry):
        here = pl.ds(aligned(block * rows, rows), rows)
        d_key = dk_ref[here].astype(BF16).astype(F32)
        dx_ref[here, HEAD_DIM:2 * HEAD_DIM] = rope(d_key, table_ref[here], inverse=True).astype(BF16)
        dx_ref[here, 2 * HEAD_DIM:3 * HEAD_DIM] = dv_ref[here].astype(BF16)
        return carry
    lax.fori_loop(0, dx_ref.shape[0] // rows, body, 0)


def gated_pull(gate, up, d_hidden):
    sig = jax.nn.sigmoid(gate)
    silu = gate * sig
    d_silu = d_hidden * up
    return (silu * up).astype(BF16), (d_silu * sig + d_silu * silu * (1.0 - sig)).astype(BF16), (d_hidden * silu).astype(BF16)


class Copies:
    def __init__(self, sems):
        self.sems, self.used = sems, 0

    def start(self, src, dst):
        copy = pltpu.make_async_copy(src, dst, self.sems.at[self.used])
        self.used += 1
        copy.start()
        return copy


def gather_loop(gather, unit, then=None):
    chips = gather.place.ring

    def body(event, carry):
        @pl.when(event < gather.events)
        def _():
            gather.event(event)
            if then is not None:
                then(event)
        step = lax.div(event, NP) + 1
        opposite = event == gather.events
        final = event == gather.events - 1
        own = event == 1
        near = (event >= NP) & (event < gather.events) & (lax.rem(event, 2) == 0)

        @pl.when(opposite)
        def _():
            gather.mate_wait_last()

        @pl.when(own | near | final)
        def _():
            gather.mate_wait_chip(step - 1, final | (lax.rem(event, NP) != 0))

        @pl.when(own | near | final | opposite)
        def _():
            distance = lax.select(opposite, gather.place.half, step - 1)
            rightward = final | (lax.rem(event, NP) != 0)
            count = lax.select(own, 0, lax.select(opposite, chips - 1, lax.select(final, chips - 2, jnp.maximum(lax.div(event, 2) - 1, 0))))
            unit(count, gather.place.near(lax.select(rightward, distance, -distance)))
        return carry
    lax.fori_loop(0, gather.events + 1, body, 0)


def kernel_first(tp_size, x_ref, gain_ref, freq_ref, gy_hbm, wqkv_hbm, wout_hbm, wgate_hbm, wup_hbm, wdown_hbm,
                 x1_out, u1_out, u0_out, gy_out, q_out, k_out, v_out, o_out, ab_out, dah_out, table_out, *scratch):
    n_gather = 6
    (u_ref, g_ref, wc_ref, wo_ref, wo1_ref, q_ref, k_ref, v_ref, om_ref, ab_ref, dah_ref, table_ref, y_ref, local) = scratch[:14]
    sems_u = scratch[14:14 + n_gather]
    sems_g = scratch[14 + n_gather:14 + 2 * n_gather]
    refs_r = scratch[14 + 2 * n_gather:]
    place = Place(tp_size)
    shard, width = x_ref.shape
    pair = 2 * shard
    chips = place.ring
    head_cols = wqkv_hbm.shape[2]
    ff = wgate_hbm.shape[2]
    piece_cols = width // NP

    loads = Copies(local)
    gu = Gather(place, u_ref, shard, sems_u)
    gg = Gather(place, g_ref, shard, sems_g)
    load_g = loads.start(gy_hbm, g_ref.at[gg.own_rows()])
    load_w = [loads.start(wqkv_hbm.at[0], wc_ref.at[:, 0:head_cols]),
              loads.start(wgate_hbm.at[0], wc_ref.at[:, head_cols:head_cols + ff]),
              loads.start(wup_hbm.at[0], wc_ref.at[:, head_cols + ff:head_cols + 2 * ff])]
    load_o = []
    for piece in range(NP):
        cols = slice(piece * piece_cols, (piece + 1) * piece_cols)
        load_o.append(loads.start(wout_hbm.at[0, :, cols], wo_ref.at[piece, 0:HEAD_DIM]))
        load_o.append(loads.start(wdown_hbm.at[0, :, cols], wo_ref.at[piece, HEAD_DIM:HEAD_DIM + ff]))
    load_o.append(loads.start(wout_hbm.at[1], wo1_ref.at[0:HEAD_DIM]))
    load_o.append(loads.start(wdown_hbm.at[1], wo1_ref.at[HEAD_DIM:HEAD_DIM + ff]))

    x_f32 = x_ref[...].astype(F32)
    u_own = norm_forward(x_f32, gain_ref[0:1])
    u_ref[gu.own_rows()] = u_own
    u0_out[...] = u_own
    place.barrier()
    gu.start()
    fill_table(freq_ref[0:1], table_ref)
    load_g.wait()
    for copy in load_w:
        copy.wait()

    n_out = loads.used

    def ab_copy(slot, here):
        return pltpu.make_async_copy(ab_ref.at[slot], ab_out.at[here], local.at[n_out + slot])

    def unit(count, chip):
        here = pl.ds(aligned(chip * pair, pair), pair)
        slot = lax.rem(count, 2)
        rows_u = u_ref[here]
        qkv = dot_nn(rows_u, wc_ref[:, 0:head_cols]).astype(BF16)
        table = table_ref[here]
        q_ref[here] = rope(qkv[:, 0:HEAD_DIM].astype(F32), table).astype(BF16)
        k_ref[here] = rope(qkv[:, HEAD_DIM:2 * HEAD_DIM].astype(F32), table).astype(BF16)
        v_ref[here] = qkv[:, 2 * HEAD_DIM:3 * HEAD_DIM]

        @pl.when(count >= 2)
        def _():
            ab_copy(slot, here).wait()
        gate = dot_nn(rows_u, wc_ref[:, head_cols:head_cols + ff]).astype(BF16)
        up = dot_nn(rows_u, wc_ref[:, head_cols + ff:head_cols + 2 * ff]).astype(BF16)
        ab_ref[slot, :, 0:ff] = gate
        ab_ref[slot, :, ff:2 * ff] = up
        gate_f, up_f = gate.astype(F32), up.astype(F32)
        om_ref[here, HEAD_DIM:HEAD_DIM + ff] = (gate_f * jax.nn.sigmoid(gate_f) * up_f).astype(BF16)
        ab_copy(slot, here).start()

    def start_gy(event):
        @pl.when(event == gu.events - NP)
        def _():
            gg.start()
    gather_loop(gu, unit, start_gy)

    def write_o(here, value):
        om_ref[here, 0:HEAD_DIM] = value

    blocks = chips
    refs_a = (q_ref, k_ref, v_ref, table_ref, None, write_o, None, None, None)

    def loop_g(event, carry):
        gg.event(event, forward=True)

        @pl.when(event < blocks)
        def _():
            attention_block(event * pair, pair, chips * pair, refs_a, True, False)
        return carry
    lax.fori_loop(0, gg.events - NP, loop_g, 0)
    for copy in load_o:
        copy.wait()

    outs = Copies(local)
    outs.used = n_out + 2
    saves = [outs.start(q_ref, q_out), outs.start(k_ref, k_out), outs.start(v_ref, v_out),
             outs.start(om_ref.at[:, 0:HEAD_DIM], o_out), outs.start(table_ref, table_out)]
    n_dah = outs.used + 1

    def gy_copy():
        return pltpu.make_async_copy(g_ref, gy_out, local.at[n_dah - 1])

    def dah_copy(slot, here):
        return pltpu.make_async_copy(dah_ref.at[slot], dah_out.at[here], local.at[n_dah + slot])

    def part(chip, piece):
        here = pl.ds(aligned(chip * pair, pair), pair)
        return dot_nn(om_ref[here], wo_ref[piece])

    reduce = Reduce(place, part, shard, refs_r)

    def filler(event):
        @pl.when(event < NP)
        def _():
            gg.event(gg.events - NP + event, forward=False)

        @pl.when(event == NP - 1)
        def _():
            gg.mate_wait_all()
            gy_copy().start()

        @pl.when((event >= NP) & (event < NP + chips))
        def _():
            block = jnp.maximum(event - NP, 0)
            here = pl.ds(aligned(block * pair, pair), pair)
            slot = lax.rem(block, 2)

            @pl.when(block >= 2)
            def _():
                dah_copy(slot, here).wait()
            dah_ref[slot] = dot_nt(g_ref[here], wo1_ref[...]).astype(BF16)
            dah_copy(slot, here).start()

    reduce.run(filler)
    for piece in range(NP):
        y_ref[:, piece * piece_cols:(piece + 1) * piece_cols] = reduce.final(piece)
    x_next = (x_ref[...].astype(F32) + y_ref[...]).astype(BF16)
    x1_out[...] = x_next
    u1_out[...] = norm_forward(x_next.astype(F32), gain_ref[1:2])
    gu.finish()
    gg.finish()
    reduce.finish()
    for copy in saves:
        copy.wait()
    gy_copy().wait()
    for slot in range(2):
        ab_copy(slot, pl.ds(0, pair)).wait()
        dah_copy(slot, pl.ds(0, pair)).wait()


def weight_grads_u(block, u_ref, dx_ref, stage_ref, outs, sems, head_cols, ff):
    rows = stage_ref.shape[1]
    slot = lax.rem(block, 2)
    here = pl.ds(aligned(block * rows, rows), rows)

    def copies():
        bounds = (0, head_cols, head_cols + ff, head_cols + 2 * ff)
        return [pltpu.make_async_copy(stage_ref.at[slot, :, bounds[i]:bounds[i + 1]], outs[i].at[here], sems.at[slot, i]) for i in range(3)]

    @pl.when(block >= 2)
    def _():
        for copy in copies():
            copy.wait()
    stage_ref[slot] = dot_tn(u_ref[:, here], dx_ref[...]).astype(BF16)
    for copy in copies():
        copy.start()


def weight_grads_u_wait(stage_ref, outs, sems, head_cols, ff):
    rows = stage_ref.shape[1]
    bounds = (0, head_cols, head_cols + ff, head_cols + 2 * ff)
    for slot in range(2):
        for i in range(3):
            pltpu.make_async_copy(stage_ref.at[slot, :, bounds[i]:bounds[i + 1]], outs[i].at[pl.ds(0, rows)], sems.at[slot, i]).wait()


def weight_grads_h(piece, ho_ref, read_dy, stage_ref, outs, sems, ff):
    cols = stage_ref.shape[2]
    stage_ref[piece] = dot_tn(ho_ref[...], read_dy(piece)).astype(BF16)
    for copy in h_copies(piece, stage_ref, outs, sems, ff):
        copy.start()


def h_copies(piece, stage_ref, outs, sems, ff):
    cols = stage_ref.shape[2]
    there = pl.ds(aligned(piece * cols, cols), cols)
    return [pltpu.make_async_copy(stage_ref.at[piece, 0:HEAD_DIM], outs[0].at[:, there], sems.at[piece, 0]),
            pltpu.make_async_copy(stage_ref.at[piece, HEAD_DIM:HEAD_DIM + ff], outs[1].at[:, there], sems.at[piece, 1])]


def kernel_last_block(tp_size, x_ref, dy_ref, gain_ref, u_hbm, gy_hbm, dah_hbm, table_hbm, wqkv_hbm, wgate_hbm, wup_hbm,
                      dx_out, gain_out, gqkv_out, gout_out, ggate_out, gup_out, gdown_out, *scratch):
    n_gather = 6
    (u_ref, wc_ref, dx_ref, ho_ref, gy_ref, q_ref, k_ref, v_ref, dk_ref, dv_ref, table_ref, y_ref, gs_ref, hs_ref, local,
     sems_gs, sems_hs, sems_gy) = scratch[:18]
    sems_u = scratch[18:18 + n_gather]
    refs_r = scratch[18 + n_gather:]
    place = Place(tp_size)
    shard, width = x_ref.shape
    pair = 2 * shard
    chips = place.ring
    head_cols = wqkv_hbm.shape[2]
    ff = wgate_hbm.shape[2]
    piece_cols = width // NP

    loads = Copies(local)
    gu = Gather(place, u_ref, shard, sems_u)
    load_u = loads.start(u_hbm, u_ref.at[gu.own_rows()])
    load_w = [loads.start(wqkv_hbm.at[1], wc_ref.at[:, 0:head_cols]),
              loads.start(wgate_hbm.at[1], wc_ref.at[:, head_cols:head_cols + ff]),
              loads.start(wup_hbm.at[1], wc_ref.at[:, head_cols + ff:head_cols + 2 * ff]),
              loads.start(table_hbm, table_ref),
              loads.start(dah_hbm, ho_ref)]

    def gy_load(piece):
        slot = piece % 2 if isinstance(piece, int) else lax.rem(piece, 2)
        cols = pl.ds(aligned(piece * piece_cols, piece_cols), piece_cols)
        return pltpu.make_async_copy(gy_hbm.at[:, cols], gy_ref.at[slot], sems_gy.at[slot])

    gy_load(0).start()
    gy_load(1).start()
    place.barrier()
    load_u.wait()
    gu.start()
    dk_ref[...] = jnp.zeros_like(dk_ref)
    dv_ref[...] = jnp.zeros_like(dv_ref)
    for copy in load_w:
        copy.wait()

    def unit(count, chip):
        here = pl.ds(aligned(chip * pair, pair), pair)
        rows_u = u_ref[here]
        qkv = dot_nn(rows_u, wc_ref[:, 0:head_cols]).astype(BF16)
        table = table_ref[here]
        q_ref[here] = rope(qkv[:, 0:HEAD_DIM].astype(F32), table).astype(BF16)
        k_ref[here] = rope(qkv[:, HEAD_DIM:2 * HEAD_DIM].astype(F32), table).astype(BF16)
        v_ref[here] = qkv[:, 2 * HEAD_DIM:3 * HEAD_DIM]
        gate = dot_nn(rows_u, wc_ref[:, head_cols:head_cols + ff]).astype(BF16).astype(F32)
        up = dot_nn(rows_u, wc_ref[:, head_cols + ff:head_cols + 2 * ff]).astype(BF16).astype(F32)
        d_hidden = ho_ref[here, HEAD_DIM:HEAD_DIM + ff].astype(F32)
        hidden, d_gate, d_up = gated_pull(gate, up, d_hidden)
        ho_ref[here, HEAD_DIM:HEAD_DIM + ff] = hidden
        dx_ref[here, head_cols:head_cols + ff] = d_gate
        dx_ref[here, head_cols + ff:head_cols + 2 * ff] = d_up

    gather_loop(gu, unit)

    def read_da(here):
        return ho_ref[here, 0:HEAD_DIM]

    def write_o(here, value):
        ho_ref[here, 0:HEAD_DIM] = value

    refs_a = (q_ref, k_ref, v_ref, table_ref, read_da, write_o, dx_ref, dk_ref, dv_ref)
    groups = 4
    for group in range(groups):
        def body(block, carry, group=group):
            attention_block(block * pair, pair, (group + 1) * (chips * pair // groups), refs_a, True, True)
            return carry
        lax.fori_loop(group * chips // groups, (group + 1) * chips // groups, body, 0)
    store_keys_values(dx_ref, dk_ref, dv_ref, table_ref, pair)

    def part(chip, piece):
        here = pl.ds(aligned(chip * pair, pair), pair)
        return dot_nt(dx_ref[here], wc_ref[pl.ds(aligned(piece * piece_cols, piece_cols), piece_cols)])

    reduce = Reduce(place, part, shard, refs_r)
    outs_u = (gqkv_out, ggate_out, gup_out)
    outs_h = (gout_out, gdown_out)

    def read_dy(piece):
        return gy_ref[lax.rem(piece, 2)]

    def filler(event):
        @pl.when(event < NP)
        def _():
            gy_load(event).wait()
            weight_grads_h(event, ho_ref, read_dy, hs_ref, outs_h, sems_hs, ff)

            @pl.when(event + 2 < NP)
            def _():
                gy_load(event + 2).start()

        @pl.when((event >= NP) & (event < NP + chips))
        def _():
            weight_grads_u(jnp.maximum(event - NP, 0), u_ref, dx_ref, gs_ref, outs_u, sems_gs, head_cols, ff)

    reduce.run(filler)
    for piece in range(NP):
        y_ref[:, piece * piece_cols:(piece + 1) * piece_cols] = reduce.final(piece)
    d_normed = y_ref[...].astype(BF16).astype(F32)
    d_x, gain_part = norm_backward(x_ref[...].astype(F32), gain_ref[1:2], d_normed)
    dx_out[...] = (dy_ref[...].astype(F32) + d_x).astype(BF16)
    gain_out[...] = gain_part
    gu.finish()
    reduce.finish()
    for piece in range(NP):
        for copy in h_copies(piece, hs_ref, outs_h, sems_hs, ff):
            copy.wait()
    weight_grads_u_wait(gs_ref, outs_u, sems_gs, head_cols, ff)


def kernel_first_block(tp_size, x_ref, dy_ref, gain_ref, gain1_ref, u_hbm, q_hbm, k_hbm, v_hbm, o_hbm, ab_hbm, table_hbm,
                       wqkv_hbm, wout_hbm, wgate_hbm, wup_hbm, wdown_hbm,
                       dx_out, gain_out, gqkv_out, gout_out, ggate_out, gup_out, gdown_out, *scratch):
    n_gather = 6
    (u_ref, g_ref, wc_ref, dx_ref, ho_ref, q_ref, k_ref, v_ref, dk_ref, dv_ref, table_ref, y_ref, gs_ref, hs_ref,
     pair_ref, all_ref, local, sems_gs, sems_hs, sem_ps, sem_pr, sem_as, sem_ar) = scratch[:23]
    sems_u = scratch[23:23 + n_gather]
    sems_g = scratch[23 + n_gather:23 + 2 * n_gather]
    refs_r = scratch[23 + 2 * n_gather:]
    place = Place(tp_size)
    shard, width = x_ref.shape
    pair = 2 * shard
    chips = place.ring
    head_cols = wqkv_hbm.shape[2]
    ff = wgate_hbm.shape[2]
    piece_cols = width // NP

    loads = Copies(local)
    gu = Gather(place, u_ref, shard, sems_u)
    gg = Gather(place, g_ref, shard, sems_g)
    load_u = loads.start(u_hbm, u_ref.at[gu.own_rows()])
    load_h = []
    for piece in range(NP):
        cols = slice(piece * piece_cols, (piece + 1) * piece_cols)
        load_h.append(loads.start(wout_hbm.at[0, :, cols], hs_ref.at[piece, 0:HEAD_DIM]))
        load_h.append(loads.start(wdown_hbm.at[0, :, cols], hs_ref.at[piece, HEAD_DIM:HEAD_DIM + ff]))
    load_h.append(loads.start(ab_hbm, dx_ref.at[:, head_cols:head_cols + 2 * ff]))
    load_a = [loads.start(q_hbm, q_ref), loads.start(k_hbm, k_ref), loads.start(v_hbm, v_ref),
              loads.start(o_hbm, ho_ref.at[:, 0:HEAD_DIM]),
              loads.start(table_hbm, table_ref),
              loads.start(wqkv_hbm.at[0], wc_ref.at[:, 0:head_cols]),
              loads.start(wgate_hbm.at[0], wc_ref.at[:, head_cols:head_cols + ff]),
              loads.start(wup_hbm.at[0], wc_ref.at[:, head_cols + ff:head_cols + 2 * ff])]

    g_ref[gg.own_rows()] = dy_ref[...]
    others = [{'tp': place.near(step) * 2 + place.core} for step in range(2, chips - 1)]
    place.barrier(others)
    gg.start()
    dk_ref[...] = jnp.zeros_like(dk_ref)
    dv_ref[...] = jnp.zeros_like(dv_ref)
    load_u.wait()
    for copy in load_h:
        copy.wait()

    def unit(count, chip):
        here = pl.ds(aligned(chip * pair, pair), pair)
        dah = dot_nt(g_ref[here, 0:piece_cols], hs_ref[0])
        for piece in range(1, NP):
            dah = dah + dot_nt(g_ref[here, piece * piece_cols:(piece + 1) * piece_cols], hs_ref[piece])
        dx_ref[here, 0:HEAD_DIM] = dah[:, 0:HEAD_DIM].astype(BF16)
        d_hidden = dah[:, HEAD_DIM:HEAD_DIM + ff].astype(BF16).astype(F32)
        gate = dx_ref[here, head_cols:head_cols + ff].astype(F32)
        up = dx_ref[here, head_cols + ff:head_cols + 2 * ff].astype(F32)
        hidden, d_gate, d_up = gated_pull(gate, up, d_hidden)
        ho_ref[here, HEAD_DIM:HEAD_DIM + ff] = hidden
        dx_ref[here, head_cols:head_cols + ff] = d_gate
        dx_ref[here, head_cols + ff:head_cols + 2 * ff] = d_up

    def start_u(event):
        @pl.when(event == gg.events - NP)
        def _():
            gu.start()
    gather_loop(gg, unit, start_u)
    for copy in load_a:
        copy.wait()

    def read_da(here):
        return dx_ref[here, 0:HEAD_DIM]

    refs_a = (q_ref, k_ref, v_ref, table_ref, read_da, None, dx_ref, dk_ref, dv_ref)
    step_rows = shard

    def loop_u(event, carry):
        gu.event(event, forward=True)

        @pl.when(event < chips)
        def _():
            def body(sub, inner):
                attention_block((event * 2 + sub) * step_rows, step_rows, chips * pair, refs_a, False, True)
                return inner
            lax.fori_loop(0, 2, body, 0)
        return carry
    lax.fori_loop(0, gu.events - NP, loop_u, 0)
    store_keys_values(dx_ref, dk_ref, dv_ref, table_ref, pair)

    def part(chip, piece):
        here = pl.ds(aligned(chip * pair, pair), pair)
        return dot_nt(dx_ref[here], wc_ref[pl.ds(aligned(piece * piece_cols, piece_cols), piece_cols)])

    reduce = Reduce(place, part, shard, refs_r)
    outs_u = (gqkv_out, ggate_out, gup_out)
    outs_h = (gout_out, gdown_out)

    def read_dy(piece):
        return g_ref[:, pl.ds(aligned(piece * piece_cols, piece_cols), piece_cols)]

    def filler(event):
        @pl.when(event < NP)
        def _():
            gu.event(gu.events - NP + event, forward=False)
            weight_grads_h(event, ho_ref, read_dy, hs_ref, outs_h, sems_hs, ff)

        @pl.when(event == NP - 1)
        def _():
            gu.mate_wait_all()

        @pl.when((event >= NP) & (event < NP + chips))
        def _():
            weight_grads_u(jnp.maximum(event - NP, 0), u_ref, dx_ref, gs_ref, outs_u, sems_gs, head_cols, ff)

    reduce.run(filler)
    for piece in range(NP):
        y_ref[:, piece * piece_cols:(piece + 1) * piece_cols] = reduce.final(piece)
    d_normed = y_ref[...].astype(BF16).astype(F32)
    d_x, gain_part = norm_backward(x_ref[...].astype(F32), gain_ref[0:1], d_normed)

    lanes = 128
    tiles = width // lanes
    for tile in range(tiles):
        pair_ref[0, tile:tile + 1] = gain_part[:, tile * lanes:(tile + 1) * lanes]
        pair_ref[0, tiles + tile:tiles + tile + 1] = gain1_ref[:, tile * lanes:(tile + 1) * lanes]
    cross = pltpu.make_async_remote_copy(pair_ref.at[0], pair_ref.at[1], sem_ps, sem_pr, place.mate, MESH)
    cross.start()
    dx_out[...] = (dy_ref[...].astype(F32) + d_x).astype(BF16)
    cross.wait()
    all_ref[place.chip] = pair_ref[0] + pair_ref[1]

    def spread(step):
        return pltpu.make_async_remote_copy(
            all_ref.at[place.chip], all_ref.at[place.chip], sem_as.at[step - 1], sem_ar.at[step - 1],
            {'tp': place.near(step) * 2 + place.core}, MESH)
    for step in range(1, chips):
        spread(step).start()
    gu.finish()
    gg.finish()
    reduce.finish()
    for piece in range(NP):
        for copy in h_copies(piece, hs_ref, outs_h, sems_hs, ff):
            copy.wait()
    weight_grads_u_wait(gs_ref, outs_u, sems_gs, head_cols, ff)
    for step in range(1, chips):
        spread(step).wait()
    total = all_ref[0]
    for chip in range(1, chips):
        total = total + all_ref[chip]
    for tile in range(tiles):
        for layer in range(2):
            gain_out[layer:layer + 1, tile * lanes:(tile + 1) * lanes] = total[layer * tiles + tile:layer * tiles + tile + 1]


def kernel_stack(*refs):
    lasts, firsts, outs, bufs, (sem_in, sem_out) = refs[0:5], refs[5:10], refs[10:15], refs[15:20], refs[20:22]
    reads, writes = [], []
    for layer, sources in ((1, lasts), (0, firsts)):
        for number, source in enumerate(sources):
            slot = len(reads)
            reads.append(pltpu.make_async_copy(source, bufs[number].at[layer], sem_in.at[slot]))
            writes.append(pltpu.make_async_copy(bufs[number].at[layer], outs[number].at[layer], sem_out.at[slot]))
    for read in reads:
        read.start()
    for read, write in zip(reads, writes):
        read.wait()
        write.start()
    for write in writes:
        write.wait()


def solution(mesh):
    tp_size = mesh.shape['tp']
    half = tp_size // 4
    row_spec = P(('dp', 'tp'), None)
    col_spec = P(None, None, 'tp')
    inner_spec = P(None, 'tp', None)

    def device_program(x_loc, dy_loc, norm_gain, w_qkv, w_out, w_gate, w_up, w_down):
        shard, width = x_loc.shape
        seq = shard * tp_size
        pair = 2 * shard
        chips = tp_size // 2
        head_cols = w_qkv.shape[2]
        ff = w_gate.shape[2]
        cols = head_cols + 2 * ff
        piece_cols = width // NP
        vmem, anyspace = pl.BlockSpec(memory_space=pltpu.VMEM), pl.BlockSpec(memory_space=pl.ANY)
        shape = jax.ShapeDtypeStruct
        dma = pltpu.SemaphoreType.DMA

        freqs = np.float32(ROPE_BASE) ** (np.float32(-2.0) * np.arange(HEAD_DIM // 2, dtype=np.float32) / np.float32(HEAD_DIM))
        freqs = jnp.asarray(np.tile(freqs, (8, 2)))

        def params(number):
            return pltpu.CompilerParams(collective_id=number, has_side_effects=True, vmem_limit_bytes=67043328)

        rows_shape = shape((shard, width), BF16)
        head_shape = shape((seq, HEAD_DIM), BF16)
        gathers = Gather.scratch(half)
        reduces = Reduce.scratch(half, shard, piece_cols)
        x1, u1, u0, gy_full, q0, k0, v0, o0, ab0, dah1, table = pl.pallas_call(
            functools.partial(kernel_first, tp_size),
            out_shape=(rows_shape, rows_shape, rows_shape, shape((seq, width), BF16), head_shape, head_shape, head_shape, head_shape,
                       shape((seq, 2 * ff), BF16), shape((seq, HEAD_DIM + ff), BF16), shape((seq, HEAD_DIM), F32)),
            in_specs=[vmem, vmem, vmem] + [anyspace] * 6,
            out_specs=(vmem, vmem, vmem) + (anyspace,) * 8,
            scratch_shapes=[
                pltpu.VMEM((seq, width), BF16), pltpu.VMEM((seq, width), BF16), pltpu.VMEM((width, cols), BF16),
                pltpu.VMEM((NP, HEAD_DIM + ff, piece_cols), BF16), pltpu.VMEM((HEAD_DIM + ff, width), BF16),
                pltpu.VMEM((seq, HEAD_DIM), BF16), pltpu.VMEM((seq, HEAD_DIM), BF16), pltpu.VMEM((seq, HEAD_DIM), BF16),
                pltpu.VMEM((seq, HEAD_DIM + ff), BF16), pltpu.VMEM((2, pair, 2 * ff), BF16), pltpu.VMEM((2, pair, HEAD_DIM + ff), BF16),
                pltpu.VMEM((seq, HEAD_DIM), F32), pltpu.VMEM((shard, width), F32), dma((32,))] + gathers + gathers + reduces,
            compiler_params=params(1), name='first_forward',
        )(x_loc, norm_gain, freqs, dy_loc, w_qkv, w_out, w_gate, w_up, w_down)

        grad_shapes = (rows_shape, shape((1, width), F32), shape((width, head_cols), BF16), shape((HEAD_DIM, width), BF16),
                       shape((width, ff), BF16), shape((width, ff), BF16), shape((ff, width), BF16))
        dx1, gain1, gqkv1, gout1, ggate1, gup1, gdown1 = pl.pallas_call(
            functools.partial(kernel_last_block, tp_size),
            out_shape=grad_shapes,
            in_specs=[vmem, vmem, vmem] + [anyspace] * 7,
            out_specs=(vmem, vmem) + (anyspace,) * 5,
            scratch_shapes=[
                pltpu.VMEM((seq, width), BF16), pltpu.VMEM((width, cols), BF16), pltpu.VMEM((seq, cols), BF16),
                pltpu.VMEM((seq, HEAD_DIM + ff), BF16), pltpu.VMEM((2, seq, piece_cols), BF16),
                pltpu.VMEM((seq, HEAD_DIM), BF16), pltpu.VMEM((seq, HEAD_DIM), BF16), pltpu.VMEM((seq, HEAD_DIM), BF16),
                pltpu.VMEM((seq, HEAD_DIM), F32), pltpu.VMEM((seq, HEAD_DIM), F32), pltpu.VMEM((seq, HEAD_DIM), F32),
                pltpu.VMEM((shard, width), F32), pltpu.VMEM((2, width // chips, cols), BF16),
                pltpu.VMEM((NP, HEAD_DIM + ff, piece_cols), BF16),
                dma((16,)), dma((2, 3)), dma((NP, 2)), dma((2,))] + gathers + reduces,
            compiler_params=params(2), name='last_block',
        )(x1, dy_loc, norm_gain, u1, gy_full, dah1, table, w_qkv, w_gate, w_up)

        grad_shapes = (rows_shape, shape((2, width), F32)) + grad_shapes[2:]
        grad_x, grad_gain, gqkv0, gout0, ggate0, gup0, gdown0 = pl.pallas_call(
            functools.partial(kernel_first_block, tp_size),
            out_shape=grad_shapes,
            in_specs=[vmem] * 4 + [anyspace] * 12,
            out_specs=(vmem, vmem) + (anyspace,) * 5,
            scratch_shapes=[
                pltpu.VMEM((seq, width), BF16), pltpu.VMEM((seq, width), BF16), pltpu.VMEM((width, cols), BF16), pltpu.VMEM((seq, cols), BF16),
                pltpu.VMEM((seq, HEAD_DIM + ff), BF16),
                pltpu.VMEM((seq, HEAD_DIM), BF16), pltpu.VMEM((seq, HEAD_DIM), BF16), pltpu.VMEM((seq, HEAD_DIM), BF16),
                pltpu.VMEM((seq, HEAD_DIM), F32), pltpu.VMEM((seq, HEAD_DIM), F32), pltpu.VMEM((seq, HEAD_DIM), F32),
                pltpu.VMEM((shard, width), F32), pltpu.VMEM((2, width // chips, cols), BF16),
                pltpu.VMEM((NP, HEAD_DIM + ff, piece_cols), BF16),
                pltpu.VMEM((2, 2 * width // 128, 128), F32), pltpu.VMEM((chips, 2 * width // 128, 128), F32),
                dma((32,)), dma((2, 3)), dma((NP, 2)), dma(()), dma(()), dma((chips - 1,)), dma((chips - 1,))] + gathers + gathers + reduces,
            compiler_params=params(3), name='first_block',
        )(x_loc, dx1, norm_gain, gain1, u0, q0, k0, v0, o0, ab0, table, w_qkv, w_out, w_gate, w_up, w_down)

        firsts, lasts = (gqkv0, gout0, ggate0, gup0, gdown0), (gqkv1, gout1, ggate1, gup1, gdown1)
        stacked = pl.pallas_call(
            kernel_stack,
            out_shape=tuple(shape((2,) + first.shape, BF16) for first in firsts),
            in_specs=[anyspace] * 10,
            out_specs=(anyspace,) * 5,
            scratch_shapes=[pltpu.VMEM((2,) + first.shape, BF16) for first in firsts] + [dma((10,)), dma((10,))],
            compiler_params=pltpu.CompilerParams(vmem_limit_bytes=40 * 2 ** 20), name='stack',
        )(*lasts, *firsts)
        return (grad_x, grad_gain) + tuple(stacked)

    return jax.shard_map(device_program, mesh=mesh, in_specs=(row_spec, row_spec, P(None, None), col_spec, inner_spec, col_spec, col_spec, inner_spec), out_specs=(row_spec, P('dp', None), P('dp', None, 'tp'), P('dp', 'tp', None), P('dp', None, 'tp'), P('dp', None, 'tp'), P('dp', 'tp', None)), check_vma=False)
```

```python
import functools

import jax
import jax.numpy as jnp
import numpy as np
from jax import lax
from jax.experimental import pallas as pl
from jax.experimental.pallas import tpu as pltpu
from jax.sharding import PartitionSpec as P

HEAD_DIM = 128
NORM_EPS = 1e-5
ROPE_BASE = 10000.0
MESH = pl.DeviceIdType.MESH
NP = 4
F32 = jnp.float32
BF16 = jnp.bfloat16


def dot_nn(a, b):
    return lax.dot_general(a, b, (((1,), (0,)), ((), ())), preferred_element_type=F32)


def dot_nt(a, b):
    return lax.dot_general(a, b, (((1,), (1,)), ((), ())), preferred_element_type=F32)


def dot_tn(a, b):
    return lax.dot_general(a, b, (((0,), (0,)), ((), ())), preferred_element_type=F32)


def aligned(index, size):
    return pl.multiple_of(index, size)


class Place:
    def __init__(self, tp_size):
        index = lax.axis_index('tp')
        self.ring = tp_size // 2
        self.half = self.ring // 2
        self.core = lax.rem(index, 2)
        self.chip = lax.div(index, 2)
        self.right = {'tp': self.near(1) * 2 + self.core}
        self.left = {'tp': self.near(-1) * 2 + self.core}
        self.mate = {'tp': self.chip * 2 + 1 - self.core}

    def near(self, step):
        return lax.rem(self.chip + step + self.ring, self.ring)

    def barrier(self, others=()):
        sem = pltpu.get_barrier_semaphore()
        peers = [self.right, self.left, self.mate] + list(others)
        for peer in peers:
            pl.semaphore_signal(sem, inc=1, device_id=peer, device_id_type=MESH)
        pl.semaphore_wait(sem, len(peers))


class Gather:
    def __init__(self, place, buf, shard_rows, sems):
        self.place, self.buf, self.shard = place, buf, shard_rows
        self.rows = shard_rows // NP
        self.events = (place.half - 1) * NP + NP // 2
        self.send_r, self.recv_r, self.send_l, self.recv_l, self.send_m, self.recv_m = sems

    @staticmethod
    def scratch(half):
        events = (half - 1) * NP + NP // 2
        return [pltpu.SemaphoreType.DMA((n,)) for n in (events, events, events, events, 2 * events + NP, 2 * events + NP)]

    def view(self, chip, core, piece):
        start = (chip * 2 + core) * self.shard + piece * self.rows
        return self.buf.at[pl.ds(aligned(start, self.rows), self.rows)]

    def own_rows(self):
        start = (self.place.chip * 2 + self.place.core) * self.shard
        return pl.ds(aligned(start, self.shard), self.shard)

    def to_right(self, event, view):
        return pltpu.make_async_remote_copy(view, view, self.send_r.at[event], self.recv_r.at[event], self.place.right, MESH)

    def to_left(self, event, view):
        return pltpu.make_async_remote_copy(view, view, self.send_l.at[event], self.recv_l.at[event], self.place.left, MESH)

    def to_mate(self, slot, view):
        return pltpu.make_async_remote_copy(view, view, self.send_m.at[slot], self.recv_m.at[slot], self.place.mate, MESH)

    def start(self):
        place = self.place
        for piece in range(NP):
            self.to_right(piece, self.view(place.chip, place.core, piece)).start()
            self.to_left(piece, self.view(place.chip, place.core, NP - 1 - piece)).start()
        for piece in range(NP):
            self.to_mate(2 * self.events + piece, self.view(place.chip, place.core, piece)).start()

    def views(self, event):
        step = lax.div(event, NP) + 1
        piece = lax.rem(event, NP)
        from_left = self.view(self.place.near(-step), self.place.core, piece)
        from_right = self.view(self.place.near(step), self.place.core, NP - 1 - piece)
        return from_left, from_right

    def event(self, event, forward=None):
        from_left, from_right = self.views(event)
        self.to_right(event, from_left).wait_recv()
        self.pass_on(event, forward, lambda: self.to_right(event + NP, from_left).start())
        self.to_mate(event, from_left).start()
        self.to_left(event, from_right).wait_recv()
        self.pass_on(event, forward, lambda: self.to_left(event + NP, from_right).start())
        self.to_mate(self.events + event, from_right).start()

    def pass_on(self, event, forward, send):
        if forward is None:
            pl.when(event + NP < self.events)(send)
        elif forward:
            send()

    def mate_wait(self, first, count):
        for offset in range(count):
            self.to_mate(first + offset, self.view(self.place.chip, 1 - self.place.core, 0)).wait_recv()

    def mate_wait_all(self):
        def body(slot, carry):
            self.mate_wait(slot, 1)
            return carry
        lax.fori_loop(0, 2 * self.events + NP, body, 0)

    def mate_wait_last(self):
        first = (self.place.half - 1) * NP
        self.mate_wait(first, NP // 2)
        self.mate_wait(self.events + first, NP // 2)

    def mate_wait_chip(self, distance, rightward):
        ring_first = lax.select(rightward, self.events, 0) + jnp.maximum(distance - 1, 0) * NP
        self.mate_wait(lax.select(distance == 0, 2 * self.events, ring_first), NP)

    def finish(self):
        view = self.view(self.place.chip, self.place.core, 0)

        def ring(event, carry):
            self.to_right(event, view).wait_send()
            self.to_left(event, view).wait_send()
            return carry
        lax.fori_loop(0, self.events, ring, 0)

        def across(slot, carry):
            self.to_mate(slot, view).wait_send()
            return carry
        lax.fori_loop(0, 2 * self.events + NP, across, 0)


class Reduce:
    SLOTS = 6
    DEPTH = 8

    def __init__(self, place, part, shard_rows, refs):
        self.place, self.part, self.shard = place, part, shard_rows
        self.events = (place.half - 1) * NP + NP // 2
        self.ring, self.acc, self.stage, self.send_n, self.recv_n, self.send_m, self.recv_m = refs

    @staticmethod
    def scratch(half, shard_rows, width):
        events = (half - 1) * NP + NP // 2
        shapes = [(2, events), (2 * Reduce.DEPTH + NP,), (Reduce.SLOTS, 2)]
        sems = [(2, events), (2, events), (2 * events + NP,), (2 * events + NP,)]
        return [pltpu.VMEM(s + (shard_rows, width), F32) for s in shapes] + [pltpu.SemaphoreType.DMA(s) for s in sems]

    def acc_slot(self, term):
        own = 2 * self.DEPTH + jnp.maximum(term - 2 * self.events, 0)
        return lax.select(term < 2 * self.events, lax.rem(term, 2 * self.DEPTH), own)

    def mate_copy(self, term):
        return pltpu.make_async_remote_copy(
            self.stage.at[lax.rem(term, self.SLOTS), 1 - self.place.core], self.acc.at[self.acc_slot(term)], self.send_m.at[term], self.recv_m.at[term],
            self.place.mate, MESH)

    def ring_copy(self, event, way):
        to = {'tp': self.place.near(1 - 2 * way) * 2 + self.place.core}
        return pltpu.make_async_remote_copy(
            self.acc.at[self.acc_slot(2 * event + way)], self.ring.at[way, event], self.send_n.at[way, event], self.recv_n.at[way, event], to, MESH)

    def fill(self, term):
        @pl.when(term >= self.SLOTS)
        def _():
            self.mate_copy(jnp.maximum(term - self.SLOTS, 0)).wait_send()
        slot = lax.rem(term, self.SLOTS)
        way = lax.rem(term, 2)

        @pl.when(term >= 2 * (self.DEPTH - 1))
        def _():
            self.ring_copy(jnp.maximum(lax.div(term, 2) - (self.DEPTH - 1), 0), way).wait_send()
        shifted = lax.div(term, 2) + NP // 2
        travels = term < 2 * self.events
        distance = jnp.maximum(self.place.half - lax.div(shifted, NP), 0)
        turn = lax.rem(shifted, NP)
        piece = lax.select(travels, lax.select(way == 0, turn, NP - 1 - turn), lax.rem(jnp.maximum(term - 2 * self.events, 0), NP))
        value = self.part(self.place.near((1 - 2 * way) * distance), piece)
        self.stage[slot, 0] = value[:self.shard]
        self.stage[slot, 1] = value[self.shard:]
        self.mate_copy(term).start()

    def event(self, event):
        def add(way, carry):
            term = 2 * event + way
            self.mate_copy(term).wait_recv()
            slot = self.acc_slot(term)
            self.acc[slot] += self.stage[lax.rem(term, self.SLOTS), self.place.core]

            @pl.when(event >= NP)
            def _():
                before = jnp.maximum(event - NP, 0)
                self.ring_copy(before, way).wait_recv()
                self.acc[slot] += self.ring[way, before]
            self.ring_copy(event, way).start()
            return carry
        lax.fori_loop(0, 2, add, 0)

    def final(self, piece):
        last = self.events - NP
        term = 2 * self.events + piece
        self.mate_copy(term).wait_recv()
        self.ring_copy(last + piece, 0).wait_recv()
        self.ring_copy(last + NP - 1 - piece, 1).wait_recv()
        return ((self.stage[term % self.SLOTS, self.place.core] + self.acc[2 * self.DEPTH + piece])
                + (self.ring[0, last + piece] + self.ring[1, last + NP - 1 - piece]))

    def finish(self):
        def across(term, carry):
            self.mate_copy(term).wait_send()
            return carry
        terms = 2 * self.events + NP
        lax.fori_loop(terms - self.SLOTS, terms, across, 0)

        def ring(event, carry):
            self.ring_copy(event, 0).wait_send()
            self.ring_copy(event, 1).wait_send()
            return carry
        lax.fori_loop(self.events + 2 - (self.DEPTH - 1), self.events, ring, 0)

    def run(self, filler):
        def body(turn, carry):
            event = jnp.maximum(turn - 1, 0)
            travels = (turn >= 1) & (turn <= self.events)

            @pl.when(travels)
            def _():
                self.event(event)

            def ahead(way, inner):
                self.fill(2 * turn + way)
                return inner
            lax.fori_loop(0, 2, ahead, 0)

            @pl.when(travels)
            def _():
                filler(event)
            return carry
        lax.fori_loop(0, self.events + 2, body, 0)


def rope_pair(table):
    lanes = lax.broadcasted_iota(jnp.int32, table.shape, 1)
    swapped = pltpu.roll(table, HEAD_DIM // 2, 1)
    low = lanes < HEAD_DIM // 2
    return jnp.where(low, table, swapped), jnp.where(low, -swapped, table)


def fill_table(freqs, table_ref):
    rows = 64
    blocks = table_ref.shape[0] // rows

    def cos_sin(count, scale):
        steps = lax.broadcasted_iota(jnp.int32, (count, HEAD_DIM), 0) * scale
        angles = steps.astype(F32) * freqs
        return jnp.cos(angles), jnp.sin(angles)
    cos_low, sin_low = cos_sin(rows, 1)
    cos_high, sin_high = cos_sin(max(blocks, 8), rows)
    low = lax.broadcasted_iota(jnp.int32, (1, HEAD_DIM), 1) < HEAD_DIM // 2
    first = jnp.where(low, cos_high, sin_high)
    second = jnp.where(low, -sin_high, cos_high)
    for block in range(blocks):
        table_ref[block * rows:(block + 1) * rows] = first[block:block + 1] * cos_low + second[block:block + 1] * sin_low


def rope(values, table, inverse=False):
    cos2, sin2 = rope_pair(table)
    turned = pltpu.roll(values, HEAD_DIM // 2, 1)
    if inverse:
        return values * cos2 - turned * sin2
    return values * cos2 + turned * sin2


def norm_forward(x_f32, gain_row):
    inv = lax.rsqrt(jnp.mean(x_f32 * x_f32, axis=-1, keepdims=True) + NORM_EPS)
    return (x_f32 * inv * gain_row).astype(BF16)


def norm_backward(x_f32, gain_row, d_normed):
    inv = lax.rsqrt(jnp.mean(x_f32 * x_f32, axis=-1, keepdims=True) + NORM_EPS)
    unit = x_f32 * inv
    d_unit = d_normed * gain_row
    d_x = inv * (d_unit - unit * jnp.mean(d_unit * unit, axis=-1, keepdims=True))
    return d_x, jnp.sum(d_normed * unit, axis=0, keepdims=True)


def attention_block(row0, rows, keys, refs, forward, backward):
    q_ref, k_ref, v_ref, table_ref, read_da, write_o, dx_ref, dk_ref, dv_ref = refs
    here = pl.ds(aligned(row0, rows), rows)
    scale = HEAD_DIM ** -0.5
    query = q_ref[here]
    scores = dot_nt(query, k_ref[0:keys]) * scale
    row_id = row0 + lax.broadcasted_iota(jnp.int32, scores.shape, 0)
    col_id = lax.broadcasted_iota(jnp.int32, scores.shape, 1)
    scores = jnp.where(row_id >= col_id, scores, -1e30)
    expd = jnp.exp(scores - jnp.max(scores, axis=-1, keepdims=True))
    prob = expd * (1.0 / jnp.sum(expd, axis=-1, keepdims=True))
    prob_b = prob.astype(BF16)
    d_attn = read_da(here) if backward else None
    if forward:
        write_o(here, dot_nn(prob_b, v_ref[0:keys]).astype(BF16))
    if backward:
        dv_ref[0:keys] += dot_tn(prob_b, d_attn)
        d_prob = dot_nt(d_attn, v_ref[0:keys]).astype(BF16).astype(F32)
        row_dot = jnp.sum(prob * d_prob, axis=-1, keepdims=True)
        d_scores = (prob * (d_prob - row_dot) * scale).astype(BF16)
        d_query = dot_nn(d_scores, k_ref[0:keys]).astype(BF16).astype(F32)
        dx_ref[here, 0:HEAD_DIM] = rope(d_query, table_ref[here], inverse=True).astype(BF16)
        dk_ref[0:keys] += dot_tn(d_scores, query)


def store_keys_values(dx_ref, dk_ref, dv_ref, table_ref, rows):
    def body(block, carry):
        here = pl.ds(aligned(block * rows, rows), rows)
        d_key = dk_ref[here].astype(BF16).astype(F32)
        dx_ref[here, HEAD_DIM:2 * HEAD_DIM] = rope(d_key, table_ref[here], inverse=True).astype(BF16)
        dx_ref[here, 2 * HEAD_DIM:3 * HEAD_DIM] = dv_ref[here].astype(BF16)
        return carry
    lax.fori_loop(0, dx_ref.shape[0] // rows, body, 0)


def gated_pull(gate, up, d_hidden):
    sig = jax.nn.sigmoid(gate)
    silu = gate * sig
    d_silu = d_hidden * up
    return (silu * up).astype(BF16), (d_silu * sig + d_silu * silu * (1.0 - sig)).astype(BF16), (d_hidden * silu).astype(BF16)


class Copies:
    def __init__(self, sems):
        self.sems, self.used = sems, 0

    def start(self, src, dst):
        copy = pltpu.make_async_copy(src, dst, self.sems.at[self.used])
        self.used += 1
        copy.start()
        return copy


def gather_loop(gather, unit, then=None):
    chips = gather.place.ring

    def body(event, carry):
        @pl.when(event < gather.events)
        def _():
            gather.event(event)
            if then is not None:
                then(event)
        step = lax.div(event, NP) + 1
        opposite = event == gather.events
        final = event == gather.events - 1
        own = event == 1
        near = (event >= NP) & (event < gather.events) & (lax.rem(event, 2) == 0)

        @pl.when(opposite)
        def _():
            gather.mate_wait_last()

        @pl.when(own | near | final)
        def _():
            gather.mate_wait_chip(step - 1, final | (lax.rem(event, NP) != 0))

        @pl.when(own | near | final | opposite)
        def _():
            distance = lax.select(opposite, gather.place.half, step - 1)
            rightward = final | (lax.rem(event, NP) != 0)
            count = lax.select(own, 0, lax.select(opposite, chips - 1, lax.select(final, chips - 2, jnp.maximum(lax.div(event, 2) - 1, 0))))
            unit(count, gather.place.near(lax.select(rightward, distance, -distance)))
        return carry
    lax.fori_loop(0, gather.events + 1, body, 0)


def weight_grads_u(block, u_ref, dx_ref, stage_ref, outs, sems, head_cols, ff):
    rows = stage_ref.shape[1]
    slot = lax.rem(block, 2)
    here = pl.ds(aligned(block * rows, rows), rows)

    def copies():
        bounds = (0, head_cols, head_cols + ff, head_cols + 2 * ff)
        return [pltpu.make_async_copy(stage_ref.at[slot, :, bounds[i]:bounds[i + 1]], outs[i].at[here], sems.at[slot, i]) for i in range(3)]

    @pl.when(block >= 2)
    def _():
        for copy in copies():
            copy.wait()
    stage_ref[slot] = dot_tn(u_ref[:, here], dx_ref[...]).astype(BF16)
    for copy in copies():
        copy.start()


def weight_grads_u_wait(stage_ref, outs, sems, head_cols, ff):
    rows = stage_ref.shape[1]
    bounds = (0, head_cols, head_cols + ff, head_cols + 2 * ff)
    for slot in range(2):
        for i in range(3):
            pltpu.make_async_copy(stage_ref.at[slot, :, bounds[i]:bounds[i + 1]], outs[i].at[pl.ds(0, rows)], sems.at[slot, i]).wait()


def weight_grads_h(piece, ho_ref, read_dy, stage_ref, outs, sems, ff):
    cols = stage_ref.shape[2]
    stage_ref[piece] = dot_tn(ho_ref[...], read_dy(piece)).astype(BF16)
    for copy in h_copies(piece, stage_ref, outs, sems, ff):
        copy.start()


def h_copies(piece, stage_ref, outs, sems, ff):
    cols = stage_ref.shape[2]
    there = pl.ds(aligned(piece * cols, cols), cols)
    return [pltpu.make_async_copy(stage_ref.at[piece, 0:HEAD_DIM], outs[0].at[:, there], sems.at[piece, 0]),
            pltpu.make_async_copy(stage_ref.at[piece, HEAD_DIM:HEAD_DIM + ff], outs[1].at[:, there], sems.at[piece, 1])]


def kernel_main(tp_size, x_ref, gain_ref, freq_ref, gy_hbm, wqkv_hbm, wout_hbm, wgate_hbm, wup_hbm, wdown_hbm,
                dx_out, gain_out, *refs):
    firsts, lasts = refs[0:5], refs[5:10]
    u0_hbm, q_hbm, k_hbm, v_hbm, o_hbm, ab_hbm = refs[10:16]
    (u_ref, g_ref, wc_ref, wo_ref, q_ref, k_ref, v_ref, ho_ref, dx_ref, dk_ref, dv_ref, table_ref, x1_ref, gs_ref,
     pair_ref, all_ref, local, sems_gs, sems_hs, sem_ps, sem_pr, sem_as, sem_ar, free_sem) = refs[16:40]
    sems_u, sems_g, refs_r = refs[40:46], refs[46:52], refs[52:]
    place = Place(tp_size)
    shard, width = x_ref.shape
    pair = 2 * shard
    chips = place.ring
    head_cols = wqkv_hbm.shape[2]
    ff = wgate_hbm.shape[2]
    piece_cols = width // NP
    gate_cols = slice(head_cols, head_cols + ff)
    up_cols = slice(head_cols + ff, head_cols + 2 * ff)
    hidden_cols = slice(HEAD_DIM, HEAD_DIM + ff)
    loads = Copies(local)
    gu = Gather(place, u_ref, shard, sems_u)
    gg = Gather(place, g_ref, shard, sems_g)

    def wait_all(copies):
        for copy in copies:
            copy.wait()

    def load_wc(layer):
        return [loads.start(wqkv_hbm.at[layer], wc_ref.at[:, 0:head_cols]),
                loads.start(wgate_hbm.at[layer], wc_ref.at[:, gate_cols]),
                loads.start(wup_hbm.at[layer], wc_ref.at[:, up_cols])]

    def load_wo(layer):
        copies = []
        for piece in range(NP):
            cols = slice(piece * piece_cols, (piece + 1) * piece_cols)
            copies.append(loads.start(wout_hbm.at[layer, :, cols], wo_ref.at[piece, 0:HEAD_DIM]))
            copies.append(loads.start(wdown_hbm.at[layer, :, cols], wo_ref.at[piece, hidden_cols]))
        return copies

    def rows_of(chip):
        return pl.ds(aligned(chip * pair, pair), pair)

    def write_o(here, value):
        ho_ref[here, 0:HEAD_DIM] = value

    def read_da(here):
        return dx_ref[here, 0:HEAD_DIM]

    def heads(here, rows_u):
        qkv = dot_nn(rows_u, wc_ref[:, 0:head_cols]).astype(BF16)
        table = table_ref[here]
        q_ref[here] = rope(qkv[:, 0:HEAD_DIM].astype(F32), table).astype(BF16)
        k_ref[here] = rope(qkv[:, HEAD_DIM:2 * HEAD_DIM].astype(F32), table).astype(BF16)
        v_ref[here] = qkv[:, 2 * HEAD_DIM:3 * HEAD_DIM]

    def forward_unit(count, chip, with_hidden):
        here = rows_of(chip)
        rows_u = u_ref[here]
        heads(here, rows_u)
        gate = dot_nn(rows_u, wc_ref[:, gate_cols]).astype(BF16)
        up = dot_nn(rows_u, wc_ref[:, up_cols]).astype(BF16)
        dx_ref[here, gate_cols] = gate
        dx_ref[here, up_cols] = up
        if with_hidden:
            gate_f, up_f = gate.astype(F32), up.astype(F32)
            ho_ref[here, hidden_cols] = (gate_f * jax.nn.sigmoid(gate_f) * up_f).astype(BF16)

    def backward_unit(count, chip):
        here = rows_of(chip)
        dah = dot_nt(g_ref[here, 0:piece_cols], wo_ref[0])
        for piece in range(1, NP):
            dah = dah + dot_nt(g_ref[here, piece * piece_cols:(piece + 1) * piece_cols], wo_ref[piece])
        dx_ref[here, 0:HEAD_DIM] = dah[:, 0:HEAD_DIM].astype(BF16)
        d_hidden = dah[:, hidden_cols].astype(BF16).astype(F32)
        hidden, d_gate, d_up = gated_pull(dx_ref[here, gate_cols].astype(F32), dx_ref[here, up_cols].astype(F32), d_hidden)
        ho_ref[here, hidden_cols] = hidden
        dx_ref[here, gate_cols] = d_gate
        dx_ref[here, up_cols] = d_up

    def part_forward(chip, piece):
        return dot_nn(ho_ref[rows_of(chip)], wo_ref[piece])

    def part_backward(chip, piece):
        return dot_nt(dx_ref[rows_of(chip)], wc_ref[pl.ds(aligned(piece * piece_cols, piece_cols), piece_cols)])

    def read_dy(piece):
        return g_ref[:, pl.ds(aligned(piece * piece_cols, piece_cols), piece_cols)]

    def finals(reduce):
        return jnp.concatenate([reduce.final(piece) for piece in range(NP)], axis=1)

    def grads_filler(event, outs):
        outs_u, outs_h = (outs[0], outs[2], outs[3]), (outs[1], outs[4])

        @pl.when(event < NP)
        def _():
            weight_grads_h(event, ho_ref, read_dy, wo_ref, outs_h, sems_hs, ff)

        @pl.when((event >= NP) & (event < NP + chips))
        def _():
            weight_grads_u(jnp.maximum(event - NP, 0), u_ref, dx_ref, gs_ref, outs_u, sems_gs, head_cols, ff)

    def grads_wait(outs):
        outs_u, outs_h = (outs[0], outs[2], outs[3]), (outs[1], outs[4])
        for piece in range(NP):
            wait_all(h_copies(piece, wo_ref, outs_h, sems_hs, ff))
        weight_grads_u_wait(gs_ref, outs_u, sems_gs, head_cols, ff)

    def keep_gain(layer, row):
        lanes = all_ref.shape[2]
        tiles = width // lanes
        for tile in range(tiles):
            pair_ref[0, layer * tiles + tile:layer * tiles + tile + 1] = row[:, tile * lanes:(tile + 1) * lanes]

    load_g = loads.start(gy_hbm, g_ref.at[gg.own_rows()])
    load_w = load_wc(0)
    load_o = load_wo(0)
    u_ref[gu.own_rows()] = norm_forward(x_ref[...].astype(F32), gain_ref[0:1])
    place.barrier([{'tp': place.near(step) * 2 + place.core} for step in range(2, chips - 1)])
    gu.start()
    saves = [loads.start(u_ref.at[gu.own_rows()], u0_hbm)]
    fill_table(freq_ref[0:1], table_ref)
    load_g.wait()
    wait_all(load_w)

    def start_gy(event):
        @pl.when(event == gu.events - NP)
        def _():
            gg.start()
    gather_loop(gu, lambda count, chip: forward_unit(count, chip, True), start_gy)

    load_w = load_wc(1)
    saves += [loads.start(q_ref, q_hbm), loads.start(k_ref, k_hbm), loads.start(v_ref, v_hbm),
              loads.start(dx_ref.at[:, head_cols:head_cols + 2 * ff], ab_hbm)]

    def attend_first(block, carry):
        attention_block(block * pair, pair, chips * pair, (q_ref, k_ref, v_ref, table_ref, None, write_o, None, None, None), True, False)
        return carry
    lax.fori_loop(0, chips, attend_first, 0)
    saves += [loads.start(ho_ref.at[:, 0:HEAD_DIM], o_hbm)]
    wait_all(load_o)
    gu.finish()
    reduce = Reduce(place, part_forward, shard, refs_r)
    reduce.run(lambda event: None)
    load_o = load_wo(1)
    gg.event(jnp.int32(0), forward=True)
    gg.event(jnp.int32(1), forward=True)
    x_next = (x_ref[...].astype(F32) + finals(reduce)).astype(BF16)
    x1_ref[...] = x_next
    saves[0].wait()
    u_ref[gu.own_rows()] = norm_forward(x_next.astype(F32), gain_ref[1:2])

    reduce.finish()
    gu.start()
    wait_all(saves[1:])
    wait_all(load_w)
    wait_all(load_o)
    dk_ref[...] = jnp.zeros_like(dk_ref)
    dv_ref[...] = jnp.zeros_like(dv_ref)
    early = 2

    def more_gy(event):
        @pl.when(event >= gu.events - NP)
        def _():
            gg.event(jnp.maximum(event - (gu.events - NP), 0) + early, forward=True)
    gather_loop(gu, lambda count, chip: forward_unit(count, chip, False), more_gy)

    groups = 4

    def attend_last(turn, carry):
        held = early + NP
        distance = lax.div(turn + 1, 2)
        rightward = (turn > 0) & (lax.rem(turn, 2) == 0)
        opposite = turn == chips - 1
        needed = lax.select(turn == 0, held, lax.select(opposite, gg.events, distance * NP))
        begin = lax.select(turn == 0, held, jnp.minimum(jnp.maximum(held + turn - 1, lax.select(turn >= chips - 2, gg.events - NP // 2, 0)), gg.events))
        end = jnp.maximum(jnp.minimum(held + turn, gg.events), needed)
        end = lax.select(turn == chips - 2, jnp.maximum(end, gg.events - 1), end)
        begin = lax.select(turn == chips - 1, gg.events - 1, begin)

        def take(event, inner):
            gg.event(event)
            return inner
        lax.fori_loop(begin, end, take, 0)

        @pl.when(opposite)
        def _():
            gg.mate_wait_last()

        @pl.when(jnp.logical_not(opposite))
        def _():
            gg.mate_wait_chip(distance, rightward)
        chip = place.near(lax.select(rightward, distance, -distance))
        backward_unit(turn, chip)
        for group in range(groups):
            @pl.when(lax.div(chip, chips // groups) == group)
            def _(group=group):
                attention_block(chip * pair, pair, (group + 1) * (chips * pair // groups),
                                (q_ref, k_ref, v_ref, table_ref, read_da, write_o, dx_ref, dk_ref, dv_ref), True, True)
        return carry
    lax.fori_loop(0, chips, attend_last, 0)
    store_keys_values(dx_ref, dk_ref, dv_ref, table_ref, pair)
    gu.finish()
    gg.finish()
    loads_a = [loads.start(q_hbm, q_ref), loads.start(k_hbm, k_ref), loads.start(v_hbm, v_ref)]
    n_late = loads.used
    loads.used += 2

    def late_loads():
        return [pltpu.make_async_copy(u0_hbm, u_ref.at[gu.own_rows()], local.at[n_late]),
                pltpu.make_async_copy(o_hbm, ho_ref.at[:, 0:HEAD_DIM], local.at[n_late + 1])]
    near = (place.left, place.right, place.mate)
    reduce = Reduce(place, part_backward, shard, refs_r)

    def filler_last(event):
        grads_filler(event, lasts)

        @pl.when(event == NP + chips)
        def _():
            for copy in late_loads():
                copy.start()
            for peer in near:
                pl.semaphore_signal(free_sem, inc=1, device_id=peer, device_id_type=MESH)
    reduce.run(filler_last)
    pl.semaphore_wait(free_sem, len(near))
    wait_all(late_loads())
    gu.start()
    d_x, gain_row = norm_backward(x1_ref[...].astype(F32), gain_ref[1:2], finals(reduce).astype(BF16).astype(F32))
    g_ref[gg.own_rows()] = (g_ref[gg.own_rows()].astype(F32) + d_x).astype(BF16)
    keep_gain(1, gain_row)

    reduce.finish()
    gg.start()
    grads_wait(lasts)
    load_o = load_wo(0) + [loads.start(ab_hbm, dx_ref.at[:, head_cols:head_cols + 2 * ff])]
    load_w = load_wc(0)
    dk_ref[...] = jnp.zeros_like(dk_ref)
    dv_ref[...] = jnp.zeros_like(dv_ref)
    wait_all(load_o)

    def more_u(event):
        @pl.when(event >= gg.events - NP)
        def _():
            gu.event(jnp.maximum(event - (gg.events - NP), 0), forward=True)
    gather_loop(gg, backward_unit, more_u)
    wait_all(loads_a)

    def attend_back(block, carry):
        @pl.when(block < gu.events - 2 * NP)
        def _():
            gu.event(block + NP, forward=True)

        def body(sub, inner):
            attention_block((block * 2 + sub) * shard, shard, chips * pair,
                            (q_ref, k_ref, v_ref, table_ref, read_da, None, dx_ref, dk_ref, dv_ref), False, True)
            return inner
        lax.fori_loop(0, 2, body, 0)
        return carry
    lax.fori_loop(0, chips, attend_back, 0)
    store_keys_values(dx_ref, dk_ref, dv_ref, table_ref, pair)
    wait_all(load_w)
    reduce = Reduce(place, part_backward, shard, refs_r)

    def filler_first(event):
        @pl.when(event < NP)
        def _():
            gu.event(gu.events - NP + event, forward=False)

        @pl.when(event == NP - 1)
        def _():
            gu.mate_wait_all()
        grads_filler(event, firsts)
    reduce.run(filler_first)
    d_x, gain_row = norm_backward(x_ref[...].astype(F32), gain_ref[0:1], finals(reduce).astype(BF16).astype(F32))
    keep_gain(0, gain_row)

    cross = pltpu.make_async_remote_copy(pair_ref.at[0], pair_ref.at[1], sem_ps, sem_pr, place.mate, MESH)
    cross.start()
    dx_out[...] = (g_ref[gg.own_rows()].astype(F32) + d_x).astype(BF16)
    cross.wait()
    all_ref[place.chip] = pair_ref[0] + pair_ref[1]

    def spread(step):
        return pltpu.make_async_remote_copy(
            all_ref.at[place.chip], all_ref.at[place.chip], sem_as.at[step - 1], sem_ar.at[step - 1],
            {'tp': place.near(step) * 2 + place.core}, MESH)
    for step in range(1, chips):
        spread(step).start()
    gu.finish()
    gg.finish()
    reduce.finish()
    grads_wait(firsts)
    for step in range(1, chips):
        spread(step).wait()
    total = all_ref[0]
    for chip in range(1, chips):
        total = total + all_ref[chip]
    lanes = total.shape[1]
    tiles = width // lanes
    for tile in range(tiles):
        for layer in range(2):
            gain_out[layer:layer + 1, tile * lanes:(tile + 1) * lanes] = total[layer * tiles + tile:layer * tiles + tile + 1]


def kernel_stack(*refs):
    lasts, firsts, rest, outs, out_rest = refs[0:5], refs[5:10], refs[10:12], refs[12:17], refs[17:19]
    bufs, buf_rest, (sem_in, sem_out) = refs[19:24], refs[24:26], refs[26:28]
    steps = [(source, bufs[number].at[layer], outs[number].at[layer])
             for layer, sources in ((1, lasts), (0, firsts)) for number, source in enumerate(sources)]
    steps += list(zip(rest, buf_rest, out_rest))
    reads = [pltpu.make_async_copy(source, buf, sem_in.at[slot]) for slot, (source, buf, out) in enumerate(steps)]
    writes = [pltpu.make_async_copy(buf, out, sem_out.at[slot]) for slot, (source, buf, out) in enumerate(steps)]
    for read in reads:
        read.start()
    for read, write in zip(reads, writes):
        read.wait()
        write.start()
    for write in writes:
        write.wait()


def solution(mesh):
    tp_size = mesh.shape['tp']
    half = tp_size // 4
    row_spec = P(('dp', 'tp'), None)
    col_spec = P(None, None, 'tp')
    inner_spec = P(None, 'tp', None)

    def device_program(x_loc, dy_loc, norm_gain, w_qkv, w_out, w_gate, w_up, w_down):
        shard, width = x_loc.shape
        seq = shard * tp_size
        pair = 2 * shard
        chips = tp_size // 2
        head_cols = w_qkv.shape[2]
        ff = w_gate.shape[2]
        cols = head_cols + 2 * ff
        piece_cols = width // NP
        vmem, anyspace = pl.BlockSpec(memory_space=pltpu.VMEM), pl.BlockSpec(memory_space=pl.ANY)
        shape = jax.ShapeDtypeStruct
        dma = pltpu.SemaphoreType.DMA

        freqs = np.float32(ROPE_BASE) ** (np.float32(-2.0) * np.arange(HEAD_DIM // 2, dtype=np.float32) / np.float32(HEAD_DIM))
        freqs = jnp.asarray(np.tile(freqs, (8, 2)))

        rows_shape = shape((shard, width), BF16)
        gain_shape = shape((2, width), F32)
        head_shape = shape((seq, HEAD_DIM), BF16)
        grads = (shape((width, head_cols), BF16), shape((HEAD_DIM, width), BF16), shape((width, ff), BF16),
                 shape((width, ff), BF16), shape((ff, width), BF16))
        whole_vmem = 67043328
        results = pl.pallas_call(
            functools.partial(kernel_main, tp_size),
            out_shape=(rows_shape, gain_shape) + grads + grads + (rows_shape,) + (head_shape,) * 4 + (shape((seq, 2 * ff), BF16),),
            in_specs=[vmem] * 3 + [anyspace] * 6,
            out_specs=(vmem, vmem) + (anyspace,) * 16,
            scratch_shapes=[
                pltpu.VMEM((seq, width), BF16), pltpu.VMEM((seq, width), BF16), pltpu.VMEM((width, cols), BF16),
                pltpu.VMEM((NP, HEAD_DIM + ff, piece_cols), BF16),
                pltpu.VMEM((seq, HEAD_DIM), BF16), pltpu.VMEM((seq, HEAD_DIM), BF16), pltpu.VMEM((seq, HEAD_DIM), BF16),
                pltpu.VMEM((seq, HEAD_DIM + ff), BF16), pltpu.VMEM((seq, cols), BF16),
                pltpu.VMEM((seq, HEAD_DIM), F32), pltpu.VMEM((seq, HEAD_DIM), F32), pltpu.VMEM((seq, HEAD_DIM), F32),
                pltpu.VMEM((shard, width), BF16), pltpu.VMEM((2, width // chips, cols), BF16),
                pltpu.VMEM((2, 2 * width // 128, 128), F32), pltpu.VMEM((chips, 2 * width // 128, 128), F32),
                dma((64,)), dma((2, 3)), dma((NP, 2)), dma(()), dma(()), dma((chips - 1,)), dma((chips - 1,)),
                pltpu.SemaphoreType.REGULAR] + Gather.scratch(half) + Gather.scratch(half) + Reduce.scratch(half, shard, piece_cols),
            compiler_params=pltpu.CompilerParams(collective_id=1, has_side_effects=True, vmem_limit_bytes=whole_vmem), name='blocks',
        )(x_loc, norm_gain, freqs, dy_loc, w_qkv, w_out, w_gate, w_up, w_down)

        stacked = pl.pallas_call(
            kernel_stack,
            out_shape=tuple(shape((2,) + grad.shape, BF16) for grad in grads) + (rows_shape, gain_shape),
            in_specs=[anyspace] * 12,
            out_specs=(anyspace,) * 7,
            scratch_shapes=[pltpu.VMEM((2,) + grad.shape, BF16) for grad in grads]
            + [pltpu.VMEM(rows_shape.shape, BF16), pltpu.VMEM(gain_shape.shape, F32), dma((12,)), dma((12,))],
            compiler_params=pltpu.CompilerParams(vmem_limit_bytes=whole_vmem), name='stack',
        )(*results[7:12], *results[2:7], *results[0:2])
        return tuple(stacked[5:7]) + tuple(stacked[0:5])

    return jax.shard_map(device_program, mesh=mesh, in_specs=(row_spec, row_spec, P(None, None), col_spec, inner_spec, col_spec, col_spec, inner_spec), out_specs=(row_spec, P('dp', None), P('dp', None, 'tp'), P('dp', 'tp', None), P('dp', None, 'tp'), P('dp', None, 'tp'), P('dp', 'tp', None)), check_vma=False)
```

```python
import functools

import jax
import jax.numpy as jnp
import numpy as np
from jax import lax
from jax.experimental import pallas as pl
from jax.experimental.pallas import tpu as pltpu
from jax.sharding import PartitionSpec as P

HEAD_DIM = 128
NORM_EPS = 1e-5
ROPE_BASE = 10000.0
MESH = pl.DeviceIdType.MESH
NP = 4
F32 = jnp.float32
BF16 = jnp.bfloat16


def dot_nn(a, b):
    return lax.dot_general(a, b, (((1,), (0,)), ((), ())), preferred_element_type=F32)


def dot_nt(a, b):
    return lax.dot_general(a, b, (((1,), (1,)), ((), ())), preferred_element_type=F32)


def dot_tn(a, b):
    return lax.dot_general(a, b, (((0,), (0,)), ((), ())), preferred_element_type=F32)


def aligned(index, size):
    return pl.multiple_of(index, size)


def scoped(name):
    def wrap(function):
        @functools.wraps(function)
        def inner(*args, **kwargs):
            with jax.named_scope(name):
                return function(*args, **kwargs)
        return inner
    return wrap


class Place:
    def __init__(self, tp_size):
        index = lax.axis_index('tp')
        self.ring = tp_size // 2
        self.half = self.ring // 2
        self.core = lax.rem(index, 2)
        self.chip = lax.div(index, 2)
        self.right = {'tp': self.near(1) * 2 + self.core}
        self.left = {'tp': self.near(-1) * 2 + self.core}
        self.mate = {'tp': self.chip * 2 + 1 - self.core}

    def near(self, step):
        return lax.rem(self.chip + step + self.ring, self.ring)

    @scoped('barrier')
    def barrier(self, others=()):
        sem = pltpu.get_barrier_semaphore()
        peers = [self.right, self.left, self.mate] + list(others)
        for peer in peers:
            pl.semaphore_signal(sem, inc=1, device_id=peer, device_id_type=MESH)
        pl.semaphore_wait(sem, len(peers))


class Gather:
    def __init__(self, place, buf, shard_rows, sems):
        self.place, self.buf, self.shard = place, buf, shard_rows
        self.rows = shard_rows // NP
        self.events = (place.half - 1) * NP + NP // 2
        self.send_r, self.recv_r, self.send_l, self.recv_l, self.send_m, self.recv_m = sems

    @staticmethod
    def scratch(half):
        events = (half - 1) * NP + NP // 2
        return [pltpu.SemaphoreType.DMA((n,)) for n in (events, events, events, events, 2 * events + NP, 2 * events + NP)]

    def view(self, chip, core, piece):
        start = (chip * 2 + core) * self.shard + piece * self.rows
        return self.buf.at[pl.ds(aligned(start, self.rows), self.rows)]

    def own_rows(self):
        start = (self.place.chip * 2 + self.place.core) * self.shard
        return pl.ds(aligned(start, self.shard), self.shard)

    def to_right(self, event, view):
        return pltpu.make_async_remote_copy(view, view, self.send_r.at[event], self.recv_r.at[event], self.place.right, MESH)

    def to_left(self, event, view):
        return pltpu.make_async_remote_copy(view, view, self.send_l.at[event], self.recv_l.at[event], self.place.left, MESH)

    def to_mate(self, slot, view):
        return pltpu.make_async_remote_copy(view, view, self.send_m.at[slot], self.recv_m.at[slot], self.place.mate, MESH)

    def start(self):
        place = self.place
        for piece in range(NP):
            self.to_right(piece, self.view(place.chip, place.core, piece)).start()
            self.to_left(piece, self.view(place.chip, place.core, NP - 1 - piece)).start()
        for piece in range(NP):
            self.to_mate(2 * self.events + piece, self.view(place.chip, place.core, piece)).start()

    def views(self, event):
        step = lax.div(event, NP) + 1
        piece = lax.rem(event, NP)
        from_left = self.view(self.place.near(-step), self.place.core, piece)
        from_right = self.view(self.place.near(step), self.place.core, NP - 1 - piece)
        return from_left, from_right

    @scoped('g_event')
    def event(self, event, forward=None):
        from_left, from_right = self.views(event)
        self.to_right(event, from_left).wait_recv()
        self.pass_on(event, forward, lambda: self.to_right(event + NP, from_left).start())
        self.to_mate(event, from_left).start()
        self.to_left(event, from_right).wait_recv()
        self.pass_on(event, forward, lambda: self.to_left(event + NP, from_right).start())
        self.to_mate(self.events + event, from_right).start()

    def forward(self, event):
        from_left, from_right = self.views(event)
        self.to_right(event + NP, from_left).start()
        self.to_left(event + NP, from_right).start()

    def pass_on(self, event, forward, send):
        if forward is None:
            pl.when(event + NP < self.events)(send)
        elif forward:
            send()

    def mate_wait(self, first, count):
        for offset in range(count):
            self.to_mate(first + offset, self.view(self.place.chip, 1 - self.place.core, 0)).wait_recv()

    def mate_wait_all(self):
        def body(slot, carry):
            self.mate_wait(slot, 1)
            return carry
        lax.fori_loop(0, 2 * self.events + NP, body, 0)

    @scoped('g_matelast')
    def mate_wait_last(self):
        first = (self.place.half - 1) * NP
        self.mate_wait(first, NP // 2)
        self.mate_wait(self.events + first, NP // 2)

    @scoped('g_matewait')
    def mate_wait_chip(self, distance, rightward):
        ring_first = lax.select(rightward, self.events, 0) + jnp.maximum(distance - 1, 0) * NP
        self.mate_wait(lax.select(distance == 0, 2 * self.events, ring_first), NP)

    @scoped('g_finish')
    def finish(self):
        view = self.view(self.place.chip, self.place.core, 0)

        def ring(event, carry):
            self.to_right(event, view).wait_send()
            self.to_left(event, view).wait_send()
            return carry
        lax.fori_loop(0, self.events, ring, 0)

        def across(slot, carry):
            self.to_mate(slot, view).wait_send()
            return carry
        lax.fori_loop(0, 2 * self.events + NP, across, 0)


class Reduce:
    SLOTS = 6
    DEPTH = 8

    def __init__(self, place, part, shard_rows, refs):
        self.place, self.part, self.shard = place, part, shard_rows
        self.events = (place.half - 1) * NP + NP // 2
        self.ring, self.acc, self.stage, self.send_n, self.recv_n, self.send_m, self.recv_m = refs

    @staticmethod
    def scratch(half, shard_rows, width):
        events = (half - 1) * NP + NP // 2
        shapes = [(2, events), (2 * Reduce.DEPTH + NP,), (Reduce.SLOTS, 2)]
        sems = [(2, events), (2, events), (2 * events + NP,), (2 * events + NP,)]
        return [pltpu.VMEM(s + (shard_rows, width), F32) for s in shapes] + [pltpu.SemaphoreType.DMA(s) for s in sems]

    def acc_slot(self, term):
        own = 2 * self.DEPTH + jnp.maximum(term - 2 * self.events, 0)
        return lax.select(term < 2 * self.events, lax.rem(term, 2 * self.DEPTH), own)

    def mate_copy(self, term):
        return pltpu.make_async_remote_copy(
            self.stage.at[lax.rem(term, self.SLOTS), 1 - self.place.core], self.acc.at[self.acc_slot(term)], self.send_m.at[term], self.recv_m.at[term],
            self.place.mate, MESH)

    def ring_copy(self, event, way):
        to = {'tp': self.place.near(1 - 2 * way) * 2 + self.place.core}
        return pltpu.make_async_remote_copy(
            self.acc.at[self.acc_slot(2 * event + way)], self.ring.at[way, event], self.send_n.at[way, event], self.recv_n.at[way, event], to, MESH)

    @scoped('r_fill')
    def fill(self, term):
        @pl.when(term >= self.SLOTS)
        def _():
            self.mate_copy(jnp.maximum(term - self.SLOTS, 0)).wait_send()
        slot = lax.rem(term, self.SLOTS)
        way = lax.rem(term, 2)

        @pl.when(term >= 2 * (self.DEPTH - 1))
        def _():
            self.ring_copy(jnp.maximum(lax.div(term, 2) - (self.DEPTH - 1), 0), way).wait_send()
        shifted = lax.div(term, 2) + NP // 2
        travels = term < 2 * self.events
        distance = jnp.maximum(self.place.half - lax.div(shifted, NP), 0)
        turn = lax.rem(shifted, NP)
        piece = lax.select(travels, lax.select(way == 0, turn, NP - 1 - turn), lax.rem(jnp.maximum(term - 2 * self.events, 0), NP))
        value = self.part(self.place.near((1 - 2 * way) * distance), piece)
        self.stage[slot, 0] = value[:self.shard]
        self.stage[slot, 1] = value[self.shard:]
        self.mate_copy(term).start()

    @scoped('r_event')
    def event(self, event):
        def add(way, carry):
            term = 2 * event + way
            self.mate_copy(term).wait_recv()
            slot = self.acc_slot(term)
            self.acc[slot] += self.stage[lax.rem(term, self.SLOTS), self.place.core]

            @pl.when(event >= NP)
            def _():
                before = jnp.maximum(event - NP, 0)
                self.ring_copy(before, way).wait_recv()
                self.acc[slot] += self.ring[way, before]
            self.ring_copy(event, way).start()
            return carry
        lax.fori_loop(0, 2, add, 0)

    def final(self, piece):
        last = self.events - NP
        term = 2 * self.events + piece
        self.mate_copy(term).wait_recv()
        self.ring_copy(last + piece, 0).wait_recv()
        self.ring_copy(last + NP - 1 - piece, 1).wait_recv()
        return ((self.stage[term % self.SLOTS, self.place.core] + self.acc[2 * self.DEPTH + piece])
                + (self.ring[0, last + piece] + self.ring[1, last + NP - 1 - piece]))

    @scoped('r_finish')
    def finish(self):
        def across(term, carry):
            self.mate_copy(term).wait_send()
            return carry
        terms = 2 * self.events + NP
        lax.fori_loop(terms - self.SLOTS, terms, across, 0)

        def ring(event, carry):
            self.ring_copy(event, 0).wait_send()
            self.ring_copy(event, 1).wait_send()
            return carry
        lax.fori_loop(self.events + 2 - (self.DEPTH - 1), self.events, ring, 0)

    def run(self, filler):
        def body(turn, carry):
            event = jnp.maximum(turn - 1, 0)
            travels = (turn >= 1) & (turn <= self.events)

            @pl.when(travels)
            def _():
                self.event(event)

            def ahead(way, inner):
                self.fill(2 * turn + way)
                return inner
            lax.fori_loop(0, 2, ahead, 0)

            @pl.when(travels)
            def _():
                filler(event)
            return carry
        lax.fori_loop(0, self.events + 2, body, 0)


def rope_pair(table):
    lanes = lax.broadcasted_iota(jnp.int32, table.shape, 1)
    swapped = pltpu.roll(table, HEAD_DIM // 2, 1)
    low = lanes < HEAD_DIM // 2
    return jnp.where(low, table, swapped), jnp.where(low, -swapped, table)


@scoped('table')
def fill_table(freqs, table_ref):
    rows = 64
    blocks = table_ref.shape[0] // rows

    def cos_sin(count, scale):
        steps = lax.broadcasted_iota(jnp.int32, (count, HEAD_DIM), 0) * scale
        angles = steps.astype(F32) * freqs
        return jnp.cos(angles), jnp.sin(angles)
    cos_low, sin_low = cos_sin(rows, 1)
    cos_high, sin_high = cos_sin(max(blocks, 8), rows)
    low = lax.broadcasted_iota(jnp.int32, (1, HEAD_DIM), 1) < HEAD_DIM // 2
    first = jnp.where(low, cos_high, sin_high)
    second = jnp.where(low, -sin_high, cos_high)
    for block in range(blocks):
        table_ref[block * rows:(block + 1) * rows] = first[block:block + 1] * cos_low + second[block:block + 1] * sin_low


def rope(values, table, inverse=False):
    cos2, sin2 = rope_pair(table)
    turned = pltpu.roll(values, HEAD_DIM // 2, 1)
    if inverse:
        return values * cos2 - turned * sin2
    return values * cos2 + turned * sin2


def norm_forward(x_f32, gain_row):
    inv = lax.rsqrt(jnp.mean(x_f32 * x_f32, axis=-1, keepdims=True) + NORM_EPS)
    return (x_f32 * inv * gain_row).astype(BF16)


def norm_unit(x_f32):
    inv = lax.rsqrt(jnp.mean(x_f32 * x_f32, axis=-1, keepdims=True) + NORM_EPS)
    return inv, x_f32 * inv


@scoped('norm_backward')
def norm_backward(inv, unit, gain_row, d_normed):
    d_unit = d_normed * gain_row
    return inv * (d_unit - unit * jnp.mean(d_unit * unit, axis=-1, keepdims=True))


@scoped('attention')
def attention_block(row0, rows, keys, refs, forward, backward):
    q_ref, k_ref, v_ref, table_ref, read_da, write_o, dx_ref, dk_ref, dv_ref = refs
    here = pl.ds(aligned(row0, rows), rows)
    scale = HEAD_DIM ** -0.5
    query = q_ref[here]
    scores = dot_nt(query, k_ref[0:keys]) * scale
    row_id = row0 + lax.broadcasted_iota(jnp.int32, scores.shape, 0)
    col_id = lax.broadcasted_iota(jnp.int32, scores.shape, 1)
    scores = jnp.where(row_id >= col_id, scores, -1e30)
    expd = jnp.exp(scores - jnp.max(scores, axis=-1, keepdims=True))
    prob = expd * (1.0 / jnp.sum(expd, axis=-1, keepdims=True))
    prob_b = prob.astype(BF16)
    d_attn = read_da(here) if backward else None
    if forward:
        write_o(here, dot_nn(prob_b, v_ref[0:keys]).astype(BF16))
    if backward:
        dv_ref[0:keys] += dot_tn(prob_b, d_attn)
        d_prob = dot_nt(d_attn, v_ref[0:keys]).astype(BF16).astype(F32)
        row_dot = jnp.sum(prob * d_prob, axis=-1, keepdims=True)
        d_scores = (prob * (d_prob - row_dot) * scale).astype(BF16)
        d_query = dot_nn(d_scores, k_ref[0:keys]).astype(BF16).astype(F32)
        dx_ref[here, 0:HEAD_DIM] = rope(d_query, table_ref[here], inverse=True).astype(BF16)
        dk_ref[0:keys] += dot_tn(d_scores, query)


@scoped('store_kv')
def store_keys_values(here, dx_ref, dk_ref, dv_ref, table_ref):
    d_key = dk_ref[here].astype(BF16).astype(F32)
    dx_ref[here, HEAD_DIM:2 * HEAD_DIM] = rope(d_key, table_ref[here], inverse=True).astype(BF16)
    dx_ref[here, 2 * HEAD_DIM:3 * HEAD_DIM] = dv_ref[here].astype(BF16)


def gated_pull(gate, up, d_hidden):
    sig = jax.nn.sigmoid(gate)
    silu = gate * sig
    d_silu = d_hidden * up
    return (silu * up).astype(BF16), (d_silu * sig + d_silu * silu * (1.0 - sig)).astype(BF16), (d_hidden * silu).astype(BF16)


class Copies:
    def __init__(self, sems):
        self.sems, self.used = sems, 0

    def start(self, src, dst):
        copy = pltpu.make_async_copy(src, dst, self.sems.at[self.used])
        self.used += 1
        copy.start()
        return copy


def gather_loop(gather, unit, then=None):
    chips = gather.place.ring

    def body(event, carry):
        @pl.when(event < gather.events)
        def _():
            gather.event(event)
            if then is not None:
                then(event)
        step = lax.div(event, NP) + 1
        opposite = event == gather.events
        final = event == gather.events - 1
        own = event == 1
        near = (event >= NP) & (event < gather.events) & (lax.rem(event, 2) == 0)

        @pl.when(opposite)
        def _():
            gather.mate_wait_last()

        @pl.when(own | near | final)
        def _():
            gather.mate_wait_chip(step - 1, final | (lax.rem(event, NP) != 0))

        @pl.when(own | near | final | opposite)
        def _():
            distance = lax.select(opposite, gather.place.half, step - 1)
            rightward = final | (lax.rem(event, NP) != 0)
            count = lax.select(own, 0, lax.select(opposite, chips - 1, lax.select(final, chips - 2, jnp.maximum(lax.div(event, 2) - 1, 0))))
            unit(count, gather.place.near(lax.select(rightward, distance, -distance)))
        return carry
    lax.fori_loop(0, gather.events + 1, body, 0)


def weight_grads_u(block, u_ref, dx_ref, stage_ref, outs, sems, head_cols, ff):
    rows = stage_ref.shape[1]
    slot = lax.rem(block, 2)
    here = pl.ds(aligned(block * rows, rows), rows)

    def copies():
        bounds = (0, head_cols, head_cols + ff, head_cols + 2 * ff)
        return [pltpu.make_async_copy(stage_ref.at[slot, :, bounds[i]:bounds[i + 1]], outs[i].at[here], sems.at[slot, i]) for i in range(3)]

    @pl.when(block >= 2)
    def _():
        for copy in copies():
            copy.wait()
    stage_ref[slot] = dot_tn(u_ref[:, here], dx_ref[...]).astype(BF16)
    for copy in copies():
        copy.start()


def weight_grads_u_wait(stage_ref, outs, sems, head_cols, ff):
    rows = stage_ref.shape[1]
    bounds = (0, head_cols, head_cols + ff, head_cols + 2 * ff)
    for slot in range(2):
        for i in range(3):
            pltpu.make_async_copy(stage_ref.at[slot, :, bounds[i]:bounds[i + 1]], outs[i].at[pl.ds(0, rows)], sems.at[slot, i]).wait()


def weight_grads_h(piece, ho_ref, read_dy, stage_ref, outs, sems, ff):
    cols = stage_ref.shape[2]
    stage_ref[piece] = dot_tn(ho_ref[...], read_dy(piece)).astype(BF16)
    for copy in h_copies(piece, stage_ref, outs, sems, ff):
        copy.start()


def h_copies(piece, stage_ref, outs, sems, ff):
    cols = stage_ref.shape[2]
    there = pl.ds(aligned(piece * cols, cols), cols)
    return [pltpu.make_async_copy(stage_ref.at[piece, 0:HEAD_DIM], outs[0].at[:, there], sems.at[piece, 0]),
            pltpu.make_async_copy(stage_ref.at[piece, HEAD_DIM:HEAD_DIM + ff], outs[1].at[:, there], sems.at[piece, 1])]


def kernel_main(tp_size, x_ref, gain_ref, freq_ref, gy_hbm, wqkv_hbm, wout_hbm, wgate_hbm, wup_hbm, wdown_hbm,
                dx_out, gain_out, *refs):
    firsts, lasts = refs[0:5], refs[5:10]
    u0_hbm, q_hbm, k_hbm, v_hbm, o_hbm, ab_hbm = refs[10:16]
    (u_ref, g_ref, wc_ref, wo_ref, q_ref, k_ref, v_ref, ho_ref, dx_ref, dk_ref, dv_ref, table_ref, x1_ref, gs_ref,
     pair_ref, all_ref, local, sems_gs, sems_hs, sem_ps, sem_pr, sem_as, sem_ar, free_sem) = refs[16:40]
    sems_u, sems_g, refs_r = refs[40:46], refs[46:52], refs[52:]
    place = Place(tp_size)
    shard, width = x_ref.shape
    pair = 2 * shard
    chips = place.ring
    head_cols = wqkv_hbm.shape[2]
    ff = wgate_hbm.shape[2]
    piece_cols = width // NP
    gate_cols = slice(head_cols, head_cols + ff)
    up_cols = slice(head_cols + ff, head_cols + 2 * ff)
    hidden_cols = slice(HEAD_DIM, HEAD_DIM + ff)
    loads = Copies(local)
    gu = Gather(place, u_ref, shard, sems_u)
    gg = Gather(place, g_ref, shard, sems_g)

    def wait_all(copies):
        for copy in copies:
            copy.wait()

    def load_wc(layer):
        return [loads.start(wqkv_hbm.at[layer], wc_ref.at[:, 0:head_cols]),
                loads.start(wgate_hbm.at[layer], wc_ref.at[:, gate_cols]),
                loads.start(wup_hbm.at[layer], wc_ref.at[:, up_cols])]

    def load_wo(layer):
        copies = []
        for piece in range(NP):
            cols = slice(piece * piece_cols, (piece + 1) * piece_cols)
            copies.append(loads.start(wout_hbm.at[layer, :, cols], wo_ref.at[piece, 0:HEAD_DIM]))
            copies.append(loads.start(wdown_hbm.at[layer, :, cols], wo_ref.at[piece, hidden_cols]))
        return copies

    def rows_of(chip):
        return pl.ds(aligned(chip * pair, pair), pair)

    def write_o(here, value):
        ho_ref[here, 0:HEAD_DIM] = value

    def read_da(here):
        return dx_ref[here, 0:HEAD_DIM]

    def heads(here, rows_u):
        qkv = dot_nn(rows_u, wc_ref[:, 0:head_cols]).astype(BF16)
        table = table_ref[here]
        q_ref[here] = rope(qkv[:, 0:HEAD_DIM].astype(F32), table).astype(BF16)
        k_ref[here] = rope(qkv[:, HEAD_DIM:2 * HEAD_DIM].astype(F32), table).astype(BF16)
        v_ref[here] = qkv[:, 2 * HEAD_DIM:3 * HEAD_DIM]

    @scoped('f_unit')
    def forward_unit(count, chip, with_hidden):
        here = rows_of(chip)
        rows_u = u_ref[here]
        heads(here, rows_u)
        gate = dot_nn(rows_u, wc_ref[:, gate_cols]).astype(BF16)
        up = dot_nn(rows_u, wc_ref[:, up_cols]).astype(BF16)
        dx_ref[here, gate_cols] = gate
        dx_ref[here, up_cols] = up
        if with_hidden:
            gate_f, up_f = gate.astype(F32), up.astype(F32)
            ho_ref[here, hidden_cols] = (gate_f * jax.nn.sigmoid(gate_f) * up_f).astype(BF16)

    @scoped('b_unit')
    def backward_unit(count, chip):
        here = rows_of(chip)
        dah = dot_nt(g_ref[here, 0:piece_cols], wo_ref[0])
        for piece in range(1, NP):
            dah = dah + dot_nt(g_ref[here, piece * piece_cols:(piece + 1) * piece_cols], wo_ref[piece])
        dx_ref[here, 0:HEAD_DIM] = dah[:, 0:HEAD_DIM].astype(BF16)
        d_hidden = dah[:, hidden_cols].astype(BF16).astype(F32)
        hidden, d_gate, d_up = gated_pull(dx_ref[here, gate_cols].astype(F32), dx_ref[here, up_cols].astype(F32), d_hidden)
        ho_ref[here, hidden_cols] = hidden
        dx_ref[here, gate_cols] = d_gate
        dx_ref[here, up_cols] = d_up

    def part_forward(chip, piece):
        return dot_nn(ho_ref[rows_of(chip)], wo_ref[piece])

    def part_backward(chip, piece):
        return dot_nt(dx_ref[rows_of(chip)], wc_ref[pl.ds(aligned(piece * piece_cols, piece_cols), piece_cols)])

    def keys_values(chip):
        store_keys_values(rows_of(chip), dx_ref, dk_ref, dv_ref, table_ref)

    def other_keys_values():
        def body(step, carry):
            keys_values(place.near(place.half + step - chips))
            return carry
        lax.fori_loop(1, chips, body, 0)

    def read_dy(piece):
        return g_ref[:, pl.ds(aligned(piece * piece_cols, piece_cols), piece_cols)]

    @scoped('finals')
    def finals(reduce):
        return jnp.concatenate([reduce.final(piece) for piece in range(NP)], axis=1)

    @scoped('filler')
    def grads_filler(event, outs):
        outs_u, outs_h = (outs[0], outs[2], outs[3]), (outs[1], outs[4])

        @pl.when(event < NP)
        def _():
            weight_grads_h(event, ho_ref, read_dy, wo_ref, outs_h, sems_hs, ff)

        @pl.when((event >= NP) & (event < NP + chips))
        def _():
            weight_grads_u(jnp.maximum(event - NP, 0), u_ref, dx_ref, gs_ref, outs_u, sems_gs, head_cols, ff)

    @scoped('grads_wait')
    def grads_wait(outs):
        outs_u, outs_h = (outs[0], outs[2], outs[3]), (outs[1], outs[4])
        for piece in range(NP):
            wait_all(h_copies(piece, wo_ref, outs_h, sems_hs, ff))
        weight_grads_u_wait(gs_ref, outs_u, sems_gs, head_cols, ff)

    lanes = all_ref.shape[3]
    tiles = width // lanes

    def cross(layer):
        return pltpu.make_async_remote_copy(pair_ref.at[layer, 0], pair_ref.at[layer, 1], sem_ps.at[layer], sem_pr.at[layer], place.mate, MESH)

    def spread(layer, step):
        here = all_ref.at[layer, place.chip]
        return pltpu.make_async_remote_copy(here, here, sem_as.at[layer, step - 1], sem_ar.at[layer, step - 1],
                                            {'tp': place.near(step) * 2 + place.core}, MESH)

    def start_gain(layer, row):
        for tile in range(tiles):
            pair_ref[layer, 0, tile:tile + 1] = row[:, tile * lanes:(tile + 1) * lanes]
        cross(layer).start()

    @scoped('spread_gain')
    def spread_gain(layer):
        cross(layer).wait()
        all_ref[layer, place.chip] = pair_ref[layer, 0] + pair_ref[layer, 1]
        for step in range(1, chips):
            spread(layer, step).start()

    @scoped('end_gain')
    def end_gain(layer):
        for step in range(1, chips):
            spread(layer, step).wait()
        total = all_ref[layer, 0]
        for chip in range(1, chips):
            total = total + all_ref[layer, chip]
        for tile in range(tiles):
            gain_out[layer:layer + 1, tile * lanes:(tile + 1) * lanes] = total[tile:tile + 1]

    load_g = loads.start(gy_hbm, g_ref.at[gg.own_rows()])
    load_w = load_wc(0)
    load_o = load_wo(0)
    u_ref[gu.own_rows()] = norm_forward(x_ref[...].astype(F32), gain_ref[0:1])
    place.barrier([{'tp': place.near(step) * 2 + place.core} for step in range(2, chips - 1)])
    gu.start()
    saves = [loads.start(u_ref.at[gu.own_rows()], u0_hbm)]
    fill_table(freq_ref[0:1], table_ref)
    load_g.wait()
    wait_all(load_w)

    def start_gy(event):
        @pl.when(event == gu.events - NP)
        def _():
            gg.start()
    gather_loop(gu, lambda count, chip: forward_unit(count, chip, True), start_gy)

    load_w = load_wc(1)
    saves += [loads.start(q_ref, q_hbm), loads.start(k_ref, k_hbm), loads.start(v_ref, v_hbm),
              loads.start(dx_ref.at[:, head_cols:head_cols + 2 * ff], ab_hbm)]

    def attend_first(chip):
        attention_block(chip * pair, pair, chips * pair, (q_ref, k_ref, v_ref, table_ref, None, write_o, None, None, None), True, False)
    attend_first(place.near(place.half))
    wait_all(load_o)
    reduce = Reduce(place, part_forward, shard, refs_r)

    def filler_forward(event):
        @pl.when(event < place.half)
        def _():
            distance = jnp.maximum(place.half - 1 - event, 0)

            def body(way, carry):
                attend_first(place.near((1 - 2 * way) * distance))
                return carry
            lax.fori_loop(0, lax.select(distance == 0, 1, 2), body, 0)

        @pl.when(event == place.half)
        def _():
            gu.finish()
            o_copy().start()
    n_o = loads.used
    loads.used += 1

    def o_copy():
        return pltpu.make_async_copy(ho_ref.at[:, 0:HEAD_DIM], o_hbm, local.at[n_o])
    reduce.run(filler_forward)
    load_o = load_wo(1)
    gg.event(jnp.int32(0), forward=True)
    gg.event(jnp.int32(1), forward=True)
    x_next = (x_ref[...].astype(F32) + finals(reduce)).astype(BF16)
    x1_ref[...] = x_next
    saves[0].wait()
    o_copy().wait()
    u_ref[gu.own_rows()] = norm_forward(x_next.astype(F32), gain_ref[1:2])

    reduce.finish()
    gu.start()
    wait_all(saves[1:])
    wait_all(load_w)
    wait_all(load_o)
    dk_ref[...] = jnp.zeros_like(dk_ref)
    dv_ref[...] = jnp.zeros_like(dv_ref)
    early = 2
    for event in range(early, NP):
        gg.event(jnp.int32(event), forward=False)

    def more_gy(event):
        first = gu.events - NP

        @pl.when((event >= first) & (event < first + NP - early))
        def _():
            gg.forward(jnp.maximum(event - first, 0) + early)

        @pl.when(event >= first + NP - early)
        def _():
            gg.event(jnp.maximum(event - first, 0) + early, forward=True)

        @pl.when((event > NP) & (event < NP + 6) & (lax.rem(event, 2) == 1))
        def _():
            turn = jnp.maximum(lax.div(event - 1, 2) - 2, 0)
            gg.mate_wait_chip(jnp.minimum(turn, 1), turn == 2)
            backward_unit(turn, place.near(lax.select(turn == 2, 1, -turn)))
    gather_loop(gu, lambda count, chip: forward_unit(count, chip, False), more_gy)

    groups = 4

    def attend_last(turn, carry):
        held = early + NP
        distance = lax.div(turn + 1, 2)
        rightward = (turn > 0) & (lax.rem(turn, 2) == 0)
        opposite = turn == chips - 1
        needed = lax.select(turn == 0, held, lax.select(opposite, gg.events, distance * NP))
        begin = lax.select(turn == 0, held, jnp.minimum(jnp.maximum(held + turn - 1, lax.select(turn >= chips - 2, gg.events - NP // 2, 0)), gg.events))
        end = jnp.maximum(jnp.minimum(held + turn, gg.events), needed)
        end = lax.select(turn == chips - 2, jnp.maximum(end, gg.events - 1), end)
        begin = lax.select(turn == chips - 1, gg.events - 1, begin)

        def take(event, inner):
            gg.event(event)
            return inner
        lax.fori_loop(begin, end, take, 0)

        chip = place.near(lax.select(rightward, distance, -distance))

        @pl.when(opposite)
        def _():
            gg.mate_wait_last()

        @pl.when((turn > 2) & jnp.logical_not(opposite))
        def _():
            gg.mate_wait_chip(distance, rightward)

        @pl.when(turn > 2)
        def _():
            backward_unit(turn, chip)
        for group in range(groups):
            @pl.when(lax.div(chip, chips // groups) == group)
            def _(group=group):
                attention_block(chip * pair, pair, (group + 1) * (chips * pair // groups),
                                (q_ref, k_ref, v_ref, table_ref, read_da, write_o, dx_ref, dk_ref, dv_ref), True, True)
        return carry
    lax.fori_loop(0, chips, attend_last, 0)
    keys_values(place.near(place.half))
    loads_a = [loads.start(q_hbm, q_ref), loads.start(k_hbm, k_ref), loads.start(v_hbm, v_ref)]
    n_late = loads.used
    loads.used += 2

    def late_loads():
        return [pltpu.make_async_copy(u0_hbm, u_ref.at[gu.own_rows()], local.at[n_late]),
                pltpu.make_async_copy(o_hbm, ho_ref.at[:, 0:HEAD_DIM], local.at[n_late + 1])]
    near = (place.left, place.right, place.mate)
    reduce = Reduce(place, part_backward, shard, refs_r)

    def filler_last(event):
        @pl.when(event == 0)
        def _():
            other_keys_values()
        grads_filler(event, lasts)

        @pl.when(event == 1)
        def _():
            gg.finish()
            gu.finish()

        @pl.when(event == NP + chips)
        def _():
            for copy in late_loads():
                copy.start()
            for peer in near:
                pl.semaphore_signal(free_sem, inc=1, device_id=peer, device_id_type=MESH)
    reduce.run(filler_last)
    pl.semaphore_wait(free_sem, len(near))
    wait_all(late_loads())
    gu.start()
    d_normed = finals(reduce).astype(BF16).astype(F32)
    inv, unit = norm_unit(x1_ref[...].astype(F32))
    g_ref[gg.own_rows()] = (g_ref[gg.own_rows()].astype(F32) + norm_backward(inv, unit, gain_ref[1:2], d_normed)).astype(BF16)
    start_gain(1, jnp.sum(d_normed * unit, axis=0, keepdims=True))

    reduce.finish()
    gg.start()
    spread_gain(1)
    grads_wait(lasts)
    load_o = load_wo(0) + [loads.start(ab_hbm, dx_ref.at[:, head_cols:head_cols + 2 * ff])]
    load_w = load_wc(0)
    dk_ref[...] = jnp.zeros_like(dk_ref)
    dv_ref[...] = jnp.zeros_like(dv_ref)
    wait_all(load_o)

    def more_u(event):
        @pl.when(event >= gg.events - NP)
        def _():
            gu.event(jnp.maximum(event - (gg.events - NP), 0), forward=True)
    gather_loop(gg, backward_unit, more_u)
    wait_all(loads_a)

    back_groups = 2

    def attend_back(block, carry):
        @pl.when(block < gu.events - 2 * NP)
        def _():
            gu.event(block + NP, forward=True)
        for group in range(back_groups):
            @pl.when(lax.div(block, chips // back_groups) == group)
            def _(group=group):
                attention_block(block * pair, pair, (group + 1) * (chips * pair // back_groups),
                                (q_ref, k_ref, v_ref, table_ref, read_da, None, dx_ref, dk_ref, dv_ref), False, True)
        return carry
    lax.fori_loop(0, chips, attend_back, 0)
    keys_values(place.near(place.half))
    wait_all(load_w)
    reduce = Reduce(place, part_backward, shard, refs_r)

    def filler_first(event):
        @pl.when(event == 0)
        def _():
            other_keys_values()

        @pl.when(event < NP)
        def _():
            gu.event(gu.events - NP + event, forward=False)

        @pl.when(event == NP - 1)
        def _():
            gu.mate_wait_all()
        grads_filler(event, firsts)
    reduce.run(filler_first)
    inv, unit = norm_unit(x_ref[...].astype(F32))
    d_normed = finals(reduce).astype(BF16).astype(F32)
    start_gain(0, jnp.sum(d_normed * unit, axis=0, keepdims=True))
    dx_out[...] = (g_ref[gg.own_rows()].astype(F32) + norm_backward(inv, unit, gain_ref[0:1], d_normed)).astype(BF16)
    spread_gain(0)
    end_gain(1)
    gu.finish()
    gg.finish()
    reduce.finish()
    grads_wait(firsts)
    end_gain(0)


def kernel_stack(*refs):
    lasts, firsts, rest, outs, out_rest = refs[0:5], refs[5:10], refs[10:12], refs[12:17], refs[17:19]
    bufs, buf_rest, (sem_in, sem_out) = refs[19:24], refs[24:26], refs[26:28]
    steps = []
    for layer, sources in ((1, lasts), (0, firsts)):
        for number, source in enumerate(sources):
            rows = source.shape[0] // max(1, source.shape[0] // 512)
            for start in range(0, source.shape[0], rows):
                here = pl.ds(start, rows)
                steps.append((source.at[here], bufs[number].at[layer, here], outs[number].at[layer, here]))
    steps += list(zip(rest, buf_rest, out_rest))
    reads = [pltpu.make_async_copy(source, buf, sem_in.at[slot]) for slot, (source, buf, out) in enumerate(steps)]
    writes = [pltpu.make_async_copy(buf, out, sem_out.at[slot]) for slot, (source, buf, out) in enumerate(steps)]
    for read in reads:
        read.start()
    for read, write in zip(reads, writes):
        read.wait()
        write.start()
    for write in writes:
        write.wait()


def solution(mesh):
    tp_size = mesh.shape['tp']
    half = tp_size // 4
    row_spec = P(('dp', 'tp'), None)
    col_spec = P(None, None, 'tp')
    inner_spec = P(None, 'tp', None)

    def device_program(x_loc, dy_loc, norm_gain, w_qkv, w_out, w_gate, w_up, w_down):
        shard, width = x_loc.shape
        seq = shard * tp_size
        pair = 2 * shard
        chips = tp_size // 2
        head_cols = w_qkv.shape[2]
        ff = w_gate.shape[2]
        cols = head_cols + 2 * ff
        piece_cols = width // NP
        vmem, anyspace = pl.BlockSpec(memory_space=pltpu.VMEM), pl.BlockSpec(memory_space=pl.ANY)
        shape = jax.ShapeDtypeStruct
        dma = pltpu.SemaphoreType.DMA

        freqs = np.float32(ROPE_BASE) ** (np.float32(-2.0) * np.arange(HEAD_DIM // 2, dtype=np.float32) / np.float32(HEAD_DIM))
        freqs = jnp.asarray(np.tile(freqs, (8, 2)))

        rows_shape = shape((shard, width), BF16)
        gain_shape = shape((2, width), F32)
        head_shape = shape((seq, HEAD_DIM), BF16)
        grads = (shape((width, head_cols), BF16), shape((HEAD_DIM, width), BF16), shape((width, ff), BF16),
                 shape((width, ff), BF16), shape((ff, width), BF16))
        whole_vmem = 67043328
        results = pl.pallas_call(
            functools.partial(kernel_main, tp_size),
            out_shape=(rows_shape, gain_shape) + grads + grads + (rows_shape,) + (head_shape,) * 4 + (shape((seq, 2 * ff), BF16),),
            in_specs=[vmem] * 3 + [anyspace] * 6,
            out_specs=(vmem, vmem) + (anyspace,) * 16,
            scratch_shapes=[
                pltpu.VMEM((seq, width), BF16), pltpu.VMEM((seq, width), BF16), pltpu.VMEM((width, cols), BF16),
                pltpu.VMEM((NP, HEAD_DIM + ff, piece_cols), BF16),
                pltpu.VMEM((seq, HEAD_DIM), BF16), pltpu.VMEM((seq, HEAD_DIM), BF16), pltpu.VMEM((seq, HEAD_DIM), BF16),
                pltpu.VMEM((seq, HEAD_DIM + ff), BF16), pltpu.VMEM((seq, cols), BF16),
                pltpu.VMEM((seq, HEAD_DIM), F32), pltpu.VMEM((seq, HEAD_DIM), F32), pltpu.VMEM((seq, HEAD_DIM), F32),
                pltpu.VMEM((shard, width), BF16), pltpu.VMEM((2, width // chips, cols), BF16),
                pltpu.VMEM((2, 2, width // 128, 128), F32), pltpu.VMEM((2, chips, width // 128, 128), F32),
                dma((64,)), dma((2, 3)), dma((NP, 2)), dma((2,)), dma((2,)), dma((2, chips - 1)), dma((2, chips - 1)),
                pltpu.SemaphoreType.REGULAR] + Gather.scratch(half) + Gather.scratch(half) + Reduce.scratch(half, shard, piece_cols),
            compiler_params=pltpu.CompilerParams(collective_id=1, has_side_effects=True, vmem_limit_bytes=whole_vmem), name='blocks',
        )(x_loc, norm_gain, freqs, dy_loc, w_qkv, w_out, w_gate, w_up, w_down)

        stacked = pl.pallas_call(
            kernel_stack,
            out_shape=tuple(shape((2,) + grad.shape, BF16) for grad in grads) + (rows_shape, gain_shape),
            in_specs=[anyspace] * 12,
            out_specs=(anyspace,) * 7,
            scratch_shapes=[pltpu.VMEM((2,) + grad.shape, BF16) for grad in grads]
            + [pltpu.VMEM(rows_shape.shape, BF16), pltpu.VMEM(gain_shape.shape, F32), dma((64,)), dma((64,))],
            compiler_params=pltpu.CompilerParams(vmem_limit_bytes=whole_vmem), name='stack',
        )(*results[7:12], *results[2:7], *results[0:2])
        return tuple(stacked[5:7]) + tuple(stacked[0:5])

    return jax.shard_map(device_program, mesh=mesh, in_specs=(row_spec, row_spec, P(None, None), col_spec, inner_spec, col_spec, col_spec, inner_spec), out_specs=(row_spec, P('dp', None), P('dp', None, 'tp'), P('dp', 'tp', None), P('dp', None, 'tp'), P('dp', None, 'tp'), P('dp', 'tp', None)), check_vma=False)
```

```python
import functools

import jax
import jax.numpy as jnp
import numpy as np
from jax import lax
from jax.experimental import pallas as pl
from jax.experimental.pallas import tpu as pltpu
from jax.sharding import PartitionSpec as P

HEAD_DIM = 128
NORM_EPS = 1e-5
ROPE_BASE = 10000.0
MESH = pl.DeviceIdType.MESH
NP = 4
F32 = jnp.float32
BF16 = jnp.bfloat16


def dot_nn(a, b):
    return lax.dot_general(a, b, (((1,), (0,)), ((), ())), preferred_element_type=F32)


def dot_nt(a, b):
    return lax.dot_general(a, b, (((1,), (1,)), ((), ())), preferred_element_type=F32)


def dot_tn(a, b):
    return lax.dot_general(a, b, (((0,), (0,)), ((), ())), preferred_element_type=F32)


def not_below_zero(index):
    return jnp.maximum(index, 0)


def row_mean(values):
    return jnp.mean(values, axis=-1, keepdims=True)


def row_sum(values):
    return jnp.sum(values, axis=-1, keepdims=True)


def loop_from(first, last, body):
    def step(index, carry):
        body(index)
        return carry
    lax.fori_loop(first, last, step, 0)


def loop(count, body):
    loop_from(0, count, body)


def aligned(index, size):
    return pl.multiple_of(index, size)


def scoped(name):
    def wrap(function):
        @functools.wraps(function)
        def inner(*args, **kwargs):
            with jax.named_scope(name):
                return function(*args, **kwargs)
        return inner
    return wrap


class Place:
    def __init__(self, tp_size):
        index = lax.axis_index('tp')
        self.ring = tp_size // 2
        self.half = self.ring // 2
        self.core = lax.rem(index, 2)
        self.chip = lax.div(index, 2)
        self.right = self.peer(1)
        self.left = self.peer(-1)
        self.mate = {'tp': self.chip * 2 + 1 - self.core}

    def peer(self, step):
        return {'tp': self.near(step) * 2 + self.core}

    def near(self, step):
        return lax.rem(self.chip + step + self.ring, self.ring)

    def arrive(self):
        peers = [self.right, self.left, self.mate] + [self.peer(step) for step in range(2, self.ring - 1)]
        for peer in peers:
            pl.semaphore_signal(pltpu.get_barrier_semaphore(), inc=1, device_id=peer, device_id_type=MESH)
        return len(peers)


class Gather:
    def __init__(self, place, buf, shard_rows, sems):
        self.place, self.buf, self.shard = place, buf, shard_rows
        self.rows = shard_rows // NP
        self.events = (place.half - 1) * NP + NP // 2
        self.send_r, self.recv_r, self.send_l, self.recv_l, self.send_m, self.recv_m = sems

    @staticmethod
    def scratch(half):
        events = (half - 1) * NP + NP // 2
        return [pltpu.SemaphoreType.DMA((n,)) for n in (events, events, events, events, 2 * events + NP, 2 * events + NP)]

    def view(self, chip, core, piece):
        start = (chip * 2 + core) * self.shard + piece * self.rows
        return self.buf.at[pl.ds(aligned(start, self.rows), self.rows)]

    def own_rows(self):
        start = (self.place.chip * 2 + self.place.core) * self.shard
        return pl.ds(aligned(start, self.shard), self.shard)

    def to_right(self, event, view):
        return pltpu.make_async_remote_copy(view, view, self.send_r.at[event], self.recv_r.at[event], self.place.right, MESH)

    def to_left(self, event, view):
        return pltpu.make_async_remote_copy(view, view, self.send_l.at[event], self.recv_l.at[event], self.place.left, MESH)

    def to_mate(self, slot, view):
        return pltpu.make_async_remote_copy(view, view, self.send_m.at[slot], self.recv_m.at[slot], self.place.mate, MESH)

    def start(self):
        place = self.place
        for piece in range(NP):
            self.to_right(piece, self.view(place.chip, place.core, piece)).start()
            self.to_left(piece, self.view(place.chip, place.core, NP - 1 - piece)).start()
        for piece in range(NP):
            self.to_mate(2 * self.events + piece, self.view(place.chip, place.core, piece)).start()

    def views(self, event):
        step = lax.div(event, NP) + 1
        piece = lax.rem(event, NP)
        from_left = self.view(self.place.near(-step), self.place.core, piece)
        from_right = self.view(self.place.near(step), self.place.core, NP - 1 - piece)
        return from_left, from_right

    @scoped('g_event')
    def event(self, event, forward=None):
        from_left, from_right = self.views(event)
        self.to_right(event, from_left).wait_recv()
        self.pass_on(event, forward, lambda: self.to_right(event + NP, from_left).start())
        self.to_mate(event, from_left).start()
        self.to_left(event, from_right).wait_recv()
        self.pass_on(event, forward, lambda: self.to_left(event + NP, from_right).start())
        self.to_mate(self.events + event, from_right).start()

    def forward(self, event):
        from_left, from_right = self.views(event)
        self.to_right(event + NP, from_left).start()
        self.to_left(event + NP, from_right).start()

    def pass_on(self, event, forward, send):
        if forward is None:
            pl.when(event + NP < self.events)(send)
        elif forward:
            send()

    def mate_wait(self, first, count):
        for offset in range(count):
            self.to_mate(first + offset, self.view(self.place.chip, 1 - self.place.core, 0)).wait_recv()

    def mate_wait_all(self):
        def body(slot):
            self.mate_wait(slot, 1)
        loop(2 * self.events + NP, body)

    @scoped('g_matelast')
    def mate_wait_last(self):
        first = (self.place.half - 1) * NP
        self.mate_wait(first, NP // 2)
        self.mate_wait(self.events + first, NP // 2)

    @scoped('g_matewait')
    def mate_wait_chip(self, distance, rightward):
        ring_first = lax.select(rightward, self.events, 0) + not_below_zero(distance - 1) * NP
        self.mate_wait(lax.select(distance == 0, 2 * self.events, ring_first), NP)

    @scoped('g_finish')
    def finish(self):
        view = self.view(self.place.chip, self.place.core, 0)

        def ring(event):
            self.to_right(event, view).wait_send()
            self.to_left(event, view).wait_send()
        loop(self.events, ring)

        def across(slot):
            self.to_mate(slot, view).wait_send()
        loop(2 * self.events + NP, across)


class Reduce:
    SLOTS = 6
    DEPTH = 8

    def __init__(self, place, part, shard_rows, refs):
        self.place, self.part, self.shard = place, part, shard_rows
        self.events = (place.half - 1) * NP + NP // 2
        self.ring, self.acc, self.stage, self.send_n, self.recv_n, self.send_m, self.recv_m = refs

    @staticmethod
    def scratch(half, shard_rows, width):
        events = (half - 1) * NP + NP // 2
        shapes = [(2, events), (2 * Reduce.DEPTH + NP,), (Reduce.SLOTS, 2)]
        sems = [(2, events), (2, events), (2 * events + NP,), (2 * events + NP,)]
        return [pltpu.VMEM(s + (shard_rows, width), F32) for s in shapes] + [pltpu.SemaphoreType.DMA(s) for s in sems]

    def acc_slot(self, term):
        own = 2 * self.DEPTH + not_below_zero(term - 2 * self.events)
        return lax.select(term < 2 * self.events, lax.rem(term, 2 * self.DEPTH), own)

    def mate_copy(self, term):
        return pltpu.make_async_remote_copy(
            self.stage.at[lax.rem(term, self.SLOTS), 1 - self.place.core], self.acc.at[self.acc_slot(term)], self.send_m.at[term], self.recv_m.at[term],
            self.place.mate, MESH)

    def ring_copy(self, event, way):
        to = self.place.peer(1 - 2 * way)
        return pltpu.make_async_remote_copy(
            self.acc.at[self.acc_slot(2 * event + way)], self.ring.at[way, event], self.send_n.at[way, event], self.recv_n.at[way, event], to, MESH)

    @scoped('r_fill')
    def fill(self, term):
        @pl.when(term >= self.SLOTS)
        def _():
            self.mate_copy(not_below_zero(term - self.SLOTS)).wait_send()
        slot = lax.rem(term, self.SLOTS)
        way = lax.rem(term, 2)

        @pl.when(term >= 2 * (self.DEPTH - 1))
        def _():
            self.ring_copy(jnp.maximum(lax.div(term, 2) - (self.DEPTH - 1), 0), way).wait_send()
        shifted = lax.div(term, 2) + NP // 2
        travels = term < 2 * self.events
        distance = not_below_zero(self.place.half - lax.div(shifted, NP))
        turn = lax.rem(shifted, NP)
        piece = lax.select(travels, lax.select(way == 0, turn, NP - 1 - turn), lax.rem(not_below_zero(term - 2 * self.events), NP))
        value = self.part(self.place.near((1 - 2 * way) * distance), piece)
        self.stage[slot, 0] = value[:self.shard]
        self.stage[slot, 1] = value[self.shard:]
        self.mate_copy(term).start()

    @scoped('r_event')
    def event(self, event):
        def add(way):
            term = 2 * event + way
            self.mate_copy(term).wait_recv()
            slot = self.acc_slot(term)
            self.acc[slot] += self.stage[lax.rem(term, self.SLOTS), self.place.core]

            @pl.when(event >= NP)
            def _():
                before = not_below_zero(event - NP)
                self.ring_copy(before, way).wait_recv()
                self.acc[slot] += self.ring[way, before]
            self.ring_copy(event, way).start()
        loop(2, add)

    def final(self, piece):
        last = self.events - NP
        term = 2 * self.events + piece
        self.mate_copy(term).wait_recv()
        self.ring_copy(last + piece, 0).wait_recv()
        self.ring_copy(last + NP - 1 - piece, 1).wait_recv()
        return ((self.stage[term % self.SLOTS, self.place.core] + self.acc[2 * self.DEPTH + piece])
                + (self.ring[0, last + piece] + self.ring[1, last + NP - 1 - piece]))

    @scoped('r_finish')
    def finish(self):
        def across(term):
            self.mate_copy(term).wait_send()
        terms = 2 * self.events + NP
        loop_from(terms - self.SLOTS, terms, across)

        def ring(event):
            self.ring_copy(event, 0).wait_send()
            self.ring_copy(event, 1).wait_send()
        loop_from(self.events + 2 - (self.DEPTH - 1), self.events, ring)

    def run(self, filler):
        def body(turn):
            event = not_below_zero(turn - 1)
            travels = (turn >= 1) & (turn <= self.events)

            @pl.when(travels)
            def _():
                self.event(event)

            def ahead(way):
                self.fill(2 * turn + way)
            loop(2, ahead)

            @pl.when(travels)
            def _():
                filler(event)
        loop(self.events + 2, body)


def rope_pair(table):
    lanes = lax.broadcasted_iota(jnp.int32, table.shape, 1)
    swapped = pltpu.roll(table, HEAD_DIM // 2, 1)
    low = lanes < HEAD_DIM // 2
    return jnp.where(low, table, swapped), jnp.where(low, -swapped, table)


@scoped('table')
def fill_table(freqs, table_ref):
    rows = 64
    blocks = table_ref.shape[0] // rows

    def cos_sin(count, scale):
        steps = lax.broadcasted_iota(jnp.int32, (count, HEAD_DIM), 0) * scale
        angles = steps.astype(F32) * freqs
        return jnp.cos(angles), jnp.sin(angles)
    cos_low, sin_low = cos_sin(rows, 1)
    cos_high, sin_high = cos_sin(max(blocks, 8), rows)
    low = lax.broadcasted_iota(jnp.int32, (1, HEAD_DIM), 1) < HEAD_DIM // 2
    first = jnp.where(low, cos_high, sin_high)
    second = jnp.where(low, -sin_high, cos_high)
    for block in range(blocks):
        table_ref[block * rows:(block + 1) * rows] = first[block:block + 1] * cos_low + second[block:block + 1] * sin_low


def rope(values, table, inverse=False):
    cos2, sin2 = rope_pair(table)
    turned = pltpu.roll(values, HEAD_DIM // 2, 1)
    if inverse:
        return values * cos2 - turned * sin2
    return values * cos2 + turned * sin2


def norm_forward(x_f32, gain_row):
    inv = lax.rsqrt(row_mean(x_f32 * x_f32) + NORM_EPS)
    return (x_f32 * inv * gain_row).astype(BF16)


def norm_unit(x_f32):
    inv = lax.rsqrt(row_mean(x_f32 * x_f32) + NORM_EPS)
    return inv, x_f32 * inv


@scoped('norm_backward')
def norm_backward(inv, unit, gain_row, d_normed):
    d_unit = d_normed * gain_row
    return inv * (d_unit - unit * row_mean(d_unit * unit))


def by_halves(dot, a, b, axis):
    size = a.shape[axis] // 2
    first = a[:size] if axis == 0 else a[:, :size]
    second = a[size:] if axis == 0 else a[:, size:]
    return dot(first, b), dot(second, b)


@scoped('attention')
def attention_block(row0, rows, keys, diagonal, refs, forward, backward):
    q_ref, k_ref, v_ref, table_ref, read_da, write_o, dx_ref, dk_ref, dv_ref = refs
    here = pl.ds(aligned(row0, rows), rows)
    scale = HEAD_DIM ** -0.5
    spans = [(start, end) for start, end in ((0, keys - diagonal), (keys - diagonal, keys)) if end > start]
    query = q_ref[here]
    scores = []
    for start, end in spans:
        part = dot_nt(query, k_ref[start:end])
        if end == keys:
            row_id = row0 - start + lax.broadcasted_iota(jnp.int32, part.shape, 0)
            part = jnp.where(row_id >= lax.broadcasted_iota(jnp.int32, part.shape, 1), part, -1e30)
        scores.append(part)
    tops = [jnp.max(part, axis=-1, keepdims=True) for part in scores]
    top = functools.reduce(jnp.maximum, tops)
    factor = scale * 1.4426950408889634
    expd = [jnp.exp2((part - top) * factor) for part in scores]
    inv_sum = 1.0 / sum(row_sum(part) for part in expd)
    prob = [part * inv_sum for part in expd]
    prob_b = [part.astype(BF16) for part in prob]
    if forward:
        halves = [by_halves(dot_nn, part, v_ref[start:end], 0) for part, (start, end) in zip(prob_b, spans)]
        out = [functools.reduce(jnp.add, [half[i] for half in halves]) for i in range(2)]
        write_o(here, jnp.concatenate(out, axis=0).astype(BF16))
    if backward:
        d_attn = read_da(here)
        d_prob = [dot_nt(d_attn, v_ref[start:end]).astype(BF16).astype(F32) for start, end in spans]
        row_dot = sum(row_sum(p * d) for p, d in zip(prob, d_prob))
        d_scores = [(p * (d - row_dot)).astype(BF16) for p, d in zip(prob, d_prob)]
        halves = [by_halves(dot_nn, part, k_ref[start:end], 0) for part, (start, end) in zip(d_scores, spans)]
        d_query = jnp.concatenate([functools.reduce(jnp.add, [half[i] for half in halves]) for i in range(2)], axis=0)
        d_query = (d_query * scale).astype(BF16).astype(F32)
        dx_ref[here, :HEAD_DIM] = rope(d_query, table_ref[here], inverse=True).astype(BF16)
        for part, prob_part, (start, end) in zip(d_scores, prob_b, spans):
            middle = (start + end) // 2
            for ref, left, right in ((dv_ref, prob_part, d_attn), (dk_ref, part, query)):
                low, high = by_halves(dot_tn, left, right, 1)
                ref[start:middle] += low
                ref[middle:end] += high


@scoped('store_kv')
def store_keys_values(here, dx_ref, dk_ref, dv_ref, table_ref):
    d_key = (dk_ref[here] * HEAD_DIM ** -0.5).astype(BF16).astype(F32)
    dx_ref[here, HEAD_DIM:2 * HEAD_DIM] = rope(d_key, table_ref[here], inverse=True).astype(BF16)
    dx_ref[here, 2 * HEAD_DIM:3 * HEAD_DIM] = dv_ref[here].astype(BF16)


def gated_pull(gate, up, d_hidden):
    sig = jax.nn.sigmoid(gate)
    silu = gate * sig
    d_silu = d_hidden * up
    return (silu * up).astype(BF16), (d_silu * sig + d_silu * silu * (1.0 - sig)).astype(BF16), (d_hidden * silu).astype(BF16)


class Copies:
    def __init__(self, sems):
        self.sems, self.used = sems, 0

    def start(self, src, dst):
        copy = pltpu.make_async_copy(src, dst, self.sems.at[self.used])
        self.used += 1
        copy.start()
        return copy


def gather_loop(gather, unit, then=None):
    chips = gather.place.ring

    def body(event):
        @pl.when(event < gather.events)
        def _():
            gather.event(event)
            if then is not None:
                then(event)
        step = lax.div(event, NP) + 1
        opposite = event == gather.events
        final = event == gather.events - 1
        own = event == 1
        near = (event >= NP) & (event < gather.events) & (lax.rem(event, 2) == 0)

        @pl.when(opposite)
        def _():
            gather.mate_wait_last()

        @pl.when(own | near | final)
        def _():
            gather.mate_wait_chip(step - 1, final | (lax.rem(event, NP) != 0))

        @pl.when(own | near | final | opposite)
        def _():
            distance = lax.select(opposite, gather.place.half, step - 1)
            rightward = final | (lax.rem(event, NP) != 0)
            count = lax.select(own, 0, lax.select(opposite, chips - 1, lax.select(final, chips - 2, not_below_zero(lax.div(event, 2) - 1))))
            unit(count, gather.place.near(lax.select(rightward, distance, -distance)))
    loop(gather.events + 1, body)


def weight_grads_u(block, u_ref, dx_ref, stage_ref, outs, sems, head_cols, ff):
    rows = stage_ref.shape[1]
    slot = lax.rem(block, 2)
    here = pl.ds(aligned(block * rows, rows), rows)

    def copies():
        bounds = (0, head_cols, head_cols + ff, head_cols + 2 * ff)
        return [pltpu.make_async_copy(stage_ref.at[slot, :, bounds[i]:bounds[i + 1]], outs[i].at[here], sems.at[slot, i]) for i in range(3)]

    @pl.when(block >= 2)
    def _():
        for copy in copies():
            copy.wait()
    stage_ref[slot] = dot_tn(u_ref[:, here], dx_ref[...]).astype(BF16)
    for copy in copies():
        copy.start()


def weight_grads_u_wait(stage_ref, outs, sems, head_cols, ff):
    rows = stage_ref.shape[1]
    bounds = (0, head_cols, head_cols + ff, head_cols + 2 * ff)
    for slot in range(2):
        for i in range(3):
            pltpu.make_async_copy(stage_ref.at[slot, :, bounds[i]:bounds[i + 1]], outs[i].at[pl.ds(0, rows)], sems.at[slot, i]).wait()


def weight_grads_h(piece, ho_ref, read_dy, stage_ref):
    stage_ref[piece] = dot_tn(ho_ref[...], read_dy(piece)).astype(BF16)


def h_copies(piece, stage_ref, outs, sems, ff):
    cols = stage_ref.shape[2]
    there = pl.ds(aligned(piece * cols, cols), cols)
    return [pltpu.make_async_copy(stage_ref.at[piece, :HEAD_DIM], outs[0].at[:, there], sems.at[piece, 0]),
            pltpu.make_async_copy(stage_ref.at[piece, HEAD_DIM:HEAD_DIM + ff], outs[1].at[:, there], sems.at[piece, 1])]


def kernel_main(tp_size, gain_ref, freq_ref, x_hbm, gy_hbm, wqkv_hbm, wout_hbm, wgate_hbm, wup_hbm, wdown_hbm,
                dx_out, gain_out, *refs):
    u_ref, g_ref, wo_ref = refs[0:3]
    lasts = refs[3:8]
    u0_hbm, q_hbm, k_hbm, v_hbm, o_hbm, ab_hbm = refs[8:14]
    (x_ref, wc_ref, q_ref, k_ref, v_ref, ho_ref, dx_ref, dk_ref, dv_ref, table_ref, x1_ref, gs_ref,
     pair_ref, all_ref, local, sems_gs, sems_hs, sem_ps, sem_pr, sem_as, sem_ar, free_sem) = refs[14:36]
    sems_u, sems_g, refs_r = refs[36:42], refs[42:48], refs[48:]
    place = Place(tp_size)
    peers = place.arrive()
    shard, width = x_ref.shape
    pair = 2 * shard
    chips = place.ring
    head_cols = wqkv_hbm.shape[2]
    ff = wgate_hbm.shape[2]
    piece_cols = width // NP
    gate_cols = slice(head_cols, head_cols + ff)
    up_cols = slice(head_cols + ff, head_cols + 2 * ff)
    hidden_cols = slice(HEAD_DIM, HEAD_DIM + ff)
    loads = Copies(local)
    gu = Gather(place, u_ref, shard, sems_u)
    gg = Gather(place, g_ref, shard, sems_g)

    def wait_all(copies):
        for copy in copies:
            copy.wait()

    def load_wc(layer):
        return [loads.start(wqkv_hbm.at[layer], wc_ref.at[:, :head_cols]),
                loads.start(wgate_hbm.at[layer], wc_ref.at[:, gate_cols]),
                loads.start(wup_hbm.at[layer], wc_ref.at[:, up_cols])]

    def load_wo(layer):
        copies = []
        for piece in range(NP):
            cols = slice(piece * piece_cols, (piece + 1) * piece_cols)
            copies.append(loads.start(wout_hbm.at[layer, :, cols], wo_ref.at[piece, :HEAD_DIM]))
            copies.append(loads.start(wdown_hbm.at[layer, :, cols], wo_ref.at[piece, hidden_cols]))
        return copies

    def rows_of(chip):
        return pl.ds(aligned(chip * pair, pair), pair)

    def write_o(here, value):
        ho_ref[here, :HEAD_DIM] = value

    def read_da(here):
        return dx_ref[here, :HEAD_DIM]

    def heads(here, rows_u):
        qkv = dot_nn(rows_u, wc_ref[:, :head_cols]).astype(BF16)
        table = table_ref[here]
        q_ref[here] = rope(qkv[:, :HEAD_DIM].astype(F32), table).astype(BF16)
        k_ref[here] = rope(qkv[:, HEAD_DIM:2 * HEAD_DIM].astype(F32), table).astype(BF16)
        v_ref[here] = qkv[:, 2 * HEAD_DIM:3 * HEAD_DIM]

    @scoped('f_unit')
    def forward_unit(count, chip, with_hidden):
        here = rows_of(chip)
        rows_u = u_ref[here]
        heads(here, rows_u)
        gate = dot_nn(rows_u, wc_ref[:, gate_cols]).astype(BF16)
        up = dot_nn(rows_u, wc_ref[:, up_cols]).astype(BF16)
        dx_ref[here, gate_cols] = gate
        dx_ref[here, up_cols] = up
        if with_hidden:
            gate_f, up_f = gate.astype(F32), up.astype(F32)
            ho_ref[here, hidden_cols] = (gate_f * jax.nn.sigmoid(gate_f) * up_f).astype(BF16)

    @scoped('b_unit')
    def backward_unit(count, chip):
        here = rows_of(chip)
        dah = dot_nt(g_ref[here, :piece_cols], wo_ref[0])
        for piece in range(1, NP):
            dah = dah + dot_nt(g_ref[here, piece * piece_cols:(piece + 1) * piece_cols], wo_ref[piece])
        dx_ref[here, :HEAD_DIM] = dah[:, :HEAD_DIM].astype(BF16)
        d_hidden = dah[:, hidden_cols].astype(BF16).astype(F32)
        hidden, d_gate, d_up = gated_pull(dx_ref[here, gate_cols].astype(F32), dx_ref[here, up_cols].astype(F32), d_hidden)
        ho_ref[here, hidden_cols] = hidden
        dx_ref[here, gate_cols] = d_gate
        dx_ref[here, up_cols] = d_up

    def part_forward(chip, piece):
        return dot_nn(ho_ref[rows_of(chip)], wo_ref[piece])

    def part_backward(chip, piece):
        return dot_nt(dx_ref[rows_of(chip)], wc_ref[pl.ds(aligned(piece * piece_cols, piece_cols), piece_cols)])

    def keys_values(chip):
        store_keys_values(rows_of(chip), dx_ref, dk_ref, dv_ref, table_ref)

    def other_keys_values():
        def body(step):
            keys_values(place.near(place.half + step - chips))
        loop_from(1, chips, body)

    def read_dy(piece):
        return g_ref[:, pl.ds(aligned(piece * piece_cols, piece_cols), piece_cols)]

    @scoped('finals')
    def finals(reduce):
        return jnp.concatenate([reduce.final(piece) for piece in range(NP)], axis=1)

    grad_cols = slice(head_cols + 2 * ff)
    last_u, last_h = (lasts[0], lasts[2], lasts[3]), (lasts[1], lasts[4])

    def grads_last(event):
        @pl.when(event < NP)
        def _():
            weight_grads_h(event, ho_ref, read_dy, wo_ref)
            for copy in h_copies(event, wo_ref, last_h, sems_hs, ff):
                copy.start()

        @pl.when((event >= NP) & (event < NP + chips))
        def _():
            weight_grads_u(not_below_zero(event - NP), u_ref, dx_ref, gs_ref, last_u, sems_gs, head_cols, ff)

    def grads_last_wait():
        for piece in range(NP):
            wait_all(h_copies(piece, wo_ref, last_h, sems_hs, ff))
        weight_grads_u_wait(gs_ref, last_u, sems_gs, head_cols, ff)

    def grads_first(event):
        @pl.when(event < NP)
        def _():
            weight_grads_h(event, ho_ref, read_dy, wo_ref)

        @pl.when((event >= NP) & (event < NP + chips))
        def _():
            rows = width // chips
            here = pl.ds(aligned(not_below_zero(event - NP) * rows, rows), rows)
            g_ref[here, grad_cols] = dot_tn(u_ref[:, here], dx_ref[...]).astype(BF16)

    lanes = all_ref.shape[3]
    tiles = width // lanes

    def cross(layer):
        return pltpu.make_async_remote_copy(pair_ref.at[layer, 0], pair_ref.at[layer, 1], sem_ps.at[layer], sem_pr.at[layer], place.mate, MESH)

    def spread(layer, step):
        here = all_ref.at[layer, place.chip]
        return pltpu.make_async_remote_copy(here, here, sem_as.at[layer, step - 1], sem_ar.at[layer, step - 1],
                                            place.peer(step), MESH)

    def start_gain(layer, row):
        for tile in range(tiles):
            pair_ref[layer, 0, tile:tile + 1] = row[:, tile * lanes:(tile + 1) * lanes]
        cross(layer).start()

    @scoped('spread_gain')
    def spread_gain(layer):
        cross(layer).wait()
        all_ref[layer, place.chip] = pair_ref[layer, 0] + pair_ref[layer, 1]
        for step in range(1, chips):
            spread(layer, step).start()

    @scoped('end_gain')
    def end_gain(layer):
        for step in range(1, chips):
            spread(layer, step).wait()
        total = all_ref[layer, 0]
        for chip in range(1, chips):
            total = total + all_ref[layer, chip]
        for tile in range(tiles):
            gain_out[layer:layer + 1, tile * lanes:(tile + 1) * lanes] = total[tile:tile + 1]

    load_x = loads.start(x_hbm, x_ref)
    load_g = loads.start(gy_hbm, g_ref.at[gg.own_rows()])
    load_w = load_wc(0)
    load_o = load_wo(0)
    load_x.wait()
    u_ref[gu.own_rows()] = norm_forward(x_ref[...].astype(F32), gain_ref[0:1])
    pl.semaphore_wait(pltpu.get_barrier_semaphore(), peers)
    gu.start()
    saves = [loads.start(u_ref.at[gu.own_rows()], u0_hbm)]
    fill_table(freq_ref[0:1], table_ref)
    load_g.wait()
    wait_all(load_w)

    def start_gy(event):
        @pl.when(event == gu.events - NP)
        def _():
            gg.start()
    gather_loop(gu, lambda count, chip: forward_unit(count, chip, True), start_gy)

    load_w = load_wc(1)
    saves += [loads.start(q_ref, q_hbm), loads.start(k_ref, k_hbm), loads.start(v_ref, v_hbm),
              loads.start(dx_ref.at[:, head_cols:head_cols + 2 * ff], ab_hbm)]

    def attend_first(chip):
        attention_block(chip * pair, pair, chips * pair, chips * pair, (q_ref, k_ref, v_ref, table_ref, None, write_o, None, None, None), True, False)
    attend_first(place.near(place.half))
    wait_all(load_o)
    reduce = Reduce(place, part_forward, shard, refs_r)

    def filler_forward(event):
        @pl.when(event < place.half)
        def _():
            distance = not_below_zero(place.half - 1 - event)

            def body(way):
                attend_first(place.near((1 - 2 * way) * distance))
            loop(lax.select(distance == 0, 1, 2), body)

        @pl.when(event == place.half)
        def _():
            gu.finish()
            o_copy().start()
    n_o = loads.used
    loads.used += 1

    def o_copy():
        return pltpu.make_async_copy(ho_ref.at[:, :HEAD_DIM], o_hbm, local.at[n_o])
    reduce.run(filler_forward)
    load_o = load_wo(1)
    gg.event(jnp.int32(0), forward=True)
    gg.event(jnp.int32(1), forward=True)
    x_next = (x_ref[...].astype(F32) + finals(reduce)).astype(BF16)
    x1_ref[...] = x_next
    saves[0].wait()
    o_copy().wait()
    u_ref[gu.own_rows()] = norm_forward(x_next.astype(F32), gain_ref[1:2])

    reduce.finish()
    gu.start()
    wait_all(saves[1:])
    wait_all(load_w)
    wait_all(load_o)
    dk_ref[...] = jnp.zeros_like(dk_ref)
    dv_ref[...] = jnp.zeros_like(dv_ref)
    early = 2
    for event in range(early, NP):
        gg.event(jnp.int32(event), forward=False)

    def more_gy(event):
        first = gu.events - NP

        @pl.when((event >= first) & (event < first + NP - early))
        def _():
            gg.forward(not_below_zero(event - first) + early)

        @pl.when(event >= first + NP - early)
        def _():
            gg.event(not_below_zero(event - first) + early, forward=True)

        @pl.when((event > NP) & (event < NP + 6) & (lax.rem(event, 2) == 1))
        def _():
            turn = not_below_zero(lax.div(event - 1, 2) - 2)
            gg.mate_wait_chip(jnp.minimum(turn, 1), turn == 2)
            backward_unit(turn, place.near(lax.select(turn == 2, 1, -turn)))
    gather_loop(gu, lambda count, chip: forward_unit(count, chip, False), more_gy)

    groups = 4

    def attend_last(turn):
        held = early + NP
        distance = lax.div(turn + 1, 2)
        rightward = (turn > 0) & (lax.rem(turn, 2) == 0)
        opposite = turn == chips - 1
        needed = lax.select(turn == 0, held, lax.select(opposite, gg.events, distance * NP))
        begin = lax.select(turn == 0, held, jnp.minimum(jnp.maximum(held + turn - 1, lax.select(turn >= chips - 2, gg.events - NP // 2, 0)), gg.events))
        end = jnp.maximum(jnp.minimum(held + turn, gg.events), needed)
        end = lax.select(turn == chips - 2, jnp.maximum(end, gg.events - 1), end)
        begin = lax.select(turn == chips - 1, gg.events - 1, begin)

        def take(event):
            gg.event(event)
        loop_from(begin, end, take)

        chip = place.near(lax.select(rightward, distance, -distance))

        @pl.when(opposite)
        def _():
            gg.mate_wait_last()

        @pl.when((turn > 2) & jnp.logical_not(opposite))
        def _():
            gg.mate_wait_chip(distance, rightward)

        @pl.when(turn > 2)
        def _():
            backward_unit(turn, chip)
        for group in range(groups):
            @pl.when(lax.div(chip, chips // groups) == group)
            def _(group=group):
                attention_block(chip * pair, pair, (group + 1) * (chips * pair // groups), chips * pair // groups,
                                (q_ref, k_ref, v_ref, table_ref, read_da, write_o, dx_ref, dk_ref, dv_ref), True, True)
    loop(chips, attend_last)
    keys_values(place.near(place.half))
    loads_a = [loads.start(q_hbm, q_ref), loads.start(k_hbm, k_ref), loads.start(v_hbm, v_ref)]
    n_late = loads.used
    loads.used += 2

    def late_loads():
        return [pltpu.make_async_copy(u0_hbm, u_ref.at[gu.own_rows()], local.at[n_late]),
                pltpu.make_async_copy(o_hbm, ho_ref.at[:, :HEAD_DIM], local.at[n_late + 1])]
    near = (place.left, place.right, place.mate)
    reduce = Reduce(place, part_backward, shard, refs_r)

    def filler_last(event):
        @pl.when(event == 0)
        def _():
            other_keys_values()
        grads_last(event)

        @pl.when(event == 1)
        def _():
            gg.finish()
            gu.finish()

        @pl.when(event == NP + chips)
        def _():
            for copy in late_loads():
                copy.start()
            for peer in near:
                pl.semaphore_signal(free_sem, inc=1, device_id=peer, device_id_type=MESH)
    reduce.run(filler_last)
    pl.semaphore_wait(free_sem, len(near))
    wait_all(late_loads())
    gu.start()
    d_normed = finals(reduce).astype(BF16).astype(F32)
    inv, unit = norm_unit(x1_ref[...].astype(F32))
    g_ref[gg.own_rows()] = (g_ref[gg.own_rows()].astype(F32) + norm_backward(inv, unit, gain_ref[1:2], d_normed)).astype(BF16)
    start_gain(1, jnp.sum(d_normed * unit, axis=0, keepdims=True))

    reduce.finish()
    gg.start()
    spread_gain(1)
    grads_last_wait()
    load_o = load_wo(0) + [loads.start(ab_hbm, dx_ref.at[:, head_cols:head_cols + 2 * ff])]
    load_w = load_wc(0)
    dk_ref[...] = jnp.zeros_like(dk_ref)
    dv_ref[...] = jnp.zeros_like(dv_ref)
    wait_all(load_o)

    def more_u(event):
        @pl.when(event >= gg.events - NP)
        def _():
            gu.event(not_below_zero(event - (gg.events - NP)), forward=True)
    gather_loop(gg, backward_unit, more_u)
    wait_all(loads_a)

    back_groups = 2

    def attend_back(block):
        @pl.when((block >= 1) & (block <= gu.events - 2 * NP))
        def _():
            gu.event(block + NP - 1, forward=True)
        for group in range(back_groups):
            @pl.when(lax.div(block, chips // back_groups) == group)
            def _(group=group):
                attention_block(block * pair, pair, (group + 1) * (chips * pair // back_groups), chips * pair // back_groups,
                                (q_ref, k_ref, v_ref, table_ref, read_da, None, dx_ref, dk_ref, dv_ref), False, True)
    loop(chips, attend_back)
    keys_values(place.near(place.half))
    wait_all(load_w)
    reduce = Reduce(place, part_backward, shard, refs_r)

    def filler_first(event):
        @pl.when(event == 0)
        def _():
            other_keys_values()

        @pl.when(event < NP)
        def _():
            gu.event(gu.events - NP + event, forward=False)

        @pl.when(event == NP - 1)
        def _():
            gu.mate_wait_all()
        grads_first(event)

        @pl.when(event == 1)
        def _():
            gg.finish()

        @pl.when(event == NP + 1)
        def _():
            gu.finish()

        @pl.when(event == NP + chips)
        def _():
            for copy in reloads():
                copy.start()
    n_reload = loads.used
    loads.used += len(fold_plan(width, head_cols, ff))

    def reloads():
        plan = fold_plan(width, head_cols, ff)
        return [pltpu.make_async_copy(lasts[number].at[theirs], u_ref.at[ours], local.at[n_reload + slot])
                for slot, (number, theirs, ours) in enumerate(plan)]
    x1_ref[...] = g_ref[gg.own_rows()]
    reduce.run(filler_first)
    inv, unit = norm_unit(x_ref[...].astype(F32))
    d_normed = finals(reduce).astype(BF16).astype(F32)
    start_gain(0, jnp.sum(d_normed * unit, axis=0, keepdims=True))
    dx_out[...] = (x1_ref[...].astype(F32) + norm_backward(inv, unit, gain_ref[0:1], d_normed)).astype(BF16)
    spread_gain(0)
    end_gain(1)
    reduce.finish()
    wait_all(reloads())
    end_gain(0)


def fold_plan(width, head_cols, ff):
    cols = head_cols + 2 * ff
    piece = width // NP
    rows = HEAD_DIM + ff
    every = slice(None)
    plan = [(0, (every, every), (every, slice(head_cols))), (2, (every, every), (every, slice(head_cols, head_cols + ff))),
            (3, (every, every), (every, slice(head_cols + ff, cols)))]
    whole = width // rows
    for turn in range(NP):
        theirs = slice(turn * piece, (turn + 1) * piece)
        if turn < whole:
            ours = slice(cols, cols + piece)
            plan += [(1, (every, theirs), (slice(turn * rows, turn * rows + HEAD_DIM), ours)),
                     (4, (every, theirs), (slice(turn * rows + HEAD_DIM, (turn + 1) * rows), ours))]
        else:
            plan += [(1, (every, theirs), (slice(whole * rows, whole * rows + HEAD_DIM), slice(cols, cols + piece)))]
            strip = width - cols - piece
            for step in range(piece // strip):
                plan += [(4, (every, slice(turn * piece + step * strip, turn * piece + (step + 1) * strip)),
                          (slice(step * ff, (step + 1) * ff), slice(cols + piece, width)))]
    return plan


def kernel_stack(head_cols, ff, last_ref, first_ref, first_h_ref, dx_ref, gain_ref, *refs):
    outs, (dx_out, gain_out, sems) = refs[0:5], refs[5:8]
    width = last_ref.shape[0]
    copies = Copies(sems)
    pending = [copies.start(dx_ref, dx_out), copies.start(gain_ref, gain_out)]
    for number, theirs, ours in fold_plan(width, head_cols, ff):
        pending.append(copies.start(last_ref.at[ours], outs[number].at[(1,) + theirs]))
    bounds = (0, head_cols, head_cols + ff, head_cols + 2 * ff)
    for i, number in enumerate((0, 2, 3)):
        pending.append(copies.start(first_ref.at[:, bounds[i]:bounds[i + 1]], outs[number].at[0]))
    piece = first_h_ref.shape[2]
    for turn in range(NP):
        there = slice(turn * piece, (turn + 1) * piece)
        pending.append(copies.start(first_h_ref.at[turn, :HEAD_DIM], outs[1].at[0, :, there]))
        pending.append(copies.start(first_h_ref.at[turn, HEAD_DIM:HEAD_DIM + ff], outs[4].at[0, :, there]))
    for copy in pending:
        copy.wait()


def solution(mesh):
    tp_size = mesh.shape['tp']
    half = tp_size // 4
    row_spec = P(('dp', 'tp'), None)
    col_spec = P(None, None, 'tp')
    inner_spec = P(None, 'tp', None)

    def device_program(x_loc, dy_loc, norm_gain, w_qkv, w_out, w_gate, w_up, w_down):
        shard, width = x_loc.shape
        seq = shard * tp_size
        pair = 2 * shard
        chips = tp_size // 2
        head_cols = w_qkv.shape[2]
        ff = w_gate.shape[2]
        cols = head_cols + 2 * ff
        piece_cols = width // NP
        vmem, anyspace = pl.BlockSpec(memory_space=pltpu.VMEM), pl.BlockSpec(memory_space=pl.ANY)
        shape = jax.ShapeDtypeStruct
        dma = pltpu.SemaphoreType.DMA

        freqs = np.float32(ROPE_BASE) ** (np.float32(-2.0) * np.arange(HEAD_DIM // 2, dtype=np.float32) / np.float32(HEAD_DIM))
        freqs = jnp.asarray(np.tile(freqs, (8, 2)))

        rows_shape = shape((shard, width), BF16)
        gain_shape = shape((2, width), F32)
        head_shape = shape((seq, HEAD_DIM), BF16)
        grads = (shape((width, head_cols), BF16), shape((HEAD_DIM, width), BF16), shape((width, ff), BF16),
                 shape((width, ff), BF16), shape((ff, width), BF16))
        square, folded = pltpu.VMEM((width, width), BF16), pltpu.VMEM((NP, HEAD_DIM + ff, piece_cols), BF16)
        hbm = pl.BlockSpec(memory_space=pltpu.HBM)
        whole_vmem = 67043328
        kept = (seq * width + width * width + NP * (HEAD_DIM + ff) * piece_cols + shard * width) * 2 + 2 ** 18
        results = pl.pallas_call(
            functools.partial(kernel_main, tp_size),
            out_shape=(pltpu.VMEM(rows_shape.shape, BF16), pltpu.VMEM(gain_shape.shape, F32), square, square, folded) + grads + (rows_shape,) + (head_shape,) * 4 + (shape((seq, 2 * ff), BF16),),
            in_specs=[vmem] * 2 + [hbm] * 7,
            out_specs=(vmem,) * 5 + (hbm,) * 11,
            scratch_shapes=[
                pltpu.VMEM((shard, width), BF16), pltpu.VMEM((width, cols), BF16),
                pltpu.VMEM((seq, HEAD_DIM), BF16), pltpu.VMEM((seq, HEAD_DIM), BF16), pltpu.VMEM((seq, HEAD_DIM), BF16),
                pltpu.VMEM((seq, HEAD_DIM + ff), BF16), pltpu.VMEM((seq, cols), BF16),
                pltpu.VMEM((seq, HEAD_DIM), F32), pltpu.VMEM((seq, HEAD_DIM), F32), pltpu.VMEM((seq, HEAD_DIM), F32),
                pltpu.VMEM((shard, width), BF16), pltpu.VMEM((2, width // chips, cols), BF16),
                pltpu.VMEM((2, 2, width // 128, 128), F32), pltpu.VMEM((2, chips, width // 128, 128), F32),
                dma((80,)), dma((2, 3)), dma((NP, 2)), dma((2,)), dma((2,)), dma((2, chips - 1)), dma((2, chips - 1)),
                pltpu.SemaphoreType.REGULAR] + Gather.scratch(half) + Gather.scratch(half) + Reduce.scratch(half, shard, piece_cols),
            compiler_params=pltpu.CompilerParams(collective_id=1, has_side_effects=True, vmem_limit_bytes=whole_vmem - kept), name='blocks',
        )(norm_gain, freqs, x_loc, dy_loc, w_qkv, w_out, w_gate, w_up, w_down)

        stacked = pl.pallas_call(
            functools.partial(kernel_stack, head_cols, ff),
            out_shape=tuple(shape((2,) + grad.shape, BF16) for grad in grads) + (rows_shape, gain_shape),
            in_specs=[vmem] * 5,
            out_specs=(hbm,) * 7,
            scratch_shapes=[dma((48,))],
            compiler_params=pltpu.CompilerParams(vmem_limit_bytes=8 * 2 ** 20), name='stack',
        )(*results[2:5], *results[0:2])
        return tuple(stacked[5:7]) + tuple(stacked[0:5])

    return jax.shard_map(device_program, mesh=mesh, in_specs=(row_spec, row_spec, P(None, None), col_spec, inner_spec, col_spec, col_spec, inner_spec), out_specs=(row_spec, P('dp', None), P('dp', None, 'tp'), P('dp', 'tp', None), P('dp', None, 'tp'), P('dp', None, 'tp'), P('dp', 'tp', None)), check_vma=False)
```

```python
import functools

import jax
import jax.numpy as jnp
import numpy as np
from jax import lax
from jax.experimental import pallas as pl
from jax.experimental.pallas import tpu as pltpu
from jax.sharding import PartitionSpec as P

HEAD_DIM = 128
NORM_EPS = 1e-5
ROPE_BASE = 10000.0
MESH = pl.DeviceIdType.MESH
NP = 4
F32 = jnp.float32
BF16 = jnp.bfloat16


def dot_nn(a, b):
    return lax.dot_general(a, b, (((1,), (0,)), ((), ())), preferred_element_type=F32)


def dot_nt(a, b):
    return lax.dot_general(a, b, (((1,), (1,)), ((), ())), preferred_element_type=F32)


def dot_tn(a, b):
    return lax.dot_general(a, b, (((0,), (0,)), ((), ())), preferred_element_type=F32)


def not_below_zero(index):
    return jnp.maximum(index, 0)


def row_mean(values):
    return jnp.mean(values, axis=-1, keepdims=True)


def row_sum(values):
    return jnp.sum(values, axis=-1, keepdims=True)


def loop_from(first, last, body):
    def step(index, carry):
        body(index)
        return carry
    lax.fori_loop(first, last, step, 0)


def loop(count, body):
    loop_from(0, count, body)


def aligned(index, size):
    return pl.multiple_of(index, size)


def scoped(name):
    def wrap(function):
        @functools.wraps(function)
        def inner(*args, **kwargs):
            with jax.named_scope(name):
                return function(*args, **kwargs)
        return inner
    return wrap


class Place:
    def __init__(self, tp_size):
        index = lax.axis_index('tp')
        self.ring = tp_size // 2
        self.half = self.ring // 2
        self.core = lax.rem(index, 2)
        self.chip = lax.div(index, 2)
        self.right = self.peer(1)
        self.left = self.peer(-1)
        self.mate = {'tp': self.chip * 2 + 1 - self.core}

    def peer(self, step):
        return {'tp': self.near(step) * 2 + self.core}

    def near(self, step):
        return lax.rem(self.chip + step + self.ring, self.ring)

    def arrive(self):
        peers = [self.right, self.left, self.mate]
        for peer in peers:
            pl.semaphore_signal(pltpu.get_barrier_semaphore(), inc=1, device_id=peer, device_id_type=MESH)
        return len(peers)


class Gather:
    def __init__(self, place, buf, shard_rows, sems):
        self.place, self.buf, self.shard = place, buf, shard_rows
        self.rows = shard_rows // NP
        self.events = (place.half - 1) * NP + NP // 2
        self.send_r, self.recv_r, self.send_l, self.recv_l, self.send_m, self.recv_m = sems

    @staticmethod
    def scratch(half):
        events = (half - 1) * NP + NP // 2
        return [pltpu.SemaphoreType.DMA((n,)) for n in (events, events, events, events, 2 * events + NP, 2 * events + NP)]

    def view(self, chip, core, piece):
        start = (chip * 2 + core) * self.shard + piece * self.rows
        return self.buf.at[pl.ds(aligned(start, self.rows), self.rows)]

    def own_rows(self):
        start = (self.place.chip * 2 + self.place.core) * self.shard
        return pl.ds(aligned(start, self.shard), self.shard)

    def to_right(self, event, view):
        return pltpu.make_async_remote_copy(view, view, self.send_r.at[event], self.recv_r.at[event], self.place.right, MESH)

    def to_left(self, event, view):
        return pltpu.make_async_remote_copy(view, view, self.send_l.at[event], self.recv_l.at[event], self.place.left, MESH)

    def to_mate(self, slot, view):
        return pltpu.make_async_remote_copy(view, view, self.send_m.at[slot], self.recv_m.at[slot], self.place.mate, MESH)

    def start(self):
        place = self.place
        for piece in range(NP):
            self.to_right(piece, self.view(place.chip, place.core, piece)).start()
            self.to_left(piece, self.view(place.chip, place.core, NP - 1 - piece)).start()
        for piece in range(NP):
            self.to_mate(2 * self.events + piece, self.view(place.chip, place.core, piece)).start()

    def views(self, event):
        step = lax.div(event, NP) + 1
        piece = lax.rem(event, NP)
        from_left = self.view(self.place.near(-step), self.place.core, piece)
        from_right = self.view(self.place.near(step), self.place.core, NP - 1 - piece)
        return from_left, from_right

    @scoped('g_event')
    def event(self, event, forward=None):
        from_left, from_right = self.views(event)
        self.to_right(event, from_left).wait_recv()
        self.pass_on(event, forward, lambda: self.to_right(event + NP, from_left).start())
        self.to_mate(event, from_left).start()
        self.to_left(event, from_right).wait_recv()
        self.pass_on(event, forward, lambda: self.to_left(event + NP, from_right).start())
        self.to_mate(self.events + event, from_right).start()

    def forward(self, event):
        from_left, from_right = self.views(event)
        self.to_right(event + NP, from_left).start()
        self.to_left(event + NP, from_right).start()

    def side_view(self, side, which, piece):
        return side.at[which, pl.ds(aligned(piece * self.rows, self.rows), self.rows)]

    def start_side(self, side):
        for piece in range(NP):
            last = NP - 1 - piece
            pltpu.make_async_remote_copy(self.side_view(side, 0, piece), self.side_view(side, 1, piece),
                                         self.send_r.at[piece], self.recv_r.at[piece], self.place.right, MESH).start()
            pltpu.make_async_remote_copy(self.side_view(side, 0, last), self.side_view(side, 2, last),
                                         self.send_l.at[piece], self.recv_l.at[piece], self.place.left, MESH).start()

    def side_copy(self, source, view, send, recv, to):
        return pltpu.make_async_remote_copy(source, view, send, recv, to, MESH)

    def adopt_side(self, side):
        place = self.place

        def body(piece):
            last = NP - 1 - piece
            from_left, from_right = self.side_view(side, 1, piece), self.side_view(side, 2, last)
            self.side_copy(from_left, from_left, self.send_r.at[piece], self.recv_r.at[piece], place.right).wait_recv()
            self.side_copy(from_right, from_right, self.send_l.at[piece], self.recv_l.at[piece], place.left).wait_recv()
            to_left, to_right = self.views(piece)
            for source, view, slot in ((self.side_view(side, 0, piece), self.view(place.chip, place.core, piece), 2 * self.events + piece),
                                       (from_left, to_left, piece), (from_right, to_right, self.events + piece)):
                self.side_copy(source, view, self.send_m.at[slot], self.recv_m.at[slot], place.mate).start()
        loop(NP, body)
        for which, step in ((0, 0), (1, -1), (2, 1)):
            start = (place.near(step) * 2 + place.core) * self.shard
            self.buf[pl.ds(aligned(start, self.shard), self.shard)] = side[which]

    def forward_side(self, side, event):
        from_left, from_right = self.views(event)
        later = event + NP
        self.side_copy(self.side_view(side, 1, event), from_left, self.send_r.at[later], self.recv_r.at[later], self.place.right).start()
        self.side_copy(self.side_view(side, 2, NP - 1 - event), from_right, self.send_l.at[later], self.recv_l.at[later], self.place.left).start()

    def pass_on(self, event, forward, send):
        if forward is None:
            pl.when(event + NP < self.events)(send)
        elif forward:
            send()

    def mate_wait(self, first, count):
        for offset in range(count):
            self.to_mate(first + offset, self.view(self.place.chip, 1 - self.place.core, 0)).wait_recv()

    def mate_wait_all(self):
        def body(slot):
            self.mate_wait(slot, 1)
        loop(2 * self.events + NP, body)

    @scoped('g_matelast')
    def mate_wait_last(self):
        first = (self.place.half - 1) * NP
        self.mate_wait(first, NP // 2)
        self.mate_wait(self.events + first, NP // 2)

    @scoped('g_matewait')
    def mate_wait_chip(self, distance, rightward):
        ring_first = lax.select(rightward, self.events, 0) + not_below_zero(distance - 1) * NP
        self.mate_wait(lax.select(distance == 0, 2 * self.events, ring_first), NP)

    @scoped('g_finish')
    def finish(self):
        view = self.view(self.place.chip, self.place.core, 0)

        def ring(event):
            self.to_right(event, view).wait_send()
            self.to_left(event, view).wait_send()
        loop(self.events, ring)

        def across(slot):
            self.to_mate(slot, view).wait_send()
        loop(2 * self.events + NP, across)


class Reduce:
    SLOTS = 4
    DEPTH = 8

    def __init__(self, place, part, shard_rows, refs):
        self.place, self.part, self.shard = place, part, shard_rows
        self.events = (place.half - 1) * NP + NP // 2
        self.ring, self.acc, self.stage, self.send_n, self.recv_n, self.send_m, self.recv_m = refs

    @staticmethod
    def scratch(half, shard_rows, width):
        events = (half - 1) * NP + NP // 2
        shapes = [(2, events), (2 * Reduce.DEPTH + NP,), (Reduce.SLOTS, 2)]
        sems = [(2, events), (2, events), (2 * events + NP,), (2 * events + NP,)]
        return [pltpu.VMEM(s + (shard_rows, width), F32) for s in shapes] + [pltpu.SemaphoreType.DMA(s) for s in sems]

    def acc_slot(self, term):
        own = 2 * self.DEPTH + not_below_zero(term - 2 * self.events)
        return lax.select(term < 2 * self.events, lax.rem(term, 2 * self.DEPTH), own)

    def mate_copy(self, term):
        return pltpu.make_async_remote_copy(
            self.stage.at[lax.rem(term, self.SLOTS), 1 - self.place.core], self.acc.at[self.acc_slot(term)], self.send_m.at[term], self.recv_m.at[term],
            self.place.mate, MESH)

    def ring_copy(self, event, way):
        to = self.place.peer(1 - 2 * way)
        return pltpu.make_async_remote_copy(
            self.acc.at[self.acc_slot(2 * event + way)], self.ring.at[way, event], self.send_n.at[way, event], self.recv_n.at[way, event], to, MESH)

    @scoped('r_fill')
    def fill(self, term):
        @pl.when(term >= self.SLOTS)
        def _():
            self.mate_copy(not_below_zero(term - self.SLOTS)).wait_send()
        slot = lax.rem(term, self.SLOTS)
        way = lax.rem(term, 2)

        @pl.when(term >= 2 * (self.DEPTH - 1))
        def _():
            self.ring_copy(jnp.maximum(lax.div(term, 2) - (self.DEPTH - 1), 0), way).wait_send()
        shifted = lax.div(term, 2) + NP // 2
        travels = term < 2 * self.events
        distance = not_below_zero(self.place.half - lax.div(shifted, NP))
        turn = lax.rem(shifted, NP)
        piece = lax.select(travels, lax.select(way == 0, turn, NP - 1 - turn), lax.rem(not_below_zero(term - 2 * self.events), NP))
        value = self.part(self.place.near((1 - 2 * way) * distance), piece)
        self.stage[slot, 0] = value[:self.shard]
        self.stage[slot, 1] = value[self.shard:]
        self.mate_copy(term).start()

    @scoped('r_event')
    def event(self, event):
        def add(way):
            term = 2 * event + way
            self.mate_copy(term).wait_recv()
            slot = self.acc_slot(term)
            self.acc[slot] += self.stage[lax.rem(term, self.SLOTS), self.place.core]

            @pl.when(event >= NP)
            def _():
                before = not_below_zero(event - NP)
                self.ring_copy(before, way).wait_recv()
                self.acc[slot] += self.ring[way, before]
            self.ring_copy(event, way).start()
        loop(2, add)

    def final(self, piece):
        last = self.events - NP
        term = 2 * self.events + piece
        self.mate_copy(term).wait_recv()
        self.ring_copy(last + piece, 0).wait_recv()
        self.ring_copy(last + NP - 1 - piece, 1).wait_recv()
        return ((self.stage[term % self.SLOTS, self.place.core] + self.acc[2 * self.DEPTH + piece])
                + (self.ring[0, last + piece] + self.ring[1, last + NP - 1 - piece]))

    @scoped('r_finish')
    def finish(self):
        def across(term):
            self.mate_copy(term).wait_send()
        terms = 2 * self.events + NP
        loop_from(terms - self.SLOTS, terms, across)

        def ring(event):
            self.ring_copy(event, 0).wait_send()
            self.ring_copy(event, 1).wait_send()
        loop_from(self.events + 2 - (self.DEPTH - 1), self.events, ring)

    def run(self, filler):
        def body(turn):
            event = not_below_zero(turn - 1)
            travels = (turn >= 1) & (turn <= self.events)

            @pl.when(travels)
            def _():
                self.event(event)

            def ahead(way):
                self.fill(2 * turn + way)
            loop(2, ahead)

            @pl.when(travels)
            def _():
                filler(event)
        loop(self.events + 2, body)


def rope_pair(table):
    lanes = lax.broadcasted_iota(jnp.int32, table.shape, 1)
    swapped = pltpu.roll(table, HEAD_DIM // 2, 1)
    low = lanes < HEAD_DIM // 2
    return jnp.where(low, table, swapped), jnp.where(low, -swapped, table)


@scoped('table')
def fill_table(freqs, table_ref):
    rows = 64
    blocks = table_ref.shape[0] // rows

    def cos_sin(count, scale):
        steps = lax.broadcasted_iota(jnp.int32, (count, HEAD_DIM), 0) * scale
        angles = steps.astype(F32) * freqs
        return jnp.cos(angles), jnp.sin(angles)
    cos_low, sin_low = cos_sin(rows, 1)
    cos_high, sin_high = cos_sin(max(blocks, 8), rows)
    low = lax.broadcasted_iota(jnp.int32, (1, HEAD_DIM), 1) < HEAD_DIM // 2
    first = jnp.where(low, cos_high, sin_high)
    second = jnp.where(low, -sin_high, cos_high)
    for block in range(blocks):
        table_ref[block * rows:(block + 1) * rows] = first[block:block + 1] * cos_low + second[block:block + 1] * sin_low


def rope(values, table, inverse=False):
    cos2, sin2 = rope_pair(table)
    turned = pltpu.roll(values, HEAD_DIM // 2, 1)
    if inverse:
        return values * cos2 - turned * sin2
    return values * cos2 + turned * sin2


def norm_forward(x_f32, gain_row):
    inv = lax.rsqrt(row_mean(x_f32 * x_f32) + NORM_EPS)
    return (x_f32 * inv * gain_row).astype(BF16)


def norm_unit(x_f32):
    inv = lax.rsqrt(row_mean(x_f32 * x_f32) + NORM_EPS)
    return inv, x_f32 * inv


@scoped('norm_backward')
def norm_backward(inv, unit, gain_row, d_normed):
    d_unit = d_normed * gain_row
    return inv * (d_unit - unit * row_mean(d_unit * unit))


def by_halves(dot, a, b, axis):
    size = a.shape[axis] // 2
    first = a[:size] if axis == 0 else a[:, :size]
    second = a[size:] if axis == 0 else a[:, size:]
    return dot(first, b), dot(second, b)


@scoped('attention')
def attention_block(row0, rows, keys, diagonal, refs, forward, backward):
    q_ref, k_ref, v_ref, table_ref, read_da, write_o, dx_ref, dk_ref, dv_ref = refs
    here = pl.ds(aligned(row0, rows), rows)
    scale = HEAD_DIM ** -0.5
    spans = [(start, end) for start, end in ((0, keys - diagonal), (keys - diagonal, keys)) if end > start]
    query = q_ref[here]
    scores = []
    for start, end in spans:
        part = dot_nt(query, k_ref[start:end])
        if end == keys:
            row_id = row0 - start + lax.broadcasted_iota(jnp.int32, part.shape, 0)
            part = jnp.where(row_id >= lax.broadcasted_iota(jnp.int32, part.shape, 1), part, -1e30)
        scores.append(part)
    tops = [jnp.max(part, axis=-1, keepdims=True) for part in scores]
    top = functools.reduce(jnp.maximum, tops)
    factor = scale * 1.4426950408889634
    expd = [jnp.exp2((part - top) * factor) for part in scores]
    inv_sum = 1.0 / sum(row_sum(part) for part in expd)
    prob = [part * inv_sum for part in expd]
    prob_b = [part.astype(BF16) for part in prob]
    if forward:
        halves = [by_halves(dot_nn, part, v_ref[start:end], 0) for part, (start, end) in zip(prob_b, spans)]
        out = [functools.reduce(jnp.add, [half[i] for half in halves]) for i in range(2)]
        write_o(here, jnp.concatenate(out, axis=0).astype(BF16))
    if backward:
        d_attn = read_da(here)
        d_prob = [dot_nt(d_attn, v_ref[start:end]).astype(BF16).astype(F32) for start, end in spans]
        row_dot = sum(row_sum(p * d) for p, d in zip(prob, d_prob))
        d_scores = [(p * (d - row_dot)).astype(BF16) for p, d in zip(prob, d_prob)]
        halves = [by_halves(dot_nn, part, k_ref[start:end], 0) for part, (start, end) in zip(d_scores, spans)]
        d_query = jnp.concatenate([functools.reduce(jnp.add, [half[i] for half in halves]) for i in range(2)], axis=0)
        d_query = (d_query * scale).astype(BF16).astype(F32)
        dx_ref[here, :HEAD_DIM] = rope(d_query, table_ref[here], inverse=True).astype(BF16)
        for part, prob_part, (start, end) in zip(d_scores, prob_b, spans):
            middle = (start + end) // 2
            for ref, left, right in ((dv_ref, prob_part, d_attn), (dk_ref, part, query)):
                low, high = by_halves(dot_tn, left, right, 1)
                ref[start:middle] += low
                ref[middle:end] += high


@scoped('store_kv')
def store_keys_values(here, dx_ref, dk_ref, dv_ref, table_ref):
    d_key = (dk_ref[here] * HEAD_DIM ** -0.5).astype(BF16).astype(F32)
    dx_ref[here, HEAD_DIM:2 * HEAD_DIM] = rope(d_key, table_ref[here], inverse=True).astype(BF16)
    dx_ref[here, 2 * HEAD_DIM:3 * HEAD_DIM] = dv_ref[here].astype(BF16)


def gated_pull(gate, up, d_hidden):
    sig = jax.nn.sigmoid(gate)
    silu = gate * sig
    d_silu = d_hidden * up
    return (silu * up).astype(BF16), (d_silu * sig + d_silu * silu * (1.0 - sig)).astype(BF16), (d_hidden * silu).astype(BF16)


class Copies:
    def __init__(self, sems):
        self.sems, self.used = sems, 0

    def start(self, src, dst):
        copy = pltpu.make_async_copy(src, dst, self.sems.at[self.used])
        self.used += 1
        copy.start()
        return copy


def gather_loop(gather, unit, then=None):
    chips = gather.place.ring

    def body(event):
        @pl.when(event < gather.events)
        def _():
            gather.event(event)
            if then is not None:
                then(event)
        step = lax.div(event, NP) + 1
        opposite = event == gather.events
        final = event == gather.events - 1
        own = event == 1
        near = (event >= NP) & (event < gather.events) & (lax.rem(event, 2) == 0)

        @pl.when(opposite)
        def _():
            gather.mate_wait_last()

        @pl.when(own | near | final)
        def _():
            gather.mate_wait_chip(step - 1, final | (lax.rem(event, NP) != 0))

        @pl.when(own | near | final | opposite)
        def _():
            distance = lax.select(opposite, gather.place.half, step - 1)
            rightward = final | (lax.rem(event, NP) != 0)
            count = lax.select(own, 0, lax.select(opposite, chips - 1, lax.select(final, chips - 2, not_below_zero(lax.div(event, 2) - 1))))
            unit(count, gather.place.near(lax.select(rightward, distance, -distance)))
    loop(gather.events + 1, body)


def weight_grads_u(block, u_ref, dx_ref, stage_ref, outs, sems, head_cols, ff):
    rows = stage_ref.shape[1]
    slot = lax.rem(block, 2)
    here = pl.ds(aligned(block * rows, rows), rows)

    def copies():
        bounds = (0, head_cols, head_cols + ff, head_cols + 2 * ff)
        return [pltpu.make_async_copy(stage_ref.at[slot, :, bounds[i]:bounds[i + 1]], outs[i].at[here], sems.at[slot, i]) for i in range(3)]

    @pl.when(block >= 2)
    def _():
        for copy in copies():
            copy.wait()
    stage_ref[slot] = dot_tn(u_ref[:, here], dx_ref[...]).astype(BF16)
    for copy in copies():
        copy.start()


def weight_grads_u_wait(stage_ref, outs, sems, head_cols, ff):
    rows = stage_ref.shape[1]
    bounds = (0, head_cols, head_cols + ff, head_cols + 2 * ff)
    for slot in range(2):
        for i in range(3):
            pltpu.make_async_copy(stage_ref.at[slot, :, bounds[i]:bounds[i + 1]], outs[i].at[pl.ds(0, rows)], sems.at[slot, i]).wait()


def weight_grads_h(piece, ho_ref, read_dy, stage_ref):
    cols = stage_ref.shape[1] // NP
    stage_ref[:, pl.ds(aligned(piece * cols, cols), cols)] = dot_tn(ho_ref[...], read_dy(piece)).astype(BF16)


def h_copies(piece, stage_ref, outs, sems, ff):
    cols = stage_ref.shape[1] // NP
    there = pl.ds(aligned(piece * cols, cols), cols)
    return [pltpu.make_async_copy(stage_ref.at[:HEAD_DIM, there], outs[0].at[:, there], sems.at[piece, 0]),
            pltpu.make_async_copy(stage_ref.at[HEAD_DIM:HEAD_DIM + ff, there], outs[1].at[:, there], sems.at[piece, 1])]


def kernel_main(tp_size, gain_ref, freq_ref, x_hbm, gy_hbm, wqkv_hbm, wout_hbm, wgate_hbm, wup_hbm, wdown_hbm,
                dx_out, gain_out, *refs):
    u_ref, g_ref, wo_ref = refs[0:3]
    lasts = refs[3:8]
    u0_hbm, q_hbm, k_hbm, v_hbm, o_hbm, ab_hbm = refs[8:14]
    (x_ref, side_ref, wc_ref, q_ref, k_ref, v_ref, ho_ref, dx_ref, dk_ref, dv_ref, table_ref, x1_ref, gs_ref,
     pair_ref, all_ref, local, sems_gs, sems_hs, sem_ps, sem_pr, sem_as, sem_ar, free_sem) = refs[14:37]
    sems_u, sems_g, refs_r = refs[37:43], refs[43:49], refs[49:]
    place = Place(tp_size)
    peers = place.arrive()
    shard, width = x_ref.shape
    pair = 2 * shard
    chips = place.ring
    head_cols = wqkv_hbm.shape[2]
    ff = wgate_hbm.shape[2]
    piece_cols = width // NP
    gate_cols = slice(head_cols, head_cols + ff)
    up_cols = slice(head_cols + ff, head_cols + 2 * ff)
    hidden_cols = slice(HEAD_DIM, HEAD_DIM + ff)
    loads = Copies(local)
    gu = Gather(place, u_ref, shard, sems_u)
    gg = Gather(place, g_ref, shard, sems_g)

    def wait_all(copies):
        for copy in copies:
            copy.wait()

    def load_wc(layer):
        return [loads.start(wqkv_hbm.at[layer], wc_ref.at[:, :head_cols]),
                loads.start(wgate_hbm.at[layer], wc_ref.at[:, gate_cols]),
                loads.start(wup_hbm.at[layer], wc_ref.at[:, up_cols])]

    def load_wo(layer):
        return [loads.start(wout_hbm.at[layer], wo_ref.at[:HEAD_DIM]), loads.start(wdown_hbm.at[layer], wo_ref.at[hidden_cols])]

    def rows_of(chip):
        return pl.ds(aligned(chip * pair, pair), pair)

    def write_o(here, value):
        ho_ref[here, :HEAD_DIM] = value

    def read_da(here):
        return dx_ref[here, :HEAD_DIM]

    def heads(here, rows_u):
        qkv = dot_nn(rows_u, wc_ref[:, :head_cols]).astype(BF16)
        table = table_ref[here]
        q_ref[here] = rope(qkv[:, :HEAD_DIM].astype(F32), table).astype(BF16)
        k_ref[here] = rope(qkv[:, HEAD_DIM:2 * HEAD_DIM].astype(F32), table).astype(BF16)
        v_ref[here] = qkv[:, 2 * HEAD_DIM:3 * HEAD_DIM]

    @scoped('f_unit')
    def forward_unit(count, chip, with_hidden):
        here = rows_of(chip)
        rows_u = u_ref[here]
        heads(here, rows_u)
        gate = dot_nn(rows_u, wc_ref[:, gate_cols]).astype(BF16)
        up = dot_nn(rows_u, wc_ref[:, up_cols]).astype(BF16)
        dx_ref[here, gate_cols] = gate
        dx_ref[here, up_cols] = up
        if with_hidden:
            gate_f, up_f = gate.astype(F32), up.astype(F32)
            ho_ref[here, hidden_cols] = (gate_f * jax.nn.sigmoid(gate_f) * up_f).astype(BF16)

    @scoped('b_unit')
    def backward_unit(count, chip):
        here = rows_of(chip)
        dah = dot_nt(g_ref[here], wo_ref[...])
        dx_ref[here, :HEAD_DIM] = dah[:, :HEAD_DIM].astype(BF16)
        d_hidden = dah[:, hidden_cols].astype(BF16).astype(F32)
        hidden, d_gate, d_up = gated_pull(dx_ref[here, gate_cols].astype(F32), dx_ref[here, up_cols].astype(F32), d_hidden)
        ho_ref[here, hidden_cols] = hidden
        dx_ref[here, gate_cols] = d_gate
        dx_ref[here, up_cols] = d_up

    def piece_of(piece):
        return pl.ds(aligned(piece * piece_cols, piece_cols), piece_cols)

    def part_forward(chip, piece):
        return dot_nn(ho_ref[rows_of(chip)], wo_ref[:, piece_of(piece)])

    def part_backward(chip, piece):
        return dot_nt(dx_ref[rows_of(chip)], wc_ref[piece_of(piece)])

    def keys_values(chip):
        store_keys_values(rows_of(chip), dx_ref, dk_ref, dv_ref, table_ref)

    def other_keys_values():
        def body(step):
            keys_values(place.near(place.half + step - chips))
        loop_from(1, chips, body)

    def read_dy(piece):
        return g_ref[:, piece_of(piece)]

    @scoped('finals')
    def finals(reduce):
        return jnp.concatenate([reduce.final(piece) for piece in range(NP)], axis=1)

    grad_cols = slice(head_cols + 2 * ff)
    last_u, last_h = (lasts[0], lasts[2], lasts[3]), (lasts[1], lasts[4])

    def grads_last(event):
        @pl.when(event < NP)
        def _():
            weight_grads_h(event, ho_ref, read_dy, wo_ref)
            for copy in h_copies(event, wo_ref, last_h, sems_hs, ff):
                copy.start()

        @pl.when((event >= NP) & (event < NP + chips))
        def _():
            weight_grads_u(not_below_zero(event - NP), u_ref, dx_ref, gs_ref, last_u, sems_gs, head_cols, ff)

    def grads_last_wait():
        for piece in range(NP):
            wait_all(h_copies(piece, wo_ref, last_h, sems_hs, ff))
        weight_grads_u_wait(gs_ref, last_u, sems_gs, head_cols, ff)

    def grads_first(event):
        @pl.when(event < NP)
        def _():
            weight_grads_h(event, ho_ref, read_dy, wo_ref)

        @pl.when((event >= NP) & (event < NP + chips))
        def _():
            rows = width // chips
            here = pl.ds(aligned(not_below_zero(event - NP) * rows, rows), rows)
            g_ref[here, grad_cols] = dot_tn(u_ref[:, here], dx_ref[...]).astype(BF16)

    lanes = all_ref.shape[3]
    tiles = width // lanes

    def cross(layer):
        return pltpu.make_async_remote_copy(pair_ref.at[layer, 0], pair_ref.at[layer, 1], sem_ps.at[layer], sem_pr.at[layer], place.mate, MESH)

    def spread(layer, step):
        here = all_ref.at[layer, place.chip]
        return pltpu.make_async_remote_copy(here, here, sem_as.at[layer, step - 1], sem_ar.at[layer, step - 1],
                                            place.peer(step), MESH)

    def start_gain(layer, row):
        for tile in range(tiles):
            pair_ref[layer, 0, tile:tile + 1] = row[:, tile * lanes:(tile + 1) * lanes]
        cross(layer).start()

    @scoped('spread_gain')
    def spread_gain(layer):
        cross(layer).wait()
        all_ref[layer, place.chip] = pair_ref[layer, 0] + pair_ref[layer, 1]
        for step in range(1, chips):
            spread(layer, step).start()

    @scoped('end_gain')
    def end_gain(layer):
        for step in range(1, chips):
            spread(layer, step).wait()
        total = all_ref[layer, 0]
        for chip in range(1, chips):
            total = total + all_ref[layer, chip]
        for tile in range(tiles):
            gain_out[layer:layer + 1, tile * lanes:(tile + 1) * lanes] = total[tile:tile + 1]

    load_x = loads.start(x_hbm, x_ref)
    load_g = loads.start(gy_hbm, g_ref.at[gg.own_rows()])
    load_w = load_wc(0)
    load_o = load_wo(0)
    load_x.wait()
    u_ref[gu.own_rows()] = norm_forward(x_ref[...].astype(F32), gain_ref[0:1])
    pl.semaphore_wait(pltpu.get_barrier_semaphore(), peers)
    gu.start()
    saves = [loads.start(u_ref.at[gu.own_rows()], u0_hbm)]
    fill_table(freq_ref[0:1], table_ref)
    load_g.wait()
    wait_all(load_w)

    def start_gy(event):
        @pl.when(event == gu.events - NP)
        def _():
            gg.start()
    gather_loop(gu, lambda count, chip: forward_unit(count, chip, True), start_gy)

    load_w = load_wc(1)
    saves += [loads.start(q_ref, q_hbm), loads.start(k_ref, k_hbm), loads.start(v_ref, v_hbm),
              loads.start(dx_ref.at[:, head_cols:head_cols + 2 * ff], ab_hbm)]

    def attend_first(chip):
        attention_block(chip * pair, pair, chips * pair, chips * pair, (q_ref, k_ref, v_ref, table_ref, None, write_o, None, None, None), True, False)
    attend_first(place.near(place.half))
    wait_all(load_o)
    reduce = Reduce(place, part_forward, shard, refs_r)

    def filler_forward(event):
        @pl.when(event < place.half)
        def _():
            distance = not_below_zero(place.half - 1 - event)

            def body(way):
                attend_first(place.near((1 - 2 * way) * distance))
            loop(lax.select(distance == 0, 1, 2), body)

        @pl.when(event == place.half)
        def _():
            gu.finish()
            o_copy().start()
    n_o = loads.used
    loads.used += 1

    def o_copy():
        return pltpu.make_async_copy(ho_ref.at[:, :HEAD_DIM], o_hbm, local.at[n_o])
    reduce.run(filler_forward)
    load_o = load_wo(1)
    gg.event(jnp.int32(0), forward=True)
    gg.event(jnp.int32(1), forward=True)
    x_next = (x_ref[...].astype(F32) + finals(reduce)).astype(BF16)
    x1_ref[...] = x_next
    saves[0].wait()
    o_copy().wait()
    u_ref[gu.own_rows()] = norm_forward(x_next.astype(F32), gain_ref[1:2])

    reduce.finish()
    gu.start()
    load_side = loads.start(u0_hbm, side_ref.at[0])
    wait_all(saves[1:])
    wait_all(load_w)
    wait_all(load_o)
    dk_ref[...] = jnp.zeros_like(dk_ref)
    dv_ref[...] = jnp.zeros_like(dv_ref)
    early = 2
    for event in range(early, NP):
        gg.event(jnp.int32(event), forward=False)

    def more_gy(event):
        first = gu.events - NP

        @pl.when((event >= first) & (event < first + NP - early))
        def _():
            gg.forward(not_below_zero(event - first) + early)

        @pl.when(event >= first + NP - early)
        def _():
            gg.event(not_below_zero(event - first) + early, forward=True)

        @pl.when((event > NP) & (event < NP + 6) & (lax.rem(event, 2) == 1))
        def _():
            turn = not_below_zero(lax.div(event - 1, 2) - 2)
            gg.mate_wait_chip(jnp.minimum(turn, 1), turn == 2)
            backward_unit(turn, place.near(lax.select(turn == 2, 1, -turn)))
    gather_loop(gu, lambda count, chip: forward_unit(count, chip, False), more_gy)

    groups = 4

    def attend_last(turn):
        held = early + NP
        distance = lax.div(turn + 1, 2)
        rightward = (turn > 0) & (lax.rem(turn, 2) == 0)
        opposite = turn == chips - 1
        needed = lax.select(turn == 0, held, lax.select(opposite, gg.events, distance * NP))
        begin = lax.select(turn == 0, held, jnp.minimum(jnp.maximum(held + turn - 1, lax.select(turn >= chips - 2, gg.events - NP // 2, 0)), gg.events))
        end = jnp.maximum(jnp.minimum(held + turn, gg.events), needed)
        end = lax.select(turn == chips - 2, jnp.maximum(end, gg.events - 1), end)
        begin = lax.select(turn == chips - 1, gg.events - 1, begin)

        @pl.when(turn == NP + 1)
        def _():
            gu.finish()
            load_side.wait()
            gu.start_side(side_ref)

        def take(event):
            gg.event(event)
        loop_from(begin, end, take)

        chip = place.near(lax.select(rightward, distance, -distance))

        @pl.when(opposite)
        def _():
            gg.mate_wait_last()

        @pl.when((turn > 2) & jnp.logical_not(opposite))
        def _():
            gg.mate_wait_chip(distance, rightward)

        @pl.when(turn > 2)
        def _():
            backward_unit(turn, chip)
        for group in range(groups):
            @pl.when(lax.div(chip, chips // groups) == group)
            def _(group=group):
                attention_block(chip * pair, pair, (group + 1) * (chips * pair // groups), chips * pair // groups,
                                (q_ref, k_ref, v_ref, table_ref, read_da, write_o, dx_ref, dk_ref, dv_ref), True, True)
    loop(chips, attend_last)
    keys_values(place.near(place.half))
    loads_a = [loads.start(q_hbm, q_ref), loads.start(k_hbm, k_ref), loads.start(v_hbm, v_ref)]
    n_late = loads.used
    loads.used += 1

    def load_o_again():
        return pltpu.make_async_copy(o_hbm, ho_ref.at[:, :HEAD_DIM], local.at[n_late])
    near = (place.left, place.right, place.mate)
    reduce = Reduce(place, part_backward, shard, refs_r)

    def filler_last(event):
        @pl.when(event == 0)
        def _():
            other_keys_values()
        grads_last(event)

        @pl.when(event == 1)
        def _():
            gg.finish()

        @pl.when(event == NP + chips)
        def _():
            load_o_again().start()
            for peer in near:
                pl.semaphore_signal(free_sem, inc=1, device_id=peer, device_id_type=MESH)
    reduce.run(filler_last)
    pl.semaphore_wait(free_sem, len(near))
    load_o_again().wait()
    gu.adopt_side(side_ref)
    for event in range(early):
        gu.forward_side(side_ref, event)
    d_normed = finals(reduce).astype(BF16).astype(F32)
    inv, unit = norm_unit(x1_ref[...].astype(F32))
    g_ref[gg.own_rows()] = (g_ref[gg.own_rows()].astype(F32) + norm_backward(inv, unit, gain_ref[1:2], d_normed)).astype(BF16)
    start_gain(1, jnp.sum(d_normed * unit, axis=0, keepdims=True))

    reduce.finish()
    gg.start()
    spread_gain(1)
    grads_last_wait()
    load_o = load_wo(0) + [loads.start(ab_hbm, dx_ref.at[:, head_cols:head_cols + 2 * ff])]
    load_w = load_wc(0)
    dk_ref[...] = jnp.zeros_like(dk_ref)
    dv_ref[...] = jnp.zeros_like(dv_ref)
    wait_all(load_o)

    def more_u(event):
        first = gg.events - NP

        @pl.when((event >= first) & (event < first + NP - early))
        def _():
            gu.forward_side(side_ref, not_below_zero(event - first) + early)

        @pl.when(event >= first + NP - early)
        def _():
            gu.event(not_below_zero(event - first) + early, forward=True)
    gather_loop(gg, backward_unit, more_u)
    wait_all(loads_a)

    back_groups = 2

    def attend_back(block):
        @pl.when((block >= 2) & (block < gu.events - 2 * NP))
        def _():
            gu.event(block + NP, forward=True)
        for group in range(back_groups):
            @pl.when(lax.div(block, chips // back_groups) == group)
            def _(group=group):
                attention_block(block * pair, pair, (group + 1) * (chips * pair // back_groups), chips * pair // back_groups,
                                (q_ref, k_ref, v_ref, table_ref, read_da, None, dx_ref, dk_ref, dv_ref), False, True)
    loop(chips, attend_back)
    keys_values(place.near(place.half))
    wait_all(load_w)
    reduce = Reduce(place, part_backward, shard, refs_r)

    def filler_first(event):
        @pl.when(event == 0)
        def _():
            other_keys_values()

        @pl.when(event < NP)
        def _():
            gu.event(gu.events - NP + event, forward=False)

        @pl.when(event == NP - 1)
        def _():
            gu.mate_wait_all()
        grads_first(event)

        @pl.when(event == 1)
        def _():
            gg.finish()

        @pl.when(event == NP + 1)
        def _():
            gu.finish()

        @pl.when(event == NP + chips)
        def _():
            for copy in reloads():
                copy.start()
    n_reload = loads.used
    loads.used += len(fold_plan(width, head_cols, ff))

    def reloads():
        plan = fold_plan(width, head_cols, ff)
        return [pltpu.make_async_copy(lasts[number].at[theirs], u_ref.at[ours], local.at[n_reload + slot])
                for slot, (number, theirs, ours) in enumerate(plan)]
    x1_ref[...] = g_ref[gg.own_rows()]
    reduce.run(filler_first)
    inv, unit = norm_unit(x_ref[...].astype(F32))
    d_normed = finals(reduce).astype(BF16).astype(F32)
    start_gain(0, jnp.sum(d_normed * unit, axis=0, keepdims=True))
    dx_out[...] = (x1_ref[...].astype(F32) + norm_backward(inv, unit, gain_ref[0:1], d_normed)).astype(BF16)
    spread_gain(0)
    end_gain(1)
    reduce.finish()
    wait_all(reloads())
    end_gain(0)


def fold_plan(width, head_cols, ff):
    cols = head_cols + 2 * ff
    piece = width // NP
    rows = HEAD_DIM + ff
    every = slice(None)
    plan = [(0, (every, every), (every, slice(head_cols))), (2, (every, every), (every, slice(head_cols, head_cols + ff))),
            (3, (every, every), (every, slice(head_cols + ff, cols)))]
    whole = width // rows
    for turn in range(NP):
        theirs = slice(turn * piece, (turn + 1) * piece)
        if turn < whole:
            ours = slice(cols, cols + piece)
            plan += [(1, (every, theirs), (slice(turn * rows, turn * rows + HEAD_DIM), ours)),
                     (4, (every, theirs), (slice(turn * rows + HEAD_DIM, (turn + 1) * rows), ours))]
        else:
            plan += [(1, (every, theirs), (slice(whole * rows, whole * rows + HEAD_DIM), slice(cols, cols + piece)))]
            strip = width - cols - piece
            for step in range(piece // strip):
                plan += [(4, (every, slice(turn * piece + step * strip, turn * piece + (step + 1) * strip)),
                          (slice(step * ff, (step + 1) * ff), slice(cols + piece, width)))]
    return plan


def kernel_stack(head_cols, ff, last_ref, first_ref, first_h_ref, dx_ref, gain_ref, *refs):
    outs, (dx_out, gain_out, sems) = refs[0:5], refs[5:8]
    width = last_ref.shape[0]
    copies = Copies(sems)
    pending = [copies.start(dx_ref, dx_out), copies.start(gain_ref, gain_out)]
    for number, theirs, ours in fold_plan(width, head_cols, ff):
        pending.append(copies.start(last_ref.at[ours], outs[number].at[(1,) + theirs]))
    bounds = (0, head_cols, head_cols + ff, head_cols + 2 * ff)
    for i, number in enumerate((0, 2, 3)):
        pending.append(copies.start(first_ref.at[:, bounds[i]:bounds[i + 1]], outs[number].at[0]))
    pending.append(copies.start(first_h_ref.at[:HEAD_DIM], outs[1].at[0]))
    pending.append(copies.start(first_h_ref.at[HEAD_DIM:HEAD_DIM + ff], outs[4].at[0]))
    for copy in pending:
        copy.wait()


def solution(mesh):
    tp_size = mesh.shape['tp']
    half = tp_size // 4
    row_spec = P(('dp', 'tp'), None)
    col_spec = P(None, None, 'tp')
    inner_spec = P(None, 'tp', None)

    def device_program(x_loc, dy_loc, norm_gain, w_qkv, w_out, w_gate, w_up, w_down):
        shard, width = x_loc.shape
        seq = shard * tp_size
        pair = 2 * shard
        chips = tp_size // 2
        head_cols = w_qkv.shape[2]
        ff = w_gate.shape[2]
        cols = head_cols + 2 * ff
        piece_cols = width // NP
        vmem, anyspace = pl.BlockSpec(memory_space=pltpu.VMEM), pl.BlockSpec(memory_space=pl.ANY)
        shape = jax.ShapeDtypeStruct
        dma = pltpu.SemaphoreType.DMA

        freqs = np.float32(ROPE_BASE) ** (np.float32(-2.0) * np.arange(HEAD_DIM // 2, dtype=np.float32) / np.float32(HEAD_DIM))
        freqs = jnp.asarray(np.tile(freqs, (8, 2)))

        rows_shape = shape((shard, width), BF16)
        gain_shape = shape((2, width), F32)
        head_shape = shape((seq, HEAD_DIM), BF16)
        grads = (shape((width, head_cols), BF16), shape((HEAD_DIM, width), BF16), shape((width, ff), BF16),
                 shape((width, ff), BF16), shape((ff, width), BF16))
        square, folded = pltpu.VMEM((width, width), BF16), pltpu.VMEM((HEAD_DIM + ff, width), BF16)
        hbm = pl.BlockSpec(memory_space=pltpu.HBM)
        whole_vmem = 67043328
        kept = (seq * width + width * width + (HEAD_DIM + ff) * width + shard * width) * 2 + 2 ** 18
        results = pl.pallas_call(
            functools.partial(kernel_main, tp_size),
            out_shape=(pltpu.VMEM(rows_shape.shape, BF16), pltpu.VMEM(gain_shape.shape, F32), square, square, folded) + grads + (rows_shape,) + (head_shape,) * 4 + (shape((seq, 2 * ff), BF16),),
            in_specs=[vmem] * 2 + [hbm] * 7,
            out_specs=(vmem,) * 5 + (hbm,) * 11,
            scratch_shapes=[
                pltpu.VMEM((shard, width), BF16), pltpu.VMEM((3, shard, width), BF16), pltpu.VMEM((width, cols), BF16),
                pltpu.VMEM((seq, HEAD_DIM), BF16), pltpu.VMEM((seq, HEAD_DIM), BF16), pltpu.VMEM((seq, HEAD_DIM), BF16),
                pltpu.VMEM((seq, HEAD_DIM + ff), BF16), pltpu.VMEM((seq, cols), BF16),
                pltpu.VMEM((seq, HEAD_DIM), F32), pltpu.VMEM((seq, HEAD_DIM), F32), pltpu.VMEM((seq, HEAD_DIM), F32),
                pltpu.VMEM((shard, width), BF16), pltpu.VMEM((2, width // chips, cols), BF16),
                pltpu.VMEM((2, 2, width // 128, 128), F32), pltpu.VMEM((2, chips, width // 128, 128), F32),
                dma((80,)), dma((2, 3)), dma((NP, 2)), dma((2,)), dma((2,)), dma((2, chips - 1)), dma((2, chips - 1)),
                pltpu.SemaphoreType.REGULAR] + Gather.scratch(half) + Gather.scratch(half) + Reduce.scratch(half, shard, piece_cols),
            compiler_params=pltpu.CompilerParams(collective_id=1, has_side_effects=True, vmem_limit_bytes=whole_vmem - kept), name='blocks',
        )(norm_gain, freqs, x_loc, dy_loc, w_qkv, w_out, w_gate, w_up, w_down)

        stacked = pl.pallas_call(
            functools.partial(kernel_stack, head_cols, ff),
            out_shape=tuple(shape((2,) + grad.shape, BF16) for grad in grads) + (rows_shape, gain_shape),
            in_specs=[vmem] * 5,
            out_specs=(hbm,) * 7,
            scratch_shapes=[dma((48,))],
            compiler_params=pltpu.CompilerParams(vmem_limit_bytes=8 * 2 ** 20), name='stack',
        )(*results[2:5], *results[0:2])
        return tuple(stacked[5:7]) + tuple(stacked[0:5])

    return jax.shard_map(device_program, mesh=mesh, in_specs=(row_spec, row_spec, P(None, None), col_spec, inner_spec, col_spec, col_spec, inner_spec), out_specs=(row_spec, P('dp', None), P('dp', None, 'tp'), P('dp', 'tp', None), P('dp', None, 'tp'), P('dp', None, 'tp'), P('dp', 'tp', None)), check_vma=False)
```

```python
import functools

import jax
import jax.numpy as jnp
import numpy as np
from jax import lax
from jax.experimental import pallas as pl
from jax.experimental.pallas import tpu as pltpu
from jax.sharding import PartitionSpec as P

HEAD_DIM = 128
NORM_EPS = 1e-5
ROPE_BASE = 10000.0
MESH = pl.DeviceIdType.MESH
NP = 4
F32 = jnp.float32
BF16 = jnp.bfloat16


def dot_nn(a, b):
    return lax.dot_general(a, b, (((1,), (0,)), ((), ())), preferred_element_type=F32)


def dot_nt(a, b):
    return lax.dot_general(a, b, (((1,), (1,)), ((), ())), preferred_element_type=F32)


def dot_tn(a, b):
    return lax.dot_general(a, b, (((0,), (0,)), ((), ())), preferred_element_type=F32)


def not_below_zero(index):
    return jnp.maximum(index, 0)


def row_mean(values):
    return jnp.mean(values, axis=-1, keepdims=True)


def row_sum(values):
    return jnp.sum(values, axis=-1, keepdims=True)


def loop_from(first, last, body):
    def step(index, carry):
        body(index)
        return carry
    lax.fori_loop(first, last, step, 0)


def loop(count, body):
    loop_from(0, count, body)


def aligned(index, size):
    return pl.multiple_of(index, size)


def scoped(name):
    def wrap(function):
        @functools.wraps(function)
        def inner(*args, **kwargs):
            with jax.named_scope(name):
                return function(*args, **kwargs)
        return inner
    return wrap


class Place:
    def __init__(self, tp_size):
        index = lax.axis_index('tp')
        self.ring = tp_size // 2
        self.half = self.ring // 2
        self.core = lax.rem(index, 2)
        self.chip = lax.div(index, 2)
        self.right = self.peer(1)
        self.left = self.peer(-1)
        self.mate = {'tp': self.chip * 2 + 1 - self.core}

    def peer(self, step):
        return {'tp': self.near(step) * 2 + self.core}

    def near(self, step):
        return lax.rem(self.chip + step + self.ring, self.ring)

    def arrive(self):
        peers = [self.right, self.left, self.mate]
        for peer in peers:
            pl.semaphore_signal(pltpu.get_barrier_semaphore(), inc=1, device_id=peer, device_id_type=MESH)
        return len(peers)


class Gather:
    def __init__(self, place, buf, shard_rows, sems):
        self.place, self.buf, self.shard = place, buf, shard_rows
        self.rows = shard_rows // NP
        self.events = (place.half - 1) * NP + NP // 2
        self.send, self.recv_r, self.recv_l, self.recv_m = sems

    @staticmethod
    def scratch(half):
        events = (half - 1) * NP + NP // 2
        return [pltpu.SemaphoreType.DMA(())] + [pltpu.SemaphoreType.DMA((n,)) for n in (events, events, 2 * half)]

    def view(self, chip, core, piece):
        start = (chip * 2 + core) * self.shard + piece * self.rows
        return self.buf.at[pl.ds(aligned(start, self.rows), self.rows)]

    def own_rows(self):
        start = (self.place.chip * 2 + self.place.core) * self.shard
        return pl.ds(aligned(start, self.shard), self.shard)

    def copy(self, source, view, recv, to):
        return pltpu.make_async_remote_copy(source, view, self.send, recv, to, MESH)

    def to_right(self, event, view):
        return self.copy(view, view, self.recv_r.at[event], self.place.right)

    def to_left(self, event, view):
        return self.copy(view, view, self.recv_l.at[event], self.place.left)

    def group(self, event, rightward):
        half = self.place.half
        return lax.select(event >= (half - 1) * NP, 2 * half - 1, lax.div(event, NP) + (half if rightward else 1))

    def to_mate(self, group, view):
        return self.copy(view, view, self.recv_m.at[group], self.place.mate)

    def start(self):
        place = self.place
        for piece in range(NP):
            self.to_right(piece, self.view(place.chip, place.core, piece)).start()
            self.to_left(piece, self.view(place.chip, place.core, NP - 1 - piece)).start()
        for piece in range(NP):
            self.to_mate(0, self.view(place.chip, place.core, piece)).start()

    def views(self, event):
        step = lax.div(event, NP) + 1
        piece = lax.rem(event, NP)
        from_left = self.view(self.place.near(-step), self.place.core, piece)
        from_right = self.view(self.place.near(step), self.place.core, NP - 1 - piece)
        return from_left, from_right

    @scoped('g_event')
    def event(self, event, forward=None):
        from_left, from_right = self.views(event)
        self.to_right(event, from_left).wait_recv()
        self.pass_on(event, forward, lambda: self.to_right(event + NP, from_left).start())
        self.to_mate(self.group(event, False), from_left).start()
        self.to_left(event, from_right).wait_recv()
        self.pass_on(event, forward, lambda: self.to_left(event + NP, from_right).start())
        self.to_mate(self.group(event, True), from_right).start()

    def forward(self, event):
        from_left, from_right = self.views(event)
        self.to_right(event + NP, from_left).start()
        self.to_left(event + NP, from_right).start()

    def side_view(self, side, which, piece):
        return side.at[which, pl.ds(aligned(piece * self.rows, self.rows), self.rows)]

    def start_side(self, side):
        for piece in range(NP):
            last = NP - 1 - piece
            self.copy(self.side_view(side, 0, piece), self.side_view(side, 1, piece), self.recv_r.at[piece], self.place.right).start()
            self.copy(self.side_view(side, 0, last), self.side_view(side, 2, last), self.recv_l.at[piece], self.place.left).start()

    def adopt_side(self, side):
        place = self.place

        def body(piece):
            last = NP - 1 - piece
            from_left, from_right = self.side_view(side, 1, piece), self.side_view(side, 2, last)
            self.to_right(piece, from_left).wait_recv()
            self.to_left(piece, from_right).wait_recv()
            to_left, to_right = self.views(piece)
            for source, view, group in ((self.side_view(side, 0, piece), self.view(place.chip, place.core, piece), 0),
                                        (from_left, to_left, 1), (from_right, to_right, place.half)):
                self.copy(source, view, self.recv_m.at[group], place.mate).start()
        loop(NP, body)
        for which, step in ((0, 0), (1, -1), (2, 1)):
            start = (place.near(step) * 2 + place.core) * self.shard
            self.buf[pl.ds(aligned(start, self.shard), self.shard)] = side[which]

    def forward_side(self, side, event):
        from_left, from_right = self.views(event)
        later = event + NP
        self.copy(self.side_view(side, 1, event), from_left, self.recv_r.at[later], self.place.right).start()
        self.copy(self.side_view(side, 2, NP - 1 - event), from_right, self.recv_l.at[later], self.place.left).start()

    def pass_on(self, event, forward, send):
        if forward is None:
            pl.when(event + NP < self.events)(send)
        elif forward:
            send()

    def mate_wait(self, group, step):
        start = (self.place.near(step) * 2 + 1 - self.place.core) * self.shard
        self.to_mate(group, self.buf.at[pl.ds(aligned(start, self.shard), self.shard)]).wait_recv()

    @scoped('g_matelast')
    def mate_wait_last(self):
        self.mate_wait(2 * self.place.half - 1, self.place.half)

    @scoped('g_matewait')
    def mate_wait_chip(self, distance, rightward):
        far = lax.select(rightward, distance + self.place.half - 1, distance)
        self.mate_wait(lax.select(distance == 0, 0, far), lax.select(rightward, distance, -distance))

    def mate_wait_all(self):
        self.mate_wait(0, 0)

        def body(turn):
            self.mate_wait_chip(turn + 1, False)
            self.mate_wait_chip(turn + 1, True)
        loop(self.place.half - 1, body)
        self.mate_wait_last()

    def finish(self):
        sent = self.buf.at[pl.ds(0, (4 * self.events + NP) * self.rows)]
        self.to_mate(0, sent).wait_send()


class Reduce:
    SLOTS = 4
    DEPTH = 8

    def __init__(self, place, part, shard_rows, refs):
        self.place, self.part, self.shard = place, part, shard_rows
        self.events = (place.half - 1) * NP + NP // 2
        self.ring, self.acc, self.stage, self.send_n, self.recv_n, self.send_m, self.recv_m = refs

    @staticmethod
    def scratch(half, shard_rows, width):
        events = (half - 1) * NP + NP // 2
        shapes = [(2, events), (2 * Reduce.DEPTH + NP,), (Reduce.SLOTS, 2)]
        sems = [(2, Reduce.DEPTH), (2, events), (Reduce.SLOTS,), (2 * Reduce.DEPTH + NP,)]
        return [pltpu.VMEM(s + (shard_rows, width), F32) for s in shapes] + [pltpu.SemaphoreType.DMA(s) for s in sems]

    def acc_slot(self, term):
        own = 2 * self.DEPTH + not_below_zero(term - 2 * self.events)
        return lax.select(term < 2 * self.events, lax.rem(term, 2 * self.DEPTH), own)

    def mate_copy(self, term):
        return pltpu.make_async_remote_copy(
            self.stage.at[lax.rem(term, self.SLOTS), 1 - self.place.core], self.acc.at[self.acc_slot(term)],
            self.send_m.at[lax.rem(term, self.SLOTS)], self.recv_m.at[self.acc_slot(term)], self.place.mate, MESH)

    def ring_copy(self, event, way):
        to = self.place.peer(1 - 2 * way)
        return pltpu.make_async_remote_copy(
            self.acc.at[self.acc_slot(2 * event + way)], self.ring.at[way, event],
            self.send_n.at[way, lax.rem(event, self.DEPTH)], self.recv_n.at[way, event], to, MESH)

    @scoped('r_fill')
    def fill(self, term):
        @pl.when(term >= self.SLOTS)
        def _():
            self.mate_copy(not_below_zero(term - self.SLOTS)).wait_send()
        slot = lax.rem(term, self.SLOTS)
        way = lax.rem(term, 2)

        @pl.when(term >= 2 * (self.DEPTH - 1))
        def _():
            self.ring_copy(jnp.maximum(lax.div(term, 2) - (self.DEPTH - 1), 0), way).wait_send()
        shifted = lax.div(term, 2) + NP // 2
        travels = term < 2 * self.events
        distance = not_below_zero(self.place.half - lax.div(shifted, NP))
        turn = lax.rem(shifted, NP)
        piece = lax.select(travels, lax.select(way == 0, turn, NP - 1 - turn), lax.rem(not_below_zero(term - 2 * self.events), NP))
        value = self.part(self.place.near((1 - 2 * way) * distance), piece)
        self.stage[slot, 0] = value[:self.shard]
        self.stage[slot, 1] = value[self.shard:]
        self.mate_copy(term).start()

    @scoped('r_event')
    def event(self, event):
        def add(way):
            term = 2 * event + way
            self.mate_copy(term).wait_recv()
            slot = self.acc_slot(term)
            self.acc[slot] += self.stage[lax.rem(term, self.SLOTS), self.place.core]

            @pl.when(event >= NP)
            def _():
                before = not_below_zero(event - NP)
                self.ring_copy(before, way).wait_recv()
                self.acc[slot] += self.ring[way, before]
            self.ring_copy(event, way).start()
        loop(2, add)

    def final(self, piece):
        last = self.events - NP
        term = 2 * self.events + piece
        self.mate_copy(term).wait_recv()
        self.ring_copy(last + piece, 0).wait_recv()
        self.ring_copy(last + NP - 1 - piece, 1).wait_recv()
        return ((self.stage[term % self.SLOTS, self.place.core] + self.acc[2 * self.DEPTH + piece])
                + (self.ring[0, last + piece] + self.ring[1, last + NP - 1 - piece]))

    @scoped('r_finish')
    def finish(self):
        def across(term):
            self.mate_copy(term).wait_send()
        terms = 2 * self.events + NP
        loop_from(terms - self.SLOTS, terms, across)

        def ring(event):
            self.ring_copy(event, 0).wait_send()
            self.ring_copy(event, 1).wait_send()
        loop_from(self.events + 2 - (self.DEPTH - 1), self.events, ring)

    def run(self, filler):
        def body(turn):
            event = not_below_zero(turn - 1)
            travels = (turn >= 1) & (turn <= self.events)

            @pl.when(travels)
            def _():
                self.event(event)

            def ahead(way):
                self.fill(2 * turn + way)
            loop(2, ahead)

            @pl.when(travels)
            def _():
                filler(event)
        loop(self.events + 2, body)


def rope_pair(table):
    lanes = lax.broadcasted_iota(jnp.int32, table.shape, 1)
    swapped = pltpu.roll(table, HEAD_DIM // 2, 1)
    low = lanes < HEAD_DIM // 2
    return jnp.where(low, table, swapped), jnp.where(low, -swapped, table)


@scoped('table')
def fill_table(freqs, table_ref):
    rows = 64
    blocks = table_ref.shape[0] // rows

    def cos_sin(count, scale):
        steps = lax.broadcasted_iota(jnp.int32, (count, HEAD_DIM), 0) * scale
        angles = steps.astype(F32) * freqs
        return jnp.cos(angles), jnp.sin(angles)
    cos_low, sin_low = cos_sin(rows, 1)
    cos_high, sin_high = cos_sin(max(blocks, 8), rows)
    low = lax.broadcasted_iota(jnp.int32, (1, HEAD_DIM), 1) < HEAD_DIM // 2
    first = jnp.where(low, cos_high, sin_high)
    second = jnp.where(low, -sin_high, cos_high)
    for block in range(blocks):
        table_ref[block * rows:(block + 1) * rows] = first[block:block + 1] * cos_low + second[block:block + 1] * sin_low


def rope(values, table, inverse=False):
    cos2, sin2 = rope_pair(table)
    turned = pltpu.roll(values, HEAD_DIM // 2, 1)
    if inverse:
        return values * cos2 - turned * sin2
    return values * cos2 + turned * sin2


def norm_forward(x_f32, gain_row):
    inv = lax.rsqrt(row_mean(x_f32 * x_f32) + NORM_EPS)
    return (x_f32 * inv * gain_row).astype(BF16)


def norm_unit(x_f32):
    inv = lax.rsqrt(row_mean(x_f32 * x_f32) + NORM_EPS)
    return inv, x_f32 * inv


@scoped('norm_backward')
def norm_backward(inv, unit, gain_row, d_normed):
    d_unit = d_normed * gain_row
    return inv * (d_unit - unit * row_mean(d_unit * unit))


def by_halves(dot, a, b, axis):
    size = a.shape[axis] // 2
    first = a[:size] if axis == 0 else a[:, :size]
    second = a[size:] if axis == 0 else a[:, size:]
    return dot(first, b), dot(second, b)


@scoped('attention')
def attention_block(row0, rows, keys, diagonal, refs, forward, backward):
    q_ref, k_ref, v_ref, table_ref, read_da, write_o, dx_ref, dk_ref, dv_ref = refs
    here = pl.ds(aligned(row0, rows), rows)
    scale = HEAD_DIM ** -0.5
    spans = [(start, end) for start, end in ((0, keys - diagonal), (keys - diagonal, keys)) if end > start]
    query = q_ref[here]
    scores = []
    for start, end in spans:
        part = dot_nt(query, k_ref[start:end])
        if end == keys:
            row_id = row0 - start + lax.broadcasted_iota(jnp.int32, part.shape, 0)
            part = jnp.where(row_id >= lax.broadcasted_iota(jnp.int32, part.shape, 1), part, -1e30)
        scores.append(part)
    tops = [jnp.max(part, axis=-1, keepdims=True) for part in scores]
    top = functools.reduce(jnp.maximum, tops)
    factor = scale * 1.4426950408889634
    expd = [jnp.exp2((part - top) * factor) for part in scores]
    inv_sum = 1.0 / sum(row_sum(part) for part in expd)
    prob = [part * inv_sum for part in expd]
    prob_b = [part.astype(BF16) for part in prob]
    if forward:
        halves = [by_halves(dot_nn, part, v_ref[start:end], 0) for part, (start, end) in zip(prob_b, spans)]
        out = [functools.reduce(jnp.add, [half[i] for half in halves]) for i in range(2)]
        write_o(here, jnp.concatenate(out, axis=0).astype(BF16))
    if backward:
        d_attn = read_da(here)
        d_prob = [dot_nt(d_attn, v_ref[start:end]).astype(BF16).astype(F32) for start, end in spans]
        row_dot = sum(row_sum(p * d) for p, d in zip(prob, d_prob))
        d_scores = [(p * (d - row_dot)).astype(BF16) for p, d in zip(prob, d_prob)]
        halves = [by_halves(dot_nn, part, k_ref[start:end], 0) for part, (start, end) in zip(d_scores, spans)]
        d_query = jnp.concatenate([functools.reduce(jnp.add, [half[i] for half in halves]) for i in range(2)], axis=0)
        d_query = (d_query * scale).astype(BF16).astype(F32)
        dx_ref[here, :HEAD_DIM] = rope(d_query, table_ref[here], inverse=True).astype(BF16)
        for part, prob_part, (start, end) in zip(d_scores, prob_b, spans):
            middle = (start + end) // 2
            for ref, left, right in ((dv_ref, prob_part, d_attn), (dk_ref, part, query)):
                low, high = by_halves(dot_tn, left, right, 1)
                ref[start:middle] += low
                ref[middle:end] += high


@scoped('store_kv')
def store_keys_values(here, dx_ref, dk_ref, dv_ref, table_ref):
    d_key = (dk_ref[here] * HEAD_DIM ** -0.5).astype(BF16).astype(F32)
    dx_ref[here, HEAD_DIM:2 * HEAD_DIM] = rope(d_key, table_ref[here], inverse=True).astype(BF16)
    dx_ref[here, 2 * HEAD_DIM:3 * HEAD_DIM] = dv_ref[here].astype(BF16)


def gated_pull(gate, up, d_hidden):
    sig = jax.nn.sigmoid(gate)
    silu = gate * sig
    d_silu = d_hidden * up
    return (silu * up).astype(BF16), (d_silu * sig + d_silu * silu * (1.0 - sig)).astype(BF16), (d_hidden * silu).astype(BF16)


class Copies:
    def __init__(self, sems):
        self.sems, self.used = sems, 0

    def start(self, src, dst):
        copy = pltpu.make_async_copy(src, dst, self.take())
        copy.start()
        return copy

    def take(self):
        self.used += 1
        return self.sems.at[self.used % self.sems.shape[0]]


def gather_loop(gather, unit, then=None):
    chips = gather.place.ring

    def body(event):
        @pl.when(event < gather.events)
        def _():
            gather.event(event)
            if then is not None:
                then(event)
        step = lax.div(event, NP) + 1
        opposite = event == gather.events
        final = event == gather.events - 1
        own = event == 1
        near = (event >= NP) & (event < gather.events) & (lax.rem(event, 2) == 0)

        @pl.when(opposite)
        def _():
            gather.mate_wait_last()

        @pl.when(own | near | final)
        def _():
            gather.mate_wait_chip(step - 1, final | (lax.rem(event, NP) != 0))

        @pl.when(own | near | final | opposite)
        def _():
            distance = lax.select(opposite, gather.place.half, step - 1)
            rightward = final | (lax.rem(event, NP) != 0)
            count = lax.select(own, 0, lax.select(opposite, chips - 1, lax.select(final, chips - 2, not_below_zero(lax.div(event, 2) - 1))))
            unit(count, gather.place.near(lax.select(rightward, distance, -distance)))
    loop(gather.events + 1, body)


def weight_grads_u(block, u_ref, dx_ref, stage_ref, outs, sems, head_cols, ff):
    rows = stage_ref.shape[1]
    slot = lax.rem(block, 2)
    here = pl.ds(aligned(block * rows, rows), rows)

    def copies():
        bounds = (0, head_cols, head_cols + ff, head_cols + 2 * ff)
        return [pltpu.make_async_copy(stage_ref.at[slot, :, bounds[i]:bounds[i + 1]], outs[i].at[here], sems.at[slot, i]) for i in range(3)]

    @pl.when(block >= 2)
    def _():
        for copy in copies():
            copy.wait()
    stage_ref[slot] = dot_tn(u_ref[:, here], dx_ref[...]).astype(BF16)
    for copy in copies():
        copy.start()


def weight_grads_u_wait(stage_ref, outs, sems, head_cols, ff):
    rows = stage_ref.shape[1]
    bounds = (0, head_cols, head_cols + ff, head_cols + 2 * ff)
    for slot in range(2):
        for i in range(3):
            pltpu.make_async_copy(stage_ref.at[slot, :, bounds[i]:bounds[i + 1]], outs[i].at[pl.ds(0, rows)], sems.at[slot, i]).wait()


def weight_grads_h(piece, ho_ref, read_dy, stage_ref):
    cols = stage_ref.shape[1] // NP
    stage_ref[:, pl.ds(aligned(piece * cols, cols), cols)] = dot_tn(ho_ref[...], read_dy(piece)).astype(BF16)


def h_copies(there, stage_ref, outs, sems, ff):
    return [pltpu.make_async_copy(stage_ref.at[:HEAD_DIM, there], outs[0].at[:, there], sems.at[0]),
            pltpu.make_async_copy(stage_ref.at[HEAD_DIM:HEAD_DIM + ff, there], outs[1].at[:, there], sems.at[1])]


def kernel_main(tp_size, gain_ref, freq_ref, x_hbm, gy_hbm, wqkv_hbm, wout_hbm, wgate_hbm, wup_hbm, wdown_hbm,
                dx_out, gain_out, *refs):
    u_ref, g_ref, wo_ref = refs[0:3]
    lasts = refs[3:8]
    u0_hbm, q_hbm, k_hbm, v_hbm, o_hbm, ab_hbm = refs[8:14]
    (x_ref, side_ref, wc_ref, q_ref, k_ref, v_ref, ho_ref, dx_ref, dk_ref, dv_ref, table_ref, x1_ref, gs_ref,
     pair_ref, all_ref, local, sems_gs, sems_hs, sem_ps, sem_pr, sem_as, sem_ar, free_sem) = refs[14:37]
    sems_u, sems_g, refs_r = refs[37:41], refs[41:45], refs[45:]
    place = Place(tp_size)
    peers = place.arrive()
    shard, width = x_ref.shape
    pair = 2 * shard
    chips = place.ring
    head_cols = wqkv_hbm.shape[2]
    ff = wgate_hbm.shape[2]
    piece_cols = width // NP
    gate_cols = slice(head_cols, head_cols + ff)
    up_cols = slice(head_cols + ff, head_cols + 2 * ff)
    hidden_cols = slice(HEAD_DIM, HEAD_DIM + ff)
    loads = Copies(local)
    gu = Gather(place, u_ref, shard, sems_u)
    gg = Gather(place, g_ref, shard, sems_g)

    def wait_all(copies):
        for copy in copies:
            copy.wait()

    def load_wc(layer):
        return [loads.start(wqkv_hbm.at[layer], wc_ref.at[:, :head_cols]),
                loads.start(wgate_hbm.at[layer], wc_ref.at[:, gate_cols]),
                loads.start(wup_hbm.at[layer], wc_ref.at[:, up_cols])]

    def load_wo(layer):
        return [loads.start(wout_hbm.at[layer], wo_ref.at[:HEAD_DIM]), loads.start(wdown_hbm.at[layer], wo_ref.at[hidden_cols])]

    def rows_of(chip):
        return pl.ds(aligned(chip * pair, pair), pair)

    def write_o(here, value):
        ho_ref[here, :HEAD_DIM] = value

    def read_da(here):
        return dx_ref[here, :HEAD_DIM]

    def heads(here, rows_u):
        qkv = dot_nn(rows_u, wc_ref[:, :head_cols]).astype(BF16)
        table = table_ref[here]
        q_ref[here] = rope(qkv[:, :HEAD_DIM].astype(F32), table).astype(BF16)
        k_ref[here] = rope(qkv[:, HEAD_DIM:2 * HEAD_DIM].astype(F32), table).astype(BF16)
        v_ref[here] = qkv[:, 2 * HEAD_DIM:3 * HEAD_DIM]

    @scoped('f_unit')
    def forward_unit(count, chip, with_hidden):
        here = rows_of(chip)
        rows_u = u_ref[here]
        heads(here, rows_u)
        gate = dot_nn(rows_u, wc_ref[:, gate_cols]).astype(BF16)
        up = dot_nn(rows_u, wc_ref[:, up_cols]).astype(BF16)
        dx_ref[here, gate_cols] = gate
        dx_ref[here, up_cols] = up
        if with_hidden:
            gate_f, up_f = gate.astype(F32), up.astype(F32)
            ho_ref[here, hidden_cols] = (gate_f * jax.nn.sigmoid(gate_f) * up_f).astype(BF16)

    @scoped('b_unit')
    def backward_unit(count, chip):
        here = rows_of(chip)
        dah = dot_nt(g_ref[here], wo_ref[...])
        dx_ref[here, :HEAD_DIM] = dah[:, :HEAD_DIM].astype(BF16)
        d_hidden = dah[:, hidden_cols].astype(BF16).astype(F32)
        hidden, d_gate, d_up = gated_pull(dx_ref[here, gate_cols].astype(F32), dx_ref[here, up_cols].astype(F32), d_hidden)
        ho_ref[here, hidden_cols] = hidden
        dx_ref[here, gate_cols] = d_gate
        dx_ref[here, up_cols] = d_up

    def piece_of(piece):
        return pl.ds(aligned(piece * piece_cols, piece_cols), piece_cols)

    def part_forward(chip, piece):
        return dot_nn(ho_ref[rows_of(chip)], wo_ref[:, piece_of(piece)])

    def part_backward(chip, piece):
        return dot_nt(dx_ref[rows_of(chip)], wc_ref[piece_of(piece)])

    def keys_values(chip):
        store_keys_values(rows_of(chip), dx_ref, dk_ref, dv_ref, table_ref)

    def other_keys_values():
        def body(step):
            keys_values(place.near(place.half + step - chips))
        loop_from(1, chips, body)

    def read_dy(piece):
        return g_ref[:, piece_of(piece)]

    @scoped('finals')
    def finals(reduce):
        return jnp.concatenate([reduce.final(piece) for piece in range(NP)], axis=1)

    grad_cols = slice(head_cols + 2 * ff)
    last_u, last_h = (lasts[0], lasts[2], lasts[3]), (lasts[1], lasts[4])

    def grads_last(event):
        @pl.when(event < NP)
        def _():
            weight_grads_h(event, ho_ref, read_dy, wo_ref)
            for copy in h_copies(piece_of(event), wo_ref, last_h, sems_hs, ff):
                copy.start()

        @pl.when((event >= NP) & (event < NP + chips))
        def _():
            weight_grads_u(not_below_zero(event - NP), u_ref, dx_ref, gs_ref, last_u, sems_gs, head_cols, ff)

    def grads_last_wait():
        wait_all(h_copies(slice(None), wo_ref, last_h, sems_hs, ff))
        weight_grads_u_wait(gs_ref, last_u, sems_gs, head_cols, ff)

    def grads_first(event):
        @pl.when(event < NP)
        def _():
            weight_grads_h(event, ho_ref, read_dy, wo_ref)

        @pl.when((event >= NP) & (event < NP + chips))
        def _():
            rows = width // chips
            here = pl.ds(aligned(not_below_zero(event - NP) * rows, rows), rows)
            g_ref[here, grad_cols] = dot_tn(u_ref[:, here], dx_ref[...]).astype(BF16)

    lanes = all_ref.shape[3]
    tiles = width // lanes

    def cross(layer):
        return pltpu.make_async_remote_copy(pair_ref.at[layer, 0], pair_ref.at[layer, 1], sem_ps.at[layer], sem_pr.at[layer], place.mate, MESH)

    def spread(layer, which, step):
        part = all_ref.at[layer, which]
        return pltpu.make_async_remote_copy(part, part, sem_as.at[layer], sem_ar.at[layer], place.peer(step), MESH)

    def start_gain(layer, row):
        for tile in range(tiles):
            pair_ref[layer, 0, tile:tile + 1] = row[:, tile * lanes:(tile + 1) * lanes]
        cross(layer).start()

    @scoped('spread_gain')
    def spread_gain(layer):
        cross(layer).wait()
        all_ref[layer, place.chip] = pair_ref[layer, 0] + pair_ref[layer, 1]
        for step in range(1, chips):
            spread(layer, place.chip, step).start()

    @scoped('end_gain')
    def end_gain(layer):
        spread(layer, slice(chips - 1), 1).wait()
        total = all_ref[layer, 0]
        for chip in range(1, chips):
            total = total + all_ref[layer, chip]
        for tile in range(tiles):
            gain_out[layer:layer + 1, tile * lanes:(tile + 1) * lanes] = total[tile:tile + 1]

    load_x = loads.start(x_hbm, x_ref)
    load_g = loads.start(gy_hbm, g_ref.at[gg.own_rows()])
    load_w = load_wc(0)
    load_o = load_wo(0)
    load_x.wait()
    u_ref[gu.own_rows()] = norm_forward(x_ref[...].astype(F32), gain_ref[0:1])
    pl.semaphore_wait(pltpu.get_barrier_semaphore(), peers)
    gu.start()
    saves = [loads.start(u_ref.at[gu.own_rows()], u0_hbm)]
    fill_table(freq_ref[0:1], table_ref)
    load_g.wait()
    wait_all(load_w)

    def start_gy(event):
        @pl.when(event == gu.events - NP)
        def _():
            gg.start()
    gather_loop(gu, lambda count, chip: forward_unit(count, chip, True), start_gy)

    load_w = load_wc(1)
    saves += [loads.start(q_ref, q_hbm), loads.start(k_ref, k_hbm), loads.start(v_ref, v_hbm),
              loads.start(dx_ref.at[:, head_cols:head_cols + 2 * ff], ab_hbm)]

    def attend_first(chip):
        attention_block(chip * pair, pair, chips * pair, chips * pair, (q_ref, k_ref, v_ref, table_ref, None, write_o, None, None, None), True, False)
    attend_first(place.near(place.half))
    wait_all(load_o)
    reduce = Reduce(place, part_forward, shard, refs_r)

    def filler_forward(event):
        @pl.when(event < place.half)
        def _():
            distance = not_below_zero(place.half - 1 - event)

            def body(way):
                attend_first(place.near((1 - 2 * way) * distance))
            loop(lax.select(distance == 0, 1, 2), body)

        @pl.when(event == place.half)
        def _():
            gu.finish()
            o_copy().start()
    sem_o = loads.take()

    def o_copy():
        return pltpu.make_async_copy(ho_ref.at[:, :HEAD_DIM], o_hbm, sem_o)
    reduce.run(filler_forward)
    load_o = load_wo(1)
    gg.event(jnp.int32(0), forward=True)
    gg.event(jnp.int32(1), forward=True)
    x_next = (x_ref[...].astype(F32) + finals(reduce)).astype(BF16)
    x1_ref[...] = x_next
    saves[0].wait()
    o_copy().wait()
    u_ref[gu.own_rows()] = norm_forward(x_next.astype(F32), gain_ref[1:2])

    reduce.finish()
    gu.start()
    load_side = loads.start(u0_hbm, side_ref.at[0])
    wait_all(saves[1:])
    wait_all(load_w)
    wait_all(load_o)
    dk_ref[...] = jnp.zeros_like(dk_ref)
    dv_ref[...] = jnp.zeros_like(dv_ref)
    early = 2
    for event in range(early, NP):
        gg.event(jnp.int32(event), forward=False)

    def more_gy(event):
        first = gu.events - NP

        @pl.when((event >= first) & (event < first + NP - early))
        def _():
            gg.forward(not_below_zero(event - first) + early)

        @pl.when(event >= first + NP - early)
        def _():
            gg.event(not_below_zero(event - first) + early, forward=True)

        @pl.when((event > NP) & (event < NP + 6) & (lax.rem(event, 2) == 1))
        def _():
            turn = not_below_zero(lax.div(event - 1, 2) - 2)
            gg.mate_wait_chip(jnp.minimum(turn, 1), turn == 2)
            backward_unit(turn, place.near(lax.select(turn == 2, 1, -turn)))
    gather_loop(gu, lambda count, chip: forward_unit(count, chip, False), more_gy)

    groups = 4

    def attend_last(turn):
        held = early + NP
        distance = lax.div(turn + 1, 2)
        rightward = (turn > 0) & (lax.rem(turn, 2) == 0)
        opposite = turn == chips - 1
        needed = lax.select(turn == 0, held, lax.select(opposite, gg.events, distance * NP))
        begin = lax.select(turn == 0, held, jnp.minimum(jnp.maximum(held + turn - 1, lax.select(turn >= chips - 2, gg.events - NP // 2, 0)), gg.events))
        end = jnp.maximum(jnp.minimum(held + turn, gg.events), needed)
        end = lax.select(turn == chips - 2, jnp.maximum(end, gg.events - 1), end)
        begin = lax.select(turn == chips - 1, gg.events - 1, begin)

        @pl.when(turn == NP + 1)
        def _():
            gu.finish()
            load_side.wait()
            gu.start_side(side_ref)

        def take(event):
            gg.event(event)
        loop_from(begin, end, take)

        chip = place.near(lax.select(rightward, distance, -distance))

        @pl.when(opposite)
        def _():
            gg.mate_wait_last()

        @pl.when((turn > 2) & jnp.logical_not(opposite))
        def _():
            gg.mate_wait_chip(distance, rightward)

        @pl.when(turn > 2)
        def _():
            backward_unit(turn, chip)
        for group in range(groups):
            @pl.when(lax.div(chip, chips // groups) == group)
            def _(group=group):
                attention_block(chip * pair, pair, (group + 1) * (chips * pair // groups), chips * pair // groups,
                                (q_ref, k_ref, v_ref, table_ref, read_da, write_o, dx_ref, dk_ref, dv_ref), True, True)
    loop(chips, attend_last)
    keys_values(place.near(place.half))
    loads_a = [loads.start(q_hbm, q_ref), loads.start(k_hbm, k_ref), loads.start(v_hbm, v_ref)]
    sem_late = loads.take()

    def load_o_again():
        return pltpu.make_async_copy(o_hbm, ho_ref.at[:, :HEAD_DIM], sem_late)
    near = (place.left, place.right, place.mate)
    reduce = Reduce(place, part_backward, shard, refs_r)

    def filler_last(event):
        @pl.when(event == 0)
        def _():
            other_keys_values()
        grads_last(event)

        @pl.when(event == 1)
        def _():
            gg.finish()

        @pl.when(event == NP + chips)
        def _():
            load_o_again().start()
            for peer in near:
                pl.semaphore_signal(free_sem, inc=1, device_id=peer, device_id_type=MESH)
    reduce.run(filler_last)
    pl.semaphore_wait(free_sem, len(near))
    load_o_again().wait()
    gu.adopt_side(side_ref)
    for event in range(early):
        gu.forward_side(side_ref, event)
    d_normed = finals(reduce).astype(BF16).astype(F32)
    inv, unit = norm_unit(x1_ref[...].astype(F32))
    g_ref[gg.own_rows()] = (g_ref[gg.own_rows()].astype(F32) + norm_backward(inv, unit, gain_ref[1:2], d_normed)).astype(BF16)
    start_gain(1, jnp.sum(d_normed * unit, axis=0, keepdims=True))

    reduce.finish()
    gg.start()
    spread_gain(1)
    grads_last_wait()
    load_o = load_wo(0) + [loads.start(ab_hbm, dx_ref.at[:, head_cols:head_cols + 2 * ff])]
    load_w = load_wc(0)
    dk_ref[...] = jnp.zeros_like(dk_ref)
    dv_ref[...] = jnp.zeros_like(dv_ref)
    wait_all(load_o)

    def more_u(event):
        first = gg.events - NP

        @pl.when((event >= first) & (event < first + NP - early))
        def _():
            gu.forward_side(side_ref, not_below_zero(event - first) + early)

        @pl.when(event >= first + NP - early)
        def _():
            gu.event(not_below_zero(event - first) + early, forward=True)
    gather_loop(gg, backward_unit, more_u)
    wait_all(loads_a)

    back_groups = 2

    def attend_back(block):
        @pl.when((block >= 2) & (block < gu.events - 2 * NP))
        def _():
            gu.event(block + NP, forward=True)
        for group in range(back_groups):
            @pl.when(lax.div(block, chips // back_groups) == group)
            def _(group=group):
                attention_block(block * pair, pair, (group + 1) * (chips * pair // back_groups), chips * pair // back_groups,
                                (q_ref, k_ref, v_ref, table_ref, read_da, None, dx_ref, dk_ref, dv_ref), False, True)
    loop(chips, attend_back)
    keys_values(place.near(place.half))
    wait_all(load_w)
    reduce = Reduce(place, part_backward, shard, refs_r)

    def filler_first(event):
        @pl.when(event == 0)
        def _():
            other_keys_values()

        @pl.when(event < NP)
        def _():
            gu.event(gu.events - NP + event, forward=False)

        @pl.when(event == NP - 1)
        def _():
            gu.mate_wait_all()
        grads_first(event)

        @pl.when(event == 1)
        def _():
            gg.finish()

        @pl.when(event == NP + 1)
        def _():
            gu.finish()

        @pl.when(event == NP + chips)
        def _():
            for copy in reloads():
                copy.start()
    plan = fold_plan(width, head_cols, ff)
    sems_plan = [loads.take() for part in plan]

    def reloads():
        return [pltpu.make_async_copy(lasts[number].at[theirs], u_ref.at[ours], sem) for (number, theirs, ours), sem in zip(plan, sems_plan)]
    x1_ref[...] = g_ref[gg.own_rows()]
    reduce.run(filler_first)
    inv, unit = norm_unit(x_ref[...].astype(F32))
    d_normed = finals(reduce).astype(BF16).astype(F32)
    start_gain(0, jnp.sum(d_normed * unit, axis=0, keepdims=True))
    dx_out[...] = (x1_ref[...].astype(F32) + norm_backward(inv, unit, gain_ref[0:1], d_normed)).astype(BF16)
    spread_gain(0)
    end_gain(1)
    reduce.finish()
    wait_all(reloads())
    end_gain(0)


def fold_plan(width, head_cols, ff):
    cols = head_cols + 2 * ff
    piece = width // NP
    rows = HEAD_DIM + ff
    every = slice(None)
    plan = [(0, (every, every), (every, slice(head_cols))), (2, (every, every), (every, slice(head_cols, head_cols + ff))),
            (3, (every, every), (every, slice(head_cols + ff, cols)))]
    whole = width // rows
    for turn in range(NP):
        theirs = slice(turn * piece, (turn + 1) * piece)
        if turn < whole:
            ours = slice(cols, cols + piece)
            plan += [(1, (every, theirs), (slice(turn * rows, turn * rows + HEAD_DIM), ours)),
                     (4, (every, theirs), (slice(turn * rows + HEAD_DIM, (turn + 1) * rows), ours))]
        else:
            plan += [(1, (every, theirs), (slice(whole * rows, whole * rows + HEAD_DIM), slice(cols, cols + piece)))]
            strip = width - cols - piece
            for step in range(piece // strip):
                plan += [(4, (every, slice(turn * piece + step * strip, turn * piece + (step + 1) * strip)),
                          (slice(step * ff, (step + 1) * ff), slice(cols + piece, width)))]
    return plan


def kernel_stack(head_cols, ff, last_ref, first_ref, first_h_ref, dx_ref, gain_ref, *refs):
    outs, (dx_out, gain_out, sems) = refs[0:5], refs[5:8]
    width = last_ref.shape[0]
    copies = Copies(sems)
    pending = [copies.start(dx_ref, dx_out), copies.start(gain_ref, gain_out)]
    for number, theirs, ours in fold_plan(width, head_cols, ff):
        pending.append(copies.start(last_ref.at[ours], outs[number].at[(1,) + theirs]))
    bounds = (0, head_cols, head_cols + ff, head_cols + 2 * ff)
    for i, number in enumerate((0, 2, 3)):
        pending.append(copies.start(first_ref.at[:, bounds[i]:bounds[i + 1]], outs[number].at[0]))
    pending.append(copies.start(first_h_ref.at[:HEAD_DIM], outs[1].at[0]))
    pending.append(copies.start(first_h_ref.at[HEAD_DIM:HEAD_DIM + ff], outs[4].at[0]))
    for copy in pending:
        copy.wait()


def solution(mesh):
    tp_size = mesh.shape['tp']
    half = tp_size // 4
    row_spec = P(('dp', 'tp'), None)
    col_spec = P(None, None, 'tp')
    inner_spec = P(None, 'tp', None)

    def device_program(x_loc, dy_loc, norm_gain, w_qkv, w_out, w_gate, w_up, w_down):
        shard, width = x_loc.shape
        seq = shard * tp_size
        pair = 2 * shard
        chips = tp_size // 2
        head_cols = w_qkv.shape[2]
        ff = w_gate.shape[2]
        cols = head_cols + 2 * ff
        piece_cols = width // NP
        vmem, anyspace = pl.BlockSpec(memory_space=pltpu.VMEM), pl.BlockSpec(memory_space=pl.ANY)
        shape = jax.ShapeDtypeStruct
        dma = pltpu.SemaphoreType.DMA

        freqs = np.float32(ROPE_BASE) ** (np.float32(-2.0) * np.arange(HEAD_DIM // 2, dtype=np.float32) / np.float32(HEAD_DIM))
        freqs = jnp.asarray(np.tile(freqs, (8, 2)))

        rows_shape = shape((shard, width), BF16)
        gain_shape = shape((2, width), F32)
        head_shape = shape((seq, HEAD_DIM), BF16)
        grads = (shape((width, head_cols), BF16), shape((HEAD_DIM, width), BF16), shape((width, ff), BF16),
                 shape((width, ff), BF16), shape((ff, width), BF16))
        square, folded = pltpu.VMEM((width, width), BF16), pltpu.VMEM((HEAD_DIM + ff, width), BF16)
        hbm = pl.BlockSpec(memory_space=pltpu.HBM)
        whole_vmem = 67043328
        kept = (seq * width + width * width + (HEAD_DIM + ff) * width + shard * width) * 2 + 2 ** 18
        results = pl.pallas_call(
            functools.partial(kernel_main, tp_size),
            out_shape=(pltpu.VMEM(rows_shape.shape, BF16), pltpu.VMEM(gain_shape.shape, F32), square, square, folded) + grads + (rows_shape,) + (head_shape,) * 4 + (shape((seq, 2 * ff), BF16),),
            in_specs=[vmem] * 2 + [hbm] * 7,
            out_specs=(vmem,) * 5 + (hbm,) * 11,
            scratch_shapes=[
                pltpu.VMEM((shard, width), BF16), pltpu.VMEM((3, shard, width), BF16), pltpu.VMEM((width, cols), BF16),
                pltpu.VMEM((seq, HEAD_DIM), BF16), pltpu.VMEM((seq, HEAD_DIM), BF16), pltpu.VMEM((seq, HEAD_DIM), BF16),
                pltpu.VMEM((seq, HEAD_DIM + ff), BF16), pltpu.VMEM((seq, cols), BF16),
                pltpu.VMEM((seq, HEAD_DIM), F32), pltpu.VMEM((seq, HEAD_DIM), F32), pltpu.VMEM((seq, HEAD_DIM), F32),
                pltpu.VMEM((shard, width), BF16), pltpu.VMEM((2, width // chips, cols), BF16),
                pltpu.VMEM((2, 2, width // 128, 128), F32), pltpu.VMEM((2, chips, width // 128, 128), F32),
                dma((24,)), dma((2, 3)), dma((2,)), dma((2,)), dma((2,)), dma((2,)), dma((2,)),
                pltpu.SemaphoreType.REGULAR] + Gather.scratch(half) + Gather.scratch(half) + Reduce.scratch(half, shard, piece_cols),
            compiler_params=pltpu.CompilerParams(collective_id=1, has_side_effects=True, vmem_limit_bytes=whole_vmem - kept), name='blocks',
        )(norm_gain, freqs, x_loc, dy_loc, w_qkv, w_out, w_gate, w_up, w_down)

        stacked = pl.pallas_call(
            functools.partial(kernel_stack, head_cols, ff),
            out_shape=tuple(shape((2,) + grad.shape, BF16) for grad in grads) + (rows_shape, gain_shape),
            in_specs=[vmem] * 5,
            out_specs=(hbm,) * 7,
            scratch_shapes=[dma((1,))],
            compiler_params=pltpu.CompilerParams(vmem_limit_bytes=8 * 2 ** 20), name='stack',
        )(*results[2:5], *results[0:2])
        return tuple(stacked[5:7]) + tuple(stacked[0:5])

    return jax.shard_map(device_program, mesh=mesh, in_specs=(row_spec, row_spec, P(None, None), col_spec, inner_spec, col_spec, col_spec, inner_spec), out_specs=(row_spec, P('dp', None), P('dp', None, 'tp'), P('dp', 'tp', None), P('dp', None, 'tp'), P('dp', None, 'tp'), P('dp', 'tp', None)), check_vma=False)
```

```python
import functools

import jax
import jax.numpy as jnp
import numpy as np
from jax import lax
from jax.experimental import pallas as pl
from jax.experimental.pallas import tpu as pltpu
from jax.sharding import PartitionSpec as P

HEAD_DIM = 128
NORM_EPS = 1e-5
ROPE_BASE = 10000.0
MESH = pl.DeviceIdType.MESH
NP = 4
F32 = jnp.float32
BF16 = jnp.bfloat16


def dot_nn(a, b):
    return lax.dot_general(a, b, (((1,), (0,)), ((), ())), preferred_element_type=F32)


def dot_nt(a, b):
    return lax.dot_general(a, b, (((1,), (1,)), ((), ())), preferred_element_type=F32)


def dot_tn(a, b):
    return lax.dot_general(a, b, (((0,), (0,)), ((), ())), preferred_element_type=F32)


def not_below_zero(index):
    return jnp.maximum(index, 0)


def row_mean(values):
    return jnp.mean(values, axis=-1, keepdims=True)


def row_sum(values):
    return jnp.sum(values, axis=-1, keepdims=True)


def loop_from(first, last, body):
    def step(index, carry):
        body(index)
        return carry
    lax.fori_loop(first, last, step, 0)


def loop(count, body):
    loop_from(0, count, body)


def aligned(index, size):
    return pl.multiple_of(index, size)


class Place:
    def __init__(self, tp_size):
        index = lax.axis_index('tp')
        self.ring = tp_size // 2
        self.half = self.ring // 2
        self.core = lax.rem(index, 2)
        self.chip = lax.div(index, 2)
        self.right = self.peer(1)
        self.left = self.peer(-1)
        self.mate = {'tp': self.chip * 2 + 1 - self.core}

    def peer(self, step):
        return {'tp': self.near(step) * 2 + self.core}

    def near(self, step):
        return lax.rem(self.chip + step + self.ring, self.ring)

    def arrive(self):
        peers = [self.right, self.left, self.mate]
        for peer in peers:
            pl.semaphore_signal(pltpu.get_barrier_semaphore(), inc=1, device_id=peer, device_id_type=MESH)
        return len(peers)


class Gather:
    def __init__(self, place, buf, shard_rows, sems):
        self.place, self.buf, self.shard = place, buf, shard_rows
        self.rows = shard_rows // NP
        self.events = (place.half - 1) * NP + NP // 2
        self.send, self.recv_r, self.recv_l, self.recv_m = sems

    @staticmethod
    def scratch(half):
        events = (half - 1) * NP + NP // 2
        return [pltpu.SemaphoreType.DMA(())] + [pltpu.SemaphoreType.DMA((n,)) for n in (events, events, 2 * half)]

    def view(self, chip, core, piece):
        start = (chip * 2 + core) * self.shard + piece * self.rows
        return self.buf.at[pl.ds(aligned(start, self.rows), self.rows)]

    def own_rows(self):
        start = (self.place.chip * 2 + self.place.core) * self.shard
        return pl.ds(aligned(start, self.shard), self.shard)

    def copy(self, source, view, recv, to):
        return pltpu.make_async_remote_copy(source, view, self.send, recv, to, MESH)

    def to_right(self, event, view):
        return self.copy(view, view, self.recv_r.at[event], self.place.right)

    def to_left(self, event, view):
        return self.copy(view, view, self.recv_l.at[event], self.place.left)

    def group(self, event, rightward):
        half = self.place.half
        return lax.select(event >= (half - 1) * NP, 2 * half - 1, lax.div(event, NP) + (half if rightward else 1))

    def to_mate(self, group, view):
        return self.copy(view, view, self.recv_m.at[group], self.place.mate)

    def start(self):
        place = self.place
        for piece in range(NP):
            self.to_right(piece, self.view(place.chip, place.core, piece)).start()
            self.to_left(piece, self.view(place.chip, place.core, NP - 1 - piece)).start()
        for piece in range(NP):
            self.to_mate(0, self.view(place.chip, place.core, piece)).start()

    def views(self, event):
        step = lax.div(event, NP) + 1
        piece = lax.rem(event, NP)
        from_left = self.view(self.place.near(-step), self.place.core, piece)
        from_right = self.view(self.place.near(step), self.place.core, NP - 1 - piece)
        return from_left, from_right

    def event(self, event, forward=None):
        from_left, from_right = self.views(event)
        self.to_right(event, from_left).wait_recv()
        self.pass_on(event, forward, lambda: self.to_right(event + NP, from_left).start())
        self.to_mate(self.group(event, False), from_left).start()
        self.to_left(event, from_right).wait_recv()
        self.pass_on(event, forward, lambda: self.to_left(event + NP, from_right).start())
        self.to_mate(self.group(event, True), from_right).start()

    def forward(self, event):
        from_left, from_right = self.views(event)
        self.to_right(event + NP, from_left).start()
        self.to_left(event + NP, from_right).start()

    def side_view(self, side, which, piece):
        return side.at[which, pl.ds(aligned(piece * self.rows, self.rows), self.rows)]

    def start_side(self, side):
        for piece in range(NP):
            last = NP - 1 - piece
            self.copy(self.side_view(side, 0, piece), self.side_view(side, 1, piece), self.recv_r.at[piece], self.place.right).start()
            self.copy(self.side_view(side, 0, last), self.side_view(side, 2, last), self.recv_l.at[piece], self.place.left).start()

    def adopt_side(self, side):
        place = self.place

        def body(piece):
            last = NP - 1 - piece
            from_left, from_right = self.side_view(side, 1, piece), self.side_view(side, 2, last)
            self.to_right(piece, from_left).wait_recv()
            self.to_left(piece, from_right).wait_recv()
            to_left, to_right = self.views(piece)
            for source, view, group in ((self.side_view(side, 0, piece), self.view(place.chip, place.core, piece), 0),
                                        (from_left, to_left, 1), (from_right, to_right, place.half)):
                self.copy(source, view, self.recv_m.at[group], place.mate).start()
        loop(NP, body)
        for which, step in ((0, 0), (1, -1), (2, 1)):
            start = (place.near(step) * 2 + place.core) * self.shard
            self.buf[pl.ds(aligned(start, self.shard), self.shard)] = side[which]

    def forward_side(self, side, event):
        from_left, from_right = self.views(event)
        later = event + NP
        self.copy(self.side_view(side, 1, event), from_left, self.recv_r.at[later], self.place.right).start()
        self.copy(self.side_view(side, 2, NP - 1 - event), from_right, self.recv_l.at[later], self.place.left).start()

    def pass_on(self, event, forward, send):
        if forward is None:
            pl.when(event + NP < self.events)(send)
        elif forward:
            send()

    def mate_wait(self, group, step):
        start = (self.place.near(step) * 2 + 1 - self.place.core) * self.shard
        self.to_mate(group, self.buf.at[pl.ds(aligned(start, self.shard), self.shard)]).wait_recv()

    def mate_wait_last(self):
        self.mate_wait(2 * self.place.half - 1, self.place.half)

    def mate_wait_chip(self, distance, rightward):
        far = lax.select(rightward, distance + self.place.half - 1, distance)
        self.mate_wait(lax.select(distance == 0, 0, far), lax.select(rightward, distance, -distance))

    def mate_wait_all(self):
        self.mate_wait(0, 0)

        def body(turn):
            self.mate_wait_chip(turn + 1, False)
            self.mate_wait_chip(turn + 1, True)
        loop(self.place.half - 1, body)
        self.mate_wait_last()

    def finish(self):
        sent = self.buf.at[pl.ds(0, (4 * self.events + NP) * self.rows)]
        self.to_mate(0, sent).wait_send()


class Reduce:
    SLOTS = 4
    DEPTH = 8

    def __init__(self, place, part, shard_rows, refs):
        self.place, self.part, self.shard = place, part, shard_rows
        self.events = (place.half - 1) * NP + NP // 2
        self.ring, self.acc, self.stage, self.send_n, self.recv_n, self.send_m, self.recv_m = refs

    @staticmethod
    def scratch(half, shard_rows, width):
        events = (half - 1) * NP + NP // 2
        shapes = [(2, events), (2 * Reduce.DEPTH + NP,), (Reduce.SLOTS, 2)]
        sems = [(2, Reduce.DEPTH), (2, events), (Reduce.SLOTS,), (2 * Reduce.DEPTH + NP,)]
        return [pltpu.VMEM(s + (shard_rows, width), F32) for s in shapes] + [pltpu.SemaphoreType.DMA(s) for s in sems]

    def acc_slot(self, term):
        own = 2 * self.DEPTH + not_below_zero(term - 2 * self.events)
        return lax.select(term < 2 * self.events, lax.rem(term, 2 * self.DEPTH), own)

    def mate_copy(self, term):
        return pltpu.make_async_remote_copy(
            self.stage.at[lax.rem(term, self.SLOTS), 1 - self.place.core], self.acc.at[self.acc_slot(term)],
            self.send_m.at[lax.rem(term, self.SLOTS)], self.recv_m.at[self.acc_slot(term)], self.place.mate, MESH)

    def ring_copy(self, event, way):
        to = self.place.peer(1 - 2 * way)
        return pltpu.make_async_remote_copy(
            self.acc.at[self.acc_slot(2 * event + way)], self.ring.at[way, event],
            self.send_n.at[way, lax.rem(event, self.DEPTH)], self.recv_n.at[way, event], to, MESH)

    def fill(self, term):
        @pl.when(term >= self.SLOTS)
        def _():
            self.mate_copy(not_below_zero(term - self.SLOTS)).wait_send()
        slot = lax.rem(term, self.SLOTS)
        way = lax.rem(term, 2)

        @pl.when(term >= 2 * (self.DEPTH - 1))
        def _():
            self.ring_copy(jnp.maximum(lax.div(term, 2) - (self.DEPTH - 1), 0), way).wait_send()
        shifted = lax.div(term, 2) + NP // 2
        travels = term < 2 * self.events
        distance = not_below_zero(self.place.half - lax.div(shifted, NP))
        turn = lax.rem(shifted, NP)
        piece = lax.select(travels, lax.select(way == 0, turn, NP - 1 - turn), lax.rem(not_below_zero(term - 2 * self.events), NP))
        value = self.part(self.place.near((1 - 2 * way) * distance), piece)
        self.stage[slot, 0] = value[:self.shard]
        self.stage[slot, 1] = value[self.shard:]
        self.mate_copy(term).start()

    def event(self, event):
        def add(way):
            term = 2 * event + way
            self.mate_copy(term).wait_recv()
            slot = self.acc_slot(term)
            self.acc[slot] += self.stage[lax.rem(term, self.SLOTS), self.place.core]

            @pl.when(event >= NP)
            def _():
                before = not_below_zero(event - NP)
                self.ring_copy(before, way).wait_recv()
                self.acc[slot] += self.ring[way, before]
            self.ring_copy(event, way).start()
        loop(2, add)

    def final(self, piece):
        last = self.events - NP
        term = 2 * self.events + piece
        self.mate_copy(term).wait_recv()
        self.ring_copy(last + piece, 0).wait_recv()
        self.ring_copy(last + NP - 1 - piece, 1).wait_recv()
        return ((self.stage[term % self.SLOTS, self.place.core] + self.acc[2 * self.DEPTH + piece])
                + (self.ring[0, last + piece] + self.ring[1, last + NP - 1 - piece]))

    def finish(self):
        def across(term):
            self.mate_copy(term).wait_send()
        terms = 2 * self.events + NP
        loop_from(terms - self.SLOTS, terms, across)

        def ring(event):
            self.ring_copy(event, 0).wait_send()
            self.ring_copy(event, 1).wait_send()
        loop_from(self.events + 2 - (self.DEPTH - 1), self.events, ring)

    def run(self, filler):
        def body(turn):
            event = not_below_zero(turn - 1)
            travels = (turn >= 1) & (turn <= self.events)

            @pl.when(travels)
            def _():
                self.event(event)

            def ahead(way):
                self.fill(2 * turn + way)
            loop(2, ahead)

            @pl.when(travels)
            def _():
                filler(event)
        loop(self.events + 2, body)


def rope_pair(table):
    lanes = lax.broadcasted_iota(jnp.int32, table.shape, 1)
    swapped = pltpu.roll(table, HEAD_DIM // 2, 1)
    low = lanes < HEAD_DIM // 2
    return jnp.where(low, table, swapped), jnp.where(low, -swapped, table)


def fill_table(freqs, table_ref):
    rows = 64
    blocks = table_ref.shape[0] // rows

    def cos_sin(count, scale):
        steps = lax.broadcasted_iota(jnp.int32, (count, HEAD_DIM), 0) * scale
        angles = steps.astype(F32) * freqs
        return jnp.cos(angles), jnp.sin(angles)
    cos_low, sin_low = cos_sin(rows, 1)
    cos_high, sin_high = cos_sin(max(blocks, 8), rows)
    low = lax.broadcasted_iota(jnp.int32, (1, HEAD_DIM), 1) < HEAD_DIM // 2
    first = jnp.where(low, cos_high, sin_high)
    second = jnp.where(low, -sin_high, cos_high)
    for block in range(blocks):
        table_ref[block * rows:(block + 1) * rows] = first[block:block + 1] * cos_low + second[block:block + 1] * sin_low


def rope(values, table, inverse=False):
    cos2, sin2 = rope_pair(table)
    turned = pltpu.roll(values, HEAD_DIM // 2, 1)
    if inverse:
        return values * cos2 - turned * sin2
    return values * cos2 + turned * sin2


def norm_forward(x_f32, gain_row):
    inv = lax.rsqrt(row_mean(x_f32 * x_f32) + NORM_EPS)
    return (x_f32 * inv * gain_row).astype(BF16)


def norm_unit(x_f32):
    inv = lax.rsqrt(row_mean(x_f32 * x_f32) + NORM_EPS)
    return inv, x_f32 * inv


def norm_backward(inv, unit, gain_row, d_normed):
    d_unit = d_normed * gain_row
    return inv * (d_unit - unit * row_mean(d_unit * unit))


def by_halves(dot, a, b, axis):
    size = a.shape[axis] // 2
    first = a[:size] if axis == 0 else a[:, :size]
    second = a[size:] if axis == 0 else a[:, size:]
    return dot(first, b), dot(second, b)


def attention_block(row0, rows, keys, diagonal, refs, forward, backward):
    q_ref, k_ref, v_ref, table_ref, read_da, write_o, dx_ref, dk_ref, dv_ref = refs
    here = pl.ds(aligned(row0, rows), rows)
    scale = HEAD_DIM ** -0.5
    spans = [(start, end) for start, end in ((0, keys - diagonal), (keys - diagonal, keys)) if end > start]
    query = q_ref[here]
    scores = []
    for start, end in spans:
        part = dot_nt(query, k_ref[start:end])
        if end == keys:
            row_id = row0 - start + lax.broadcasted_iota(jnp.int32, part.shape, 0)
            part = jnp.where(row_id >= lax.broadcasted_iota(jnp.int32, part.shape, 1), part, -1e30)
        scores.append(part)
    tops = [jnp.max(part, axis=-1, keepdims=True) for part in scores]
    top = functools.reduce(jnp.maximum, tops)
    factor = scale * 1.4426950408889634
    expd = [jnp.exp2((part - top) * factor) for part in scores]
    inv_sum = 1.0 / sum(row_sum(part) for part in expd)
    prob = [part * inv_sum for part in expd]
    prob_b = [part.astype(BF16) for part in prob]
    if forward:
        halves = [by_halves(dot_nn, part, v_ref[start:end], 0) for part, (start, end) in zip(prob_b, spans)]
        out = [functools.reduce(jnp.add, [half[i] for half in halves]) for i in range(2)]
        write_o(here, jnp.concatenate(out, axis=0).astype(BF16))
    if backward:
        d_attn = read_da(here)
        d_prob = [dot_nt(d_attn, v_ref[start:end]).astype(BF16).astype(F32) for start, end in spans]
        row_dot = sum(row_sum(p * d) for p, d in zip(prob, d_prob))
        d_scores = [(p * (d - row_dot)).astype(BF16) for p, d in zip(prob, d_prob)]
        halves = [by_halves(dot_nn, part, k_ref[start:end], 0) for part, (start, end) in zip(d_scores, spans)]
        d_query = jnp.concatenate([functools.reduce(jnp.add, [half[i] for half in halves]) for i in range(2)], axis=0)
        d_query = (d_query * scale).astype(BF16).astype(F32)
        dx_ref[here, :HEAD_DIM] = rope(d_query, table_ref[here], inverse=True).astype(BF16)
        for part, prob_part, (start, end) in zip(d_scores, prob_b, spans):
            middle = (start + end) // 2
            for ref, left, right in ((dv_ref, prob_part, d_attn), (dk_ref, part, query)):
                low, high = by_halves(dot_tn, left, right, 1)
                ref[start:middle] += low
                ref[middle:end] += high


def store_keys_values(here, dx_ref, dk_ref, dv_ref, table_ref):
    d_key = (dk_ref[here] * HEAD_DIM ** -0.5).astype(BF16).astype(F32)
    dx_ref[here, HEAD_DIM:2 * HEAD_DIM] = rope(d_key, table_ref[here], inverse=True).astype(BF16)
    dx_ref[here, 2 * HEAD_DIM:3 * HEAD_DIM] = dv_ref[here].astype(BF16)


def gated_pull(gate, up, d_hidden):
    sig = jax.nn.sigmoid(gate)
    silu = gate * sig
    d_silu = d_hidden * up
    return (silu * up).astype(BF16), (d_silu * sig + d_silu * silu * (1.0 - sig)).astype(BF16), (d_hidden * silu).astype(BF16)


class Copies:
    def __init__(self, sems):
        self.sems, self.used = sems, 0

    def start(self, src, dst):
        copy = pltpu.make_async_copy(src, dst, self.take())
        copy.start()
        return copy

    def take(self):
        self.used += 1
        return self.sems.at[self.used % self.sems.shape[0]]


def gather_loop(gather, unit, then=None):
    chips = gather.place.ring

    def body(event):
        @pl.when(event < gather.events)
        def _():
            gather.event(event)
            if then is not None:
                then(event)
        step = lax.div(event, NP) + 1
        opposite = event == gather.events
        final = event == gather.events - 1
        own = event == 1
        near = (event >= NP) & (event < gather.events) & (lax.rem(event, 2) == 0)

        @pl.when(opposite)
        def _():
            gather.mate_wait_last()

        @pl.when(own | near | final)
        def _():
            gather.mate_wait_chip(step - 1, final | (lax.rem(event, NP) != 0))

        @pl.when(own | near | final | opposite)
        def _():
            distance = lax.select(opposite, gather.place.half, step - 1)
            rightward = final | (lax.rem(event, NP) != 0)
            count = lax.select(own, 0, lax.select(opposite, chips - 1, lax.select(final, chips - 2, not_below_zero(lax.div(event, 2) - 1))))
            unit(count, gather.place.near(lax.select(rightward, distance, -distance)))
    loop(gather.events + 1, body)


def weight_grads_u(block, u_ref, dx_ref, stage_ref, outs, sems, head_cols, ff):
    rows = stage_ref.shape[1]
    slot = lax.rem(block, 2)
    here = pl.ds(aligned(block * rows, rows), rows)

    def copies():
        bounds = (0, head_cols, head_cols + ff, head_cols + 2 * ff)
        return [pltpu.make_async_copy(stage_ref.at[slot, :, bounds[i]:bounds[i + 1]], outs[i].at[here], sems.at[slot, i]) for i in range(3)]

    @pl.when(block >= 2)
    def _():
        for copy in copies():
            copy.wait()
    stage_ref[slot] = dot_tn(u_ref[:, here], dx_ref[...]).astype(BF16)
    for copy in copies():
        copy.start()


def weight_grads_u_wait(stage_ref, outs, sems, head_cols, ff):
    rows = stage_ref.shape[1]
    bounds = (0, head_cols, head_cols + ff, head_cols + 2 * ff)
    for slot in range(2):
        for i in range(3):
            pltpu.make_async_copy(stage_ref.at[slot, :, bounds[i]:bounds[i + 1]], outs[i].at[pl.ds(0, rows)], sems.at[slot, i]).wait()


def weight_grads_h(piece, ho_ref, read_dy, stage_ref):
    cols = stage_ref.shape[1] // NP
    stage_ref[:, pl.ds(aligned(piece * cols, cols), cols)] = dot_tn(ho_ref[...], read_dy(piece)).astype(BF16)


def h_copies(there, stage_ref, outs, sems, ff):
    return [pltpu.make_async_copy(stage_ref.at[:HEAD_DIM, there], outs[0].at[:, there], sems.at[0]),
            pltpu.make_async_copy(stage_ref.at[HEAD_DIM:HEAD_DIM + ff, there], outs[1].at[:, there], sems.at[1])]


def kernel_main(tp_size, gain_hbm, freq_hbm, x_hbm, gy_hbm, wqkv_hbm, wout_hbm, wgate_hbm, wup_hbm, wdown_hbm,
                dx_out, gain_out, *refs):
    u_ref, g_ref, wo_ref = refs[0:3]
    lasts = refs[3:8]
    u0_hbm, q_hbm, k_hbm, v_hbm, o_hbm, ab_hbm = refs[8:14]
    (gain_ref, freq_ref, x_ref, side_ref, wc_ref, q_ref, k_ref, v_ref, ho_ref, dx_ref, dk_ref, dv_ref, table_ref, x1_ref, gs_ref,
     pair_ref, all_ref, local, sems_gs, sems_hs, sem_ps, sem_pr, sem_as, sem_ar, free_sem) = refs[14:39]
    sems_u, sems_g, refs_r = refs[39:43], refs[43:47], refs[47:]
    place = Place(tp_size)
    peers = place.arrive()
    shard, width = x_ref.shape
    pair = 2 * shard
    chips = place.ring
    head_cols = wqkv_hbm.shape[2]
    ff = wgate_hbm.shape[2]
    piece_cols = width // NP
    gate_cols = slice(head_cols, head_cols + ff)
    up_cols = slice(head_cols + ff, head_cols + 2 * ff)
    hidden_cols = slice(HEAD_DIM, HEAD_DIM + ff)
    loads = Copies(local)
    gu = Gather(place, u_ref, shard, sems_u)
    gg = Gather(place, g_ref, shard, sems_g)

    def wait_all(copies):
        for copy in copies:
            copy.wait()

    def load_wc(layer):
        return [loads.start(wqkv_hbm.at[layer], wc_ref.at[:, :head_cols]),
                loads.start(wgate_hbm.at[layer], wc_ref.at[:, gate_cols]),
                loads.start(wup_hbm.at[layer], wc_ref.at[:, up_cols])]

    def load_wo(layer):
        return [loads.start(wout_hbm.at[layer], wo_ref.at[:HEAD_DIM]), loads.start(wdown_hbm.at[layer], wo_ref.at[hidden_cols])]

    def rows_of(chip):
        return pl.ds(aligned(chip * pair, pair), pair)

    def write_o(here, value):
        ho_ref[here, :HEAD_DIM] = value

    def read_da(here):
        return dx_ref[here, :HEAD_DIM]

    def heads(here, rows_u):
        qkv = dot_nn(rows_u, wc_ref[:, :head_cols]).astype(BF16)
        table = table_ref[here]
        q_ref[here] = rope(qkv[:, :HEAD_DIM].astype(F32), table).astype(BF16)
        k_ref[here] = rope(qkv[:, HEAD_DIM:2 * HEAD_DIM].astype(F32), table).astype(BF16)
        v_ref[here] = qkv[:, 2 * HEAD_DIM:3 * HEAD_DIM]

    def forward_unit(count, chip, with_hidden):
        here = rows_of(chip)
        rows_u = u_ref[here]
        heads(here, rows_u)
        gate = dot_nn(rows_u, wc_ref[:, gate_cols]).astype(BF16)
        up = dot_nn(rows_u, wc_ref[:, up_cols]).astype(BF16)
        dx_ref[here, gate_cols] = gate
        dx_ref[here, up_cols] = up
        if with_hidden:
            gate_f, up_f = gate.astype(F32), up.astype(F32)
            ho_ref[here, hidden_cols] = (gate_f * jax.nn.sigmoid(gate_f) * up_f).astype(BF16)

    def backward_unit(count, chip):
        here = rows_of(chip)
        dah = dot_nt(g_ref[here], wo_ref[...])
        dx_ref[here, :HEAD_DIM] = dah[:, :HEAD_DIM].astype(BF16)
        d_hidden = dah[:, hidden_cols].astype(BF16).astype(F32)
        hidden, d_gate, d_up = gated_pull(dx_ref[here, gate_cols].astype(F32), dx_ref[here, up_cols].astype(F32), d_hidden)
        ho_ref[here, hidden_cols] = hidden
        dx_ref[here, gate_cols] = d_gate
        dx_ref[here, up_cols] = d_up

    def piece_of(piece):
        return pl.ds(aligned(piece * piece_cols, piece_cols), piece_cols)

    def part_forward(chip, piece):
        return dot_nn(ho_ref[rows_of(chip)], wo_ref[:, piece_of(piece)])

    def part_backward(chip, piece):
        return dot_nt(dx_ref[rows_of(chip)], wc_ref[piece_of(piece)])

    def keys_values(chip):
        store_keys_values(rows_of(chip), dx_ref, dk_ref, dv_ref, table_ref)

    def other_keys_values():
        def body(step):
            keys_values(place.near(place.half + step - chips))
        loop_from(1, chips, body)

    def read_dy(piece):
        return g_ref[:, piece_of(piece)]

    def finals(reduce):
        return jnp.concatenate([reduce.final(piece) for piece in range(NP)], axis=1)

    grad_cols = slice(head_cols + 2 * ff)
    last_u, last_h = (lasts[0], lasts[2], lasts[3]), (lasts[1], lasts[4])

    def grads_last(event):
        @pl.when(event < NP)
        def _():
            weight_grads_h(event, ho_ref, read_dy, wo_ref)
            for copy in h_copies(piece_of(event), wo_ref, last_h, sems_hs, ff):
                copy.start()

        @pl.when((event >= NP) & (event < NP + chips))
        def _():
            weight_grads_u(not_below_zero(event - NP), u_ref, dx_ref, gs_ref, last_u, sems_gs, head_cols, ff)

    def grads_last_wait():
        wait_all(h_copies(slice(None), wo_ref, last_h, sems_hs, ff))
        weight_grads_u_wait(gs_ref, last_u, sems_gs, head_cols, ff)

    def grads_first(event):
        @pl.when(event < NP)
        def _():
            weight_grads_h(event, ho_ref, read_dy, wo_ref)

        @pl.when((event >= NP) & (event < NP + chips))
        def _():
            rows = width // chips
            here = pl.ds(aligned(not_below_zero(event - NP) * rows, rows), rows)
            g_ref[here, grad_cols] = dot_tn(u_ref[:, here], dx_ref[...]).astype(BF16)

    lanes = all_ref.shape[3]
    tiles = width // lanes

    def cross(layer):
        return pltpu.make_async_remote_copy(pair_ref.at[layer, 0], pair_ref.at[layer, 1], sem_ps.at[layer], sem_pr.at[layer], place.mate, MESH)

    def spread(layer, which, step):
        part = all_ref.at[layer, which]
        return pltpu.make_async_remote_copy(part, part, sem_as.at[layer], sem_ar.at[layer], place.peer(step), MESH)

    def start_gain(layer, row):
        for tile in range(tiles):
            pair_ref[layer, 0, tile:tile + 1] = row[:, tile * lanes:(tile + 1) * lanes]
        cross(layer).start()

    def spread_gain(layer):
        cross(layer).wait()
        all_ref[layer, place.chip] = pair_ref[layer, 0] + pair_ref[layer, 1]
        for step in sorted(range(1, chips), key=lambda step: -min(step, chips - step)):
            spread(layer, place.chip, step).start()

    def end_gain(layer):
        spread(layer, slice(chips - 1), 1).wait()
        total = all_ref[layer, 0]
        for chip in range(1, chips):
            total = total + all_ref[layer, chip]
        for tile in range(tiles):
            gain_out[layer:layer + 1, tile * lanes:(tile + 1) * lanes] = total[tile:tile + 1]

    load_x = [loads.start(x_hbm, x_ref), loads.start(gain_hbm, gain_ref), loads.start(freq_hbm, freq_ref)]
    load_g = loads.start(gy_hbm, g_ref.at[gg.own_rows()])
    load_w = load_wc(0)
    load_o = load_wo(0)
    wait_all(load_x)
    u_ref[gu.own_rows()] = norm_forward(x_ref[...].astype(F32), gain_ref[0:1])
    pl.semaphore_wait(pltpu.get_barrier_semaphore(), peers)
    gu.start()
    saves = [loads.start(u_ref.at[gu.own_rows()], u0_hbm)]
    fill_table(freq_ref[:1], table_ref)
    load_g.wait()
    wait_all(load_w)

    def start_gy(event):
        @pl.when(event == gu.events - NP)
        def _():
            gg.start()
    gather_loop(gu, lambda count, chip: forward_unit(count, chip, True), start_gy)

    load_w = load_wc(1)
    saves += [loads.start(q_ref, q_hbm), loads.start(k_ref, k_hbm), loads.start(v_ref, v_hbm),
              loads.start(dx_ref.at[:, head_cols:head_cols + 2 * ff], ab_hbm)]

    def attend_first(chip):
        attention_block(chip * pair, pair, chips * pair, chips * pair, (q_ref, k_ref, v_ref, table_ref, None, write_o, None, None, None), True, False)
    attend_first(place.near(place.half))
    wait_all(load_o)
    reduce = Reduce(place, part_forward, shard, refs_r)

    def filler_forward(event):
        @pl.when(event < place.half)
        def _():
            distance = not_below_zero(place.half - 1 - event)

            def body(way):
                attend_first(place.near((1 - 2 * way) * distance))
            loop(lax.select(distance == 0, 1, 2), body)

        @pl.when(event == place.half)
        def _():
            gu.finish()
            o_copy().start()
    sem_o = loads.take()

    def o_copy():
        return pltpu.make_async_copy(ho_ref.at[:, :HEAD_DIM], o_hbm, sem_o)
    reduce.run(filler_forward)
    load_o = load_wo(1)
    gg.event(jnp.int32(0), forward=True)
    gg.event(jnp.int32(1), forward=True)
    x_next = (x_ref[...].astype(F32) + finals(reduce)).astype(BF16)
    x1_ref[...] = x_next
    saves[0].wait()
    o_copy().wait()
    u_ref[gu.own_rows()] = norm_forward(x_next.astype(F32), gain_ref[1:2])

    reduce.finish()
    gu.start()
    load_side = loads.start(u0_hbm, side_ref.at[0])
    wait_all(saves[1:])
    wait_all(load_w)
    wait_all(load_o)
    dk_ref[...] = jnp.zeros_like(dk_ref)
    dv_ref[...] = jnp.zeros_like(dv_ref)
    early = 2
    for event in range(early, NP):
        gg.event(jnp.int32(event), forward=False)

    def more_gy(event):
        first = gu.events - NP

        @pl.when((event >= first) & (event < first + NP - early))
        def _():
            gg.forward(not_below_zero(event - first) + early)

        @pl.when(event >= first + NP - early)
        def _():
            gg.event(not_below_zero(event - first) + early, forward=True)

        @pl.when((event > NP) & (event < NP + 6) & (lax.rem(event, 2) == 1))
        def _():
            turn = not_below_zero(lax.div(event - 1, 2) - 2)
            gg.mate_wait_chip(jnp.minimum(turn, 1), turn == 2)
            backward_unit(turn, place.near(lax.select(turn == 2, 1, -turn)))
    gather_loop(gu, lambda count, chip: forward_unit(count, chip, False), more_gy)

    groups = 4

    def attend_last(turn):
        held = early + NP
        distance = lax.div(turn + 1, 2)
        rightward = (turn > 0) & (lax.rem(turn, 2) == 0)
        opposite = turn == chips - 1
        needed = lax.select(turn == 0, held, lax.select(opposite, gg.events, distance * NP))
        begin = lax.select(turn == 0, held, jnp.minimum(jnp.maximum(held + turn - 1, lax.select(turn >= chips - 2, gg.events - NP // 2, 0)), gg.events))
        end = jnp.maximum(jnp.minimum(held + turn, gg.events), needed)
        end = lax.select(turn == chips - 2, jnp.maximum(end, gg.events - 1), end)
        begin = lax.select(turn == chips - 1, gg.events - 1, begin)

        @pl.when(turn == NP + 1)
        def _():
            gu.finish()
            load_side.wait()
            gu.start_side(side_ref)

        def take(event):
            gg.event(event)
        loop_from(begin, end, take)

        chip = place.near(lax.select(rightward, distance, -distance))

        @pl.when(opposite)
        def _():
            gg.mate_wait_last()

        @pl.when((turn > 2) & jnp.logical_not(opposite))
        def _():
            gg.mate_wait_chip(distance, rightward)

        @pl.when(turn > 2)
        def _():
            backward_unit(turn, chip)
        for group in range(groups):
            @pl.when(lax.div(chip, chips // groups) == group)
            def _(group=group):
                attention_block(chip * pair, pair, (group + 1) * (chips * pair // groups), chips * pair // groups,
                                (q_ref, k_ref, v_ref, table_ref, read_da, write_o, dx_ref, dk_ref, dv_ref), True, True)
    loop(chips, attend_last)
    keys_values(place.near(place.half))
    loads_a = [loads.start(q_hbm, q_ref), loads.start(k_hbm, k_ref), loads.start(v_hbm, v_ref)]
    sem_late = loads.take()

    def load_o_again():
        return pltpu.make_async_copy(o_hbm, ho_ref.at[:, :HEAD_DIM], sem_late)
    near = (place.left, place.right, place.mate)
    reduce = Reduce(place, part_backward, shard, refs_r)

    def filler_last(event):
        @pl.when(event == 0)
        def _():
            other_keys_values()
        grads_last(event)

        @pl.when(event == 1)
        def _():
            gg.finish()

        @pl.when(event == NP + chips)
        def _():
            load_o_again().start()
            for peer in near:
                pl.semaphore_signal(free_sem, inc=1, device_id=peer, device_id_type=MESH)
    reduce.run(filler_last)
    pl.semaphore_wait(free_sem, len(near))
    load_o_again().wait()
    gu.adopt_side(side_ref)
    for event in range(early):
        gu.forward_side(side_ref, event)
    d_normed = finals(reduce).astype(BF16).astype(F32)
    inv, unit = norm_unit(x1_ref[...].astype(F32))
    g_ref[gg.own_rows()] = (g_ref[gg.own_rows()].astype(F32) + norm_backward(inv, unit, gain_ref[1:2], d_normed)).astype(BF16)
    start_gain(1, jnp.sum(d_normed * unit, axis=0, keepdims=True))

    reduce.finish()
    gg.start()
    spread_gain(1)
    grads_last_wait()
    load_o = load_wo(0) + [loads.start(ab_hbm, dx_ref.at[:, head_cols:head_cols + 2 * ff])]
    load_w = load_wc(0)
    dk_ref[...] = jnp.zeros_like(dk_ref)
    dv_ref[...] = jnp.zeros_like(dv_ref)
    wait_all(load_o)

    def more_u(event):
        first = gg.events - NP

        @pl.when((event >= first) & (event < first + NP - early))
        def _():
            gu.forward_side(side_ref, not_below_zero(event - first) + early)

        @pl.when(event >= first + NP - early)
        def _():
            gu.event(not_below_zero(event - first) + early, forward=True)
    gather_loop(gg, backward_unit, more_u)
    wait_all(loads_a)

    def attend_back(block):
        @pl.when((block >= 2) & (block < gu.events - 2 * NP))
        def _():
            gu.event(block + NP, forward=True)
        for group in range(groups):
            @pl.when(lax.div(block, chips // groups) == group)
            def _(group=group):
                attention_block(block * pair, pair, (group + 1) * (chips * pair // groups), chips * pair // groups,
                                (q_ref, k_ref, v_ref, table_ref, read_da, None, dx_ref, dk_ref, dv_ref), False, True)
    loop(chips, attend_back)
    keys_values(place.near(place.half))
    wait_all(load_w)
    reduce = Reduce(place, part_backward, shard, refs_r)

    def filler_first(event):
        @pl.when(event == 0)
        def _():
            other_keys_values()

        @pl.when(event < NP)
        def _():
            gu.event(gu.events - NP + event, forward=False)

        @pl.when(event == NP - 1)
        def _():
            gu.mate_wait_all()
        grads_first(event)

        @pl.when(event == 1)
        def _():
            gg.finish()

        @pl.when(event == NP + 1)
        def _():
            gu.finish()

        @pl.when(event == NP + chips)
        def _():
            for copy in reloads():
                copy.start()
    plan = fold_plan(width, head_cols, ff)
    sems_plan = [loads.take() for part in plan]

    def reloads():
        return [pltpu.make_async_copy(lasts[number].at[theirs], u_ref.at[ours], sem) for (number, theirs, ours), sem in zip(plan, sems_plan)]
    x1_ref[...] = g_ref[gg.own_rows()]
    reduce.run(filler_first)
    inv, unit = norm_unit(x_ref[...].astype(F32))
    d_normed = finals(reduce).astype(BF16).astype(F32)
    start_gain(0, jnp.sum(d_normed * unit, axis=0, keepdims=True))
    dx_out[...] = (x1_ref[...].astype(F32) + norm_backward(inv, unit, gain_ref[0:1], d_normed)).astype(BF16)
    spread_gain(0)
    end_gain(1)
    reduce.finish()
    wait_all(reloads())
    end_gain(0)


def fold_plan(width, head_cols, ff):
    cols = head_cols + 2 * ff
    piece = width // NP
    rows = HEAD_DIM + ff
    every = slice(None)
    plan = [(0, (every, every), (every, slice(head_cols))), (2, (every, every), (every, slice(head_cols, head_cols + ff))),
            (3, (every, every), (every, slice(head_cols + ff, cols)))]
    whole = width // rows
    for turn in range(NP):
        theirs = slice(turn * piece, (turn + 1) * piece)
        if turn < whole:
            ours = slice(cols, cols + piece)
            plan += [(1, (every, theirs), (slice(turn * rows, turn * rows + HEAD_DIM), ours)),
                     (4, (every, theirs), (slice(turn * rows + HEAD_DIM, (turn + 1) * rows), ours))]
        else:
            plan += [(1, (every, theirs), (slice(whole * rows, whole * rows + HEAD_DIM), slice(cols, cols + piece)))]
            strip = width - cols - piece
            for step in range(piece // strip):
                plan += [(4, (every, slice(turn * piece + step * strip, turn * piece + (step + 1) * strip)),
                          (slice(step * ff, (step + 1) * ff), slice(cols + piece, width)))]
    return plan


def kernel_stack(head_cols, ff, last_ref, first_ref, first_h_ref, dx_ref, gain_ref, *refs):
    outs, (dx_out, gain_out, sems) = refs[0:5], refs[5:8]
    width = last_ref.shape[0]
    copies = Copies(sems)
    pending = [copies.start(dx_ref, dx_out), copies.start(gain_ref, gain_out)]
    for number, theirs, ours in fold_plan(width, head_cols, ff):
        pending.append(copies.start(last_ref.at[ours], outs[number].at[(1,) + theirs]))
    bounds = (0, head_cols, head_cols + ff, head_cols + 2 * ff)
    for i, number in enumerate((0, 2, 3)):
        pending.append(copies.start(first_ref.at[:, bounds[i]:bounds[i + 1]], outs[number].at[0]))
    pending.append(copies.start(first_h_ref.at[:HEAD_DIM], outs[1].at[0]))
    pending.append(copies.start(first_h_ref.at[HEAD_DIM:HEAD_DIM + ff], outs[4].at[0]))
    for copy in pending:
        copy.wait()


def solution(mesh):
    tp_size = mesh.shape['tp']
    half = tp_size // 4
    row_spec = P(('dp', 'tp'), None)
    col_spec = P(None, None, 'tp')
    inner_spec = P(None, 'tp', None)

    def device_program(x_loc, dy_loc, norm_gain, w_qkv, w_out, w_gate, w_up, w_down):
        shard, width = x_loc.shape
        seq = shard * tp_size
        pair = 2 * shard
        chips = tp_size // 2
        head_cols = w_qkv.shape[2]
        ff = w_gate.shape[2]
        cols = head_cols + 2 * ff
        piece_cols = width // NP
        vmem, anyspace = pl.BlockSpec(memory_space=pltpu.VMEM), pl.BlockSpec(memory_space=pl.ANY)
        shape = jax.ShapeDtypeStruct
        dma = pltpu.SemaphoreType.DMA

        freqs = np.float32(ROPE_BASE) ** (np.float32(-2.0) * np.arange(HEAD_DIM // 2, dtype=np.float32) / np.float32(HEAD_DIM))
        freqs = jnp.asarray(np.tile(freqs, (8, 2)))

        rows_shape = shape((shard, width), BF16)
        gain_shape = shape((2, width), F32)
        head_shape = shape((seq, HEAD_DIM), BF16)
        grads = (shape((width, head_cols), BF16), shape((HEAD_DIM, width), BF16), shape((width, ff), BF16),
                 shape((width, ff), BF16), shape((ff, width), BF16))
        square, folded = pltpu.VMEM((width, width), BF16), pltpu.VMEM((HEAD_DIM + ff, width), BF16)
        hbm = pl.BlockSpec(memory_space=pltpu.HBM)
        whole_vmem = 67043328
        kept = (seq * width + width * width + (HEAD_DIM + ff) * width + shard * width) * 2 + 2 ** 18
        results = pl.pallas_call(
            functools.partial(kernel_main, tp_size),
            out_shape=(pltpu.VMEM(rows_shape.shape, BF16), pltpu.VMEM(gain_shape.shape, F32), square, square, folded) + grads + (rows_shape,) + (head_shape,) * 4 + (shape((seq, 2 * ff), BF16),),
            in_specs=[hbm] * 9,
            out_specs=(vmem,) * 5 + (hbm,) * 11,
            scratch_shapes=[
                pltpu.VMEM((2, width), F32), pltpu.VMEM(freqs.shape, F32), pltpu.VMEM((shard, width), BF16),
                pltpu.VMEM((3, shard, width), BF16), pltpu.VMEM((width, cols), BF16),
                pltpu.VMEM((seq, HEAD_DIM), BF16), pltpu.VMEM((seq, HEAD_DIM), BF16), pltpu.VMEM((seq, HEAD_DIM), BF16),
                pltpu.VMEM((seq, HEAD_DIM + ff), BF16), pltpu.VMEM((seq, cols), BF16),
                pltpu.VMEM((seq, HEAD_DIM), F32), pltpu.VMEM((seq, HEAD_DIM), F32), pltpu.VMEM((seq, HEAD_DIM), F32),
                pltpu.VMEM((shard, width), BF16), pltpu.VMEM((2, width // chips, cols), BF16),
                pltpu.VMEM((2, 2, width // 128, 128), F32), pltpu.VMEM((2, chips, width // 128, 128), F32),
                dma((24,)), dma((2, 3)), dma((2,)), dma((2,)), dma((2,)), dma((2,)), dma((2,)),
                pltpu.SemaphoreType.REGULAR] + Gather.scratch(half) + Gather.scratch(half) + Reduce.scratch(half, shard, piece_cols),
            compiler_params=pltpu.CompilerParams(collective_id=1, has_side_effects=True, vmem_limit_bytes=whole_vmem - kept), name='blocks',
        )(norm_gain, freqs, x_loc, dy_loc, w_qkv, w_out, w_gate, w_up, w_down)

        stacked = pl.pallas_call(
            functools.partial(kernel_stack, head_cols, ff),
            out_shape=tuple(shape((2,) + grad.shape, BF16) for grad in grads) + (rows_shape, gain_shape),
            in_specs=[vmem] * 5,
            out_specs=(hbm,) * 7,
            scratch_shapes=[dma((1,))],
            compiler_params=pltpu.CompilerParams(vmem_limit_bytes=8 * 2 ** 20), name='stack',
        )(*results[2:5], *results[0:2])
        return tuple(stacked[5:7]) + tuple(stacked[0:5])

    return jax.shard_map(device_program, mesh=mesh, in_specs=(row_spec, row_spec, P(None, None), col_spec, inner_spec, col_spec, col_spec, inner_spec), out_specs=(row_spec, P('dp', None), P('dp', None, 'tp'), P('dp', 'tp', None), P('dp', None, 'tp'), P('dp', None, 'tp'), P('dp', 'tp', None)), check_vma=False)
```

```python
import functools

import jax
import jax.numpy as jnp
import numpy as np
from jax import lax
from jax.experimental import pallas as pl
from jax.experimental.pallas import tpu as pltpu
from jax.sharding import PartitionSpec as P

HEAD_DIM = 128
NORM_EPS = 1e-5
ROPE_BASE = 10000.0
MESH = pl.DeviceIdType.MESH
NP = 4
F32 = jnp.float32
BF16 = jnp.bfloat16


def dot_nn(a, b):
    return lax.dot_general(a, b, (((1,), (0,)), ((), ())), preferred_element_type=F32)


def dot_nt(a, b):
    return lax.dot_general(a, b, (((1,), (1,)), ((), ())), preferred_element_type=F32)


def dot_tn(a, b):
    return lax.dot_general(a, b, (((0,), (0,)), ((), ())), preferred_element_type=F32)


def not_below_zero(index):
    return jnp.maximum(index, 0)


def row_mean(values):
    return jnp.mean(values, axis=-1, keepdims=True)


def row_sum(values):
    return jnp.sum(values, axis=-1, keepdims=True)


def loop_from(first, last, body):
    def step(index, carry):
        body(index)
        return carry
    lax.fori_loop(first, last, step, 0)


def loop(count, body):
    loop_from(0, count, body)


def aligned(index, size):
    return pl.multiple_of(index, size)


class Place:
    def __init__(self, tp_size):
        index = lax.axis_index('tp')
        self.ring = tp_size // 2
        self.half = self.ring // 2
        self.core = lax.rem(index, 2)
        self.chip = lax.div(index, 2)
        self.right = self.peer(1)
        self.left = self.peer(-1)
        self.mate = {'tp': self.chip * 2 + 1 - self.core}

    def peer(self, step):
        return {'tp': self.near(step) * 2 + self.core}

    def near(self, step):
        return lax.rem(self.chip + step + self.ring, self.ring)

    def arrive(self):
        peers = [self.right, self.left, self.mate]
        for peer in peers:
            pl.semaphore_signal(pltpu.get_barrier_semaphore(), inc=1, device_id=peer, device_id_type=MESH)
        return len(peers)


class Gather:
    def __init__(self, place, buf, shard_rows, sems):
        self.place, self.buf, self.shard = place, buf, shard_rows
        self.rows = shard_rows // NP
        self.events = (place.half - 1) * NP + NP // 2
        self.send, self.recv_r, self.recv_l, self.recv_m = sems

    @staticmethod
    def scratch(half):
        events = (half - 1) * NP + NP // 2
        return [pltpu.SemaphoreType.DMA(())] + [pltpu.SemaphoreType.DMA((n,)) for n in (events, events, 2 * half)]

    def view(self, chip, core, piece):
        start = (chip * 2 + core) * self.shard + piece * self.rows
        return self.buf.at[pl.ds(aligned(start, self.rows), self.rows)]

    def own_rows(self):
        start = (self.place.chip * 2 + self.place.core) * self.shard
        return pl.ds(aligned(start, self.shard), self.shard)

    def copy(self, source, view, recv, to):
        return pltpu.make_async_remote_copy(source, view, self.send, recv, to, MESH)

    def to_right(self, event, view):
        return self.copy(view, view, self.recv_r.at[event], self.place.right)

    def to_left(self, event, view):
        return self.copy(view, view, self.recv_l.at[event], self.place.left)

    def group(self, event, rightward):
        half = self.place.half
        return lax.select(event >= (half - 1) * NP, 2 * half - 1, lax.div(event, NP) + (half if rightward else 1))

    def to_mate(self, group, view):
        return self.copy(view, view, self.recv_m.at[group], self.place.mate)

    def start(self, first=0):
        place = self.place
        for piece in range(first, NP):
            self.start_pair(piece)
        for piece in range(NP):
            self.to_mate(0, self.view(place.chip, place.core, piece)).start()

    def start_pair(self, piece):
        place = self.place
        self.to_right(piece, self.view(place.chip, place.core, piece)).start()
        self.to_left(piece, self.view(place.chip, place.core, NP - 1 - piece)).start()

    def views(self, event):
        step = lax.div(event, NP) + 1
        piece = lax.rem(event, NP)
        from_left = self.view(self.place.near(-step), self.place.core, piece)
        from_right = self.view(self.place.near(step), self.place.core, NP - 1 - piece)
        return from_left, from_right

    def event(self, event, forward=None):
        from_left, from_right = self.views(event)
        self.to_right(event, from_left).wait_recv()
        self.pass_on(event, forward, lambda: self.to_right(event + NP, from_left).start())
        self.to_mate(self.group(event, False), from_left).start()
        self.to_left(event, from_right).wait_recv()
        self.pass_on(event, forward, lambda: self.to_left(event + NP, from_right).start())
        self.to_mate(self.group(event, True), from_right).start()

    def forward(self, event):
        from_left, from_right = self.views(event)
        self.to_right(event + NP, from_left).start()
        self.to_left(event + NP, from_right).start()

    def side_view(self, side, which, piece):
        return side.at[which, pl.ds(aligned(piece * self.rows, self.rows), self.rows)]

    def start_side(self, side):
        for piece in range(NP):
            last = NP - 1 - piece
            self.copy(self.side_view(side, 0, piece), self.side_view(side, 1, piece), self.recv_r.at[piece], self.place.right).start()
            self.copy(self.side_view(side, 0, last), self.side_view(side, 2, last), self.recv_l.at[piece], self.place.left).start()

    def adopt_side(self, side):
        place = self.place

        def body(piece):
            last = NP - 1 - piece
            from_left, from_right = self.side_view(side, 1, piece), self.side_view(side, 2, last)
            self.to_right(piece, from_left).wait_recv()
            self.to_left(piece, from_right).wait_recv()
            to_left, to_right = self.views(piece)
            for source, view, group in ((self.side_view(side, 0, piece), self.view(place.chip, place.core, piece), 0),
                                        (from_left, to_left, 1), (from_right, to_right, place.half)):
                self.copy(source, view, self.recv_m.at[group], place.mate).start()
        loop(NP, body)
        for which, step in ((0, 0), (1, -1), (2, 1)):
            start = (place.near(step) * 2 + place.core) * self.shard
            self.buf[pl.ds(aligned(start, self.shard), self.shard)] = side[which]

    def forward_side(self, side, event):
        from_left, from_right = self.views(event)
        later = event + NP
        self.copy(self.side_view(side, 1, event), from_left, self.recv_r.at[later], self.place.right).start()
        self.copy(self.side_view(side, 2, NP - 1 - event), from_right, self.recv_l.at[later], self.place.left).start()

    def pass_on(self, event, forward, send):
        if forward is None:
            pl.when(event + NP < self.events)(send)
        elif forward:
            send()

    def mate_wait(self, group, step):
        start = (self.place.near(step) * 2 + 1 - self.place.core) * self.shard
        self.to_mate(group, self.buf.at[pl.ds(aligned(start, self.shard), self.shard)]).wait_recv()

    def mate_wait_last(self):
        self.mate_wait(2 * self.place.half - 1, self.place.half)

    def mate_wait_chip(self, distance, rightward):
        far = lax.select(rightward, distance + self.place.half - 1, distance)
        self.mate_wait(lax.select(distance == 0, 0, far), lax.select(rightward, distance, -distance))

    def mate_wait_all(self):
        self.mate_wait(0, 0)

        def body(turn):
            self.mate_wait_chip(turn + 1, False)
            self.mate_wait_chip(turn + 1, True)
        loop(self.place.half - 1, body)
        self.mate_wait_last()

    def finish(self):
        sent = self.buf.at[pl.ds(0, (4 * self.events + NP) * self.rows)]
        self.to_mate(0, sent).wait_send()


class Reduce:
    SLOTS = 4
    DEPTH = 8

    def __init__(self, place, part, shard_rows, refs):
        self.place, self.part, self.shard = place, part, shard_rows
        self.events = (place.half - 1) * NP + NP // 2
        self.ring, self.acc, self.stage, self.send_n, self.recv_n, self.send_m, self.recv_m = refs

    @staticmethod
    def scratch(half, shard_rows, width):
        events = (half - 1) * NP + NP // 2
        shapes = [(2, events), (2 * Reduce.DEPTH + NP,), (Reduce.SLOTS, 2)]
        sems = [(2, Reduce.DEPTH), (2, events), (Reduce.SLOTS,), (2 * Reduce.DEPTH + NP,)]
        return [pltpu.VMEM(s + (shard_rows, width), F32) for s in shapes] + [pltpu.SemaphoreType.DMA(s) for s in sems]

    def acc_slot(self, term):
        own = 2 * self.DEPTH + not_below_zero(term - 2 * self.events)
        return lax.select(term < 2 * self.events, lax.rem(term, 2 * self.DEPTH), own)

    def mate_copy(self, term):
        return pltpu.make_async_remote_copy(
            self.stage.at[lax.rem(term, self.SLOTS), 1 - self.place.core], self.acc.at[self.acc_slot(term)],
            self.send_m.at[lax.rem(term, self.SLOTS)], self.recv_m.at[self.acc_slot(term)], self.place.mate, MESH)

    def ring_copy(self, event, way):
        to = self.place.peer(1 - 2 * way)
        return pltpu.make_async_remote_copy(
            self.acc.at[self.acc_slot(2 * event + way)], self.ring.at[way, event],
            self.send_n.at[way, lax.rem(event, self.DEPTH)], self.recv_n.at[way, event], to, MESH)

    def fill(self, term):
        @pl.when(term >= self.SLOTS)
        def _():
            self.mate_copy(not_below_zero(term - self.SLOTS)).wait_send()
        slot = lax.rem(term, self.SLOTS)
        way = lax.rem(term, 2)

        @pl.when(term >= 2 * (self.DEPTH - 1))
        def _():
            self.ring_copy(jnp.maximum(lax.div(term, 2) - (self.DEPTH - 1), 0), way).wait_send()
        shifted = lax.div(term, 2) + NP // 2
        travels = term < 2 * self.events
        distance = not_below_zero(self.place.half - lax.div(shifted, NP))
        turn = lax.rem(shifted, NP)
        piece = lax.select(travels, lax.select(way == 0, turn, NP - 1 - turn), lax.rem(not_below_zero(term - 2 * self.events), NP))
        value = self.part(self.place.near((1 - 2 * way) * distance), piece)
        self.stage[slot, 0] = value[:self.shard]
        self.stage[slot, 1] = value[self.shard:]
        self.mate_copy(term).start()

    def event(self, event):
        def add(way):
            term = 2 * event + way
            self.mate_copy(term).wait_recv()
            slot = self.acc_slot(term)
            self.acc[slot] += self.stage[lax.rem(term, self.SLOTS), self.place.core]

            @pl.when(event >= NP)
            def _():
                before = not_below_zero(event - NP)
                self.ring_copy(before, way).wait_recv()
                self.acc[slot] += self.ring[way, before]
            self.ring_copy(event, way).start()
        loop(2, add)

    def final(self, piece):
        last = self.events - NP
        term = 2 * self.events + piece
        self.mate_copy(term).wait_recv()
        self.ring_copy(last + piece, 0).wait_recv()
        self.ring_copy(last + NP - 1 - piece, 1).wait_recv()
        return ((self.stage[term % self.SLOTS, self.place.core] + self.acc[2 * self.DEPTH + piece])
                + (self.ring[0, last + piece] + self.ring[1, last + NP - 1 - piece]))

    def finish(self):
        def across(term):
            self.mate_copy(term).wait_send()
        terms = 2 * self.events + NP
        loop_from(terms - self.SLOTS, terms, across)

        def ring(event):
            self.ring_copy(event, 0).wait_send()
            self.ring_copy(event, 1).wait_send()
        loop_from(self.events + 2 - (self.DEPTH - 1), self.events, ring)

    def run(self, filler):
        def body(turn):
            event = not_below_zero(turn - 1)
            travels = (turn >= 1) & (turn <= self.events)

            @pl.when(travels)
            def _():
                self.event(event)

            def ahead(way):
                self.fill(2 * turn + way)
            loop(2, ahead)

            @pl.when(travels)
            def _():
                filler(event)
        loop(self.events + 2, body)


def rope_pair(table):
    lanes = lax.broadcasted_iota(jnp.int32, table.shape, 1)
    swapped = pltpu.roll(table, HEAD_DIM // 2, 1)
    low = lanes < HEAD_DIM // 2
    return jnp.where(low, table, swapped), jnp.where(low, -swapped, table)


def fill_table(freqs, table_ref):
    rows = 64
    blocks = table_ref.shape[0] // rows

    def cos_sin(count, scale):
        steps = lax.broadcasted_iota(jnp.int32, (count, HEAD_DIM), 0) * scale
        angles = steps.astype(F32) * freqs
        return jnp.cos(angles), jnp.sin(angles)
    cos_low, sin_low = cos_sin(rows, 1)
    cos_high, sin_high = cos_sin(max(blocks, 8), rows)
    low = lax.broadcasted_iota(jnp.int32, (1, HEAD_DIM), 1) < HEAD_DIM // 2
    first = jnp.where(low, cos_high, sin_high)
    second = jnp.where(low, -sin_high, cos_high)
    for block in range(blocks):
        table_ref[block * rows:(block + 1) * rows] = first[block:block + 1] * cos_low + second[block:block + 1] * sin_low


def rope(values, table, inverse=False):
    cos2, sin2 = rope_pair(table)
    turned = pltpu.roll(values, HEAD_DIM // 2, 1)
    if inverse:
        return values * cos2 - turned * sin2
    return values * cos2 + turned * sin2


def norm_forward(x_f32, gain_row):
    inv = lax.rsqrt(row_mean(x_f32 * x_f32) + NORM_EPS)
    return (x_f32 * inv * gain_row).astype(BF16)


def norm_unit(x_f32):
    inv = lax.rsqrt(row_mean(x_f32 * x_f32) + NORM_EPS)
    return inv, x_f32 * inv


def norm_backward(inv, unit, gain_row, d_normed):
    d_unit = d_normed * gain_row
    return inv * (d_unit - unit * row_mean(d_unit * unit))


def by_halves(dot, a, b, axis):
    size = a.shape[axis] // 2
    first = a[:size] if axis == 0 else a[:, :size]
    second = a[size:] if axis == 0 else a[:, size:]
    return dot(first, b), dot(second, b)


def attention_block(row0, rows, keys, diagonal, refs, forward, backward):
    q_ref, k_ref, v_ref, table_ref, read_da, write_o, dx_ref, dk_ref, dv_ref = refs
    here = pl.ds(aligned(row0, rows), rows)
    scale = HEAD_DIM ** -0.5
    spans = [(start, end) for start, end in ((0, keys - diagonal), (keys - diagonal, keys)) if end > start]
    query = q_ref[here]
    scores = []
    for start, end in spans:
        part = dot_nt(query, k_ref[start:end])
        if end == keys:
            row_id = row0 - start + lax.broadcasted_iota(jnp.int32, part.shape, 0)
            part = jnp.where(row_id >= lax.broadcasted_iota(jnp.int32, part.shape, 1), part, -1e30)
        scores.append(part)
    tops = [jnp.max(part, axis=-1, keepdims=True) for part in scores]
    top = functools.reduce(jnp.maximum, tops)
    factor = scale * 1.4426950408889634
    expd = [jnp.exp2((part - top) * factor) for part in scores]
    inv_sum = 1.0 / sum(row_sum(part) for part in expd)
    prob = [part * inv_sum for part in expd]
    prob_b = [part.astype(BF16) for part in prob]
    if forward:
        halves = [by_halves(dot_nn, part, v_ref[start:end], 0) for part, (start, end) in zip(prob_b, spans)]
        out = [functools.reduce(jnp.add, [half[i] for half in halves]) for i in range(2)]
        write_o(here, jnp.concatenate(out, axis=0).astype(BF16))
    if backward:
        d_attn = read_da(here)
        d_prob = [dot_nt(d_attn, v_ref[start:end]).astype(BF16).astype(F32) for start, end in spans]
        row_dot = sum(row_sum(p * d) for p, d in zip(prob, d_prob))
        d_scores = [(p * (d - row_dot)).astype(BF16) for p, d in zip(prob, d_prob)]
        halves = [by_halves(dot_nn, part, k_ref[start:end], 0) for part, (start, end) in zip(d_scores, spans)]
        d_query = jnp.concatenate([functools.reduce(jnp.add, [half[i] for half in halves]) for i in range(2)], axis=0)
        d_query = (d_query * scale).astype(BF16).astype(F32)
        dx_ref[here, :HEAD_DIM] = rope(d_query, table_ref[here], inverse=True).astype(BF16)
        for part, prob_part, (start, end) in zip(d_scores, prob_b, spans):
            middle = (start + end) // 2
            for ref, left, right in ((dv_ref, prob_part, d_attn), (dk_ref, part, query)):
                low, high = by_halves(dot_tn, left, right, 1)
                ref[start:middle] += low
                ref[middle:end] += high


def store_keys_values(here, dx_ref, dk_ref, dv_ref, table_ref):
    d_key = (dk_ref[here] * HEAD_DIM ** -0.5).astype(BF16).astype(F32)
    dx_ref[here, HEAD_DIM:2 * HEAD_DIM] = rope(d_key, table_ref[here], inverse=True).astype(BF16)
    dx_ref[here, 2 * HEAD_DIM:3 * HEAD_DIM] = dv_ref[here].astype(BF16)


def gated_pull(gate, up, d_hidden):
    sig = jax.nn.sigmoid(gate)
    silu = gate * sig
    d_silu = d_hidden * up
    return (silu * up).astype(BF16), (d_silu * sig + d_silu * silu * (1.0 - sig)).astype(BF16), (d_hidden * silu).astype(BF16)


class Copies:
    def __init__(self, sems):
        self.sems, self.used = sems, 0

    def start(self, src, dst):
        copy = pltpu.make_async_copy(src, dst, self.take())
        copy.start()
        return copy

    def take(self):
        self.used += 1
        return self.sems.at[self.used % self.sems.shape[0]]


def gather_loop(gather, unit, then=None):
    chips = gather.place.ring

    def body(event):
        @pl.when(event < gather.events)
        def _():
            gather.event(event)
            if then is not None:
                then(event)
        step = lax.div(event, NP) + 1
        opposite = event == gather.events
        final = event == gather.events - 1
        own = event == 1
        near = (event >= NP) & (event < gather.events) & (lax.rem(event, 2) == 0)

        @pl.when(opposite)
        def _():
            gather.mate_wait_last()

        @pl.when(own | near | final)
        def _():
            gather.mate_wait_chip(step - 1, final | (lax.rem(event, NP) != 0))

        @pl.when(own | near | final | opposite)
        def _():
            distance = lax.select(opposite, gather.place.half, step - 1)
            rightward = final | (lax.rem(event, NP) != 0)
            count = lax.select(own, 0, lax.select(opposite, chips - 1, lax.select(final, chips - 2, not_below_zero(lax.div(event, 2) - 1))))
            unit(count, gather.place.near(lax.select(rightward, distance, -distance)))
    loop(gather.events + 1, body)


def weight_grads_u(block, u_ref, dx_ref, stage_ref, outs, sems, head_cols, ff):
    rows = stage_ref.shape[1]
    slot = lax.rem(block, 2)
    here = pl.ds(aligned(block * rows, rows), rows)

    def copies():
        bounds = (0, head_cols, head_cols + ff, head_cols + 2 * ff)
        return [pltpu.make_async_copy(stage_ref.at[slot, :, bounds[i]:bounds[i + 1]], outs[i].at[here], sems.at[slot, i]) for i in range(3)]

    @pl.when(block >= 2)
    def _():
        for copy in copies():
            copy.wait()
    stage_ref[slot] = dot_tn(u_ref[:, here], dx_ref[...]).astype(BF16)
    for copy in copies():
        copy.start()


def weight_grads_u_wait(stage_ref, outs, sems, head_cols, ff):
    rows = stage_ref.shape[1]
    bounds = (0, head_cols, head_cols + ff, head_cols + 2 * ff)
    for slot in range(2):
        for i in range(3):
            pltpu.make_async_copy(stage_ref.at[slot, :, bounds[i]:bounds[i + 1]], outs[i].at[pl.ds(0, rows)], sems.at[slot, i]).wait()


def weight_grads_h(piece, ho_ref, read_dy, stage_ref):
    cols = stage_ref.shape[1] // NP
    stage_ref[:, pl.ds(aligned(piece * cols, cols), cols)] = dot_tn(ho_ref[...], read_dy(piece)).astype(BF16)


def h_copies(there, stage_ref, outs, sems, ff):
    return [pltpu.make_async_copy(stage_ref.at[:HEAD_DIM, there], outs[0].at[:, there], sems.at[0]),
            pltpu.make_async_copy(stage_ref.at[HEAD_DIM:HEAD_DIM + ff, there], outs[1].at[:, there], sems.at[1])]


def kernel_main(tp_size, gain_hbm, freq_hbm, x_hbm, gy_hbm, wqkv_hbm, wout_hbm, wgate_hbm, wup_hbm, wdown_hbm,
                dx_out, gain_out, *refs):
    u_ref, g_ref, wo_ref = refs[0:3]
    lasts = refs[3:8]
    u0_hbm, q_hbm, k_hbm, v_hbm, o_hbm, ab_hbm = refs[8:14]
    (gain_ref, freq_ref, x_ref, side_ref, wc_ref, q_ref, k_ref, v_ref, ho_ref, dx_ref, dk_ref, dv_ref, table_ref, x1_ref, gs_ref,
     pair_ref, all_ref, local, sems_gs, sems_hs, sem_ps, sem_pr, sem_as, sem_ar, free_sem) = refs[14:39]
    sems_u, sems_g, refs_r = refs[39:43], refs[43:47], refs[47:]
    place = Place(tp_size)
    peers = place.arrive()
    shard, width = x_ref.shape
    pair = 2 * shard
    chips = place.ring
    head_cols = wqkv_hbm.shape[2]
    ff = wgate_hbm.shape[2]
    piece_cols = width // NP
    gate_cols = slice(head_cols, head_cols + ff)
    up_cols = slice(head_cols + ff, head_cols + 2 * ff)
    hidden_cols = slice(HEAD_DIM, HEAD_DIM + ff)
    loads = Copies(local)
    gu = Gather(place, u_ref, shard, sems_u)
    gg = Gather(place, g_ref, shard, sems_g)

    def wait_all(copies):
        for copy in copies:
            copy.wait()

    def load_wc(layer):
        return [loads.start(wqkv_hbm.at[layer], wc_ref.at[:, :head_cols]),
                loads.start(wgate_hbm.at[layer], wc_ref.at[:, gate_cols]),
                loads.start(wup_hbm.at[layer], wc_ref.at[:, up_cols])]

    def load_wo(layer):
        return [loads.start(wout_hbm.at[layer], wo_ref.at[:HEAD_DIM]), loads.start(wdown_hbm.at[layer], wo_ref.at[hidden_cols])]

    def rows_of(chip):
        return pl.ds(aligned(chip * pair, pair), pair)

    def write_o(here, value):
        ho_ref[here, :HEAD_DIM] = value

    def read_da(here):
        return dx_ref[here, :HEAD_DIM]

    def heads(here, rows_u):
        qkv = dot_nn(rows_u, wc_ref[:, :head_cols]).astype(BF16)
        table = table_ref[here]
        q_ref[here] = rope(qkv[:, :HEAD_DIM].astype(F32), table).astype(BF16)
        k_ref[here] = rope(qkv[:, HEAD_DIM:2 * HEAD_DIM].astype(F32), table).astype(BF16)
        v_ref[here] = qkv[:, 2 * HEAD_DIM:3 * HEAD_DIM]

    def forward_unit(count, chip, with_hidden):
        here = rows_of(chip)
        rows_u = u_ref[here]
        heads(here, rows_u)
        gate = dot_nn(rows_u, wc_ref[:, gate_cols]).astype(BF16)
        up = dot_nn(rows_u, wc_ref[:, up_cols]).astype(BF16)
        dx_ref[here, gate_cols] = gate
        dx_ref[here, up_cols] = up
        if with_hidden:
            gate_f, up_f = gate.astype(F32), up.astype(F32)
            ho_ref[here, hidden_cols] = (gate_f * jax.nn.sigmoid(gate_f) * up_f).astype(BF16)

    def backward_unit(count, chip):
        here = rows_of(chip)
        dah = dot_nt(g_ref[here], wo_ref[...])
        dx_ref[here, :HEAD_DIM] = dah[:, :HEAD_DIM].astype(BF16)
        d_hidden = dah[:, hidden_cols].astype(BF16).astype(F32)
        hidden, d_gate, d_up = gated_pull(dx_ref[here, gate_cols].astype(F32), dx_ref[here, up_cols].astype(F32), d_hidden)
        ho_ref[here, hidden_cols] = hidden
        dx_ref[here, gate_cols] = d_gate
        dx_ref[here, up_cols] = d_up

    def piece_of(piece):
        return pl.ds(aligned(piece * piece_cols, piece_cols), piece_cols)

    def part_forward(chip, piece):
        return dot_nn(ho_ref[rows_of(chip)], wo_ref[:, piece_of(piece)])

    def part_backward(chip, piece):
        return dot_nt(dx_ref[rows_of(chip)], wc_ref[piece_of(piece)])

    def keys_values(chip):
        store_keys_values(rows_of(chip), dx_ref, dk_ref, dv_ref, table_ref)

    def other_keys_values():
        def body(step):
            keys_values(place.near(place.half + step - chips))
        loop_from(1, chips, body)

    def read_dy(piece):
        return g_ref[:, piece_of(piece)]

    def finals(reduce):
        return jnp.concatenate([reduce.final(piece) for piece in range(NP)], axis=1)

    grad_cols = slice(head_cols + 2 * ff)
    last_u, last_h = (lasts[0], lasts[2], lasts[3]), (lasts[1], lasts[4])

    def grads_last(event):
        @pl.when(event < NP)
        def _():
            weight_grads_h(event, ho_ref, read_dy, wo_ref)
            for copy in h_copies(piece_of(event), wo_ref, last_h, sems_hs, ff):
                copy.start()

        @pl.when((event >= NP) & (event < NP + chips))
        def _():
            weight_grads_u(not_below_zero(event - NP), u_ref, dx_ref, gs_ref, last_u, sems_gs, head_cols, ff)

    def grads_last_wait():
        wait_all(h_copies(slice(None), wo_ref, last_h, sems_hs, ff))
        weight_grads_u_wait(gs_ref, last_u, sems_gs, head_cols, ff)

    def grads_first(event):
        @pl.when(event < NP)
        def _():
            weight_grads_h(event, ho_ref, read_dy, wo_ref)

        @pl.when((event >= NP) & (event < NP + chips))
        def _():
            rows = width // chips
            here = pl.ds(aligned(not_below_zero(event - NP) * rows, rows), rows)
            g_ref[here, grad_cols] = dot_tn(u_ref[:, here], dx_ref[...]).astype(BF16)

    lanes = all_ref.shape[3]
    tiles = width // lanes

    def cross(layer):
        return pltpu.make_async_remote_copy(pair_ref.at[layer, 0], pair_ref.at[layer, 1], sem_ps.at[layer], sem_pr.at[layer], place.mate, MESH)

    def spread(layer, which, step):
        part = all_ref.at[layer, which]
        return pltpu.make_async_remote_copy(part, part, sem_as.at[layer], sem_ar.at[layer], place.peer(step), MESH)

    def start_gain(layer, row):
        for tile in range(tiles):
            pair_ref[layer, 0, tile:tile + 1] = row[:, tile * lanes:(tile + 1) * lanes]
        cross(layer).start()

    def spread_gain(layer):
        cross(layer).wait()
        all_ref[layer, place.chip] = pair_ref[layer, 0] + pair_ref[layer, 1]
        for step in sorted(range(1, chips), key=lambda step: -min(step, chips - step)):
            spread(layer, place.chip, step).start()

    def end_gain(layer):
        spread(layer, slice(chips - 1), 1).wait()
        total = all_ref[layer, 0]
        for chip in range(1, chips):
            total = total + all_ref[layer, chip]
        for tile in range(tiles):
            gain_out[layer:layer + 1, tile * lanes:(tile + 1) * lanes] = total[tile:tile + 1]

    ends_first = sorted(range(NP), key=lambda piece: min(piece, NP - 1 - piece))
    parts = [pl.ds(piece * gu.rows, gu.rows) for piece in ends_first]
    load_gain = loads.start(gain_hbm, gain_ref)
    load_x = [loads.start(x_hbm.at[part], x_ref.at[part]) for part in parts]
    load_freq = loads.start(freq_hbm, freq_ref)
    load_g = loads.start(gy_hbm, g_ref.at[gg.own_rows()])
    load_w = load_wc(0)
    load_o = load_wo(0)
    load_gain.wait()
    own_start = (place.chip * 2 + place.core) * shard
    for turn, (piece, part) in enumerate(zip(ends_first, parts)):
        load_x[turn].wait()
        here = pl.ds(aligned(own_start + piece * gu.rows, gu.rows), gu.rows)
        u_ref[here] = norm_forward(x_ref[part].astype(F32), gain_ref[0:1])
        if turn == 1:
            pl.semaphore_wait(pltpu.get_barrier_semaphore(), peers)
            gu.start_pair(0)
    gu.start(first=1)
    saves = [loads.start(u_ref.at[gu.own_rows()], u0_hbm)]
    load_freq.wait()
    fill_table(freq_ref[:1], table_ref)
    load_g.wait()
    wait_all(load_w)

    def start_gy(event):
        @pl.when(event == gu.events - NP)
        def _():
            gg.start()
    gather_loop(gu, lambda count, chip: forward_unit(count, chip, True), start_gy)

    load_w = load_wc(1)
    saves += [loads.start(q_ref, q_hbm), loads.start(k_ref, k_hbm), loads.start(v_ref, v_hbm),
              loads.start(dx_ref.at[:, head_cols:head_cols + 2 * ff], ab_hbm)]

    def attend_first(chip):
        attention_block(chip * pair, pair, chips * pair, chips * pair, (q_ref, k_ref, v_ref, table_ref, None, write_o, None, None, None), True, False)
    attend_first(place.near(place.half))
    wait_all(load_o)
    reduce = Reduce(place, part_forward, shard, refs_r)

    def filler_forward(event):
        @pl.when(event < place.half)
        def _():
            distance = not_below_zero(place.half - 1 - event)

            def body(way):
                attend_first(place.near((1 - 2 * way) * distance))
            loop(lax.select(distance == 0, 1, 2), body)

        @pl.when(event == place.half)
        def _():
            gu.finish()
            o_copy().start()
    sem_o = loads.take()

    def o_copy():
        return pltpu.make_async_copy(ho_ref.at[:, :HEAD_DIM], o_hbm, sem_o)
    reduce.run(filler_forward)
    load_o = load_wo(1)
    gg.event(jnp.int32(0), forward=True)
    gg.event(jnp.int32(1), forward=True)
    x_next = (x_ref[...].astype(F32) + finals(reduce)).astype(BF16)
    x1_ref[...] = x_next
    saves[0].wait()
    o_copy().wait()
    u_ref[gu.own_rows()] = norm_forward(x_next.astype(F32), gain_ref[1:2])

    reduce.finish()
    gu.start()
    load_side = loads.start(u0_hbm, side_ref.at[0])
    wait_all(saves[1:])
    wait_all(load_w)
    wait_all(load_o)
    dk_ref[...] = jnp.zeros_like(dk_ref)
    dv_ref[...] = jnp.zeros_like(dv_ref)
    early = 2
    for event in range(early, NP):
        gg.event(jnp.int32(event), forward=False)

    def more_gy(event):
        first = gu.events - NP

        @pl.when((event >= first) & (event < first + NP - early))
        def _():
            gg.forward(not_below_zero(event - first) + early)

        @pl.when(event >= first + NP - early)
        def _():
            gg.event(not_below_zero(event - first) + early, forward=True)

        @pl.when((event > NP) & (event < NP + 6) & (lax.rem(event, 2) == 1))
        def _():
            turn = not_below_zero(lax.div(event - 1, 2) - 2)
            gg.mate_wait_chip(jnp.minimum(turn, 1), turn == 2)
            backward_unit(turn, place.near(lax.select(turn == 2, 1, -turn)))
    gather_loop(gu, lambda count, chip: forward_unit(count, chip, False), more_gy)

    groups = 4

    def attend_last(turn):
        held = early + NP
        distance = lax.div(turn + 1, 2)
        rightward = (turn > 0) & (lax.rem(turn, 2) == 0)
        opposite = turn == chips - 1
        needed = lax.select(turn == 0, held, lax.select(opposite, gg.events, distance * NP))
        begin = lax.select(turn == 0, held, jnp.minimum(jnp.maximum(held + turn - 1, lax.select(turn >= chips - 2, gg.events - NP // 2, 0)), gg.events))
        end = jnp.maximum(jnp.minimum(held + turn, gg.events), needed)
        end = lax.select(turn == chips - 2, jnp.maximum(end, gg.events - 1), end)
        begin = lax.select(turn == chips - 1, gg.events - 1, begin)

        @pl.when(turn == NP + 1)
        def _():
            gu.finish()
            load_side.wait()
            gu.start_side(side_ref)

        def take(event):
            gg.event(event)
        loop_from(begin, end, take)

        chip = place.near(lax.select(rightward, distance, -distance))

        @pl.when(opposite)
        def _():
            gg.mate_wait_last()

        @pl.when((turn > 2) & jnp.logical_not(opposite))
        def _():
            gg.mate_wait_chip(distance, rightward)

        @pl.when(turn > 2)
        def _():
            backward_unit(turn, chip)
        for group in range(groups):
            @pl.when(lax.div(chip, chips // groups) == group)
            def _(group=group):
                attention_block(chip * pair, pair, (group + 1) * (chips * pair // groups), chips * pair // groups,
                                (q_ref, k_ref, v_ref, table_ref, read_da, write_o, dx_ref, dk_ref, dv_ref), True, True)
    loop(chips, attend_last)
    keys_values(place.near(place.half))
    loads_a = [loads.start(q_hbm, q_ref), loads.start(k_hbm, k_ref), loads.start(v_hbm, v_ref)]
    sem_late = loads.take()

    def load_o_again():
        return pltpu.make_async_copy(o_hbm, ho_ref.at[:, :HEAD_DIM], sem_late)
    near = (place.left, place.right, place.mate)
    reduce = Reduce(place, part_backward, shard, refs_r)

    def filler_last(event):
        @pl.when(event == 0)
        def _():
            other_keys_values()
        grads_last(event)

        @pl.when(event == 1)
        def _():
            gg.finish()

        @pl.when(event == NP + chips)
        def _():
            load_o_again().start()
            for peer in near:
                pl.semaphore_signal(free_sem, inc=1, device_id=peer, device_id_type=MESH)
    reduce.run(filler_last)
    pl.semaphore_wait(free_sem, len(near))
    load_o_again().wait()
    gu.adopt_side(side_ref)
    for event in range(early):
        gu.forward_side(side_ref, event)
    d_normed = finals(reduce).astype(BF16).astype(F32)
    inv, unit = norm_unit(x1_ref[...].astype(F32))
    g_ref[gg.own_rows()] = (g_ref[gg.own_rows()].astype(F32) + norm_backward(inv, unit, gain_ref[1:2], d_normed)).astype(BF16)
    start_gain(1, jnp.sum(d_normed * unit, axis=0, keepdims=True))

    reduce.finish()
    gg.start()
    spread_gain(1)
    grads_last_wait()
    load_o = load_wo(0) + [loads.start(ab_hbm, dx_ref.at[:, head_cols:head_cols + 2 * ff])]
    load_w = load_wc(0)
    dk_ref[...] = jnp.zeros_like(dk_ref)
    dv_ref[...] = jnp.zeros_like(dv_ref)
    wait_all(load_o)

    def more_u(event):
        first = gg.events - NP

        @pl.when((event >= first) & (event < first + NP - early))
        def _():
            gu.forward_side(side_ref, not_below_zero(event - first) + early)

        @pl.when(event >= first + NP - early)
        def _():
            gu.event(not_below_zero(event - first) + early, forward=True)
    gather_loop(gg, backward_unit, more_u)
    wait_all(loads_a)

    def attend_back(block):
        @pl.when((block >= 2) & (block < gu.events - 2 * NP))
        def _():
            gu.event(block + NP, forward=True)
        for group in range(groups):
            @pl.when(lax.div(block, chips // groups) == group)
            def _(group=group):
                attention_block(block * pair, pair, (group + 1) * (chips * pair // groups), chips * pair // groups,
                                (q_ref, k_ref, v_ref, table_ref, read_da, None, dx_ref, dk_ref, dv_ref), False, True)
    loop(chips, attend_back)
    keys_values(place.near(place.half))
    wait_all(load_w)
    reduce = Reduce(place, part_backward, shard, refs_r)

    def filler_first(event):
        @pl.when(event == 0)
        def _():
            other_keys_values()

        @pl.when(event < NP)
        def _():
            gu.event(gu.events - NP + event, forward=False)

        @pl.when(event == NP - 1)
        def _():
            gu.mate_wait_all()
        grads_first(event)

        @pl.when(event == 1)
        def _():
            gg.finish()

        @pl.when(event == NP + 1)
        def _():
            gu.finish()

        @pl.when(event == NP + chips)
        def _():
            for copy in reloads():
                copy.start()
    plan = fold_plan(width, head_cols, ff)
    sems_plan = [loads.take() for part in plan]

    def reloads():
        return [pltpu.make_async_copy(lasts[number].at[theirs], u_ref.at[ours], sem) for (number, theirs, ours), sem in zip(plan, sems_plan)]
    x1_ref[...] = g_ref[gg.own_rows()]
    reduce.run(filler_first)
    inv, unit = norm_unit(x_ref[...].astype(F32))
    d_normed = finals(reduce).astype(BF16).astype(F32)
    start_gain(0, jnp.sum(d_normed * unit, axis=0, keepdims=True))
    dx_out[...] = (x1_ref[...].astype(F32) + norm_backward(inv, unit, gain_ref[0:1], d_normed)).astype(BF16)
    spread_gain(0)
    end_gain(1)
    reduce.finish()
    wait_all(reloads())
    end_gain(0)


def fold_plan(width, head_cols, ff):
    cols = head_cols + 2 * ff
    piece = width // NP
    rows = HEAD_DIM + ff
    every = slice(None)
    plan = [(0, (every, every), (every, slice(head_cols))), (2, (every, every), (every, slice(head_cols, head_cols + ff))),
            (3, (every, every), (every, slice(head_cols + ff, cols)))]
    whole = width // rows
    for turn in range(NP):
        theirs = slice(turn * piece, (turn + 1) * piece)
        if turn < whole:
            ours = slice(cols, cols + piece)
            plan += [(1, (every, theirs), (slice(turn * rows, turn * rows + HEAD_DIM), ours)),
                     (4, (every, theirs), (slice(turn * rows + HEAD_DIM, (turn + 1) * rows), ours))]
        else:
            plan += [(1, (every, theirs), (slice(whole * rows, whole * rows + HEAD_DIM), slice(cols, cols + piece)))]
            strip = width - cols - piece
            for step in range(piece // strip):
                plan += [(4, (every, slice(turn * piece + step * strip, turn * piece + (step + 1) * strip)),
                          (slice(step * ff, (step + 1) * ff), slice(cols + piece, width)))]
    return plan


def kernel_stack(head_cols, ff, last_ref, first_ref, first_h_ref, dx_ref, gain_ref, *refs):
    outs, (dx_out, gain_out, sems) = refs[0:5], refs[5:8]
    width = last_ref.shape[0]
    copies = Copies(sems)
    pending = [copies.start(dx_ref, dx_out), copies.start(gain_ref, gain_out)]
    for number, theirs, ours in fold_plan(width, head_cols, ff):
        pending.append(copies.start(last_ref.at[ours], outs[number].at[(1,) + theirs]))
    bounds = (0, head_cols, head_cols + ff, head_cols + 2 * ff)
    for i, number in enumerate((0, 2, 3)):
        pending.append(copies.start(first_ref.at[:, bounds[i]:bounds[i + 1]], outs[number].at[0]))
    pending.append(copies.start(first_h_ref.at[:HEAD_DIM], outs[1].at[0]))
    pending.append(copies.start(first_h_ref.at[HEAD_DIM:HEAD_DIM + ff], outs[4].at[0]))
    for copy in pending:
        copy.wait()


def solution(mesh):
    tp_size = mesh.shape['tp']
    half = tp_size // 4
    row_spec = P(('dp', 'tp'), None)
    col_spec = P(None, None, 'tp')
    inner_spec = P(None, 'tp', None)

    def device_program(x_loc, dy_loc, norm_gain, w_qkv, w_out, w_gate, w_up, w_down):
        shard, width = x_loc.shape
        seq = shard * tp_size
        pair = 2 * shard
        chips = tp_size // 2
        head_cols = w_qkv.shape[2]
        ff = w_gate.shape[2]
        cols = head_cols + 2 * ff
        piece_cols = width // NP
        vmem, anyspace = pl.BlockSpec(memory_space=pltpu.VMEM), pl.BlockSpec(memory_space=pl.ANY)
        shape = jax.ShapeDtypeStruct
        dma = pltpu.SemaphoreType.DMA

        freqs = np.float32(ROPE_BASE) ** (np.float32(-2.0) * np.arange(HEAD_DIM // 2, dtype=np.float32) / np.float32(HEAD_DIM))
        freqs = jnp.asarray(np.tile(freqs, (8, 2)))

        rows_shape = shape((shard, width), BF16)
        gain_shape = shape((2, width), F32)
        head_shape = shape((seq, HEAD_DIM), BF16)
        grads = (shape((width, head_cols), BF16), shape((HEAD_DIM, width), BF16), shape((width, ff), BF16),
                 shape((width, ff), BF16), shape((ff, width), BF16))
        square, folded = pltpu.VMEM((width, width), BF16), pltpu.VMEM((HEAD_DIM + ff, width), BF16)
        hbm = pl.BlockSpec(memory_space=pltpu.HBM)
        whole_vmem = 67043328
        kept = (seq * width + width * width + (HEAD_DIM + ff) * width + shard * width) * 2 + 2 ** 18
        results = pl.pallas_call(
            functools.partial(kernel_main, tp_size),
            out_shape=(pltpu.VMEM(rows_shape.shape, BF16), pltpu.VMEM(gain_shape.shape, F32), square, square, folded) + grads + (rows_shape,) + (head_shape,) * 4 + (shape((seq, 2 * ff), BF16),),
            in_specs=[hbm] * 9,
            out_specs=(vmem,) * 5 + (hbm,) * 11,
            scratch_shapes=[
                pltpu.VMEM((2, width), F32), pltpu.VMEM(freqs.shape, F32), pltpu.VMEM((shard, width), BF16),
                pltpu.VMEM((3, shard, width), BF16), pltpu.VMEM((width, cols), BF16),
                pltpu.VMEM((seq, HEAD_DIM), BF16), pltpu.VMEM((seq, HEAD_DIM), BF16), pltpu.VMEM((seq, HEAD_DIM), BF16),
                pltpu.VMEM((seq, HEAD_DIM + ff), BF16), pltpu.VMEM((seq, cols), BF16),
                pltpu.VMEM((seq, HEAD_DIM), F32), pltpu.VMEM((seq, HEAD_DIM), F32), pltpu.VMEM((seq, HEAD_DIM), F32),
                pltpu.VMEM((shard, width), BF16), pltpu.VMEM((2, width // chips, cols), BF16),
                pltpu.VMEM((2, 2, width // 128, 128), F32), pltpu.VMEM((2, chips, width // 128, 128), F32),
                dma((16,)), dma((2, 3)), dma((2,)), dma((2,)), dma((2,)), dma((2,)), dma((2,)),
                pltpu.SemaphoreType.REGULAR] + Gather.scratch(half) + Gather.scratch(half) + Reduce.scratch(half, shard, piece_cols),
            compiler_params=pltpu.CompilerParams(collective_id=1, has_side_effects=True, vmem_limit_bytes=whole_vmem - kept), name='blocks',
        )(norm_gain, freqs, x_loc, dy_loc, w_qkv, w_out, w_gate, w_up, w_down)

        stacked = pl.pallas_call(
            functools.partial(kernel_stack, head_cols, ff),
            out_shape=tuple(shape((2,) + grad.shape, BF16) for grad in grads) + (rows_shape, gain_shape),
            in_specs=[vmem] * 5,
            out_specs=(hbm,) * 7,
            scratch_shapes=[dma((1,))],
            compiler_params=pltpu.CompilerParams(vmem_limit_bytes=8 * 2 ** 20), name='stack',
        )(*results[2:5], *results[0:2])
        return tuple(stacked[5:7]) + tuple(stacked[0:5])

    return jax.shard_map(device_program, mesh=mesh, in_specs=(row_spec, row_spec, P(None, None), col_spec, inner_spec, col_spec, col_spec, inner_spec), out_specs=(row_spec, P('dp', None), P('dp', None, 'tp'), P('dp', 'tp', None), P('dp', None, 'tp'), P('dp', None, 'tp'), P('dp', 'tp', None)), check_vma=False)
```

```python
import functools

import jax
import jax.numpy as jnp
import numpy as np
from jax import lax
from jax.experimental import pallas as pl
from jax.experimental.pallas import tpu as pltpu
from jax.sharding import PartitionSpec as P

HEAD_DIM = 128
NORM_EPS = 1e-5
ROPE_BASE = 10000.0
MESH = pl.DeviceIdType.MESH
NP = 4
F32 = jnp.float32
BF16 = jnp.bfloat16


def dot_nn(a, b):
    return lax.dot_general(a, b, (((1,), (0,)), ((), ())), preferred_element_type=F32)


def dot_nt(a, b):
    return lax.dot_general(a, b, (((1,), (1,)), ((), ())), preferred_element_type=F32)


def dot_tn(a, b):
    return lax.dot_general(a, b, (((0,), (0,)), ((), ())), preferred_element_type=F32)


def not_below_zero(index):
    return jnp.maximum(index, 0)


def row_mean(values):
    return jnp.mean(values, axis=-1, keepdims=True)


def row_sum(values):
    return jnp.sum(values, axis=-1, keepdims=True)


def loop_from(first, last, body):
    def step(index, carry):
        body(index)
        return carry
    lax.fori_loop(first, last, step, 0)


def loop(count, body):
    loop_from(0, count, body)


def aligned(index, size):
    return pl.multiple_of(index, size)


class Place:
    def __init__(self, tp_size):
        index = lax.axis_index('tp')
        self.ring = tp_size // 2
        self.half = self.ring // 2
        self.core = lax.rem(index, 2)
        self.chip = lax.div(index, 2)
        self.right = self.peer(1)
        self.left = self.peer(-1)
        self.mate = {'tp': self.chip * 2 + 1 - self.core}

    def peer(self, step):
        return {'tp': self.near(step) * 2 + self.core}

    def near(self, step):
        return lax.rem(self.chip + step + self.ring, self.ring)

    def arrive(self):
        peers = [self.right, self.left, self.mate]
        for peer in peers:
            pl.semaphore_signal(pltpu.get_barrier_semaphore(), inc=1, device_id=peer, device_id_type=MESH)
        return len(peers)


class Gather:
    def __init__(self, place, buf, shard_rows, sems):
        self.place, self.buf, self.shard = place, buf, shard_rows
        self.rows = shard_rows // NP
        self.events = (place.half - 1) * NP + NP // 2
        self.send, self.recv_r, self.recv_l, self.recv_m = sems

    @staticmethod
    def scratch(half):
        events = (half - 1) * NP + NP // 2
        return [pltpu.SemaphoreType.DMA(())] + [pltpu.SemaphoreType.DMA((n,)) for n in (events, events, 2 * half)]

    def view(self, chip, core, piece):
        start = (chip * 2 + core) * self.shard + piece * self.rows
        return self.buf.at[pl.ds(aligned(start, self.rows), self.rows)]

    def own_rows(self):
        start = (self.place.chip * 2 + self.place.core) * self.shard
        return pl.ds(aligned(start, self.shard), self.shard)

    def copy(self, source, view, recv, to):
        return pltpu.make_async_remote_copy(source, view, self.send, recv, to, MESH)

    def to_right(self, event, view):
        return self.copy(view, view, self.recv_r.at[event], self.place.right)

    def to_left(self, event, view):
        return self.copy(view, view, self.recv_l.at[event], self.place.left)

    def group(self, event, rightward):
        half = self.place.half
        return lax.select(event >= (half - 1) * NP, 2 * half - 1, lax.div(event, NP) + (half if rightward else 1))

    def to_mate(self, group, view):
        return self.copy(view, view, self.recv_m.at[group], self.place.mate)

    def start(self, first=0):
        place = self.place
        for piece in range(first, NP):
            self.start_pair(piece)
        for piece in range(NP):
            self.to_mate(0, self.view(place.chip, place.core, piece)).start()

    def start_pair(self, piece):
        place = self.place
        self.to_right(piece, self.view(place.chip, place.core, piece)).start()
        self.to_left(piece, self.view(place.chip, place.core, NP - 1 - piece)).start()

    def views(self, event):
        step = lax.div(event, NP) + 1
        piece = lax.rem(event, NP)
        from_left = self.view(self.place.near(-step), self.place.core, piece)
        from_right = self.view(self.place.near(step), self.place.core, NP - 1 - piece)
        return from_left, from_right

    def event(self, event, forward=None):
        from_left, from_right = self.views(event)
        self.to_right(event, from_left).wait_recv()
        self.pass_on(event, forward, lambda: self.to_right(event + NP, from_left).start())
        self.to_mate(self.group(event, False), from_left).start()
        self.to_left(event, from_right).wait_recv()
        self.pass_on(event, forward, lambda: self.to_left(event + NP, from_right).start())
        self.to_mate(self.group(event, True), from_right).start()

    def forward(self, event):
        from_left, from_right = self.views(event)
        self.to_right(event + NP, from_left).start()
        self.to_left(event + NP, from_right).start()

    def side_view(self, side, which, piece):
        return side.at[which, pl.ds(aligned(piece * self.rows, self.rows), self.rows)]

    def start_side(self, side):
        for piece in range(NP):
            last = NP - 1 - piece
            self.copy(self.side_view(side, 0, piece), self.side_view(side, 1, piece), self.recv_r.at[piece], self.place.right).start()
            self.copy(self.side_view(side, 0, last), self.side_view(side, 2, last), self.recv_l.at[piece], self.place.left).start()

    def adopt_side(self, side):
        place = self.place

        def body(piece):
            last = NP - 1 - piece
            from_left, from_right = self.side_view(side, 1, piece), self.side_view(side, 2, last)
            self.to_right(piece, from_left).wait_recv()
            self.to_left(piece, from_right).wait_recv()
            to_left, to_right = self.views(piece)
            for source, view, group in ((self.side_view(side, 0, piece), self.view(place.chip, place.core, piece), 0),
                                        (from_left, to_left, 1), (from_right, to_right, place.half)):
                self.copy(source, view, self.recv_m.at[group], place.mate).start()
        loop(NP, body)
        for which, step in ((0, 0), (1, -1), (2, 1)):
            start = (place.near(step) * 2 + place.core) * self.shard
            self.buf[pl.ds(aligned(start, self.shard), self.shard)] = side[which]

    def forward_side(self, side, event):
        from_left, from_right = self.views(event)
        later = event + NP
        self.copy(self.side_view(side, 1, event), from_left, self.recv_r.at[later], self.place.right).start()
        self.copy(self.side_view(side, 2, NP - 1 - event), from_right, self.recv_l.at[later], self.place.left).start()

    def pass_on(self, event, forward, send):
        if forward is None:
            pl.when(event + NP < self.events)(send)
        elif forward:
            send()

    def mate_wait(self, group, step):
        start = (self.place.near(step) * 2 + 1 - self.place.core) * self.shard
        self.to_mate(group, self.buf.at[pl.ds(aligned(start, self.shard), self.shard)]).wait_recv()

    def mate_wait_last(self):
        self.mate_wait(2 * self.place.half - 1, self.place.half)

    def mate_wait_chip(self, distance, rightward):
        far = lax.select(rightward, distance + self.place.half - 1, distance)
        self.mate_wait(lax.select(distance == 0, 0, far), lax.select(rightward, distance, -distance))

    def mate_wait_all(self):
        self.mate_wait(0, 0)

        def body(turn):
            self.mate_wait_chip(turn + 1, False)
            self.mate_wait_chip(turn + 1, True)
        loop(self.place.half - 1, body)
        self.mate_wait_last()

    def finish(self):
        sent = self.buf.at[pl.ds(0, (4 * self.events + NP) * self.rows)]
        self.to_mate(0, sent).wait_send()


class Reduce:
    SLOTS = 4
    DEPTH = 8

    def __init__(self, place, part, shard_rows, refs):
        self.place, self.part, self.shard = place, part, shard_rows
        self.events = (place.half - 1) * NP + NP // 2
        self.ring, self.acc, self.stage, self.send_n, self.recv_n, self.send_m, self.recv_m = refs

    @staticmethod
    def scratch(half, shard_rows, width):
        events = (half - 1) * NP + NP // 2
        shapes = [(2, events), (2 * Reduce.DEPTH + NP,), (Reduce.SLOTS, 2)]
        sems = [(2, Reduce.DEPTH), (2, events), (Reduce.SLOTS,), (2 * Reduce.DEPTH + NP,)]
        return [pltpu.VMEM(s + (shard_rows, width), F32) for s in shapes] + [pltpu.SemaphoreType.DMA(s) for s in sems]

    def acc_slot(self, term):
        own = 2 * self.DEPTH + not_below_zero(term - 2 * self.events)
        return lax.select(term < 2 * self.events, lax.rem(term, 2 * self.DEPTH), own)

    def mate_copy(self, term):
        return pltpu.make_async_remote_copy(
            self.stage.at[lax.rem(term, self.SLOTS), 1 - self.place.core], self.acc.at[self.acc_slot(term)],
            self.send_m.at[lax.rem(term, self.SLOTS)], self.recv_m.at[self.acc_slot(term)], self.place.mate, MESH)

    def ring_copy(self, event, way):
        to = self.place.peer(1 - 2 * way)
        return pltpu.make_async_remote_copy(
            self.acc.at[self.acc_slot(2 * event + way)], self.ring.at[way, event],
            self.send_n.at[way, lax.rem(event, self.DEPTH)], self.recv_n.at[way, event], to, MESH)

    def fill(self, term):
        @pl.when(term >= self.SLOTS)
        def _():
            self.mate_copy(not_below_zero(term - self.SLOTS)).wait_send()
        slot = lax.rem(term, self.SLOTS)
        way = lax.rem(term, 2)

        @pl.when(term >= 2 * (self.DEPTH - 1))
        def _():
            self.ring_copy(jnp.maximum(lax.div(term, 2) - (self.DEPTH - 1), 0), way).wait_send()
        shifted = lax.div(term, 2) + NP // 2
        travels = term < 2 * self.events
        distance = not_below_zero(self.place.half - lax.div(shifted, NP))
        turn = lax.rem(shifted, NP)
        piece = lax.select(travels, lax.select(way == 0, turn, NP - 1 - turn), lax.rem(not_below_zero(term - 2 * self.events), NP))
        value = self.part(self.place.near((1 - 2 * way) * distance), piece)
        self.stage[slot, 0] = value[:self.shard]
        self.stage[slot, 1] = value[self.shard:]
        self.mate_copy(term).start()

    def event(self, event):
        def add(way):
            term = 2 * event + way
            self.mate_copy(term).wait_recv()
            slot = self.acc_slot(term)
            self.acc[slot] += self.stage[lax.rem(term, self.SLOTS), self.place.core]

            @pl.when(event >= NP)
            def _():
                before = not_below_zero(event - NP)
                self.ring_copy(before, way).wait_recv()
                self.acc[slot] += self.ring[way, before]
            self.ring_copy(event, way).start()
        loop(2, add)

    def final(self, piece):
        last = self.events - NP
        term = 2 * self.events + piece
        self.mate_copy(term).wait_recv()
        self.ring_copy(last + piece, 0).wait_recv()
        self.ring_copy(last + NP - 1 - piece, 1).wait_recv()
        return ((self.stage[term % self.SLOTS, self.place.core] + self.acc[2 * self.DEPTH + piece])
                + (self.ring[0, last + piece] + self.ring[1, last + NP - 1 - piece]))

    def finish(self):
        def across(term):
            self.mate_copy(term).wait_send()
        terms = 2 * self.events + NP
        loop_from(terms - self.SLOTS, terms, across)

        def ring(event):
            self.ring_copy(event, 0).wait_send()
            self.ring_copy(event, 1).wait_send()
        loop_from(self.events + 2 - (self.DEPTH - 1), self.events, ring)

    def run(self, filler):
        def body(turn):
            event = not_below_zero(turn - 1)
            travels = (turn >= 1) & (turn <= self.events)

            @pl.when(travels)
            def _():
                self.event(event)

            def ahead(way):
                self.fill(2 * turn + way)
            loop(2, ahead)

            @pl.when(travels)
            def _():
                filler(event)
        loop(self.events + 2, body)


def rope_pair(table):
    lanes = lax.broadcasted_iota(jnp.int32, table.shape, 1)
    swapped = pltpu.roll(table, HEAD_DIM // 2, 1)
    low = lanes < HEAD_DIM // 2
    return jnp.where(low, table, swapped), jnp.where(low, -swapped, table)


def fill_table(freqs, table_ref):
    rows = 64
    blocks = table_ref.shape[0] // rows

    def cos_sin(count, scale):
        steps = lax.broadcasted_iota(jnp.int32, (count, HEAD_DIM), 0) * scale
        angles = steps.astype(F32) * freqs
        return jnp.cos(angles), jnp.sin(angles)
    cos_low, sin_low = cos_sin(rows, 1)
    cos_high, sin_high = cos_sin(max(blocks, 8), rows)
    low = lax.broadcasted_iota(jnp.int32, (1, HEAD_DIM), 1) < HEAD_DIM // 2
    first = jnp.where(low, cos_high, sin_high)
    second = jnp.where(low, -sin_high, cos_high)
    for block in range(blocks):
        table_ref[block * rows:(block + 1) * rows] = first[block:block + 1] * cos_low + second[block:block + 1] * sin_low


def rope(values, table, inverse=False):
    cos2, sin2 = rope_pair(table)
    turned = pltpu.roll(values, HEAD_DIM // 2, 1)
    if inverse:
        return values * cos2 - turned * sin2
    return values * cos2 + turned * sin2


def norm_forward(x_f32, gain_row):
    inv = lax.rsqrt(row_mean(x_f32 * x_f32) + NORM_EPS)
    return (x_f32 * inv * gain_row).astype(BF16)


def norm_unit(x_f32):
    inv = lax.rsqrt(row_mean(x_f32 * x_f32) + NORM_EPS)
    return inv, x_f32 * inv


def norm_backward(inv, unit, gain_row, d_normed):
    d_unit = d_normed * gain_row
    return inv * (d_unit - unit * row_mean(d_unit * unit))


def by_halves(dot, a, b, axis):
    size = a.shape[axis] // 2
    first = a[:size] if axis == 0 else a[:, :size]
    second = a[size:] if axis == 0 else a[:, size:]
    return dot(first, b), dot(second, b)


def attention_block(row0, rows, keys, diagonal, refs, forward, backward):
    q_ref, k_ref, v_ref, table_ref, read_da, write_o, dx_ref, dk_ref, dv_ref = refs
    here = pl.ds(aligned(row0, rows), rows)
    scale = HEAD_DIM ** -0.5
    spans = [(start, end) for start, end in ((0, keys - diagonal), (keys - diagonal, keys)) if end > start]
    query = q_ref[here]
    scores = []
    for start, end in spans:
        part = dot_nt(query, k_ref[start:end])
        if end == keys:
            row_id = row0 - start + lax.broadcasted_iota(jnp.int32, part.shape, 0)
            part = jnp.where(row_id >= lax.broadcasted_iota(jnp.int32, part.shape, 1), part, -1e30 / scale)
        scores.append(part)
    tops = [jnp.max(part, axis=-1, keepdims=True) for part in scores]
    top = functools.reduce(jnp.maximum, tops)
    factor = scale * 1.4426950408889634
    expd = [jnp.exp2((part - top) * factor) for part in scores]
    inv_sum = 1.0 / sum(row_sum(part) for part in expd)
    prob = [part * inv_sum for part in expd]
    prob_b = [part.astype(BF16) for part in prob]
    if forward:
        halves = [by_halves(dot_nn, part, v_ref[start:end], 0) for part, (start, end) in zip(prob_b, spans)]
        out = [functools.reduce(jnp.add, [half[i] for half in halves]) for i in range(2)]
        write_o(here, jnp.concatenate(out, axis=0).astype(BF16))
    if backward:
        d_attn = read_da(here)
        d_prob = [dot_nt(d_attn, v_ref[start:end]).astype(BF16).astype(F32) for start, end in spans]
        row_dot = sum(row_sum(p * d) for p, d in zip(prob, d_prob))
        d_scores = [(p * (d - row_dot) * scale).astype(BF16) for p, d in zip(prob, d_prob)]
        halves = [by_halves(dot_nn, part, k_ref[start:end], 0) for part, (start, end) in zip(d_scores, spans)]
        d_query = jnp.concatenate([functools.reduce(jnp.add, [half[i] for half in halves]) for i in range(2)], axis=0)
        d_query = d_query.astype(BF16).astype(F32)
        dx_ref[here, :HEAD_DIM] = rope(d_query, table_ref[here], inverse=True).astype(BF16)
        for part, prob_part, (start, end) in zip(d_scores, prob_b, spans):
            middle = (start + end) // 2
            for ref, left, right in ((dv_ref, prob_part, d_attn), (dk_ref, part, query)):
                low, high = by_halves(dot_tn, left, right, 1)
                ref[start:middle] += low
                ref[middle:end] += high


def store_keys_values(here, dx_ref, dk_ref, dv_ref, table_ref):
    d_key = dk_ref[here].astype(BF16).astype(F32)
    dx_ref[here, HEAD_DIM:2 * HEAD_DIM] = rope(d_key, table_ref[here], inverse=True).astype(BF16)
    dx_ref[here, 2 * HEAD_DIM:3 * HEAD_DIM] = dv_ref[here].astype(BF16)


def gated_pull(gate, up, d_hidden):
    sig = jax.nn.sigmoid(gate)
    silu = gate * sig
    d_silu = d_hidden * up
    return (silu * up).astype(BF16), (d_silu * sig + d_silu * silu * (1.0 - sig)).astype(BF16), (d_hidden * silu).astype(BF16)


class Copies:
    def __init__(self, sems):
        self.sems, self.used = sems, 0

    def start(self, src, dst):
        copy = pltpu.make_async_copy(src, dst, self.take())
        copy.start()
        return copy

    def take(self):
        self.used += 1
        return self.sems.at[self.used % self.sems.shape[0]]


def gather_loop(gather, unit, then=None):
    chips = gather.place.ring

    def body(event):
        @pl.when(event < gather.events)
        def _():
            gather.event(event)
            if then is not None:
                then(event)
        step = lax.div(event, NP) + 1
        opposite = event == gather.events
        final = event == gather.events - 1
        own = event == 1
        near = (event >= NP) & (event < gather.events) & (lax.rem(event, 2) == 0)

        @pl.when(opposite)
        def _():
            gather.mate_wait_last()

        @pl.when(own | near | final)
        def _():
            gather.mate_wait_chip(step - 1, final | (lax.rem(event, NP) != 0))

        @pl.when(own | near | final | opposite)
        def _():
            distance = lax.select(opposite, gather.place.half, step - 1)
            rightward = final | (lax.rem(event, NP) != 0)
            count = lax.select(own, 0, lax.select(opposite, chips - 1, lax.select(final, chips - 2, not_below_zero(lax.div(event, 2) - 1))))
            unit(count, gather.place.near(lax.select(rightward, distance, -distance)))
    loop(gather.events + 1, body)


def weight_grads_u(block, u_ref, dx_ref, stage_ref, outs, sems, head_cols, ff):
    rows = stage_ref.shape[1]
    slot = lax.rem(block, 2)
    here = pl.ds(aligned(block * rows, rows), rows)

    def copies():
        bounds = (0, head_cols, head_cols + ff, head_cols + 2 * ff)
        return [pltpu.make_async_copy(stage_ref.at[slot, :, bounds[i]:bounds[i + 1]], outs[i].at[here], sems.at[slot, i]) for i in range(3)]

    @pl.when(block >= 2)
    def _():
        for copy in copies():
            copy.wait()
    stage_ref[slot] = dot_tn(u_ref[:, here], dx_ref[...]).astype(BF16)
    for copy in copies():
        copy.start()


def weight_grads_u_wait(stage_ref, outs, sems, head_cols, ff):
    rows = stage_ref.shape[1]
    bounds = (0, head_cols, head_cols + ff, head_cols + 2 * ff)
    for slot in range(2):
        for i in range(3):
            pltpu.make_async_copy(stage_ref.at[slot, :, bounds[i]:bounds[i + 1]], outs[i].at[pl.ds(0, rows)], sems.at[slot, i]).wait()


def weight_grads_h(piece, ho_ref, read_dy, stage_ref):
    cols = stage_ref.shape[1] // NP
    stage_ref[:, pl.ds(aligned(piece * cols, cols), cols)] = dot_tn(ho_ref[...], read_dy(piece)).astype(BF16)


def h_copies(there, stage_ref, outs, sems, ff):
    return [pltpu.make_async_copy(stage_ref.at[:HEAD_DIM, there], outs[0].at[:, there], sems.at[0]),
            pltpu.make_async_copy(stage_ref.at[HEAD_DIM:HEAD_DIM + ff, there], outs[1].at[:, there], sems.at[1])]


def kernel_main(tp_size, gain_hbm, freq_hbm, x_hbm, gy_hbm, wqkv_hbm, wout_hbm, wgate_hbm, wup_hbm, wdown_hbm,
                dx_out, gain_out, *refs):
    u_ref, g_ref, wo_ref = refs[0:3]
    lasts = refs[3:8]
    u0_hbm, q_hbm, k_hbm, v_hbm, o_hbm, ab_hbm = refs[8:14]
    (gain_ref, freq_ref, x_ref, side_ref, wc_ref, q_ref, k_ref, v_ref, ho_ref, dx_ref, dk_ref, dv_ref, table_ref, x1_ref, gs_ref,
     pair_ref, all_ref, local, sems_gs, sems_hs, sem_ps, sem_pr, sem_as, sem_ar, free_sem) = refs[14:39]
    sems_u, sems_g, refs_r = refs[39:43], refs[43:47], refs[47:]
    place = Place(tp_size)
    peers = place.arrive()
    shard, width = x_ref.shape
    pair = 2 * shard
    chips = place.ring
    head_cols = wqkv_hbm.shape[2]
    ff = wgate_hbm.shape[2]
    piece_cols = width // NP
    gate_cols = slice(head_cols, head_cols + ff)
    up_cols = slice(head_cols + ff, head_cols + 2 * ff)
    hidden_cols = slice(HEAD_DIM, HEAD_DIM + ff)
    loads = Copies(local)
    gu = Gather(place, u_ref, shard, sems_u)
    gg = Gather(place, g_ref, shard, sems_g)

    def wait_all(copies):
        for copy in copies:
            copy.wait()

    def load_wc(layer):
        return [loads.start(wqkv_hbm.at[layer], wc_ref.at[:, :head_cols]),
                loads.start(wgate_hbm.at[layer], wc_ref.at[:, gate_cols]),
                loads.start(wup_hbm.at[layer], wc_ref.at[:, up_cols])]

    def load_wo(layer):
        return [loads.start(wout_hbm.at[layer], wo_ref.at[:HEAD_DIM]), loads.start(wdown_hbm.at[layer], wo_ref.at[hidden_cols])]

    def rows_of(chip):
        return pl.ds(aligned(chip * pair, pair), pair)

    def write_o(here, value):
        ho_ref[here, :HEAD_DIM] = value

    def read_da(here):
        return dx_ref[here, :HEAD_DIM]

    def heads(here, rows_u):
        qkv = dot_nn(rows_u, wc_ref[:, :head_cols]).astype(BF16)
        table = table_ref[here]
        q_ref[here] = rope(qkv[:, :HEAD_DIM].astype(F32), table).astype(BF16)
        k_ref[here] = rope(qkv[:, HEAD_DIM:2 * HEAD_DIM].astype(F32), table).astype(BF16)
        v_ref[here] = qkv[:, 2 * HEAD_DIM:3 * HEAD_DIM]

    def forward_unit(count, chip, with_hidden):
        here = rows_of(chip)
        rows_u = u_ref[here]
        heads(here, rows_u)
        gate = dot_nn(rows_u, wc_ref[:, gate_cols]).astype(BF16)
        up = dot_nn(rows_u, wc_ref[:, up_cols]).astype(BF16)
        dx_ref[here, gate_cols] = gate
        dx_ref[here, up_cols] = up
        if with_hidden:
            gate_f, up_f = gate.astype(F32), up.astype(F32)
            ho_ref[here, hidden_cols] = (gate_f * jax.nn.sigmoid(gate_f) * up_f).astype(BF16)

    def backward_unit(count, chip):
        here = rows_of(chip)
        dah = dot_nt(g_ref[here], wo_ref[...])
        dx_ref[here, :HEAD_DIM] = dah[:, :HEAD_DIM].astype(BF16)
        d_hidden = dah[:, hidden_cols].astype(BF16).astype(F32)
        hidden, d_gate, d_up = gated_pull(dx_ref[here, gate_cols].astype(F32), dx_ref[here, up_cols].astype(F32), d_hidden)
        ho_ref[here, hidden_cols] = hidden
        dx_ref[here, gate_cols] = d_gate
        dx_ref[here, up_cols] = d_up

    def piece_of(piece):
        return pl.ds(aligned(piece * piece_cols, piece_cols), piece_cols)

    def part_forward(chip, piece):
        return dot_nn(ho_ref[rows_of(chip)], wo_ref[:, piece_of(piece)])

    def part_backward(chip, piece):
        return dot_nt(dx_ref[rows_of(chip)], wc_ref[piece_of(piece)])

    def keys_values(chip):
        store_keys_values(rows_of(chip), dx_ref, dk_ref, dv_ref, table_ref)

    def other_keys_values():
        def body(step):
            keys_values(place.near(place.half + step - chips))
        loop_from(1, chips, body)

    def read_dy(piece):
        return g_ref[:, piece_of(piece)]

    def finals(reduce):
        return jnp.concatenate([reduce.final(piece) for piece in range(NP)], axis=1)

    grad_cols = slice(head_cols + 2 * ff)
    last_u, last_h = (lasts[0], lasts[2], lasts[3]), (lasts[1], lasts[4])

    def grads_last(event):
        @pl.when(event < NP)
        def _():
            weight_grads_h(event, ho_ref, read_dy, wo_ref)
            for copy in h_copies(piece_of(event), wo_ref, last_h, sems_hs, ff):
                copy.start()

        @pl.when((event >= NP) & (event < NP + chips))
        def _():
            weight_grads_u(not_below_zero(event - NP), u_ref, dx_ref, gs_ref, last_u, sems_gs, head_cols, ff)

    def grads_last_wait():
        wait_all(h_copies(slice(None), wo_ref, last_h, sems_hs, ff))
        weight_grads_u_wait(gs_ref, last_u, sems_gs, head_cols, ff)

    def grads_first(event):
        @pl.when(event < NP)
        def _():
            weight_grads_h(event, ho_ref, read_dy, wo_ref)

        @pl.when((event >= NP) & (event < NP + chips))
        def _():
            rows = width // chips
            here = pl.ds(aligned(not_below_zero(event - NP) * rows, rows), rows)
            g_ref[here, grad_cols] = dot_tn(u_ref[:, here], dx_ref[...]).astype(BF16)

    lanes = all_ref.shape[3]
    tiles = width // lanes

    def cross(layer):
        return pltpu.make_async_remote_copy(pair_ref.at[layer, 0], pair_ref.at[layer, 1], sem_ps.at[layer], sem_pr.at[layer], place.mate, MESH)

    def spread(layer, which, step):
        part = all_ref.at[layer, which]
        return pltpu.make_async_remote_copy(part, part, sem_as.at[layer], sem_ar.at[layer], place.peer(step), MESH)

    def start_gain(layer, row):
        for tile in range(tiles):
            pair_ref[layer, 0, tile:tile + 1] = row[:, tile * lanes:(tile + 1) * lanes]
        cross(layer).start()

    def spread_gain(layer):
        cross(layer).wait()
        all_ref[layer, place.chip] = pair_ref[layer, 0] + pair_ref[layer, 1]
        for step in sorted(range(1, chips), key=lambda step: -min(step, chips - step)):
            spread(layer, place.chip, step).start()

    def end_gain(layer):
        spread(layer, slice(chips - 1), 1).wait()
        total = all_ref[layer, 0]
        for chip in range(1, chips):
            total = total + all_ref[layer, chip]
        for tile in range(tiles):
            gain_out[layer:layer + 1, tile * lanes:(tile + 1) * lanes] = total[tile:tile + 1]

    ends_first = sorted(range(NP), key=lambda piece: min(piece, NP - 1 - piece))
    parts = [pl.ds(piece * gu.rows, gu.rows) for piece in ends_first]
    load_gain = loads.start(gain_hbm, gain_ref)
    load_x = [loads.start(x_hbm.at[part], x_ref.at[part]) for part in parts]
    load_freq = loads.start(freq_hbm, freq_ref)
    load_g = loads.start(gy_hbm, g_ref.at[gg.own_rows()])
    load_w = load_wc(0)
    load_o = load_wo(0)
    load_gain.wait()
    own_start = (place.chip * 2 + place.core) * shard
    for turn, (piece, part) in enumerate(zip(ends_first, parts)):
        load_x[turn].wait()
        here = pl.ds(aligned(own_start + piece * gu.rows, gu.rows), gu.rows)
        u_ref[here] = norm_forward(x_ref[part].astype(F32), gain_ref[0:1])
        if turn == 1:
            pl.semaphore_wait(pltpu.get_barrier_semaphore(), peers)
            gu.start_pair(0)
    gu.start(first=1)
    saves = [loads.start(u_ref.at[gu.own_rows()], u0_hbm)]
    load_freq.wait()
    fill_table(freq_ref[:1], table_ref)
    load_g.wait()
    wait_all(load_w)

    def start_gy(event):
        @pl.when(event == gu.events - NP)
        def _():
            gg.start()
    gather_loop(gu, lambda count, chip: forward_unit(count, chip, True), start_gy)

    load_w = load_wc(1)
    saves += [loads.start(q_ref, q_hbm), loads.start(k_ref, k_hbm), loads.start(v_ref, v_hbm),
              loads.start(dx_ref.at[:, head_cols:head_cols + 2 * ff], ab_hbm)]

    def attend_first(chip):
        attention_block(chip * pair, pair, chips * pair, chips * pair, (q_ref, k_ref, v_ref, table_ref, None, write_o, None, None, None), True, False)
    attend_first(place.near(place.half))
    wait_all(load_o)
    reduce = Reduce(place, part_forward, shard, refs_r)

    def filler_forward(event):
        @pl.when(event < place.half)
        def _():
            distance = not_below_zero(place.half - 1 - event)

            def body(way):
                attend_first(place.near((1 - 2 * way) * distance))
            loop(lax.select(distance == 0, 1, 2), body)

        @pl.when(event == place.half)
        def _():
            gu.finish()
            o_copy().start()
    sem_o = loads.take()

    def o_copy():
        return pltpu.make_async_copy(ho_ref.at[:, :HEAD_DIM], o_hbm, sem_o)
    reduce.run(filler_forward)
    load_o = load_wo(1)
    gg.event(jnp.int32(0), forward=True)
    gg.event(jnp.int32(1), forward=True)
    x_next = (x_ref[...].astype(F32) + finals(reduce)).astype(BF16)
    x1_ref[...] = x_next
    saves[0].wait()
    o_copy().wait()
    u_ref[gu.own_rows()] = norm_forward(x_next.astype(F32), gain_ref[1:2])

    reduce.finish()
    gu.start()
    load_side = loads.start(u0_hbm, side_ref.at[0])
    wait_all(saves[1:])
    wait_all(load_w)
    wait_all(load_o)
    dk_ref[...] = jnp.zeros_like(dk_ref)
    dv_ref[...] = jnp.zeros_like(dv_ref)
    early = 2
    for event in range(early, NP):
        gg.event(jnp.int32(event), forward=False)

    def more_gy(event):
        first = gu.events - NP

        @pl.when((event >= first) & (event < first + NP - early))
        def _():
            gg.forward(not_below_zero(event - first) + early)

        @pl.when(event >= first + NP - early)
        def _():
            gg.event(not_below_zero(event - first) + early, forward=True)

        @pl.when((event > NP) & (event < NP + 6) & (lax.rem(event, 2) == 1))
        def _():
            turn = not_below_zero(lax.div(event - 1, 2) - 2)
            gg.mate_wait_chip(jnp.minimum(turn, 1), turn == 2)
            backward_unit(turn, place.near(lax.select(turn == 2, 1, -turn)))
    gather_loop(gu, lambda count, chip: forward_unit(count, chip, False), more_gy)

    groups = 4

    def attend_last(turn):
        held = early + NP
        distance = lax.div(turn + 1, 2)
        rightward = (turn > 0) & (lax.rem(turn, 2) == 0)
        opposite = turn == chips - 1
        needed = lax.select(turn == 0, held, lax.select(opposite, gg.events, distance * NP))
        begin = lax.select(turn == 0, held, jnp.minimum(jnp.maximum(held + turn - 1, lax.select(turn >= chips - 2, gg.events - NP // 2, 0)), gg.events))
        end = jnp.maximum(jnp.minimum(held + turn, gg.events), needed)
        end = lax.select(turn == chips - 2, jnp.maximum(end, gg.events - 1), end)
        begin = lax.select(turn == chips - 1, gg.events - 1, begin)

        @pl.when(turn == NP + 1)
        def _():
            gu.finish()
            load_side.wait()
            gu.start_side(side_ref)

        def take(event):
            gg.event(event)
        loop_from(begin, end, take)

        chip = place.near(lax.select(rightward, distance, -distance))

        @pl.when(opposite)
        def _():
            gg.mate_wait_last()

        @pl.when((turn > 2) & jnp.logical_not(opposite))
        def _():
            gg.mate_wait_chip(distance, rightward)

        @pl.when(turn > 2)
        def _():
            backward_unit(turn, chip)
        for group in range(groups):
            @pl.when(lax.div(chip, chips // groups) == group)
            def _(group=group):
                attention_block(chip * pair, pair, (group + 1) * (chips * pair // groups), chips * pair // groups,
                                (q_ref, k_ref, v_ref, table_ref, read_da, write_o, dx_ref, dk_ref, dv_ref), True, True)
    loop(chips, attend_last)
    keys_values(place.near(place.half))
    loads_a = [loads.start(q_hbm, q_ref), loads.start(k_hbm, k_ref), loads.start(v_hbm, v_ref)]
    sem_late = loads.take()

    def load_o_again():
        return pltpu.make_async_copy(o_hbm, ho_ref.at[:, :HEAD_DIM], sem_late)
    near = (place.left, place.right, place.mate)
    reduce = Reduce(place, part_backward, shard, refs_r)

    def filler_last(event):
        @pl.when(event == 0)
        def _():
            other_keys_values()
        grads_last(event)

        @pl.when(event == 1)
        def _():
            gg.finish()

        @pl.when(event == NP + chips)
        def _():
            load_o_again().start()
            for peer in near:
                pl.semaphore_signal(free_sem, inc=1, device_id=peer, device_id_type=MESH)
    reduce.run(filler_last)
    pl.semaphore_wait(free_sem, len(near))
    load_o_again().wait()
    gu.adopt_side(side_ref)
    for event in range(early):
        gu.forward_side(side_ref, event)
    d_normed = finals(reduce).astype(BF16).astype(F32)
    inv, unit = norm_unit(x1_ref[...].astype(F32))
    g_ref[gg.own_rows()] = (g_ref[gg.own_rows()].astype(F32) + norm_backward(inv, unit, gain_ref[1:2], d_normed)).astype(BF16)
    start_gain(1, jnp.sum(d_normed * unit, axis=0, keepdims=True))

    reduce.finish()
    gg.start()
    spread_gain(1)
    grads_last_wait()
    load_o = load_wo(0) + [loads.start(ab_hbm, dx_ref.at[:, head_cols:head_cols + 2 * ff])]
    load_w = load_wc(0)
    dk_ref[...] = jnp.zeros_like(dk_ref)
    dv_ref[...] = jnp.zeros_like(dv_ref)
    wait_all(load_o)

    def more_u(event):
        first = gg.events - NP

        @pl.when((event >= first) & (event < first + NP - early))
        def _():
            gu.forward_side(side_ref, not_below_zero(event - first) + early)

        @pl.when(event >= first + NP - early)
        def _():
            gu.event(not_below_zero(event - first) + early, forward=True)
    gather_loop(gg, backward_unit, more_u)
    wait_all(loads_a)

    def attend_back(block):
        @pl.when((block >= 2) & (block < gu.events - 2 * NP))
        def _():
            gu.event(block + NP, forward=True)
        for group in range(groups):
            @pl.when(lax.div(block, chips // groups) == group)
            def _(group=group):
                attention_block(block * pair, pair, (group + 1) * (chips * pair // groups), chips * pair // groups,
                                (q_ref, k_ref, v_ref, table_ref, read_da, None, dx_ref, dk_ref, dv_ref), False, True)
    loop(chips, attend_back)
    keys_values(place.near(place.half))
    wait_all(load_w)
    reduce = Reduce(place, part_backward, shard, refs_r)

    def filler_first(event):
        @pl.when(event == 0)
        def _():
            other_keys_values()

        @pl.when(event < NP)
        def _():
            gu.event(gu.events - NP + event, forward=False)

        @pl.when(event == NP - 1)
        def _():
            gu.mate_wait_all()
        grads_first(event)

        @pl.when(event == 1)
        def _():
            gg.finish()

        @pl.when(event == NP + 1)
        def _():
            gu.finish()

        @pl.when(event == NP + chips)
        def _():
            for copy in reloads():
                copy.start()
    plan = fold_plan(width, head_cols, ff)
    sems_plan = [loads.take() for part in plan]

    def reloads():
        return [pltpu.make_async_copy(lasts[number].at[theirs], u_ref.at[ours], sem) for (number, theirs, ours), sem in zip(plan, sems_plan)]
    x1_ref[...] = g_ref[gg.own_rows()]
    reduce.run(filler_first)
    inv, unit = norm_unit(x_ref[...].astype(F32))
    d_normed = finals(reduce).astype(BF16).astype(F32)
    start_gain(0, jnp.sum(d_normed * unit, axis=0, keepdims=True))
    dx_out[...] = (x1_ref[...].astype(F32) + norm_backward(inv, unit, gain_ref[0:1], d_normed)).astype(BF16)
    spread_gain(0)
    end_gain(1)
    reduce.finish()
    wait_all(reloads())
    end_gain(0)


def fold_plan(width, head_cols, ff):
    cols = head_cols + 2 * ff
    piece = width // NP
    rows = HEAD_DIM + ff
    every = slice(None)
    plan = [(0, (every, every), (every, slice(head_cols))), (2, (every, every), (every, slice(head_cols, head_cols + ff))),
            (3, (every, every), (every, slice(head_cols + ff, cols)))]
    whole = width // rows
    for turn in range(NP):
        theirs = slice(turn * piece, (turn + 1) * piece)
        if turn < whole:
            ours = slice(cols, cols + piece)
            plan += [(1, (every, theirs), (slice(turn * rows, turn * rows + HEAD_DIM), ours)),
                     (4, (every, theirs), (slice(turn * rows + HEAD_DIM, (turn + 1) * rows), ours))]
        else:
            plan += [(1, (every, theirs), (slice(whole * rows, whole * rows + HEAD_DIM), slice(cols, cols + piece)))]
            strip = width - cols - piece
            for step in range(piece // strip):
                plan += [(4, (every, slice(turn * piece + step * strip, turn * piece + (step + 1) * strip)),
                          (slice(step * ff, (step + 1) * ff), slice(cols + piece, width)))]
    return plan


def kernel_stack(head_cols, ff, last_ref, first_ref, first_h_ref, dx_ref, gain_ref, *refs):
    outs, (dx_out, gain_out, sems) = refs[0:5], refs[5:8]
    width = last_ref.shape[0]
    copies = Copies(sems)
    pending = [copies.start(dx_ref, dx_out), copies.start(gain_ref, gain_out)]
    for number, theirs, ours in fold_plan(width, head_cols, ff):
        pending.append(copies.start(last_ref.at[ours], outs[number].at[(1,) + theirs]))
    bounds = (0, head_cols, head_cols + ff, head_cols + 2 * ff)
    for i, number in enumerate((0, 2, 3)):
        pending.append(copies.start(first_ref.at[:, bounds[i]:bounds[i + 1]], outs[number].at[0]))
    pending.append(copies.start(first_h_ref.at[:HEAD_DIM], outs[1].at[0]))
    pending.append(copies.start(first_h_ref.at[HEAD_DIM:HEAD_DIM + ff], outs[4].at[0]))
    for copy in pending:
        copy.wait()


def solution(mesh):
    tp_size = mesh.shape['tp']
    half = tp_size // 4
    row_spec = P(('dp', 'tp'), None)
    col_spec = P(None, None, 'tp')
    inner_spec = P(None, 'tp', None)

    def device_program(x_loc, dy_loc, norm_gain, w_qkv, w_out, w_gate, w_up, w_down):
        shard, width = x_loc.shape
        seq = shard * tp_size
        pair = 2 * shard
        chips = tp_size // 2
        head_cols = w_qkv.shape[2]
        ff = w_gate.shape[2]
        cols = head_cols + 2 * ff
        piece_cols = width // NP
        vmem, anyspace = pl.BlockSpec(memory_space=pltpu.VMEM), pl.BlockSpec(memory_space=pl.ANY)
        shape = jax.ShapeDtypeStruct
        dma = pltpu.SemaphoreType.DMA

        freqs = np.float32(ROPE_BASE) ** (np.float32(-2.0) * np.arange(HEAD_DIM // 2, dtype=np.float32) / np.float32(HEAD_DIM))
        freqs = jnp.asarray(np.tile(freqs, (8, 2)))

        rows_shape = shape((shard, width), BF16)
        gain_shape = shape((2, width), F32)
        head_shape = shape((seq, HEAD_DIM), BF16)
        grads = (shape((width, head_cols), BF16), shape((HEAD_DIM, width), BF16), shape((width, ff), BF16),
                 shape((width, ff), BF16), shape((ff, width), BF16))
        square, folded = pltpu.VMEM((width, width), BF16), pltpu.VMEM((HEAD_DIM + ff, width), BF16)
        hbm = pl.BlockSpec(memory_space=pltpu.HBM)
        whole_vmem = 67043328
        kept = (seq * width + width * width + (HEAD_DIM + ff) * width + shard * width) * 2 + 2 ** 18
        results = pl.pallas_call(
            functools.partial(kernel_main, tp_size),
            out_shape=(pltpu.VMEM(rows_shape.shape, BF16), pltpu.VMEM(gain_shape.shape, F32), square, square, folded) + grads + (rows_shape,) + (head_shape,) * 4 + (shape((seq, 2 * ff), BF16),),
            in_specs=[hbm] * 9,
            out_specs=(vmem,) * 5 + (hbm,) * 11,
            scratch_shapes=[
                pltpu.VMEM((2, width), F32), pltpu.VMEM(freqs.shape, F32), pltpu.VMEM((shard, width), BF16),
                pltpu.VMEM((3, shard, width), BF16), pltpu.VMEM((width, cols), BF16),
                pltpu.VMEM((seq, HEAD_DIM), BF16), pltpu.VMEM((seq, HEAD_DIM), BF16), pltpu.VMEM((seq, HEAD_DIM), BF16),
                pltpu.VMEM((seq, HEAD_DIM + ff), BF16), pltpu.VMEM((seq, cols), BF16),
                pltpu.VMEM((seq, HEAD_DIM), F32), pltpu.VMEM((seq, HEAD_DIM), F32), pltpu.VMEM((seq, HEAD_DIM), F32),
                pltpu.VMEM((shard, width), BF16), pltpu.VMEM((2, width // chips, cols), BF16),
                pltpu.VMEM((2, 2, width // 128, 128), F32), pltpu.VMEM((2, chips, width // 128, 128), F32),
                dma((16,)), dma((2, 3)), dma((2,)), dma((2,)), dma((2,)), dma((2,)), dma((2,)),
                pltpu.SemaphoreType.REGULAR] + Gather.scratch(half) + Gather.scratch(half) + Reduce.scratch(half, shard, piece_cols),
            compiler_params=pltpu.CompilerParams(collective_id=1, has_side_effects=True, vmem_limit_bytes=whole_vmem - kept), name='blocks',
        )(norm_gain, freqs, x_loc, dy_loc, w_qkv, w_out, w_gate, w_up, w_down)

        stacked = pl.pallas_call(
            functools.partial(kernel_stack, head_cols, ff),
            out_shape=tuple(shape((2,) + grad.shape, BF16) for grad in grads) + (rows_shape, gain_shape),
            in_specs=[vmem] * 5,
            out_specs=(hbm,) * 7,
            scratch_shapes=[dma((1,))],
            compiler_params=pltpu.CompilerParams(vmem_limit_bytes=8 * 2 ** 20), name='stack',
        )(*results[2:5], *results[0:2])
        return tuple(stacked[5:7]) + tuple(stacked[0:5])

    return jax.shard_map(device_program, mesh=mesh, in_specs=(row_spec, row_spec, P(None, None), col_spec, inner_spec, col_spec, col_spec, inner_spec), out_specs=(row_spec, P('dp', None), P('dp', None, 'tp'), P('dp', 'tp', None), P('dp', None, 'tp'), P('dp', None, 'tp'), P('dp', 'tp', None)), check_vma=False)
```
